32 devices in a mesh: dp: 8 (over y, x, core), tensor: 4 (over z).
Axes of the slice: x: 2, y: 2, z: 4, core: 2. Of those that a mesh axis runs over, the one named last changes fastest.
Arguments:
- hidden_in: bfloat16 [16384, 1024], P(('dp', 'tensor')), may hold values from -6 to 6
- cotangent: bfloat16 [16384, 1024], P(('dp', 'tensor')), may hold values from -6 to 6
- w_query: float32 [1024, 1024], P('dp', 'tensor'), may hold values from -0.1875 to 0.1875
- w_key: float32 [1024, 1024], P('dp', 'tensor'), may hold values from -0.1875 to 0.1875
- w_value: float32 [1024, 1024], P('dp', 'tensor'), may hold values from -0.1875 to 0.1875
- w_out: float32 [1024, 1024], P('dp', 'tensor'), may hold values from -2 to 2
- w_up: float32 [1024, 4096], P('dp', 'tensor'), may hold values from -0.1875 to 0.1875
- w_down: float32 [1024, 4096], P('dp', 'tensor'), may hold values from -0.09375 to 0.09375
- bias_query: float32 [1024], replicated, may hold values from -3 to 3
- bias_value: float32 [1024], replicated, may hold values from -3 to 3
- bias_out: float32 [1024], replicated, may hold values from -3 to 3
- bias_up: float32 [4096], replicated, may hold values from -3 to 3
- bias_down: float32 [1024], replicated, may hold values from -3 to 3
- gain_attn: float32 [1024], replicated, may hold values from 0.5 to 1.5
- shift_attn: float32 [1024], replicated, may hold values from -3 to 3
- gain_ffn: float32 [1024], replicated, may hold values from 0.5 to 1.5
- shift_ffn: float32 [1024], replicated, may hold values from -3 to 3
- valid_lengths: int32 [32], P('dp'), may hold values from 64 to 512, as said below
Outputs:
- output: bfloat16 [16384, 1024], P(('dp', 'tensor'))
- grad_hidden_in: bfloat16 [16384, 1024], P(('dp', 'tensor'))
- grad_w_query: float32 [1024, 1024], P('dp', 'tensor')
- grad_w_key: float32 [1024, 1024], P('dp', 'tensor')
- grad_w_value: float32 [1024, 1024], P('dp', 'tensor')
- grad_w_out: float32 [1024, 1024], P('dp', 'tensor')
- grad_w_up: float32 [1024, 4096], P('dp', 'tensor')
- grad_w_down: float32 [1024, 4096], P('dp', 'tensor')
- grad_bias_query: float32 [1024], replicated
- grad_bias_value: float32 [1024], replicated
- grad_bias_out: float32 [1024], replicated
- grad_bias_up: float32 [4096], replicated
- grad_bias_down: float32 [1024], replicated
- grad_gain_attn: float32 [1024], replicated
- grad_shift_attn: float32 [1024], replicated
- grad_gain_ffn: float32 [1024], replicated
- grad_shift_ffn: float32 [1024], replicated
The draws below stay inside these ranges and needn't reach their ends.
Inputs may be any that keep to these rules, and one draw needn't show every extreme that they name: Each sequence's real tokens are its first valid_lengths positions; some sequence has all 512.
All inputs are finite; a program needn't handle non-finite values.
Results may differ from the reference program's by a relative error of at most 0.02.
Values may be sent and summed in bfloat16 or wider, within the bound.
A program may use at most 128 MiB of HBM per device.

```python
import jax
import jax.numpy as jnp
from jax import lax

D = 1024
HEADS = 16
FF = 4096
SEQ = 512
SEQS = 32
TOKENS = 16384
N_DP = 8


def draw_valid_lengths(key, part):
    drawn = jax.random.randint(key, (SEQS,), SEQ // 8, SEQ + 1).astype(jnp.int32)
    drawn = drawn.at[0].set(SEQ)
    return drawn.at[SEQS - 1].set(SEQ // 8)


def level_of(key, shape, shards, smallest, top_value):
    level, own = 1.0, jax.random.fold_in(key, 6)
    for dim, parts in shards:
        heights = jnp.exp(jax.random.uniform(jax.random.fold_in(own, dim), (parts,), jnp.float32, smallest / len(shards), top_value / len(shards)))
        level = level * jnp.repeat(heights, shape[dim] // parts).reshape([-1 if axis == dim else 1 for axis in range(len(shape))])
    return level


def noise(stream_key, extent, scale, limit, pieces=(), dtype=jnp.bfloat16):
    values = jax.random.normal(stream_key, extent, jnp.float32) * scale
    if len(pieces) > 0:
        values = level_of(stream_key, extent, pieces, -0.22, 0.18) * values
    return jnp.clip(values, min=-limit, max=limit).astype(dtype)


def setup_inputs(seed: int = 0) -> dict:
    arg_keys = jax.random.split(jax.random.key(seed), 19)
    hidden_in = noise(arg_keys[0], (TOKENS, D), 1.0, 6.0, ((0, 32),))
    cotangent = noise(arg_keys[1], (TOKENS, D), 1.0, 6.0, ((0, 32),))
    w_query = noise(arg_keys[2], (D, D), D ** -0.5, 0.1875, ((0, 8), (1, 4)), jnp.float32)
    w_key = noise(arg_keys[3], (D, D), D ** -0.5, 0.1875, ((0, 8), (1, 4)), jnp.float32)
    w_value = noise(arg_keys[4], (D, D), D ** -0.5, 0.1875, ((0, 8), (1, 4)), jnp.float32)
    w_out = noise(arg_keys[5], (D, D), (4 * D // SEQ) ** -0.5, 2.0, ((0, 8), (1, 4)), jnp.float32)
    w_up = noise(arg_keys[6], (D, FF), D ** -0.5, 0.1875, ((0, 8), (1, 4)), jnp.float32)
    w_down = noise(arg_keys[7], (D, FF), FF ** -0.5, 0.09375, ((0, 8), (1, 4)), jnp.float32)
    bias_query = noise(arg_keys[8], (D,), 0.5, 3.0, (), jnp.float32)
    bias_value = noise(arg_keys[9], (D,), 0.5, 3.0, (), jnp.float32)
    bias_out = noise(arg_keys[10], (D,), 0.3, 3.0, (), jnp.float32)
    bias_up = noise(arg_keys[11], (FF,), 0.5, 3.0, (), jnp.float32)
    bias_down = noise(arg_keys[12], (D,), 0.3, 3.0, (), jnp.float32)
    gain_attn = jnp.clip(1.0 + 0.1 * jax.random.normal(arg_keys[13], (D,), jnp.float32), 0.5, 1.5)
    shift_attn = noise(arg_keys[14], (D,), 0.3, 3.0, (), jnp.float32)
    gain_ffn = jnp.clip(1.0 + 0.1 * jax.random.normal(arg_keys[15], (D,), jnp.float32), 0.5, 1.5)
    shift_ffn = noise(arg_keys[16], (D,), 0.3, 3.0, (), jnp.float32)
    valid_lengths = draw_valid_lengths(jax.random.fold_in(arg_keys[18], 71), 0)
    return dict(hidden_in=hidden_in, cotangent=cotangent, w_query=w_query, w_key=w_key, w_value=w_value, w_out=w_out, w_up=w_up, w_down=w_down, bias_query=bias_query, bias_value=bias_value, bias_out=bias_out, bias_up=bias_up, bias_down=bias_down, gain_attn=gain_attn, shift_attn=shift_attn, gain_ffn=gain_ffn, shift_ffn=shift_ffn, valid_lengths=valid_lengths)


@jax.custom_vjp
def low(v):
    return lax.optimization_barrier(v.astype(jnp.bfloat16)).astype(jnp.float32)

@jax.custom_vjp
def low_back(v):
    return v

def low_keep(v):
    return (low(v), None)

def low_pass(kept, grad):
    return (grad,)

def back_keep(v):
    return (v, None)

def back_low(kept, grad):
    return (low(grad),)
low.defvjp(low_keep, low_pass)
low_back.defvjp(back_keep, back_low)
EPSILON = 1e-12
MASKED = -1e+30
HIGHEST = lax.Precision.HIGHEST

def matmul(left_side, right_side):
    return jnp.dot(left_side, right_side, precision=HIGHEST)

def both_ways(value_in):
    return low(low_back(value_in))

def layer_norm(hidden, gain_vec, shift_vec):
    center = hidden - lax.optimization_barrier(jnp.mean(hidden, axis=-1, keepdims=True))
    variance = lax.optimization_barrier(jnp.mean(center * center, axis=-1, keepdims=True))
    return center * lax.rsqrt(variance + EPSILON) * gain_vec + shift_vec

def attend_one(sliced):
    queries, keys_in, values, length = sliced
    scale = float(queries.shape[-1]) ** (-0.5)
    scores = low_back(jnp.einsum('qhd,khd->hqk', queries, keys_in, precision=HIGHEST) * scale)
    visible = jnp.arange(queries.shape[0]) < length
    scores = jnp.where(visible[None, None, :], scores, MASKED)
    weights_soft = low(jax.nn.softmax(scores, axis=-1))
    return jnp.einsum('hqk,khd->qhd', weights_soft, values, precision=HIGHEST)

def forward(params, inputs, lengths):
    w_query, w_key, w_value, w_out, w_up, w_down, bias_query, bias_value, bias_out, bias_up, bias_down, gain_attn, shift_attn, gain_ffn, shift_ffn = params
    row_count = inputs.shape[0]
    head_size = inputs.shape[1] // HEADS

    def shaped(matrix):
        return matrix.reshape(row_count // SEQ, SEQ, HEADS, head_size)
    queries = both_ways(matmul(inputs, low(w_query)) + bias_query)
    keys_all = both_ways(matmul(inputs, low(w_key)))
    values = both_ways(matmul(inputs, low(w_value)) + bias_value)
    context = lax.map(jax.checkpoint(attend_one), (shaped(queries), shaped(keys_all), shaped(values), lengths))
    context = both_ways(context.reshape(row_count, -1))
    attention = low_back(matmul(context, low(w_out).T))
    normed = layer_norm(inputs + attention + bias_out, gain_attn, shift_attn)
    upper_pre = low_back(matmul(low(normed), low(w_up)) + bias_up)
    active = low(jax.nn.gelu(upper_pre, approximate=False))
    mixed_out = low_back(matmul(active, low(w_down).T))
    return layer_norm(normed + mixed_out + bias_down, gain_ffn, shift_ffn)

def reference(hidden_in, cotangent, w_query, w_key, w_value, w_out, w_up, w_down, bias_query, bias_value, bias_out, bias_up, bias_down, gain_attn, shift_attn, gain_ffn, shift_ffn, valid_lengths):
    params = (w_query, w_key, w_value, w_out, w_up, w_down, bias_query, bias_value, bias_out, bias_up, bias_down, gain_attn, shift_attn, gain_ffn, shift_ffn)
    groups = N_DP
    per_group = hidden_in.shape[0] // groups
    model_width = hidden_in.shape[1]
    blocks = (hidden_in.astype(jnp.float32).reshape(groups, per_group, model_width), cotangent.astype(jnp.float32).reshape(groups, per_group, model_width), valid_lengths.reshape(groups, -1))

    def group_step(totals, sliced):
        block_in, block_cot, block_len = sliced

        def run_block(params_in, inputs_in):
            return forward(params_in, inputs_in, block_len)
        out_block, pullback = jax.vjp(run_block, params, block_in)
        grad_params, grad_in = pullback(block_cot)
        totals = jax.tree.map(jnp.add, totals, grad_params)
        return (totals, (out_block, grad_in))
    initial = jax.tree.map(jnp.zeros_like, params)
    totals, (outputs, grads_in) = lax.scan(group_step, initial, blocks)
    factor = 1.0 / float(TOKENS) ** 0.5
    g_wq, g_wk, g_wv, g_wo, g_wu, g_wd, g_bq, g_bv, g_bo, g_bu, g_bd, g_ga, g_sa, g_gf, g_sf = totals
    return (outputs.reshape(-1, model_width).astype(jnp.bfloat16), grads_in.reshape(-1, model_width).astype(jnp.bfloat16), g_wq * factor, g_wk * factor, g_wv * factor, g_wo * factor, g_wu * factor, g_wd * factor, g_bq * factor, g_bv * factor, g_bo * factor, g_bu * factor, g_bd * factor, g_ga * factor, g_sa * factor, g_gf * factor, g_sf * factor)
```

```python
import math

import jax
import jax.numpy as jnp
from jax import lax
from jax.experimental import pallas as pl
from jax.experimental.pallas import tpu as pltpu
from jax.sharding import PartitionSpec as P

HEADS = 16
EPSILON = 1e-12
MASKED = -1e30
BF16 = jnp.bfloat16
F32 = jnp.float32


ORDER = (0, 2, 4, 6, 1, 3, 5, 7)
BIT_CORE, BIT_X, BIT_Y = 1, 2, 4


def matmul(left_side, right_side):
    return jnp.dot(left_side, right_side, preferred_element_type=F32)


def contract_rows(left_side, right_side):
    return lax.dot_general(
        left_side, right_side, (((0,), (0,)), ((), ())), preferred_element_type=F32
    )


def contract_cols(left_side, right_side):
    return lax.dot_general(
        left_side, right_side, (((1,), (1,)), ((), ())), preferred_element_type=F32
    )


def swap(array, bit):
    return lax.ppermute(array, "dp", [(i, i ^ bit) for i in range(lax.axis_size("dp"))])


def shift(array, step):
    size = lax.axis_size("tensor")
    return lax.ppermute(array, "tensor", [(i, (i + step) % size) for i in range(size)])


def gather_near(shard):
    size = lax.axis_size("tensor")
    rows = shard.shape[0]
    column = jnp.concatenate([shard] + [shift(shard, r) for r in range(1, size)], axis=1)
    by_x, by_y = swap(column, BIT_X), swap(column, BIT_Y)
    corner = [swap(by_x[: rows // 2], BIT_Y), swap(by_y[rows // 2 :], BIT_X)]
    plane = jnp.concatenate([column, by_x, by_y] + corner, axis=0)
    return jnp.concatenate([plane, swap(plane, BIT_CORE)], axis=0)


def scatter_near(own_half, other_half):
    size = lax.axis_size("tensor")
    arrived = swap(other_half.astype(BF16), BIT_CORE)
    plane = (own_half + arrived.astype(F32)).astype(BF16)
    rows = plane.shape[0] // 4
    cols = plane.shape[1] // size
    half = rows // 2
    part = [plane[k * rows : (k + 1) * rows] for k in range(4)]
    to_y = swap(part[3][:half], BIT_X)
    to_x = swap(part[3][half:], BIT_Y)

    def add(first, second):
        return (first.astype(F32) + second.astype(F32)).astype(BF16)

    x_part = jnp.concatenate([part[1][:half], add(part[1][half:], to_x)], axis=0)
    y_part = jnp.concatenate([add(part[2][:half], to_y), part[2][half:]], axis=0)
    column = (
        part[0].astype(F32)
        + swap(x_part, BIT_X).astype(F32)
        + swap(y_part, BIT_Y).astype(F32)
    )
    total = column[:, :cols]
    for r in range(1, size):
        total += shift(column[:, r * cols : (r + 1) * cols].astype(BF16), -r).astype(F32)
    return total


def gather_far(shard):
    return lax.all_gather(
        lax.all_gather(shard, "tensor", axis=1, tiled=True), "dp", axis=0, tiled=True
    )


def scatter_far(own_half, other_half):
    whole = jnp.concatenate([own_half, other_half], axis=0).astype(BF16)
    part = lax.psum_scatter(whole, "dp", scatter_dimension=0, tiled=True)
    return lax.psum_scatter(part, "tensor", scatter_dimension=1, tiled=True).astype(F32)


def sum_near(vector):
    for axis in ("tensor", "dp"):
        size, bit = lax.axis_size(axis), 1
        while bit < size:
            vector = vector + lax.ppermute(vector, axis, [(i, i ^ bit) for i in range(size)])
            bit *= 2
    return vector


def permute_blocks(array, index, width):
    rows, cols = array.shape

    def body(index_ref, in_ref, out_ref):
        out_ref[...] = in_ref[...]

    return pl.pallas_call(
        body,
        out_shape=jax.ShapeDtypeStruct(array.shape, array.dtype),
        grid_spec=pltpu.PrefetchScalarGridSpec(
            num_scalar_prefetch=1,
            grid=(cols // width,),
            in_specs=[pl.BlockSpec((rows, width), lambda k, index_ref: (0, index_ref[k]))],
            out_specs=pl.BlockSpec((rows, width), lambda k, index_ref: (0, k)),
        ),
        cost_estimate=pl.CostEstimate(
            flops=0, bytes_accessed=2 * array.size * array.dtype.itemsize, transcendentals=0
        ),
        name="permute_blocks",
    )(index, array)


def soft_weights(queries, keys, visible, scale):
    scores = contract_cols(queries, keys) * scale
    scores = jnp.where(visible, scores, MASKED)
    exponent = jnp.exp(scores - jnp.max(scores, axis=-1, keepdims=True))
    return exponent / jnp.sum(exponent, axis=-1, keepdims=True)


def pairs_of(width, head_size):
    lanes = max(128, head_size)
    return [(start, lanes, lanes // head_size) for start in range(0, width, lanes)]


def keep_head(array, which, head_size):
    lane = lax.broadcasted_iota(jnp.int32, array.shape, 1)
    return jnp.where(lane // head_size == which, array, jnp.zeros_like(array))


def attend_forward(qkv_q, qkv_kv, length, head_size, groups):
    q_rows = qkv_q.shape[0]
    k_rows = qkv_kv.shape[0]
    block = qkv_q.shape[1] // groups
    width = block // 3
    scale = float(head_size) ** (-0.5)

    def body(length_ref, q_ref, kv_ref, out_ref):
        visible = lax.broadcasted_iota(jnp.int32, (q_rows, k_rows), 1) < length_ref[0]
        for start, lanes, held in pairs_of(width, head_size):
            queries = q_ref[:, start : start + lanes]
            keys = kv_ref[:, width + start : width + start + lanes]
            values = kv_ref[:, 2 * width + start : 2 * width + start + lanes]
            total = jnp.zeros((q_rows, lanes), F32)
            for which in range(held):
                probs = soft_weights(keep_head(queries, which, head_size), keys, visible, scale)
                total += keep_head(matmul(probs.astype(BF16), values), which, head_size)
            out_ref[:, start : start + lanes] = total.astype(BF16)

    return pl.pallas_call(
        body,
        out_shape=jax.ShapeDtypeStruct((q_rows, groups * width), BF16),
        grid_spec=pltpu.PrefetchScalarGridSpec(
            num_scalar_prefetch=1,
            grid=(groups,),
            in_specs=[
                pl.BlockSpec((q_rows, block), lambda g, length_ref: (0, g)),
                pl.BlockSpec((k_rows, block), lambda g, length_ref: (0, g)),
            ],
            out_specs=pl.BlockSpec((q_rows, width), lambda g, length_ref: (0, g)),
        ),
        cost_estimate=pl.CostEstimate(
            flops=4 * q_rows * k_rows * width * groups,
            bytes_accessed=2 * (2 * q_rows + 2 * k_rows) * width * groups,
            transcendentals=q_rows * k_rows * groups * width // head_size,
        ),
        name="attend_forward",
    )(length, qkv_q, qkv_kv)


def attend_backward(qkv_q, qkv_kv, grad_context, length, head_size, groups):
    q_rows = qkv_q.shape[0]
    k_rows = qkv_kv.shape[0]
    block = qkv_q.shape[1] // groups
    width = block // 3
    scale = float(head_size) ** (-0.5)

    def body(length_ref, q_ref, kv_ref, grad_ref, dq_ref, dkv_ref):
        visible = lax.broadcasted_iota(jnp.int32, (q_rows, k_rows), 1) < length_ref[0]
        for start, lanes, held in pairs_of(width, head_size):
            queries = q_ref[:, start : start + lanes]
            keys = kv_ref[:, width + start : width + start + lanes]
            values = kv_ref[:, 2 * width + start : 2 * width + start + lanes]
            grads = grad_ref[:, start : start + lanes]
            grad_q = jnp.zeros((q_rows, lanes), F32)
            grad_k = jnp.zeros((k_rows, lanes), F32)
            grad_v = jnp.zeros((k_rows, lanes), F32)
            for which in range(held):
                mine = keep_head(grads, which, head_size)
                query = keep_head(queries, which, head_size)
                probs = soft_weights(query, keys, visible, scale)
                grad_v += contract_rows(probs.astype(BF16), mine)
                grad_probs = contract_cols(mine, values)
                inner = jnp.sum(probs * grad_probs, axis=-1, keepdims=True)
                grad_scores = (probs * (grad_probs - inner)).astype(BF16)
                grad_q += keep_head(matmul(grad_scores, keys), which, head_size)
                grad_k += contract_rows(grad_scores, query)
            dq_ref[:, start : start + lanes] = (grad_q * scale).astype(BF16)
            dkv_ref[:, start : start + lanes] = (grad_k * scale).astype(BF16)
            dkv_ref[:, width + start : width + start + lanes] = grad_v.astype(BF16)

    return pl.pallas_call(
        body,
        out_shape=(
            jax.ShapeDtypeStruct((q_rows, groups * width), BF16),
            jax.ShapeDtypeStruct((k_rows, groups * 2 * width), BF16),
        ),
        grid_spec=pltpu.PrefetchScalarGridSpec(
            num_scalar_prefetch=1,
            grid=(groups,),
            in_specs=[
                pl.BlockSpec((q_rows, block), lambda g, length_ref: (0, g)),
                pl.BlockSpec((k_rows, block), lambda g, length_ref: (0, g)),
                pl.BlockSpec((q_rows, width), lambda g, length_ref: (0, g)),
            ],
            out_specs=[
                pl.BlockSpec((q_rows, width), lambda g, length_ref: (0, g)),
                pl.BlockSpec((k_rows, 2 * width), lambda g, length_ref: (0, g)),
            ],
        ),
        cost_estimate=pl.CostEstimate(
            flops=10 * q_rows * k_rows * width * groups,
            bytes_accessed=2 * (3 * q_rows + 4 * k_rows) * width * groups,
            transcendentals=q_rows * k_rows * groups * width // head_size,
        ),
        name="attend_backward",
    )(length, qkv_q, qkv_kv, grad_context)


def norm_forward(hidden, gain_vec, shift_vec):
    center = hidden - jnp.mean(hidden, axis=-1, keepdims=True)
    variance = jnp.mean(center * center, axis=-1, keepdims=True)
    inv_root = lax.rsqrt(variance + EPSILON)
    normal = center * inv_root
    return (normal * gain_vec + shift_vec, normal, inv_root)


def norm_backward(grad_in, normal, inv_root, gain_vec):
    grad_normal = grad_in * gain_vec
    grad_gain = jnp.sum(grad_in * normal, axis=0)
    grad_shift = jnp.sum(grad_in, axis=0)
    grad_hidden = inv_root * (
        grad_normal
        - jnp.mean(grad_normal, axis=-1, keepdims=True)
        - normal * jnp.mean(grad_normal * normal, axis=-1, keepdims=True)
    )
    return (grad_hidden, grad_gain, grad_shift)


def per_device(
    hidden_in,
    cotangent,
    w_query,
    w_key,
    w_value,
    w_out,
    w_up,
    w_down,
    bias_query,
    bias_value,
    bias_out,
    bias_up,
    bias_down,
    gain_attn,
    shift_attn,
    gain_ffn,
    shift_ffn,
    valid_lengths,
):
    rows, model_width = hidden_in.shape
    n_tensor = lax.axis_size("tensor")
    n_data = lax.axis_size("dp")
    tensor_at = lax.axis_index("tensor")
    data_at = lax.axis_index("dp")
    seq_len = rows * n_tensor // valid_lengths.shape[0]
    spread_over = seq_len // rows
    head_size = model_width // HEADS
    head_cols = w_query.shape[1]
    unit_cols = w_up.shape[1]
    factor = 1.0 / math.sqrt(rows * n_tensor * n_data)
    near = n_data == len(ORDER) and spread_over == 1
    width = model_width // n_data
    gather = gather_near if near else gather_far
    scatter = scatter_near if near else scatter_far

    if near:
        order = jnp.array(ORDER, jnp.int32)
        back = jnp.array([ORDER.index(k) for k in range(n_data)], jnp.int32)
        block_at = jnp.bitwise_xor(order, data_at)
        place_of = back[jnp.bitwise_xor(jnp.arange(n_data, dtype=jnp.int32), data_at)]
        column_at = (tensor_at - jnp.arange(n_tensor)) % n_tensor
    else:
        column_at = jnp.arange(n_tensor)

    def arrange(array):
        return permute_blocks(array, block_at, width) if near else array

    def restore(array):
        return permute_blocks(array, place_of, width) if near else array

    def column_vector(vector):
        return vector.reshape(n_tensor, -1)[column_at] if near else vector.reshape(n_tensor, -1)

    def column_vector_back(blocks):
        return (blocks[column_at] if near else blocks).reshape(-1)

    vectors = jnp.stack([bias_out, bias_down, gain_attn, shift_attn, gain_ffn, shift_ffn])
    if near:
        vectors = vectors.reshape(-1, n_data, width)[:, block_at].reshape(-1, model_width)
    bias_out, bias_down, gain_attn, shift_attn, gain_ffn, shift_ffn = vectors
    query_bias, value_bias = column_vector(bias_query), column_vector(bias_value)
    bias_qkv = jnp.concatenate(
        [query_bias, jnp.zeros_like(query_bias), value_bias], axis=1
    ).reshape(-1)
    bias_units = column_vector(bias_up).reshape(-1)
    length = lax.dynamic_slice_in_dim(valid_lengths, tensor_at // spread_over, 1)

    qkv_full = gather(
        jnp.concatenate([w_query.astype(BF16), w_key.astype(BF16), w_value.astype(BF16)], axis=1)
    )
    out_full = gather(w_out.astype(BF16))
    up_full = gather(w_up.astype(BF16))
    down_full = gather(w_down.astype(BF16))

    inputs = arrange(hidden_in)
    grad_output = arrange(cotangent).astype(F32)

    qkv = (matmul(inputs, qkv_full) + bias_qkv).astype(BF16)
    if spread_over > 1:
        members = [
            list(range(k, k + spread_over)) for k in range(0, n_tensor, spread_over)
        ]
        qkv_seq = lax.all_gather(qkv, "tensor", axis_index_groups=members, axis=0, tiled=True)
    else:
        qkv_seq = qkv
    context = attend_forward(qkv, qkv_seq, length, head_size, n_tensor)
    attention = contract_cols(context, out_full)
    normed, normal_attn, root_attn = norm_forward(
        inputs.astype(F32) + attention + bias_out, gain_attn, shift_attn
    )
    normed_low = normed.astype(BF16)
    upper = matmul(normed_low, up_full) + bias_units
    cumulative = 0.5 * (1.0 + lax.erf(upper * math.sqrt(0.5)))
    slope = cumulative + upper * jnp.exp(-0.5 * upper * upper) * (1.0 / math.sqrt(2.0 * math.pi))
    active = (upper * cumulative).astype(BF16)
    slope, active = lax.optimization_barrier((slope, active))
    mixed = contract_cols(active, down_full)
    result, normal_ffn, root_ffn = norm_forward(normed + mixed + bias_down, gain_ffn, shift_ffn)

    half = model_width // 2
    grad_second, grad_gain_ffn, grad_shift_ffn = norm_backward(
        grad_output, normal_ffn, root_ffn, gain_ffn
    )
    grad_bias_down = jnp.sum(grad_second, axis=0)
    mixed_low = grad_second.astype(BF16)
    grad_down = scatter(
        contract_rows(mixed_low[:, :half], active), contract_rows(mixed_low[:, half:], active)
    )
    grad_upper = (matmul(mixed_low, down_full) * slope).astype(BF16)
    grad_bias_up = jnp.sum(grad_upper, axis=0, dtype=F32)
    grad_up = scatter(
        contract_rows(normed_low[:, :half], grad_upper),
        contract_rows(normed_low[:, half:], grad_upper),
    )
    grad_normed = grad_second + contract_cols(grad_upper, up_full)
    grad_first, grad_gain_attn, grad_shift_attn = norm_backward(
        grad_normed, normal_attn, root_attn, gain_attn
    )
    grad_bias_out = jnp.sum(grad_first, axis=0)
    attn_low = grad_first.astype(BF16)
    grad_context = matmul(attn_low, out_full).astype(BF16)
    grad_out = scatter(
        contract_rows(attn_low[:, :half], context), contract_rows(attn_low[:, half:], context)
    )
    grad_q, grad_kv = attend_backward(qkv, qkv_seq, grad_context, length, head_size, n_tensor)
    if spread_over > 1:
        grad_kv = lax.psum_scatter(
            grad_kv.astype(F32),
            "tensor",
            scatter_dimension=0,
            axis_index_groups=members,
            tiled=True,
        ).astype(BF16)
    grad_qkv = jnp.concatenate(
        [grad_q.reshape(rows, n_tensor, -1), grad_kv.reshape(rows, n_tensor, -1)], axis=2
    ).reshape(rows, -1)
    grad_bias_qkv = jnp.sum(grad_qkv, axis=0, dtype=F32).reshape(n_tensor, 3, head_cols)
    grad_qkv_w = scatter(
        contract_rows(inputs[:, :half], grad_qkv), contract_rows(inputs[:, half:], grad_qkv)
    )
    grad_input = restore((grad_first + contract_cols(grad_qkv, qkv_full)).astype(BF16))
    output = restore(result.astype(BF16))

    sums = jnp.stack(
        [
            grad_bias_out,
            grad_bias_down,
            grad_gain_attn,
            grad_shift_attn,
            grad_gain_ffn,
            grad_shift_ffn,
        ]
    )
    if near:
        sums = sums.reshape(-1, n_data, width)[:, place_of]
    sums = jnp.concatenate(
        [
            sums.reshape(-1),
            column_vector_back(grad_bias_qkv[:, 0]),
            column_vector_back(grad_bias_qkv[:, 2]),
            column_vector_back(grad_bias_up.reshape(n_tensor, -1)),
        ]
    ).reshape(-1, 128)
    sums = (sum_near(sums) if near else lax.psum(sums, ("dp", "tensor"))).reshape(-1) * factor
    v_out, v_down, v_gain_attn, v_shift_attn, v_gain_ffn, v_shift_ffn, v_query, v_value = (
        sums[k * model_width : (k + 1) * model_width] for k in range(8)
    )
    v_up = sums[8 * model_width :]
    return (
        output,
        grad_input,
        grad_qkv_w[:, :head_cols] * factor,
        grad_qkv_w[:, head_cols : 2 * head_cols] * factor,
        grad_qkv_w[:, 2 * head_cols :] * factor,
        grad_out * factor,
        grad_up * factor,
        grad_down * factor,
        v_query,
        v_value,
        v_out,
        v_up,
        v_down,
        v_gain_attn,
        v_shift_attn,
        v_gain_ffn,
        v_shift_ffn,
    )


def solution(mesh):
    tokens, matrix, copied = P(("dp", "tensor"), None), P("dp", "tensor"), P()
    return jax.shard_map(
        per_device,
        mesh=mesh,
        in_specs=(tokens,) * 2 + (matrix,) * 6 + (copied,) * 9 + (P("dp"),),
        out_specs=(tokens,) * 2 + (matrix,) * 6 + (copied,) * 9,
        check_vma=False,
    )
```

```python
import math

import jax
import jax.numpy as jnp
from jax import lax
from jax.experimental import pallas as pl
from jax.experimental.pallas import tpu as pltpu
from jax.sharding import PartitionSpec as P

HEADS = 16
EPSILON = 1e-12
MASKED = -1e30
BF16 = jnp.bfloat16
F32 = jnp.float32

ORDER = (0, 2, 4, 6, 1, 3, 5, 7)
BIT_CORE, BIT_X, BIT_Y = 1, 2, 4


def matmul(left_side, right_side):
    return jnp.dot(left_side, right_side, preferred_element_type=F32)


def contract_rows(left_side, right_side):
    return lax.dot_general(
        left_side, right_side, (((0,), (0,)), ((), ())), preferred_element_type=F32
    )


def contract_cols(left_side, right_side):
    return lax.dot_general(
        left_side, right_side, (((1,), (1,)), ((), ())), preferred_element_type=F32
    )


FORWARD_ID = 1


def neighbour(index, bit):
    return index + bit - 2 * bit * ((index // bit) % 2)


def greet(partners):
    barrier = pltpu.get_barrier_semaphore()
    for partner in partners:
        pl.semaphore_signal(
            barrier, inc=1, device_id=partner, device_id_type=pl.DeviceIdType.MESH
        )
    pl.semaphore_wait(barrier, len(partners))


def forward_near(shards, inputs, visible, bias_qkv, bias_out, gain, shift_vec, bias_units, head_size):
    size = lax.axis_size("tensor")
    rows, width = inputs.shape
    block = shards[0].shape[0]
    cols = [shard.shape[1] for shard in shards]
    full = [(len(ORDER) * block, size * c) for c in cols]
    units = full[2][1]
    tile = 512
    half = block // 2
    attn = cols[0] // 3

    def body(
        a_in, o_in, u_in, d_in, x_ref, visible_ref, bias_qkv_ref, bias_out_ref, gain_ref, shift_ref,
        bias_units_ref, a_out, o_out, u_out, d_out, qkv_ref, context_ref, hidden_ref, active_out,
        slope_out, a_ref, o_ref, u_ref, low_ref, active_ref, slope_ref, local_sem, own_sem, send_sem,
        recv_sem, tile_sem,
    ):
        data_at, tensor_at = lax.axis_index("dp"), lax.axis_index("tensor")
        shard_refs = (a_in, o_in, u_in, d_in)
        places = (a_ref, o_ref, u_ref, d_out)

        def dp_partner(bit):
            return (neighbour(data_at, bit), tensor_at)

        def z_partner(step):
            return (data_at, (tensor_at + step) % size)

        by_x, by_y, by_core = dp_partner(BIT_X), dp_partner(BIT_Y), dp_partner(BIT_CORE)
        greet([by_x, by_y, by_core] + [z_partner(r) for r in range(1, size)])
        copies = {}

        def send(g, slot, source, target, device):
            copy = pltpu.make_async_remote_copy(
                src_ref=source,
                dst_ref=target,
                send_sem=send_sem.at[g, slot],
                recv_sem=recv_sem.at[g, slot],
                device_id=device,
                device_id_type=pl.DeviceIdType.MESH,
            )
            copies[g, slot] = copy
            copy.start()

        def arrived(g, *slots):
            for slot in slots:
                copies[g, slot].wait_recv()

        def part(g, start, count):
            return places[g].at[start : start + count, :]

        def send_column(g):
            own[g].wait()
            arrived(g, 0, 1, 2)
            send(g, 3, part(g, 0, block), part(g, block, block), by_x)
            send(g, 4, part(g, 0, block), part(g, 2 * block, block), by_y)

        def send_corner(g):
            arrived(g, 3, 4)
            send(g, 5, part(g, block, half), part(g, 3 * block, half), by_y)
            send(g, 6, part(g, 2 * block + half, half), part(g, 3 * block + half, half), by_x)
            for k in range(3):
                send(g, 7 + k, part(g, k * block, block), part(g, (4 + k) * block, block), by_core)

        def send_last(g):
            arrived(g, 5, 6)
            send(g, 10, part(g, 3 * block, block), part(g, 7 * block, block), by_core)

        def finish(g):
            arrived(g, 7, 8, 9, 10)

        saves = []

        def save(g, target):
            copy = pltpu.make_async_copy(places[g], target, local_sem.at[g])
            copy.start()
            saves.append(copy)

        own = []
        for g in range(4):
            copy = pltpu.make_async_copy(
                shard_refs[g], places[g].at[0:block, 0 : cols[g]], own_sem.at[g]
            )
            copy.start()
            own.append(copy)
            for r in range(1, size):
                send(
                    g,
                    r - 1,
                    shard_refs[g],
                    places[g].at[0:block, r * cols[g] : (r + 1) * cols[g]],
                    z_partner(r),
                )

        send_column(0)
        send_column(1)
        send_corner(0)
        send_column(2)
        send_corner(1)
        send_last(0)
        finish(0)
        save(0, a_out)

        def project(r, carry):
            at = pl.multiple_of(r * cols[0], 128)
            total = matmul(x_ref[...], a_ref[:, pl.ds(at, cols[0])])
            qkv_ref[:, pl.ds(at, cols[0])] = (total + bias_qkv_ref[:, pl.ds(at, cols[0])]).astype(BF16)
            return carry

        lax.fori_loop(0, size, project, 0)
        scale = float(head_size) ** (-0.5)

        def attend(r, carry):
            at = pl.multiple_of(r * cols[0], 128)
            to = pl.multiple_of(r * attn, 128)
            seen = visible_ref[...] > 0.0
            for start, lanes, held in pairs_of(attn, head_size):
                queries = qkv_ref[:, pl.ds(at + start, lanes)]
                keys = qkv_ref[:, pl.ds(at + attn + start, lanes)]
                values = qkv_ref[:, pl.ds(at + 2 * attn + start, lanes)]
                total = jnp.zeros((rows, lanes), F32)
                for which in range(held):
                    probs = soft_weights(keep_head(queries, which, head_size), keys, seen, scale)
                    total += keep_head(matmul(probs.astype(BF16), values), which, head_size)
                context_ref[:, pl.ds(to + start, lanes)] = total.astype(BF16)
            return carry

        lax.fori_loop(0, size, attend, 0)
        send_last(1)
        send_corner(2)
        send_column(3)
        finish(1)
        save(1, o_out)

        def output(j, carry):
            at = pl.multiple_of(j * 256, 256)
            total = contract_cols(context_ref[...], o_ref[pl.ds(at, 256), :])
            given = x_ref[:, pl.ds(at, 256)].astype(F32)
            hidden_ref[:, pl.ds(at, 256)] = given + total + bias_out_ref[:, pl.ds(at, 256)]
            return carry

        lax.fori_loop(0, width // 256, output, 0)

        def norm(j, carry):
            at = pl.multiple_of(j * 64, 64)
            normed = norm_forward(hidden_ref[pl.ds(at, 64), :], gain_ref[...], shift_ref[...])[0]
            low_ref[pl.ds(at, 64), :] = normed.astype(BF16)
            return carry

        lax.fori_loop(0, rows // 64, norm, 0)
        send_last(2)
        finish(2)
        save(2, u_out)

        def tile_copies(j, at):
            return (
                pltpu.make_async_copy(
                    active_ref.at[:, pl.ds(at, tile)], active_out.at[:, pl.ds(at, tile)], tile_sem.at[0, j]
                ),
                pltpu.make_async_copy(
                    slope_ref.at[:, pl.ds(at, tile)], slope_out.at[:, pl.ds(at, tile)], tile_sem.at[1, j]
                ),
            )

        def raise_up(j, carry):
            at = pl.multiple_of(j * tile, tile)
            total = matmul(low_ref[...], u_ref[:, pl.ds(at, tile)])
            active, slope = activate(total, bias_units_ref[:, pl.ds(at, tile)])
            active_ref[:, pl.ds(at, tile)] = active.astype(BF16)
            slope_ref[:, pl.ds(at, tile)] = slope
            for copy in tile_copies(j, at):
                copy.start()
            return carry

        lax.fori_loop(0, units // tile, raise_up, 0)
        send_corner(3)
        send_last(3)
        finish(3)

        def settle(j, carry):
            for copy in tile_copies(j, pl.multiple_of(j * tile, tile)):
                copy.wait()
            return carry

        lax.fori_loop(0, units // tile, settle, 0)
        for copy in saves:
            copy.wait()
        for copy in copies.values():
            copy.wait_send()

    anywhere, inside = pl.BlockSpec(memory_space=pl.ANY), pl.BlockSpec(memory_space=pltpu.VMEM)
    sent = sum(2 * block * c * size * 7 for c in cols)
    return pl.pallas_call(
        body,
        out_shape=[jax.ShapeDtypeStruct(shape, BF16) for shape in full]
        + [
            jax.ShapeDtypeStruct((rows, full[0][1]), BF16),
            jax.ShapeDtypeStruct((rows, width), BF16),
            jax.ShapeDtypeStruct((rows, width), F32),
            jax.ShapeDtypeStruct((rows, units), BF16),
            jax.ShapeDtypeStruct((rows, units), F32),
        ],
        in_specs=[anywhere] * 4 + [inside] * 7,
        out_specs=[anywhere] * 4 + [inside] * 3 + [anywhere] * 2,
        scratch_shapes=[pltpu.VMEM(shape, BF16) for shape in full[:3]]
        + [
            pltpu.VMEM((rows, width), BF16),
            pltpu.VMEM((rows, units), BF16),
            pltpu.VMEM((rows, units), F32),
            pltpu.SemaphoreType.DMA((4,)),
            pltpu.SemaphoreType.DMA((4,)),
            pltpu.SemaphoreType.DMA((4, 11)),
            pltpu.SemaphoreType.DMA((4, 11)),
            pltpu.SemaphoreType.DMA((2, units // tile)),
        ],
        compiler_params=pltpu.CompilerParams(
            collective_id=FORWARD_ID, has_side_effects=True, vmem_limit_bytes=60 * 2**20
        ),
        cost_estimate=pl.CostEstimate(
            flops=2 * rows * (full[0][1] + width + units) * width,
            bytes_accessed=2 * sent,
            transcendentals=rows * units,
        ),
        name="forward_near",
    )(*shards, inputs, visible, bias_qkv, bias_out, gain, shift_vec, bias_units)


BACKWARD_ID = 2
TILE = 512


def backward_near(mixed_low, normed_low, inputs, context, grad_second, normal, root, gain, visible,
                  active, slope, qkv, weights, vectors, head_size):
    size = lax.axis_size("tensor")
    rows, width = mixed_low.shape
    block = width // len(ORDER)
    middle = width // 2
    half = block // 2
    full = [weight.shape[1] for weight in weights]
    cols = [c // size for c in full]
    attn = cols[0] // 3
    units = full[2]
    A, O, U, D = range(4)
    vector_rows = (6 * width + 2 * full[1] + units) // 128
    v_query, v_value, v_up = 6 * width // 128, (6 * width + full[1]) // 128, (6 * width + 2 * full[1]) // 128
    scale = float(head_size) ** (-0.5)

    def body(
        mixed_ref, mixed_t, normed_t, input_t, context_ref, second_in, normal_in, root_ref, gain_ref,
        visible_ref, active_in, slope_in, qkv_in, a_in, o_in, u_in, d_in, vectors_ref,
        a_out, o_out, u_out, d_out, grad_out, sums_out,
        w_buf, act_buf, slope_buf, gu_ref, grad_ref, low_ref, low_t, gctx_ref, qkv_buf, send_buf,
        send_o, a_plane, o_plane, u_plane, d_plane, a_corner, o_corner, u_corner, d_corner, a_side,
        o_side, u_side, d_side, a_zin, o_zin, u_zin, d_zin, v_ref, v_in, load_sem, second_sem, core_send,
        core_recv, send_sem, recv_sem, v_send, v_recv,
    ):
        data_at, tensor_at = lax.axis_index("dp"), lax.axis_index("tensor")
        planes = (a_plane, o_plane, u_plane, d_plane)
        corners = (a_corner, o_corner, u_corner, d_corner)
        sides = (a_side, o_side, u_side, d_side)
        zins = (a_zin, o_zin, u_zin, d_zin)
        outs = (a_out, o_out, u_out, d_out)
        sources = (send_buf, send_o, send_buf, send_buf)

        def dp_partner(bit):
            return (neighbour(data_at, bit), tensor_at)

        def z_partner(step):
            return (data_at, (tensor_at + size + step) % size)

        by_x, by_y, by_core = dp_partner(BIT_X), dp_partner(BIT_Y), dp_partner(BIT_CORE)

        def column(j, span=TILE):
            return pl.ds(pl.multiple_of(j * span, 128), span)

        def load(row, source, buffer, j):
            return pltpu.make_async_copy(
                source.at[:, column(j)], buffer.at[j % 2], load_sem.at[row, j % 2]
            )

        def over_tiles(count, loads, step):
            for row, source, buffer in loads:
                load(row, source, buffer, 0).start()

            def one(j, carry):
                @pl.when(j + 1 < count)
                def _():
                    for row, source, buffer in loads:
                        load(row, source, buffer, j + 1).start()

                for row, source, buffer in loads:
                    load(row, source, buffer, j).wait()
                step(j)
                return carry

            lax.fori_loop(0, count, one, 0)

        def remote(source, target, send, receive, device):
            return pltpu.make_async_remote_copy(
                src_ref=source,
                dst_ref=target,
                send_sem=send,
                recv_sem=receive,
                device_id=device,
                device_id_type=pl.DeviceIdType.MESH,
            )

        def core_copy(g, j):
            return remote(
                sources[g].at[:, column(j)],
                planes[g].at[:, column(j)],
                core_send.at[g, j],
                core_recv.at[g, j],
                by_core,
            )

        copies = {}

        def send(g, slot, source, target, device):
            copies[g, slot] = remote(
                source, target, send_sem.at[g, slot], recv_sem.at[g, slot], device
            )
            copies[g, slot].start()

        def arrived(g, *slots):
            for slot in slots:
                copies[g, slot].wait_recv()

        def other_tile(g, left_t, right, j):
            sources[g][:, column(j)] = matmul(left_t[middle:, :], right).astype(BF16)
            core_copy(g, j).start()

        def own_tile(g, left_t, right, j):
            core_copy(g, j).wait_recv()
            total = matmul(left_t[:middle, :], right) + planes[g][:, column(j)].astype(F32)
            planes[g][:, column(j)] = total.astype(BF16)

        def send_corner(g):
            plane = planes[g]
            send(g, 0, plane.at[3 * block : 3 * block + half], corners[g].at[0], by_x)
            send(g, 1, plane.at[3 * block + half :], corners[g].at[1], by_y)

        def add_rows(g, start, more):
            def one(j, carry):
                at = column(j, cols[g])
                total = planes[g][start : start + half, at].astype(F32) + more[:, at].astype(F32)
                planes[g][start : start + half, at] = total.astype(BF16)
                return carry

            lax.fori_loop(0, size, one, 0)

        def send_sides(g):
            arrived(g, 0, 1)
            add_rows(g, 2 * block, corners[g].at[0])
            add_rows(g, block + half, corners[g].at[1])
            send(g, 2, planes[g].at[block : 2 * block], sides[g].at[0], by_x)
            send(g, 3, planes[g].at[2 * block : 3 * block], sides[g].at[1], by_y)

        def send_column(g):
            arrived(g, 2, 3)
            for r in range(size):
                at = slice(r * cols[g], (r + 1) * cols[g])
                total = planes[g][:block, at].astype(F32)
                total += sides[g][0, :, at].astype(F32) + sides[g][1, :, at].astype(F32)
                if r == 0:
                    outs[g][...] = total
                else:
                    planes[g][:block, at] = total.astype(BF16)
                    send(g, 3 + r, planes[g].at[:block, at], zins[g].at[r - 1], z_partner(-r))

        def finish(g):
            arrived(g, *range(4, 3 + size))
            total = outs[g][...]
            for r in range(1, size):
                total += zins[g][r - 1].astype(F32)
            outs[g][...] = total

        def feature_rows(k, vector):
            for place, mask in enumerate(ORDER):
                at = data_at
                for bit in (BIT_CORE, BIT_X, BIT_Y):
                    if mask & bit:
                        at = neighbour(at, bit)
                v_ref[0, pl.ds(k * len(ORDER) + at, 1), :] = vector[:, place * 128 : (place + 1) * 128]

        z_near = tensor_at + 1 - 2 * (tensor_at % 2)
        z_across = tensor_at + 2 - 4 * ((tensor_at // 2) % 2)
        v_partners = (by_core, (data_at, z_near), (data_at, z_across), by_x, by_y)

        def v_copy(k):
            return remote(v_ref.at[k], v_in.at[k], v_send.at[k], v_recv.at[k], v_partners[k])

        def v_add(k):
            v_copy(k).wait_recv()
            v_ref[k + 1] = v_ref[k] + v_in[k]

        grad_load = pltpu.make_async_copy(second_in, grad_ref, second_sem)
        grad_load.start()
        greet([by_x, by_y, by_core] + [z_partner(r) for r in range(1, size)])
        for k in range(3):
            feature_rows((1, 4, 5)[k], vectors_ref[k : k + 1, :])

        def gelu_step(j):
            other_tile(D, mixed_t, act_buf[j % 2], j)
            low = (matmul(mixed_ref[...], w_buf[j % 2]) * slope_buf[j % 2]).astype(BF16)
            gu_ref[:, column(j)] = low
            sums = jnp.sum(low.astype(F32), axis=0, keepdims=True)
            count = TILE // 128
            per = cols[U] // TILE
            first = v_up + ((tensor_at + size - j // per) % size) * (cols[U] // 128) + (j % per) * count
            for k in range(count):
                v_ref[0, pl.ds(first + k, 1), :] = sums[:, k * 128 : (k + 1) * 128]

        over_tiles(
            units // TILE,
            [(0, active_in, act_buf), (1, d_in, w_buf), (2, slope_in, slope_buf)],
            gelu_step,
        )
        normal_loads = [
            pltpu.make_async_copy(normal_in.at[:, column(k)], slope_buf.at[k], load_sem.at[2, k])
            for k in range(2)
        ]
        for copy in normal_loads:
            copy.start()
        over_tiles(
            units // TILE,
            [(0, active_in, act_buf)],
            lambda j: own_tile(D, mixed_t, act_buf[j % 2], j),
        )
        send_corner(D)
        grad_load.wait()

        def up_step(j):
            core_copy(D, j).wait_send()
            tile = gu_ref[:, column(j)]
            other_tile(U, normed_t, tile, j)
            grad_ref[...] += contract_cols(tile, w_buf[j % 2])

        over_tiles(units // TILE, [(1, u_in, w_buf)], up_step)
        send_sides(D)

        def own_up(j, carry):
            own_tile(U, normed_t, gu_ref[:, column(j)], j)
            return carry

        lax.fori_loop(0, units // TILE, own_up, 0)
        send_corner(U)

        for copy in normal_loads:
            copy.wait()
        chunk = 64

        def norm_step(j, sums):
            at = pl.ds(pl.multiple_of(j * chunk, chunk), chunk)
            normal_rows = jnp.concatenate([slope_buf[0, at, :], slope_buf[1, at, :]], axis=1)
            grads = grad_ref[at, :]
            hidden, more_gain, more_shift = norm_backward(
                grads, normal_rows, root_ref[at, :], gain_ref[...]
            )
            grad_ref[at, :] = hidden
            low_ref[at, :] = hidden.astype(BF16)
            more = (jnp.sum(hidden, axis=0), more_gain, more_shift)
            return tuple(a + b[None] for a, b in zip(sums, more))

        zero = jnp.zeros((1, width), F32)
        sums = lax.fori_loop(0, rows // chunk, norm_step, (zero, zero, zero))
        for k in range(3):
            feature_rows((0, 2, 3)[k], sums[k])
        for k in range(width // 128):
            at = slice(k * 128, (k + 1) * 128)
            low_t[at, :] = low_ref[:, at].astype(F32).T.astype(BF16)

        def out_step(j):
            gctx_ref[:, column(j)] = matmul(low_ref[...], w_buf[j % 2]).astype(BF16)
            other_tile(O, low_t, context_ref[:, column(j)], j)

        over_tiles(full[O] // TILE, [(1, o_in, w_buf)], out_step)

        def qkv_load(r):
            return pltpu.make_async_copy(
                qkv_in.at[:, column(r, cols[A])], qkv_buf.at[r % 2], load_sem.at[0, r % 2]
            )

        def attend_step(r, carry):
            @pl.when(r + 1 < size)
            def _():
                qkv_load(r + 1).start()

            qkv_load(r).wait()
            slot = r % 2
            seen = visible_ref[...] > 0.0
            for start, lanes, held in pairs_of(attn, head_size):
                queries = qkv_buf[slot, :, start : start + lanes]
                keys = qkv_buf[slot, :, attn + start : attn + start + lanes]
                values = qkv_buf[slot, :, 2 * attn + start : 2 * attn + start + lanes]
                grads = gctx_ref[:, pl.ds(pl.multiple_of(r * attn + start, 128), lanes)]
                grad_q = jnp.zeros((rows, lanes), F32)
                grad_k = jnp.zeros((rows, lanes), F32)
                grad_v = jnp.zeros((rows, lanes), F32)
                for which in range(held):
                    mine = keep_head(grads, which, head_size)
                    query = keep_head(queries, which, head_size)
                    scores = jnp.where(seen, contract_cols(keys, query) * scale, MASKED)
                    exponent = jnp.exp(scores - jnp.max(scores, axis=0, keepdims=True))
                    probs = exponent * (1.0 / jnp.sum(exponent, axis=0, keepdims=True))
                    grad_v += matmul(probs.astype(BF16), mine)
                    grad_probs = contract_cols(values, mine)
                    inner = jnp.sum(probs * grad_probs, axis=0, keepdims=True)
                    grad_scores = (probs * (grad_probs - inner)).astype(BF16)
                    grad_q += keep_head(contract_rows(grad_scores, keys), which, head_size)
                    grad_k += matmul(grad_scores, query)
                low_q = (grad_q * scale).astype(BF16)
                low_v = grad_v.astype(BF16)
                at = r * cols[A] + start
                gu_ref[:, pl.ds(pl.multiple_of(at, 128), lanes)] = low_q
                gu_ref[:, pl.ds(pl.multiple_of(at + attn, 128), lanes)] = (grad_k * scale).astype(BF16)
                gu_ref[:, pl.ds(pl.multiple_of(at + 2 * attn, 128), lanes)] = low_v
                place = ((tensor_at + size - r) % size) * (attn // 128) + start // 128
                v_ref[0, pl.ds(v_query + place, 1), :] = jnp.sum(
                    low_q.astype(F32), axis=0, keepdims=True
                )
                v_ref[0, pl.ds(v_value + place, 1), :] = jnp.sum(
                    low_v.astype(F32), axis=0, keepdims=True
                )
            return carry

        qkv_load(0).start()
        lax.fori_loop(0, size // 2, attend_step, 0)
        for j in range(full[O] // TILE):
            own_tile(O, low_t, context_ref[:, j * TILE : (j + 1) * TILE], j)
        send_column(D)
        lax.fori_loop(size // 2, size, attend_step, 0)
        v_copy(0).start()
        send_sides(U)

        def qkv_step(j):
            core_copy(U, j).wait_send()
            tile = gu_ref[:, column(j)]
            other_tile(A, input_t, tile, j)
            grad_ref[...] += contract_cols(tile, w_buf[j % 2])

        over_tiles(full[A] // TILE, [(1, a_in, w_buf)], qkv_step)
        for j in range(full[A] // TILE, units // TILE):
            core_copy(U, j).wait_send()
        v_add(0)
        v_copy(1).start()

        def own_qkv(j, carry):
            own_tile(A, input_t, gu_ref[:, column(j)], j)
            return carry

        lax.fori_loop(0, full[A] // TILE, own_qkv, 0)
        send_corner(A)
        send_corner(O)
        v_add(1)
        v_copy(2).start()
        for place, mask in enumerate(ORDER):
            at = data_at
            for bit in (BIT_CORE, BIT_X, BIT_Y):
                if mask & bit:
                    at = neighbour(at, bit)
            grad_out[:, pl.ds(pl.multiple_of(at * block, block), block)] = grad_ref[
                :, place * block : (place + 1) * block
            ].astype(BF16)
        finish(D)
        v_add(2)
        send_column(U)
        send_sides(A)
        send_sides(O)
        v_copy(3).start()
        send_column(A)
        send_column(O)
        v_add(3)
        v_copy(4).start()
        finish(U)
        v_add(4)
        sums_out[...] = v_ref[5]
        finish(A)
        finish(O)
        for j in range(full[A] // TILE):
            core_copy(A, j).wait_send()
        for j in range(full[O] // TILE):
            core_copy(O, j).wait_send()
        for k in range(5):
            v_copy(k).wait_send()
        for copy in copies.values():
            copy.wait_send()

    anywhere, inside = pl.BlockSpec(memory_space=pl.ANY), pl.BlockSpec(memory_space=pltpu.VMEM)
    results = pl.pallas_call(
        body,
        out_shape=[jax.ShapeDtypeStruct((block, c), F32) for c in cols]
        + [
            jax.ShapeDtypeStruct((rows, width), BF16),
            jax.ShapeDtypeStruct((vector_rows, 128), F32),
        ],
        in_specs=[inside] * 5 + [anywhere] * 2 + [inside] * 3 + [anywhere] * 7 + [inside],
        out_specs=[inside] * 6,
        scratch_shapes=[
            pltpu.VMEM((2, width, TILE), BF16),
            pltpu.VMEM((2, rows, TILE), BF16),
            pltpu.VMEM((2, rows, TILE), F32),
            pltpu.VMEM((rows, units), BF16),
            pltpu.VMEM((rows, width), F32),
            pltpu.VMEM((rows, width), BF16),
            pltpu.VMEM((width, rows), BF16),
            pltpu.VMEM((rows, full[1]), BF16),
            pltpu.VMEM((2, rows, cols[0]), BF16),
            pltpu.VMEM((middle, units), BF16),
            pltpu.VMEM((middle, full[1]), BF16),
        ]
        + [pltpu.VMEM((middle, c), BF16) for c in full]
        + [pltpu.VMEM((2, half, c), BF16) for c in full]
        + [pltpu.VMEM((2, block, c), BF16) for c in full]
        + [pltpu.VMEM((size - 1, block, c), BF16) for c in cols]
        + [
            pltpu.VMEM((6, vector_rows, 128), F32),
            pltpu.VMEM((5, vector_rows, 128), F32),
            pltpu.SemaphoreType.DMA((3, 2)),
            pltpu.SemaphoreType.DMA,
            pltpu.SemaphoreType.DMA((4, units // TILE)),
            pltpu.SemaphoreType.DMA((4, units // TILE)),
            pltpu.SemaphoreType.DMA((4, 3 + size)),
            pltpu.SemaphoreType.DMA((4, 3 + size)),
            pltpu.SemaphoreType.DMA((5,)),
            pltpu.SemaphoreType.DMA((5,)),
        ],
        compiler_params=pltpu.CompilerParams(
            collective_id=BACKWARD_ID, has_side_effects=True, vmem_limit_bytes=63 * 2**20
        ),
        cost_estimate=pl.CostEstimate(
            flops=4 * rows * sum(full) * width,
            bytes_accessed=4 * sum(full) * width,
            transcendentals=0,
        ),
        name="backward_near",
    )(
        mixed_low, mixed_low.T, normed_low.T, inputs.T, context, grad_second, normal, root, gain,
        visible, active, slope, qkv, *weights, vectors,
    )
    return results[:4], results[4], results[5]


def gather_far(shard):
    return lax.all_gather(
        lax.all_gather(shard, "tensor", axis=1, tiled=True), "dp", axis=0, tiled=True
    )


def scatter_far(left_side, right_side):
    whole = contract_rows(left_side, right_side).astype(BF16)
    part = lax.psum_scatter(whole, "dp", scatter_dimension=0, tiled=True)
    return lax.psum_scatter(part, "tensor", scatter_dimension=1, tiled=True).astype(F32)


def permute_blocks(array, index, width):
    def body(index_ref, in_ref, out_ref):
        for k in range(array.shape[1] // width):
            start = pl.multiple_of(index_ref[k] * width, width)
            out_ref[:, k * width : (k + 1) * width] = in_ref[:, pl.ds(start, width)]

    return pl.pallas_call(
        body,
        out_shape=jax.ShapeDtypeStruct(array.shape, array.dtype),
        grid_spec=pltpu.PrefetchScalarGridSpec(
            num_scalar_prefetch=1,
            grid=(1,),
            in_specs=[pl.BlockSpec(array.shape, lambda k, index_ref: (0, 0))],
            out_specs=pl.BlockSpec(array.shape, lambda k, index_ref: (0, 0)),
        ),
        cost_estimate=pl.CostEstimate(
            flops=0, bytes_accessed=2 * array.size * array.dtype.itemsize, transcendentals=0
        ),
        name="permute_blocks",
    )(index, array)


def soft_weights(queries, keys, visible, scale):
    scores = contract_cols(queries, keys) * scale
    scores = jnp.where(visible, scores, MASKED)
    exponent = jnp.exp(scores - jnp.max(scores, axis=-1, keepdims=True))
    return exponent * (1.0 / jnp.sum(exponent, axis=-1, keepdims=True))


def pairs_of(width, head_size):
    lanes = max(128, head_size)
    return [(start, lanes, lanes // head_size) for start in range(0, width, lanes)]


def keep_head(array, which, head_size):
    lane = lax.broadcasted_iota(jnp.int32, array.shape, 1)
    return jnp.where(lane // head_size == which, array, jnp.zeros_like(array))


def attend_forward(qkv_q, qkv_kv, length, head_size, groups):
    q_rows = qkv_q.shape[0]
    k_rows = qkv_kv.shape[0]
    block = qkv_q.shape[1] // groups
    width = block // 3
    scale = float(head_size) ** (-0.5)

    def body(length_ref, q_ref, kv_ref, out_ref):
        visible = lax.broadcasted_iota(jnp.int32, (q_rows, k_rows), 1) < length_ref[0]
        for start, lanes, held in pairs_of(width, head_size):
            queries = q_ref[:, start : start + lanes]
            keys = kv_ref[:, width + start : width + start + lanes]
            values = kv_ref[:, 2 * width + start : 2 * width + start + lanes]
            total = jnp.zeros((q_rows, lanes), F32)
            for which in range(held):
                probs = soft_weights(keep_head(queries, which, head_size), keys, visible, scale)
                total += keep_head(matmul(probs.astype(BF16), values), which, head_size)
            out_ref[:, start : start + lanes] = total.astype(BF16)

    return pl.pallas_call(
        body,
        out_shape=jax.ShapeDtypeStruct((q_rows, groups * width), BF16),
        grid_spec=pltpu.PrefetchScalarGridSpec(
            num_scalar_prefetch=1,
            grid=(groups,),
            in_specs=[
                pl.BlockSpec((q_rows, block), lambda g, length_ref: (0, g)),
                pl.BlockSpec((k_rows, block), lambda g, length_ref: (0, g)),
            ],
            out_specs=pl.BlockSpec((q_rows, width), lambda g, length_ref: (0, g)),
        ),
        cost_estimate=pl.CostEstimate(
            flops=4 * q_rows * k_rows * width * groups,
            bytes_accessed=2 * (2 * q_rows + 2 * k_rows) * width * groups,
            transcendentals=q_rows * k_rows * groups * width // head_size,
        ),
        name="attend_forward",
    )(length, qkv_q, qkv_kv)


def attend_backward(qkv_q, qkv_kv, grad_context, length, head_size, groups):
    q_rows = qkv_q.shape[0]
    k_rows = qkv_kv.shape[0]
    block = qkv_q.shape[1] // groups
    width = block // 3
    scale = float(head_size) ** (-0.5)

    def body(length_ref, q_ref, kv_ref, grad_ref, dq_ref, dkv_ref):
        visible = lax.broadcasted_iota(jnp.int32, (q_rows, k_rows), 1) < length_ref[0]
        for start, lanes, held in pairs_of(width, head_size):
            queries = q_ref[:, start : start + lanes]
            keys = kv_ref[:, width + start : width + start + lanes]
            values = kv_ref[:, 2 * width + start : 2 * width + start + lanes]
            grads = grad_ref[:, start : start + lanes]
            grad_q = jnp.zeros((q_rows, lanes), F32)
            grad_k = jnp.zeros((k_rows, lanes), F32)
            grad_v = jnp.zeros((k_rows, lanes), F32)
            for which in range(held):
                mine = keep_head(grads, which, head_size)
                query = keep_head(queries, which, head_size)
                probs = soft_weights(query, keys, visible, scale)
                grad_v += contract_rows(probs.astype(BF16), mine)
                grad_probs = contract_cols(mine, values)
                inner = jnp.sum(probs * grad_probs, axis=-1, keepdims=True)
                grad_scores = (probs * (grad_probs - inner)).astype(BF16)
                grad_q += keep_head(matmul(grad_scores, keys), which, head_size)
                grad_k += contract_rows(grad_scores, query)
            dq_ref[:, start : start + lanes] = (grad_q * scale).astype(BF16)
            dkv_ref[:, start : start + lanes] = (grad_k * scale).astype(BF16)
            dkv_ref[:, width + start : width + start + lanes] = grad_v.astype(BF16)

    return pl.pallas_call(
        body,
        out_shape=(
            jax.ShapeDtypeStruct((q_rows, groups * width), BF16),
            jax.ShapeDtypeStruct((k_rows, groups * 2 * width), BF16),
        ),
        grid_spec=pltpu.PrefetchScalarGridSpec(
            num_scalar_prefetch=1,
            grid=(groups,),
            in_specs=[
                pl.BlockSpec((q_rows, block), lambda g, length_ref: (0, g)),
                pl.BlockSpec((k_rows, block), lambda g, length_ref: (0, g)),
                pl.BlockSpec((q_rows, width), lambda g, length_ref: (0, g)),
            ],
            out_specs=[
                pl.BlockSpec((q_rows, width), lambda g, length_ref: (0, g)),
                pl.BlockSpec((k_rows, 2 * width), lambda g, length_ref: (0, g)),
            ],
        ),
        cost_estimate=pl.CostEstimate(
            flops=10 * q_rows * k_rows * width * groups,
            bytes_accessed=2 * (3 * q_rows + 4 * k_rows) * width * groups,
            transcendentals=q_rows * k_rows * groups * width // head_size,
        ),
        name="attend_backward",
    )(length, qkv_q, qkv_kv, grad_context)


def activate(total, bias):
    upper = total + bias
    cumulative = 0.5 * (1.0 + lax.erf(upper * math.sqrt(0.5)))
    density = jnp.exp(-0.5 * upper * upper) * (1.0 / math.sqrt(2.0 * math.pi))
    return upper * cumulative, cumulative + upper * density


def norm_forward(hidden, gain_vec, shift_vec):
    center = hidden - jnp.mean(hidden, axis=-1, keepdims=True)
    variance = jnp.mean(center * center, axis=-1, keepdims=True)
    inv_root = lax.rsqrt(variance + EPSILON)
    normal = center * inv_root
    return (normal * gain_vec + shift_vec, normal, inv_root)


def norm_backward(grad_in, normal, inv_root, gain_vec):
    grad_normal = grad_in * gain_vec
    grad_gain = jnp.sum(grad_in * normal, axis=0)
    grad_shift = jnp.sum(grad_in, axis=0)
    grad_hidden = inv_root * (
        grad_normal
        - jnp.mean(grad_normal, axis=-1, keepdims=True)
        - normal * jnp.mean(grad_normal * normal, axis=-1, keepdims=True)
    )
    return (grad_hidden, grad_gain, grad_shift)


def layer(
    hidden_in,
    cotangent,
    w_query,
    w_key,
    w_value,
    w_out,
    w_up,
    w_down,
    bias_query,
    bias_value,
    bias_out,
    bias_up,
    bias_down,
    gain_attn,
    shift_attn,
    gain_ffn,
    shift_ffn,
    valid_lengths,
):
    rows, model_width = hidden_in.shape
    n_tensor = lax.axis_size("tensor")
    n_data = lax.axis_size("dp")
    tensor_at = lax.axis_index("tensor")
    data_at = lax.axis_index("dp")
    seq_len = rows * n_tensor // valid_lengths.shape[0]
    spread_over = seq_len // rows
    head_size = model_width // HEADS
    head_cols = w_query.shape[1]
    factor = 1.0 / math.sqrt(rows * n_tensor * n_data)
    near = n_data == len(ORDER) and spread_over == 1
    width = model_width // n_data

    if near:
        order = jnp.array(ORDER, jnp.int32)
        back = jnp.array([ORDER.index(k) for k in range(n_data)], jnp.int32)
        block_at = jnp.bitwise_xor(order, data_at)
        place_of = back[jnp.bitwise_xor(jnp.arange(n_data, dtype=jnp.int32), data_at)]
        column_at = (tensor_at - jnp.arange(n_tensor)) % n_tensor
    else:
        column_at = jnp.arange(n_tensor)

    def arrange(array):
        return permute_blocks(array, block_at, width) if near else array

    def restore(array):
        return permute_blocks(array, place_of, width) if near else array

    def column_vector(vector):
        return vector.reshape(n_tensor, -1)[column_at] if near else vector.reshape(n_tensor, -1)

    vectors = jnp.stack([bias_out, bias_down, gain_attn, shift_attn, gain_ffn, shift_ffn])
    if near:
        vectors = vectors.reshape(-1, n_data, width)[:, block_at].reshape(-1, model_width)
    bias_out, bias_down, gain_attn, shift_attn, gain_ffn, shift_ffn = vectors
    query_bias, value_bias = column_vector(bias_query), column_vector(bias_value)
    bias_qkv = jnp.concatenate(
        [query_bias, jnp.zeros_like(query_bias), value_bias], axis=1
    ).reshape(1, -1)
    bias_units = column_vector(bias_up).reshape(1, -1)
    length = lax.dynamic_slice_in_dim(valid_lengths, tensor_at // spread_over, 1)

    inputs = arrange(hidden_in)
    grad_output = arrange(cotangent).astype(F32)

    w_attend = jnp.concatenate([w_query.astype(BF16), w_key.astype(BF16), w_value.astype(BF16)], axis=1)
    shards = (w_attend, w_out.astype(BF16), w_up.astype(BF16), w_down.astype(BF16))
    if near:
        visible = (jnp.arange(seq_len)[None, :] < length).astype(F32)
        qkv_full, out_full, up_full, down_full, qkv, context, hidden, active, slope = forward_near(
            shards, inputs, visible, bias_qkv, bias_out[None], gain_attn[None], shift_attn[None],
            bias_units, head_size,
        )
        qkv_seq = qkv
    else:
        qkv_full, out_full, up_full, down_full = (gather_far(shard) for shard in shards)
        qkv = (matmul(inputs, qkv_full) + bias_qkv).astype(BF16)
        members = [
            list(range(k, k + spread_over)) for k in range(0, n_tensor, spread_over)
        ]
        qkv_seq = lax.all_gather(qkv, "tensor", axis_index_groups=members, axis=0, tiled=True)
        context = attend_forward(qkv, qkv_seq, length, head_size, n_tensor)
        hidden = inputs.astype(F32) + contract_cols(context, out_full) + bias_out
    normed, normal_attn, root_attn = norm_forward(hidden, gain_attn, shift_attn)
    normed_low = normed.astype(BF16)
    if not near:
        active, slope = activate(matmul(normed_low, up_full), bias_units)
        active = active.astype(BF16)
    mixed = contract_cols(active, down_full)
    result, normal_ffn, root_ffn = norm_forward(normed + mixed + bias_down, gain_ffn, shift_ffn)

    grad_second, grad_gain_ffn, grad_shift_ffn = norm_backward(
        grad_output, normal_ffn, root_ffn, gain_ffn
    )
    grad_bias_down = jnp.sum(grad_second, axis=0)
    mixed_low = grad_second.astype(BF16)
    output = restore(result.astype(BF16))
    if near:
        given = jnp.stack([grad_bias_down, grad_gain_ffn, grad_shift_ffn])
        (grad_qkv_w, grad_out, grad_up, grad_down), grad_input, sums = backward_near(
            mixed_low, normed_low, inputs, context, grad_second, normal_attn, root_attn,
            gain_attn[None], visible.T, active, slope, qkv,
            (qkv_full, out_full, up_full, down_full), given, head_size,
        )
        sums = sums.reshape(-1) * factor
    else:
        grad_down = scatter_far(mixed_low, active)
        grad_upper = (matmul(mixed_low, down_full) * slope).astype(BF16)
        grad_bias_up = jnp.sum(grad_upper, axis=0, dtype=F32)
        grad_up = scatter_far(normed_low, grad_upper)
        grad_normed = grad_second + contract_cols(grad_upper, up_full)
        grad_first, grad_gain_attn, grad_shift_attn = norm_backward(
            grad_normed, normal_attn, root_attn, gain_attn
        )
        grad_bias_out = jnp.sum(grad_first, axis=0)
        attn_low = grad_first.astype(BF16)
        grad_context = matmul(attn_low, out_full).astype(BF16)
        grad_out = scatter_far(attn_low, context)
        grad_q, grad_kv = attend_backward(qkv, qkv_seq, grad_context, length, head_size, n_tensor)
        grad_kv = lax.psum_scatter(
            grad_kv.astype(F32),
            "tensor",
            scatter_dimension=0,
            axis_index_groups=members,
            tiled=True,
        ).astype(BF16)
        grad_qkv = jnp.concatenate(
            [grad_q.reshape(rows, n_tensor, -1), grad_kv.reshape(rows, n_tensor, -1)], axis=2
        ).reshape(rows, -1)
        grad_bias_qkv = jnp.sum(grad_qkv, axis=0, dtype=F32).reshape(n_tensor, 3, head_cols)
        grad_qkv_w = scatter_far(inputs, grad_qkv)
        grad_input = (grad_first + contract_cols(grad_qkv, qkv_full)).astype(BF16)
        sums = jnp.concatenate(
            [
                grad_bias_out,
                grad_bias_down,
                grad_gain_attn,
                grad_shift_attn,
                grad_gain_ffn,
                grad_shift_ffn,
                grad_bias_qkv[:, 0].reshape(-1),
                grad_bias_qkv[:, 2].reshape(-1),
                grad_bias_up,
            ]
        )
        sums = lax.psum(sums, ("dp", "tensor")) * factor
    v_out, v_down, v_gain_attn, v_shift_attn, v_gain_ffn, v_shift_ffn, v_query, v_value = (
        sums[k * model_width : (k + 1) * model_width] for k in range(8)
    )
    v_up = sums[8 * model_width :]
    return (
        output,
        grad_input,
        grad_qkv_w[:, :head_cols] * factor,
        grad_qkv_w[:, head_cols : 2 * head_cols] * factor,
        grad_qkv_w[:, 2 * head_cols :] * factor,
        grad_out * factor,
        grad_up * factor,
        grad_down * factor,
        v_query,
        v_value,
        v_out,
        v_up,
        v_down,
        v_gain_attn,
        v_shift_attn,
        v_gain_ffn,
        v_shift_ffn,
    )


def solution(mesh):
    tokens, matrix, copied = P(("dp", "tensor"), None), P("dp", "tensor"), P()
    return jax.shard_map(
        layer,
        mesh=mesh,
        in_specs=(tokens,) * 2 + (matrix,) * 6 + (copied,) * 9 + (P("dp"),),
        out_specs=(tokens,) * 2 + (matrix,) * 6 + (copied,) * 9,
        check_vma=False,
    )
```

```python
import math

import jax
import jax.numpy as jnp
from jax import lax
from jax.experimental import pallas as pl
from jax.experimental.pallas import tpu as pltpu
from jax.sharding import PartitionSpec as P

HEADS = 16
EPSILON = 1e-12
MASKED = -1e30
BF16 = jnp.bfloat16
F32 = jnp.float32

ORDER = (0, 2, 4, 6, 1, 3, 5, 7)
BIT_CORE, BIT_X, BIT_Y = 1, 2, 4


def matmul(left_side, right_side):
    return jnp.dot(left_side, right_side, preferred_element_type=F32)


def contract_rows(left_side, right_side):
    return lax.dot_general(
        left_side, right_side, (((0,), (0,)), ((), ())), preferred_element_type=F32
    )


def contract_cols(left_side, right_side):
    return lax.dot_general(
        left_side, right_side, (((1,), (1,)), ((), ())), preferred_element_type=F32
    )


FORWARD_ID = 1
BACKWARD_ID = 2
TILE = 512


def neighbour(index, bit):
    return index + bit - 2 * bit * ((index // bit) % 2)


def block_of(index, mask):
    for bit in (BIT_CORE, BIT_X, BIT_Y):
        if mask & bit:
            index = neighbour(index, bit)
    return index


def greet(partners):
    barrier = pltpu.get_barrier_semaphore()
    for partner in partners:
        pl.semaphore_signal(
            barrier, inc=1, device_id=partner, device_id_type=pl.DeviceIdType.MESH
        )
    pl.semaphore_wait(barrier, len(partners))


def forward_near(weights, hidden_in, cotangent, wide, bias_query, bias_value, bias_units, lengths, head_size):
    size = lax.axis_size("tensor")
    rows, width = hidden_in.shape
    block = width // len(ORDER)
    attn, units_each = weights[0].shape[1], weights[4].shape[1]
    cols = [3 * attn, attn, units_each, units_each]
    full = [(width, size * c) for c in cols]
    units = size * units_each
    half = block // 2
    A, O, U, D = range(4)
    B_OUT, B_DOWN, G_ATTN, S_ATTN, G_FFN, S_FFN = range(6)

    def body(
        q_in, k_in, v_in, o_in, u_in, d_in, hidden_raw, cotangent_ref, bias_out_in, bias_down_in,
        gain_attn_in, shift_attn_in, gain_ffn_in, shift_ffn_in, bias_q_ref, bias_v_ref, bias_u_ref,
        lengths_ref,
        a_out, o_out, u_out, d_out, qkv_ref, context_ref, hidden_ref, active_out, slope_out, output_ref,
        mixed_ref, mixed_t, normed_t, input_t, second_ref, sums_ref, wide_ref,
        a_ref, o_ref, u_ref, d_ref, x_ref, low_ref, active_ref, slope_ref, local_sem, send_sem, recv_sem,
        tile_sem,
    ):
        data_at, tensor_at = lax.axis_index("dp"), lax.axis_index("tensor")
        places = (a_ref, o_ref, u_ref, d_ref)

        def dp_partner(bit):
            return (neighbour(data_at, bit), tensor_at)

        def z_partner(step):
            return (data_at, (tensor_at + step) % size)

        by_x, by_y, by_core = dp_partner(BIT_X), dp_partner(BIT_Y), dp_partner(BIT_CORE)
        owners = [block_of(data_at, mask) for mask in ORDER]
        copies = {}

        def send(g, slot, source, target, device):
            copy = pltpu.make_async_remote_copy(
                src_ref=source,
                dst_ref=target,
                send_sem=send_sem.at[g, slot],
                recv_sem=recv_sem.at[g, slot],
                device_id=device,
                device_id_type=pl.DeviceIdType.MESH,
            )
            copies[g, slot] = copy
            copy.start()

        def arrived(g, *slots):
            for slot in slots:
                copies[g, slot].wait_recv()

        def part(g, start, count):
            return places[g].at[start : start + count, :]

        def send_z(g):
            for r in range(1, size):
                send(
                    g,
                    r - 1,
                    places[g].at[0:block, 0 : cols[g]],
                    places[g].at[0:block, r * cols[g] : (r + 1) * cols[g]],
                    z_partner(r),
                )

        def send_column(g):
            arrived(g, 0, 1, 2)
            send(g, 3, part(g, 0, block), part(g, block, block), by_x)
            send(g, 4, part(g, 0, block), part(g, 2 * block, block), by_y)

        def send_corner(g):
            arrived(g, 3, 4)
            send(g, 5, part(g, block, half), part(g, 3 * block, half), by_y)
            send(g, 6, part(g, 2 * block + half, half), part(g, 3 * block + half, half), by_x)
            for k in range(3):
                send(g, 7 + k, part(g, k * block, block), part(g, (4 + k) * block, block), by_core)

        def send_last(g):
            arrived(g, 5, 6)
            send(g, 10, part(g, 3 * block, block), part(g, 7 * block, block), by_core)

        saves = []

        def save(g, target):
            copy = pltpu.make_async_copy(places[g], target, local_sem.at[g])
            copy.start()
            saves.append(copy)

        for k, ref in enumerate((q_in, k_in, v_in)):
            a_ref[:block, k * attn : (k + 1) * attn] = ref[...].astype(BF16)
        o_ref[:block, :attn] = o_in[...].astype(BF16)
        greet([by_x, by_y, by_core] + [z_partner(r) for r in range(1, size)])
        send_z(A)
        send_z(O)
        u_ref[:block, :units_each] = u_in[...].astype(BF16)
        send_z(U)
        d_ref[:block, :units_each] = d_in[...].astype(BF16)
        send_z(D)

        def lanes_of(owner):
            return pl.ds(pl.multiple_of(owner * block, block), block)

        def transpose_into(target, source):
            for k in range(width // 128):
                at = slice(k * 128, (k + 1) * 128)
                target[at, :] = source[:, at].astype(F32).T.astype(BF16)

        for place, owner in enumerate(owners):
            at = slice(place * block, (place + 1) * block)
            x_ref[:, at] = hidden_raw[:, lanes_of(owner)]
            for k, ref in enumerate(
                (bias_out_in, bias_down_in, gain_attn_in, shift_attn_in, gain_ffn_in, shift_ffn_in)
            ):
                wide_ref[k : k + 1, at] = ref[:, lanes_of(owner)]

        def vector(k):
            return wide_ref[k : k + 1, :]

        send_column(A)
        transpose_into(input_t, x_ref)
        send_column(O)
        send_corner(A)
        send_column(U)
        send_corner(O)
        send_last(A)
        arrived(A, 7, 8, 9, 10)
        save(A, a_out)

        def column_of(r, span):
            return pl.ds(pl.multiple_of(((tensor_at + size - r) % size) * span, 128), span)

        def project(r, carry):
            at = r * cols[A]
            total = matmul(x_ref[...], a_ref[:, pl.ds(pl.multiple_of(at, 128), cols[A])])
            biases = (bias_q_ref[:, column_of(r, attn)], 0.0, bias_v_ref[:, column_of(r, attn)])
            for k, bias in enumerate(biases):
                piece = total[:, k * attn : (k + 1) * attn] + bias
                qkv_ref[:, pl.ds(pl.multiple_of(at + k * attn, 128), attn)] = piece.astype(BF16)
            return carry

        lax.fori_loop(0, size, project, 0)
        scale = float(head_size) ** (-0.5)
        length = lengths_ref[tensor_at]

        def attend(r, carry):
            at = pl.multiple_of(r * cols[A], 128)
            to = pl.multiple_of(r * attn, 128)
            seen = lax.broadcasted_iota(jnp.int32, (rows, rows), 1) < length
            for start, lanes, held in pairs_of(attn, head_size):
                queries = qkv_ref[:, pl.ds(at + start, lanes)]
                keys = qkv_ref[:, pl.ds(at + attn + start, lanes)]
                values = qkv_ref[:, pl.ds(at + 2 * attn + start, lanes)]
                total = jnp.zeros((rows, lanes), F32)
                for which in range(held):
                    probs = soft_weights(keep_head(queries, which, head_size), keys, seen, scale)
                    total += keep_head(matmul(probs.astype(BF16), values), which, head_size)
                context_ref[:, pl.ds(to + start, lanes)] = total.astype(BF16)
            return carry

        lax.fori_loop(0, size, attend, 0)
        send_last(O)
        send_corner(U)
        send_column(D)
        arrived(O, 7, 8, 9, 10)
        save(O, o_out)

        def output(j, carry):
            at = pl.ds(pl.multiple_of(j * 256, 256), 256)
            total = contract_cols(context_ref[...], o_ref[at, :])
            hidden_ref[:, at] = x_ref[:, at].astype(F32) + total + wide_ref[B_OUT : B_OUT + 1, at]
            return carry

        lax.fori_loop(0, width // 256, output, 0)
        chunk = 64

        def norm(j, carry):
            at = pl.ds(pl.multiple_of(j * chunk, chunk), chunk)
            normed = norm_forward(hidden_ref[at, :], vector(G_ATTN), vector(S_ATTN))[0]
            low_ref[at, :] = normed.astype(BF16)
            second_ref[at, :] = normed + vector(B_DOWN)
            return carry

        lax.fori_loop(0, rows // chunk, norm, 0)
        send_last(U)
        arrived(U, 7, 8, 9, 10)
        save(U, u_out)
        per = units_each // TILE

        def tile_at(j):
            return pl.ds(pl.multiple_of(j * TILE, TILE), TILE)

        def slope_copy(j):
            return pltpu.make_async_copy(
                slope_ref.at[j % 2], slope_out.at[:, tile_at(j)], tile_sem.at[1, j % 2]
            )

        def active_copy(j):
            return pltpu.make_async_copy(
                active_ref.at[:, tile_at(j)], active_out.at[:, tile_at(j)], tile_sem.at[0, j]
            )

        def raise_up(j, carry):
            @pl.when(j >= 2)
            def _():
                slope_copy(j - 2).wait()

            total = matmul(low_ref[...], u_ref[:, tile_at(j)])
            first = ((tensor_at + size - j // per) % size) * units_each + (j % per) * TILE
            bias = bias_u_ref[:, pl.ds(pl.multiple_of(first, TILE), TILE)]
            active, slope = activate(total, bias)
            active_ref[:, tile_at(j)] = active.astype(BF16)
            slope_ref[j % 2] = slope
            active_copy(j).start()
            slope_copy(j).start()
            return carry

        lax.fori_loop(0, units // TILE, raise_up, 0)
        send_corner(D)
        transpose_into(normed_t, low_ref)

        def lower(start):
            at = slice(start, start + 256)
            second_ref[:, at] += contract_cols(active_ref[...], d_ref[at, :])

        lower(0)
        arrived(D, 7, 8)
        lower(4 * block)
        send_last(D)
        lower(2 * block)
        arrived(D, 9, 10)
        save(D, d_out)
        lower(6 * block)

        def second(j, sums):
            at = pl.ds(pl.multiple_of(j * chunk, chunk), chunk)
            result, normal, root = norm_forward(second_ref[at, :], vector(G_FFN), vector(S_FFN))
            grads = jnp.concatenate([cotangent_ref[at, lanes_of(owner)] for owner in owners], axis=1)
            for place, owner in enumerate(owners):
                output_ref[at, lanes_of(owner)] = result[:, place * block : (place + 1) * block].astype(BF16)
            hidden, more_gain, more_shift = norm_backward(
                grads.astype(F32), normal, root, vector(G_FFN)
            )
            second_ref[at, :] = hidden
            mixed_ref[at, :] = hidden.astype(BF16)
            more = (jnp.sum(hidden, axis=0), more_gain, more_shift)
            return tuple(a + b[None] for a, b in zip(sums, more))

        zero = jnp.zeros((1, width), F32)
        sums = lax.fori_loop(0, rows // chunk, second, (zero, zero, zero))
        for k in range(3):
            sums_ref[k : k + 1, :] = sums[k]
        transpose_into(mixed_t, mixed_ref)

        def settle(j, carry):
            active_copy(j).wait()
            return carry

        lax.fori_loop(0, units // TILE, settle, 0)
        for j in (units // TILE - 2, units // TILE - 1):
            slope_copy(j).wait()
        for copy in saves:
            copy.wait()
        for copy in copies.values():
            copy.wait_send()

    anywhere, inside = pl.BlockSpec(memory_space=pl.ANY), pl.BlockSpec(memory_space=pltpu.VMEM)
    tall = jax.ShapeDtypeStruct((rows, width), BF16)
    turned = jax.ShapeDtypeStruct((width, rows), BF16)
    return pl.pallas_call(
        body,
        out_shape=[jax.ShapeDtypeStruct(shape, BF16) for shape in full]
        + [
            jax.ShapeDtypeStruct((rows, full[A][1]), BF16),
            tall,
            jax.ShapeDtypeStruct((rows, width), F32),
            jax.ShapeDtypeStruct((rows, units), BF16),
            jax.ShapeDtypeStruct((rows, units), F32),
            tall,
            tall,
            turned,
            turned,
            turned,
            jax.ShapeDtypeStruct((rows, width), F32),
            jax.ShapeDtypeStruct((3, width), F32),
            jax.ShapeDtypeStruct((6, width), F32),
        ],
        in_specs=[inside] * 17 + [pl.BlockSpec(memory_space=pltpu.SMEM)],
        out_specs=[anywhere] * 4 + [inside] * 3 + [anywhere] * 2 + [inside] * 8,
        scratch_shapes=[pltpu.VMEM(shape, BF16) for shape in full]
        + [
            pltpu.VMEM((rows, width), BF16),
            pltpu.VMEM((rows, width), BF16),
            pltpu.VMEM((rows, units), BF16),
            pltpu.VMEM((2, rows, TILE), F32),
            pltpu.SemaphoreType.DMA((4,)),
            pltpu.SemaphoreType.DMA((4, 11)),
            pltpu.SemaphoreType.DMA((4, 11)),
            pltpu.SemaphoreType.DMA((2, units // TILE)),
        ],
        compiler_params=pltpu.CompilerParams(
            collective_id=FORWARD_ID, has_side_effects=True, vmem_limit_bytes=63 * 2**20
        ),
        cost_estimate=pl.CostEstimate(
            flops=2 * rows * width * sum(shape[1] for shape in full),
            bytes_accessed=4 * width * sum(shape[1] for shape in full),
            transcendentals=rows * units,
        ),
        name="forward_near",
    )(
        *weights, hidden_in, cotangent, *(vector[None] for vector in wide), bias_query[None],
        bias_value[None], bias_units[None], lengths,
    )


def backward_near(mixed_low, mixed_t, normed_t, input_t, context, grad_second, hidden, wide, lengths,
                  active, slope, qkv, weights, vectors, head_size):
    size = lax.axis_size("tensor")
    rows, width = mixed_low.shape
    block = width // len(ORDER)
    middle = width // 2
    half = block // 2
    full = [weight.shape[1] for weight in weights]
    cols = [c // size for c in full]
    attn = cols[0] // 3
    units = full[2]
    A, O, U, D = range(4)
    vector_rows = (6 * width + 2 * full[1] + units) // 128
    v_query, v_value, v_up = 6 * width // 128, (6 * width + full[1]) // 128, (6 * width + 2 * full[1]) // 128
    scale = float(head_size) ** (-0.5)

    def body(
        mixed_ref, mixed_t, normed_t, input_t, context_ref, second_in, hidden_in, wide_ref,
        lengths_ref, active_in, slope_in, qkv_in, a_in, o_in, u_in, d_in, vectors_ref,
        a_out, o_out, u_out, d_out, grad_out, sums_out,
        w_buf, act_buf, slope_buf, gu_ref, grad_ref, low_ref, low_t, gctx_ref, qkv_buf, send_buf,
        send_o, a_plane, o_plane, u_plane, d_plane, a_corner, o_corner, u_corner, d_corner, a_side,
        o_side, u_side, d_side, a_zin, o_zin, u_zin, d_zin, v_ref, v_in, load_sem, second_sem, core_send,
        core_recv, send_sem, recv_sem, v_send, v_recv,
    ):
        data_at, tensor_at = lax.axis_index("dp"), lax.axis_index("tensor")
        planes = (a_plane, o_plane, u_plane, d_plane)
        corners = (a_corner, o_corner, u_corner, d_corner)
        sides = (a_side, o_side, u_side, d_side)
        zins = (a_zin, o_zin, u_zin, d_zin)
        outs = (a_out, o_out, u_out, d_out)
        sources = (send_buf, send_o, send_buf, send_buf)

        def dp_partner(bit):
            return (neighbour(data_at, bit), tensor_at)

        def z_partner(step):
            return (data_at, (tensor_at + size + step) % size)

        by_x, by_y, by_core = dp_partner(BIT_X), dp_partner(BIT_Y), dp_partner(BIT_CORE)

        def column(j, span=TILE):
            return pl.ds(pl.multiple_of(j * span, 128), span)

        def load(row, source, buffer, j):
            return pltpu.make_async_copy(
                source.at[:, column(j)], buffer.at[j % 2], load_sem.at[row, j % 2]
            )

        def over_tiles(count, loads, step):
            for row, source, buffer in loads:
                load(row, source, buffer, 0).start()

            def one(j, carry):
                @pl.when(j + 1 < count)
                def _():
                    for row, source, buffer in loads:
                        load(row, source, buffer, j + 1).start()

                for row, source, buffer in loads:
                    load(row, source, buffer, j).wait()
                step(j)
                return carry

            lax.fori_loop(0, count, one, 0)

        def remote(source, target, send, receive, device):
            return pltpu.make_async_remote_copy(
                src_ref=source,
                dst_ref=target,
                send_sem=send,
                recv_sem=receive,
                device_id=device,
                device_id_type=pl.DeviceIdType.MESH,
            )

        def core_copy(g, j):
            return remote(
                sources[g].at[:, column(j)],
                planes[g].at[:, column(j)],
                core_send.at[g, j],
                core_recv.at[g, j],
                by_core,
            )

        copies = {}

        def send(g, slot, source, target, device):
            copies[g, slot] = remote(
                source, target, send_sem.at[g, slot], recv_sem.at[g, slot], device
            )
            copies[g, slot].start()

        def arrived(g, *slots):
            for slot in slots:
                copies[g, slot].wait_recv()

        def other_tile(g, left_t, right, j):
            sources[g][:, column(j)] = matmul(left_t[middle:, :], right).astype(BF16)
            core_copy(g, j).start()

        def own_tile(g, left_t, right, j):
            core_copy(g, j).wait_recv()
            total = matmul(left_t[:middle, :], right) + planes[g][:, column(j)].astype(F32)
            planes[g][:, column(j)] = total.astype(BF16)

        def send_corner(g):
            plane = planes[g]
            send(g, 0, plane.at[3 * block : 3 * block + half], corners[g].at[0], by_x)
            send(g, 1, plane.at[3 * block + half :], corners[g].at[1], by_y)

        def add_rows(g, start, more):
            def one(j, carry):
                at = column(j, cols[g])
                total = planes[g][start : start + half, at].astype(F32) + more[:, at].astype(F32)
                planes[g][start : start + half, at] = total.astype(BF16)
                return carry

            lax.fori_loop(0, size, one, 0)

        def send_sides(g):
            arrived(g, 0, 1)
            add_rows(g, 2 * block, corners[g].at[0])
            add_rows(g, block + half, corners[g].at[1])
            send(g, 2, planes[g].at[block : 2 * block], sides[g].at[0], by_x)
            send(g, 3, planes[g].at[2 * block : 3 * block], sides[g].at[1], by_y)

        def send_column(g):
            arrived(g, 2, 3)
            for r in range(size):
                at = slice(r * cols[g], (r + 1) * cols[g])
                total = planes[g][:block, at].astype(F32)
                total += sides[g][0, :, at].astype(F32) + sides[g][1, :, at].astype(F32)
                if r == 0:
                    outs[g][...] = total
                else:
                    planes[g][:block, at] = total.astype(BF16)
                    send(g, 3 + r, planes[g].at[:block, at], zins[g].at[r - 1], z_partner(-r))

        def finish(g):
            arrived(g, *range(4, 3 + size))
            total = outs[g][...]
            for r in range(1, size):
                total += zins[g][r - 1].astype(F32)
            outs[g][...] = total

        def feature_rows(k, vector):
            for place, mask in enumerate(ORDER):
                at = block_of(data_at, mask)
                v_ref[0, pl.ds(k * len(ORDER) + at, 1), :] = vector[:, place * 128 : (place + 1) * 128]

        z_near = tensor_at + 1 - 2 * (tensor_at % 2)
        z_across = tensor_at + 2 - 4 * ((tensor_at // 2) % 2)
        v_partners = (by_core, (data_at, z_near), (data_at, z_across), by_x, by_y)

        def v_copy(k):
            return remote(v_ref.at[k], v_in.at[k], v_send.at[k], v_recv.at[k], v_partners[k])

        def v_add(k):
            v_copy(k).wait_recv()
            v_ref[k + 1] = v_ref[k] + v_in[k]

        grad_load = pltpu.make_async_copy(second_in, grad_ref, second_sem)
        grad_load.start()
        greet([by_x, by_y, by_core] + [z_partner(r) for r in range(1, size)])
        for k in range(3):
            feature_rows((1, 4, 5)[k], vectors_ref[k : k + 1, :])

        def gelu_step(j):
            other_tile(D, mixed_t, act_buf[j % 2], j)
            low = (matmul(mixed_ref[...], w_buf[j % 2]) * slope_buf[j % 2]).astype(BF16)
            gu_ref[:, column(j)] = low
            sums = jnp.sum(low.astype(F32), axis=0, keepdims=True)
            count = TILE // 128
            per = cols[U] // TILE
            first = v_up + ((tensor_at + size - j // per) % size) * (cols[U] // 128) + (j % per) * count
            for k in range(count):
                v_ref[0, pl.ds(first + k, 1), :] = sums[:, k * 128 : (k + 1) * 128]

        over_tiles(
            units // TILE,
            [(0, active_in, act_buf), (1, d_in, w_buf), (2, slope_in, slope_buf)],
            gelu_step,
        )
        hidden_loads = [
            pltpu.make_async_copy(hidden_in.at[:, column(k)], slope_buf.at[k], load_sem.at[2, k])
            for k in range(2)
        ]
        for copy in hidden_loads:
            copy.start()
        over_tiles(
            units // TILE,
            [(0, active_in, act_buf)],
            lambda j: own_tile(D, mixed_t, act_buf[j % 2], j),
        )
        send_corner(D)
        grad_load.wait()

        def up_step(j):
            core_copy(D, j).wait_send()
            tile = gu_ref[:, column(j)]
            other_tile(U, normed_t, tile, j)
            grad_ref[...] += contract_cols(tile, w_buf[j % 2])

        over_tiles(units // TILE, [(1, u_in, w_buf)], up_step)
        send_sides(D)

        def own_up(j, carry):
            own_tile(U, normed_t, gu_ref[:, column(j)], j)
            return carry

        lax.fori_loop(0, units // TILE, own_up, 0)
        send_corner(U)

        for copy in hidden_loads:
            copy.wait()
        chunk = 64

        def norm_step(j, sums):
            at = pl.ds(pl.multiple_of(j * chunk, chunk), chunk)
            hidden_rows = jnp.concatenate([slope_buf[0, at, :], slope_buf[1, at, :]], axis=1)
            gain = wide_ref[2:3, :]
            normal, root = norm_forward(hidden_rows, gain, gain)[1:]
            hidden, more_gain, more_shift = norm_backward(grad_ref[at, :], normal, root, gain)
            grad_ref[at, :] = hidden
            low_ref[at, :] = hidden.astype(BF16)
            more = (jnp.sum(hidden, axis=0), more_gain, more_shift)
            return tuple(a + b[None] for a, b in zip(sums, more))

        zero = jnp.zeros((1, width), F32)
        sums = lax.fori_loop(0, rows // chunk, norm_step, (zero, zero, zero))
        for k in range(3):
            feature_rows((0, 2, 3)[k], sums[k])
        for k in range(width // 128):
            at = slice(k * 128, (k + 1) * 128)
            low_t[at, :] = low_ref[:, at].astype(F32).T.astype(BF16)

        def out_step(j):
            gctx_ref[:, column(j)] = matmul(low_ref[...], w_buf[j % 2]).astype(BF16)
            other_tile(O, low_t, context_ref[:, column(j)], j)

        over_tiles(full[O] // TILE, [(1, o_in, w_buf)], out_step)

        def qkv_load(r):
            return pltpu.make_async_copy(
                qkv_in.at[:, column(r, cols[A])], qkv_buf.at[r % 2], load_sem.at[0, r % 2]
            )

        def attend_step(r, carry):
            @pl.when(r + 1 < size)
            def _():
                qkv_load(r + 1).start()

            qkv_load(r).wait()
            slot = r % 2
            seen = lax.broadcasted_iota(jnp.int32, (rows, rows), 0) < length
            for start, lanes, held in pairs_of(attn, head_size):
                queries = qkv_buf[slot, :, start : start + lanes]
                keys = qkv_buf[slot, :, attn + start : attn + start + lanes]
                values = qkv_buf[slot, :, 2 * attn + start : 2 * attn + start + lanes]
                grads = gctx_ref[:, pl.ds(pl.multiple_of(r * attn + start, 128), lanes)]
                grad_q = jnp.zeros((rows, lanes), F32)
                grad_k = jnp.zeros((rows, lanes), F32)
                grad_v = jnp.zeros((rows, lanes), F32)
                for which in range(held):
                    mine = keep_head(grads, which, head_size)
                    query = keep_head(queries, which, head_size)
                    scores = jnp.where(seen, contract_cols(keys, query) * scale, MASKED)
                    exponent = jnp.exp(scores - jnp.max(scores, axis=0, keepdims=True))
                    probs = exponent * (1.0 / jnp.sum(exponent, axis=0, keepdims=True))
                    grad_v += matmul(probs.astype(BF16), mine)
                    grad_probs = contract_cols(values, mine)
                    inner = jnp.sum(probs * grad_probs, axis=0, keepdims=True)
                    grad_scores = (probs * (grad_probs - inner)).astype(BF16)
                    grad_q += keep_head(contract_rows(grad_scores, keys), which, head_size)
                    grad_k += matmul(grad_scores, query)
                low_q = (grad_q * scale).astype(BF16)
                low_v = grad_v.astype(BF16)
                at = r * cols[A] + start
                gu_ref[:, pl.ds(pl.multiple_of(at, 128), lanes)] = low_q
                gu_ref[:, pl.ds(pl.multiple_of(at + attn, 128), lanes)] = (grad_k * scale).astype(BF16)
                gu_ref[:, pl.ds(pl.multiple_of(at + 2 * attn, 128), lanes)] = low_v
                place = ((tensor_at + size - r) % size) * (attn // 128) + start // 128
                v_ref[0, pl.ds(v_query + place, 1), :] = jnp.sum(
                    low_q.astype(F32), axis=0, keepdims=True
                )
                v_ref[0, pl.ds(v_value + place, 1), :] = jnp.sum(
                    low_v.astype(F32), axis=0, keepdims=True
                )
            return carry

        length = lengths_ref[tensor_at]
        qkv_load(0).start()
        lax.fori_loop(0, size // 2, attend_step, 0)
        for j in range(full[O] // TILE):
            own_tile(O, low_t, context_ref[:, j * TILE : (j + 1) * TILE], j)
        send_column(D)
        lax.fori_loop(size // 2, size, attend_step, 0)
        v_copy(0).start()
        send_sides(U)

        def qkv_step(j):
            core_copy(U, j).wait_send()
            tile = gu_ref[:, column(j)]
            other_tile(A, input_t, tile, j)
            grad_ref[...] += contract_cols(tile, w_buf[j % 2])

        over_tiles(full[A] // TILE, [(1, a_in, w_buf)], qkv_step)
        for j in range(full[A] // TILE, units // TILE):
            core_copy(U, j).wait_send()
        v_add(0)
        v_copy(1).start()

        def own_qkv(j, carry):
            own_tile(A, input_t, gu_ref[:, column(j)], j)
            return carry

        lax.fori_loop(0, full[A] // TILE, own_qkv, 0)
        send_corner(A)
        send_corner(O)
        v_add(1)
        v_copy(2).start()
        for place, mask in enumerate(ORDER):
            at = block_of(data_at, mask)
            grad_out[:, pl.ds(pl.multiple_of(at * block, block), block)] = grad_ref[
                :, place * block : (place + 1) * block
            ].astype(BF16)
        finish(D)
        v_add(2)
        send_column(U)
        send_sides(A)
        send_sides(O)
        v_copy(3).start()
        send_column(A)
        send_column(O)
        v_add(3)
        v_copy(4).start()
        finish(U)
        v_add(4)
        sums_out[...] = v_ref[5]
        finish(A)
        finish(O)
        for j in range(full[A] // TILE):
            core_copy(A, j).wait_send()
        for j in range(full[O] // TILE):
            core_copy(O, j).wait_send()
        for k in range(5):
            v_copy(k).wait_send()
        for copy in copies.values():
            copy.wait_send()

    anywhere, inside = pl.BlockSpec(memory_space=pl.ANY), pl.BlockSpec(memory_space=pltpu.VMEM)
    results = pl.pallas_call(
        body,
        out_shape=[jax.ShapeDtypeStruct((block, c), F32) for c in cols]
        + [
            jax.ShapeDtypeStruct((rows, width), BF16),
            jax.ShapeDtypeStruct((vector_rows, 128), F32),
        ],
        in_specs=[inside] * 5
        + [anywhere] * 2
        + [inside, pl.BlockSpec(memory_space=pltpu.SMEM)]
        + [anywhere] * 7
        + [inside],
        out_specs=[inside] * 6,
        scratch_shapes=[
            pltpu.VMEM((2, width, TILE), BF16),
            pltpu.VMEM((2, rows, TILE), BF16),
            pltpu.VMEM((2, rows, TILE), F32),
            pltpu.VMEM((rows, units), BF16),
            pltpu.VMEM((rows, width), F32),
            pltpu.VMEM((rows, width), BF16),
            pltpu.VMEM((width, rows), BF16),
            pltpu.VMEM((rows, full[1]), BF16),
            pltpu.VMEM((2, rows, cols[0]), BF16),
            pltpu.VMEM((middle, units), BF16),
            pltpu.VMEM((middle, full[1]), BF16),
        ]
        + [pltpu.VMEM((middle, c), BF16) for c in full]
        + [pltpu.VMEM((2, half, c), BF16) for c in full]
        + [pltpu.VMEM((2, block, c), BF16) for c in full]
        + [pltpu.VMEM((size - 1, block, c), BF16) for c in cols]
        + [
            pltpu.VMEM((6, vector_rows, 128), F32),
            pltpu.VMEM((5, vector_rows, 128), F32),
            pltpu.SemaphoreType.DMA((3, 2)),
            pltpu.SemaphoreType.DMA,
            pltpu.SemaphoreType.DMA((4, units // TILE)),
            pltpu.SemaphoreType.DMA((4, units // TILE)),
            pltpu.SemaphoreType.DMA((4, 3 + size)),
            pltpu.SemaphoreType.DMA((4, 3 + size)),
            pltpu.SemaphoreType.DMA((5,)),
            pltpu.SemaphoreType.DMA((5,)),
        ],
        compiler_params=pltpu.CompilerParams(
            collective_id=BACKWARD_ID, has_side_effects=True, vmem_limit_bytes=63 * 2**20
        ),
        cost_estimate=pl.CostEstimate(
            flops=4 * rows * sum(full) * width,
            bytes_accessed=4 * sum(full) * width,
            transcendentals=0,
        ),
        name="backward_near",
    )(
        mixed_low, mixed_t, normed_t, input_t, context, grad_second, hidden, wide, lengths, active,
        slope, qkv, *weights, vectors,
    )
    return results[:4], results[4], results[5]


def gather_far(shard):
    return lax.all_gather(
        lax.all_gather(shard, "tensor", axis=1, tiled=True), "dp", axis=0, tiled=True
    )


def scatter_far(left_side, right_side):
    whole = contract_rows(left_side, right_side).astype(BF16)
    part = lax.psum_scatter(whole, "dp", scatter_dimension=0, tiled=True)
    return lax.psum_scatter(part, "tensor", scatter_dimension=1, tiled=True).astype(F32)


def soft_weights(queries, keys, visible, scale):
    scores = contract_cols(queries, keys) * scale
    scores = jnp.where(visible, scores, MASKED)
    exponent = jnp.exp(scores - jnp.max(scores, axis=-1, keepdims=True))
    return exponent * (1.0 / jnp.sum(exponent, axis=-1, keepdims=True))


def pairs_of(width, head_size):
    lanes = max(128, head_size)
    return [(start, lanes, lanes // head_size) for start in range(0, width, lanes)]


def keep_head(array, which, head_size):
    lane = lax.broadcasted_iota(jnp.int32, array.shape, 1)
    return jnp.where(lane // head_size == which, array, jnp.zeros_like(array))


def attend_forward(qkv_q, qkv_kv, length, head_size, groups):
    q_rows = qkv_q.shape[0]
    k_rows = qkv_kv.shape[0]
    block = qkv_q.shape[1] // groups
    width = block // 3
    scale = float(head_size) ** (-0.5)

    def body(length_ref, q_ref, kv_ref, out_ref):
        visible = lax.broadcasted_iota(jnp.int32, (q_rows, k_rows), 1) < length_ref[0]
        for start, lanes, held in pairs_of(width, head_size):
            queries = q_ref[:, start : start + lanes]
            keys = kv_ref[:, width + start : width + start + lanes]
            values = kv_ref[:, 2 * width + start : 2 * width + start + lanes]
            total = jnp.zeros((q_rows, lanes), F32)
            for which in range(held):
                probs = soft_weights(keep_head(queries, which, head_size), keys, visible, scale)
                total += keep_head(matmul(probs.astype(BF16), values), which, head_size)
            out_ref[:, start : start + lanes] = total.astype(BF16)

    return pl.pallas_call(
        body,
        out_shape=jax.ShapeDtypeStruct((q_rows, groups * width), BF16),
        grid_spec=pltpu.PrefetchScalarGridSpec(
            num_scalar_prefetch=1,
            grid=(groups,),
            in_specs=[
                pl.BlockSpec((q_rows, block), lambda g, length_ref: (0, g)),
                pl.BlockSpec((k_rows, block), lambda g, length_ref: (0, g)),
            ],
            out_specs=pl.BlockSpec((q_rows, width), lambda g, length_ref: (0, g)),
        ),
        cost_estimate=pl.CostEstimate(
            flops=4 * q_rows * k_rows * width * groups,
            bytes_accessed=2 * (2 * q_rows + 2 * k_rows) * width * groups,
            transcendentals=q_rows * k_rows * groups * width // head_size,
        ),
        name="attend_forward",
    )(length, qkv_q, qkv_kv)


def attend_backward(qkv_q, qkv_kv, grad_context, length, head_size, groups):
    q_rows = qkv_q.shape[0]
    k_rows = qkv_kv.shape[0]
    block = qkv_q.shape[1] // groups
    width = block // 3
    scale = float(head_size) ** (-0.5)

    def body(length_ref, q_ref, kv_ref, grad_ref, dq_ref, dkv_ref):
        visible = lax.broadcasted_iota(jnp.int32, (q_rows, k_rows), 1) < length_ref[0]
        for start, lanes, held in pairs_of(width, head_size):
            queries = q_ref[:, start : start + lanes]
            keys = kv_ref[:, width + start : width + start + lanes]
            values = kv_ref[:, 2 * width + start : 2 * width + start + lanes]
            grads = grad_ref[:, start : start + lanes]
            grad_q = jnp.zeros((q_rows, lanes), F32)
            grad_k = jnp.zeros((k_rows, lanes), F32)
            grad_v = jnp.zeros((k_rows, lanes), F32)
            for which in range(held):
                mine = keep_head(grads, which, head_size)
                query = keep_head(queries, which, head_size)
                probs = soft_weights(query, keys, visible, scale)
                grad_v += contract_rows(probs.astype(BF16), mine)
                grad_probs = contract_cols(mine, values)
                inner = jnp.sum(probs * grad_probs, axis=-1, keepdims=True)
                grad_scores = (probs * (grad_probs - inner)).astype(BF16)
                grad_q += keep_head(matmul(grad_scores, keys), which, head_size)
                grad_k += contract_rows(grad_scores, query)
            dq_ref[:, start : start + lanes] = (grad_q * scale).astype(BF16)
            dkv_ref[:, start : start + lanes] = (grad_k * scale).astype(BF16)
            dkv_ref[:, width + start : width + start + lanes] = grad_v.astype(BF16)

    return pl.pallas_call(
        body,
        out_shape=(
            jax.ShapeDtypeStruct((q_rows, groups * width), BF16),
            jax.ShapeDtypeStruct((k_rows, groups * 2 * width), BF16),
        ),
        grid_spec=pltpu.PrefetchScalarGridSpec(
            num_scalar_prefetch=1,
            grid=(groups,),
            in_specs=[
                pl.BlockSpec((q_rows, block), lambda g, length_ref: (0, g)),
                pl.BlockSpec((k_rows, block), lambda g, length_ref: (0, g)),
                pl.BlockSpec((q_rows, width), lambda g, length_ref: (0, g)),
            ],
            out_specs=[
                pl.BlockSpec((q_rows, width), lambda g, length_ref: (0, g)),
                pl.BlockSpec((k_rows, 2 * width), lambda g, length_ref: (0, g)),
            ],
        ),
        cost_estimate=pl.CostEstimate(
            flops=10 * q_rows * k_rows * width * groups,
            bytes_accessed=2 * (3 * q_rows + 4 * k_rows) * width * groups,
            transcendentals=q_rows * k_rows * groups * width // head_size,
        ),
        name="attend_backward",
    )(length, qkv_q, qkv_kv, grad_context)


def activate(total, bias):
    upper = total + bias
    cumulative = 0.5 * (1.0 + lax.erf(upper * math.sqrt(0.5)))
    density = jnp.exp(-0.5 * upper * upper) * (1.0 / math.sqrt(2.0 * math.pi))
    return upper * cumulative, cumulative + upper * density


def norm_forward(hidden, gain_vec, shift_vec):
    center = hidden - jnp.mean(hidden, axis=-1, keepdims=True)
    variance = jnp.mean(center * center, axis=-1, keepdims=True)
    inv_root = lax.rsqrt(variance + EPSILON)
    normal = center * inv_root
    return (normal * gain_vec + shift_vec, normal, inv_root)


def norm_backward(grad_in, normal, inv_root, gain_vec):
    grad_normal = grad_in * gain_vec
    grad_gain = jnp.sum(grad_in * normal, axis=0)
    grad_shift = jnp.sum(grad_in, axis=0)
    grad_hidden = inv_root * (
        grad_normal
        - jnp.mean(grad_normal, axis=-1, keepdims=True)
        - normal * jnp.mean(grad_normal * normal, axis=-1, keepdims=True)
    )
    return (grad_hidden, grad_gain, grad_shift)


def layer(
    hidden_in,
    cotangent,
    w_query,
    w_key,
    w_value,
    w_out,
    w_up,
    w_down,
    bias_query,
    bias_value,
    bias_out,
    bias_up,
    bias_down,
    gain_attn,
    shift_attn,
    gain_ffn,
    shift_ffn,
    valid_lengths,
):
    rows, model_width = hidden_in.shape
    n_tensor = lax.axis_size("tensor")
    n_data = lax.axis_size("dp")
    tensor_at = lax.axis_index("tensor")
    spread_over = rows * n_tensor // valid_lengths.shape[0] // rows
    head_size = model_width // HEADS
    head_cols = w_query.shape[1]
    factor = 1.0 / math.sqrt(rows * n_tensor * n_data)
    matrices = (w_query, w_key, w_value, w_out, w_up, w_down)
    wide = (bias_out, bias_down, gain_attn, shift_attn, gain_ffn, shift_ffn)

    if n_data == len(ORDER) and spread_over == 1:
        (
            qkv_full, out_full, up_full, down_full, qkv, context, hidden, active, slope, output,
            mixed_low, mixed_t, normed_t, input_t, grad_second, given, arranged,
        ) = forward_near(
            matrices, hidden_in, cotangent, wide, bias_query, bias_value, bias_up, valid_lengths,
            head_size,
        )
        (grad_qkv_w, grad_out, grad_up, grad_down), grad_input, sums = backward_near(
            mixed_low, mixed_t, normed_t, input_t, context, grad_second, hidden, arranged,
            valid_lengths, active, slope, qkv, (qkv_full, out_full, up_full, down_full), given,
            head_size,
        )
        sums = sums.reshape(-1) * factor
    else:

        def column_part(vector):
            return vector.reshape(n_tensor, -1)

        query_bias, value_bias = column_part(bias_query), column_part(bias_value)
        bias_qkv = jnp.concatenate(
            [query_bias, jnp.zeros_like(query_bias), value_bias], axis=1
        ).reshape(1, -1)
        length = lax.dynamic_slice_in_dim(valid_lengths, tensor_at // spread_over, 1)
        low = [matrix.astype(BF16) for matrix in matrices]
        shards = [jnp.concatenate(low[:3], axis=1)] + low[3:]
        qkv_full, out_full, up_full, down_full = (gather_far(shard) for shard in shards)
        qkv = (matmul(hidden_in, qkv_full) + bias_qkv).astype(BF16)
        members = [list(range(k, k + spread_over)) for k in range(0, n_tensor, spread_over)]
        qkv_seq = lax.all_gather(qkv, "tensor", axis_index_groups=members, axis=0, tiled=True)
        context = attend_forward(qkv, qkv_seq, length, head_size, n_tensor)
        hidden = hidden_in.astype(F32) + contract_cols(context, out_full) + bias_out
        normed, normal_attn, root_attn = norm_forward(hidden, gain_attn, shift_attn)
        normed_low = normed.astype(BF16)
        active, slope = activate(matmul(normed_low, up_full), bias_up)
        active = active.astype(BF16)
        mixed = contract_cols(active, down_full)
        result, normal_ffn, root_ffn = norm_forward(normed + mixed + bias_down, gain_ffn, shift_ffn)
        output = result.astype(BF16)
        grad_second, grad_gain_ffn, grad_shift_ffn = norm_backward(
            cotangent.astype(F32), normal_ffn, root_ffn, gain_ffn
        )
        grad_bias_down = jnp.sum(grad_second, axis=0)
        mixed_low = grad_second.astype(BF16)
        grad_down = scatter_far(mixed_low, active)
        grad_upper = (matmul(mixed_low, down_full) * slope).astype(BF16)
        grad_bias_up = jnp.sum(grad_upper, axis=0, dtype=F32)
        grad_up = scatter_far(normed_low, grad_upper)
        grad_normed = grad_second + contract_cols(grad_upper, up_full)
        grad_first, grad_gain_attn, grad_shift_attn = norm_backward(
            grad_normed, normal_attn, root_attn, gain_attn
        )
        grad_bias_out = jnp.sum(grad_first, axis=0)
        attn_low = grad_first.astype(BF16)
        grad_context = matmul(attn_low, out_full).astype(BF16)
        grad_out = scatter_far(attn_low, context)
        grad_q, grad_kv = attend_backward(qkv, qkv_seq, grad_context, length, head_size, n_tensor)
        grad_kv = lax.psum_scatter(
            grad_kv.astype(F32),
            "tensor",
            scatter_dimension=0,
            axis_index_groups=members,
            tiled=True,
        ).astype(BF16)
        grad_qkv = jnp.concatenate(
            [grad_q.reshape(rows, n_tensor, -1), grad_kv.reshape(rows, n_tensor, -1)], axis=2
        ).reshape(rows, -1)
        grad_bias_qkv = jnp.sum(grad_qkv, axis=0, dtype=F32).reshape(n_tensor, 3, head_cols)
        grad_qkv_w = scatter_far(hidden_in, grad_qkv)
        grad_input = (grad_first + contract_cols(grad_qkv, qkv_full)).astype(BF16)
        sums = jnp.concatenate(
            [
                grad_bias_out,
                grad_bias_down,
                grad_gain_attn,
                grad_shift_attn,
                grad_gain_ffn,
                grad_shift_ffn,
                grad_bias_qkv[:, 0].reshape(-1),
                grad_bias_qkv[:, 2].reshape(-1),
                grad_bias_up,
            ]
        )
        sums = lax.psum(sums, ("dp", "tensor")) * factor
    v_out, v_down, v_gain_attn, v_shift_attn, v_gain_ffn, v_shift_ffn, v_query, v_value = (
        sums[k * model_width : (k + 1) * model_width] for k in range(8)
    )
    v_up = sums[8 * model_width :]
    return (
        output,
        grad_input,
        grad_qkv_w[:, :head_cols] * factor,
        grad_qkv_w[:, head_cols : 2 * head_cols] * factor,
        grad_qkv_w[:, 2 * head_cols :] * factor,
        grad_out * factor,
        grad_up * factor,
        grad_down * factor,
        v_query,
        v_value,
        v_out,
        v_up,
        v_down,
        v_gain_attn,
        v_shift_attn,
        v_gain_ffn,
        v_shift_ffn,
    )


def solution(mesh):
    tokens, matrix, copied = P(("dp", "tensor"), None), P("dp", "tensor"), P()
    return jax.shard_map(
        layer,
        mesh=mesh,
        in_specs=(tokens,) * 2 + (matrix,) * 6 + (copied,) * 9 + (P("dp"),),
        out_specs=(tokens,) * 2 + (matrix,) * 6 + (copied,) * 9,
        check_vma=False,
    )
```

```python
import math

import jax
import jax.numpy as jnp
from jax import lax
from jax.experimental import pallas as pl
from jax.experimental.pallas import tpu as pltpu
from jax.sharding import PartitionSpec as P

HEADS = 16
EPSILON = 1e-12
MASKED = -1e30
BF16 = jnp.bfloat16
F32 = jnp.float32

ORDER = (0, 2, 4, 6, 1, 3, 5, 7)
BIT_CORE, BIT_X, BIT_Y = 1, 2, 4


def matmul(left_side, right_side):
    return jnp.dot(left_side, right_side, preferred_element_type=F32)


def contract_rows(left_side, right_side):
    return lax.dot_general(
        left_side, right_side, (((0,), (0,)), ((), ())), preferred_element_type=F32
    )


def contract_cols(left_side, right_side):
    return lax.dot_general(
        left_side, right_side, (((1,), (1,)), ((), ())), preferred_element_type=F32
    )


FORWARD_ID = 1
BACKWARD_ID = 2
TILE = 512


def neighbour(index, bit):
    return index + bit - 2 * bit * ((index // bit) % 2)


def block_of(index, mask):
    for bit in (BIT_CORE, BIT_X, BIT_Y):
        if mask & bit:
            index = neighbour(index, bit)
    return index


def pieces_of(size, attn, units_each):
    pieces = [(0, k * size * attn, attn) for k in range(3)] + [(1, 0, attn)]
    for weight in (2, 3):
        start = 0
        for count in (units_each // 2, units_each // 4, units_each // 4):
            pieces.append((weight, start * size, count))
            start += count
    return pieces


def greet(partners):
    barrier = pltpu.get_barrier_semaphore()
    for partner in partners:
        pl.semaphore_signal(
            barrier, inc=1, device_id=partner, device_id_type=pl.DeviceIdType.MESH
        )
    pl.semaphore_wait(barrier, len(partners))


def forward_near(weights, hidden_in, cotangent, wide, bias_query, bias_value, bias_units, lengths, head_size):
    size = lax.axis_size("tensor")
    rows, width = hidden_in.shape
    block = width // len(ORDER)
    attn, units_each = weights[0].shape[1], weights[4].shape[1]
    cols = [3 * attn, attn, units_each, units_each]
    full = [(width, size * c) for c in cols]
    units = size * units_each
    half = block // 2
    pieces = pieces_of(size, attn, units_each)
    X = len(pieces) - 1
    A, O, U, D = range(4)
    B_OUT, B_DOWN, G_ATTN, S_ATTN, G_FFN, S_FFN = range(6)

    def body(
        q_in, k_in, v_in, o_in, u_in, d_in, hidden_raw, cotangent_ref, bias_out_in, bias_down_in,
        gain_attn_in, shift_attn_in, gain_ffn_in, shift_ffn_in, bias_q_ref, bias_v_ref, bias_u_ref,
        lengths_ref,
        a_out, o_out, u_out, d_out, qkv_ref, context_ref, hidden_ref, active_out, slope_out, output_ref,
        mixed_ref, mixed_t, normed_t, input_t, second_ref, sums_ref, wide_ref,
        a_ref, o_ref, u_ref, d_ref, x_ref, low_ref, active_ref, slope_ref, bias_ref, units_ref, local_sem, send_sem, recv_sem,
        tile_sem,
    ):
        data_at, tensor_at = lax.axis_index("dp"), lax.axis_index("tensor")
        places = (a_ref, o_ref, u_ref, d_ref)

        def dp_partner(bit):
            return (neighbour(data_at, bit), tensor_at)

        def z_partner(step):
            return (data_at, (tensor_at + step) % size)

        by_x, by_y, by_core = dp_partner(BIT_X), dp_partner(BIT_Y), dp_partner(BIT_CORE)
        owners = [block_of(data_at, mask) for mask in ORDER]
        copies = {}

        def send(g, slot, source, target, device):
            copy = pltpu.make_async_remote_copy(
                src_ref=source,
                dst_ref=target,
                send_sem=send_sem.at[g, slot],
                recv_sem=recv_sem.at[g, slot],
                device_id=device,
                device_id_type=pl.DeviceIdType.MESH,
            )
            copies[g, slot] = copy
            copy.start()

        def arrived(g, *slots):
            for slot in slots:
                copies[g, slot].wait_recv()

        def whole(g, start, count):
            weight, first, wide_by = pieces[g]
            return places[weight].at[start : start + count, first : first + size * wide_by]

        def cell(g, start, count, r):
            weight, first, wide_by = pieces[g]
            at = first + r * wide_by
            return places[weight].at[start : start + count, at : at + wide_by]

        def send_z(g):
            for r in range(1, size):
                send(g, r - 1, cell(g, 0, block, 0), cell(g, 0, block, r), z_partner(r))

        def send_column(g):
            arrived(g, 0, 1, 2)
            send(g, 3, whole(g, 0, block), whole(g, block, block), by_x)
            send(g, 4, whole(g, 0, block), whole(g, 2 * block, block), by_y)

        def send_corner(g):
            arrived(g, 3, 4)
            send(g, 5, whole(g, block, half), whole(g, 3 * block, half), by_y)
            send(g, 6, whole(g, 2 * block + half, half), whole(g, 3 * block + half, half), by_x)
            send(g, 7, whole(g, 0, 3 * block), whole(g, 4 * block, 3 * block), by_core)

        def send_last(g):
            arrived(g, 5, 6)
            send(g, 8, whole(g, 3 * block, block), whole(g, 7 * block, block), by_core)

        def complete(*group):
            for g in group:
                arrived(g, 7, 8)

        def late_plane():
            send(X, 3, cell(X, 0, block, 0), cell(X, block, block, 0), by_x)
            send(X, 4, cell(X, 0, block, 0), cell(X, 2 * block, block, 0), by_y)

        def late_corner():
            arrived(X, 3, 4)
            send(X, 5, cell(X, block, half, 0), cell(X, 3 * block, half, 0), by_y)
            send(X, 6, cell(X, 2 * block + half, half, 0), cell(X, 3 * block + half, half, 0), by_x)

        def late_z():
            arrived(X, 5, 6)
            for r in range(1, size):
                send(X, r - 1, cell(X, 0, 4 * block, 0), cell(X, 0, 4 * block, r), z_partner(r))

        def late_core():
            arrived(X, 0, 1, 2)
            send(X, 7, whole(X, 0, 4 * block), whole(X, 4 * block, 4 * block), by_core)

        saves = []

        def save(g, target):
            copy = pltpu.make_async_copy(places[g], target, local_sem.at[g])
            copy.start()
            saves.append(copy)

        sources = (q_in, k_in, v_in, o_in, u_in, u_in, u_in, d_in, d_in, d_in)

        def cast(g):
            weight, first, wide_by = pieces[g]
            start = first // size if weight >= U else 0
            places[weight][:block, first : first + wide_by] = sources[g][
                :, start : start + wide_by
            ].astype(BF16)

        cast(0)
        cast(X)
        greet([by_x, by_y, by_core] + [z_partner(r) for r in range(1, size)])
        late_plane()
        send_z(0)
        for g in range(1, X):
            cast(g)
            send_z(g)

        def lanes_of(owner):
            return pl.ds(pl.multiple_of(owner * block, block), block)

        def transpose_into(target, source):
            for k in range(width // 128):
                at = slice(k * 128, (k + 1) * 128)
                target[at, :] = source[:, at].astype(F32).T.astype(BF16)

        for place, owner in enumerate(owners):
            at = slice(place * block, (place + 1) * block)
            x_ref[:, at] = hidden_raw[:, lanes_of(owner)]
            for k, ref in enumerate(
                (bias_out_in, bias_down_in, gain_attn_in, shift_attn_in, gain_ffn_in, shift_ffn_in)
            ):
                wide_ref[k : k + 1, at] = ref[:, lanes_of(owner)]

        def vector(k):
            return wide_ref[k : k + 1, :]

        def column_of(r, first, span):
            at = ((tensor_at + size - r) % size) * (first[1]) + first[0]
            return pl.ds(pl.multiple_of(at, 128), span)

        for r in range(size):
            at = slice(r * attn, (r + 1) * attn)
            bias_ref[0:1, at] = bias_q_ref[:, column_of(r, (0, attn), attn)]
            bias_ref[1:2, at] = bias_v_ref[:, column_of(r, (0, attn), attn)]
            for weight, first, wide_by in pieces:
                if weight == U:
                    at = slice(first + r * wide_by, first + (r + 1) * wide_by)
                    units_ref[:, at] = bias_u_ref[:, column_of(r, (first // size, units_each), wide_by)]

        late_corner()
        send_column(0)
        late_z()
        send_column(1)
        send_corner(0)
        send_column(2)
        send_corner(1)
        send_last(0)
        transpose_into(input_t, x_ref)
        send_column(3)
        send_corner(2)
        send_last(1)
        send_column(4)
        send_corner(3)
        send_last(2)
        complete(0, 1, 2)
        save(A, a_out)

        def project(j, carry):
            at = pl.ds(pl.multiple_of(j * attn, attn), attn)
            total = matmul(x_ref[...], a_ref[:, at])
            which = j // size
            bias = bias_ref[:, pl.ds(pl.multiple_of((j % size) * attn, attn), attn)]
            bias = jnp.where(which == 0, bias[0:1], jnp.where(which == 2, bias[1:2], 0.0))
            qkv_ref[:, at] = (total + bias).astype(BF16)
            return carry

        lax.fori_loop(0, 3 * size, project, 0)
        scale = float(head_size) ** (-0.5)
        length = lengths_ref[tensor_at]

        def attend(r, carry):
            seen = lax.broadcasted_iota(jnp.int32, (rows, rows), 1) < length
            for start, lanes, held in pairs_of(attn, head_size):
                at = [
                    pl.ds(pl.multiple_of((k * size + r) * attn + start, 128), lanes) for k in range(3)
                ]
                queries, keys, values = (qkv_ref[:, where] for where in at)
                total = jnp.zeros((rows, lanes), F32)
                for which in range(held):
                    probs = soft_weights(keep_head(queries, which, head_size), keys, seen, scale)
                    total += keep_head(matmul(probs.astype(BF16), values), which, head_size)
                context_ref[:, at[0]] = total.astype(BF16)
            return carry

        send_column(5)
        lax.fori_loop(0, 1, attend, 0)
        send_corner(4)
        send_last(3)
        send_column(6)
        lax.fori_loop(1, 2, attend, 0)
        send_corner(5)
        send_last(4)
        send_column(7)
        lax.fori_loop(2, 3, attend, 0)
        send_corner(6)
        send_last(5)
        lax.fori_loop(3, size, attend, 0)
        complete(3)
        save(O, o_out)
        send_column(8)

        def output(j, carry):
            at = pl.ds(pl.multiple_of(j * 256, 256), 256)
            total = contract_cols(context_ref[...], o_ref[at, :])
            hidden_ref[:, at] = x_ref[:, at].astype(F32) + total + wide_ref[B_OUT : B_OUT + 1, at]
            return carry

        lax.fori_loop(0, width // 256, output, 0)
        chunk = 64

        def norm(j, carry):
            at = pl.ds(pl.multiple_of(j * chunk, chunk), chunk)
            normed = norm_forward(hidden_ref[at, :], vector(G_ATTN), vector(S_ATTN))[0]
            low_ref[at, :] = normed.astype(BF16)
            second_ref[at, :] = normed + vector(B_DOWN)
            return carry

        lax.fori_loop(0, rows // chunk, norm, 0)
        send_corner(7)
        send_last(6)
        complete(4, 5, 6)
        save(U, u_out)

        def tile_at(j):
            return pl.ds(pl.multiple_of(j * TILE, TILE), TILE)

        def slope_copy(j):
            return pltpu.make_async_copy(
                slope_ref.at[j % 2], slope_out.at[:, tile_at(j)], tile_sem.at[1, j % 2]
            )

        def active_copy(j):
            return pltpu.make_async_copy(
                active_ref.at[:, tile_at(j)], active_out.at[:, tile_at(j)], tile_sem.at[0, j]
            )

        def raise_up(j, carry):
            @pl.when(j >= 2)
            def _():
                slope_copy(j - 2).wait()

            total = matmul(low_ref[...], u_ref[:, tile_at(j)])
            active, slope = activate(total, units_ref[:, tile_at(j)])
            active_ref[:, tile_at(j)] = active.astype(BF16)
            slope_ref[j % 2] = slope
            active_copy(j).start()
            slope_copy(j).start()
            return carry

        tiles = units // TILE
        lax.fori_loop(0, tiles // 2, raise_up, 0)
        send_corner(8)
        send_last(7)
        lax.fori_loop(tiles // 2, tiles, raise_up, 0)
        late_core()
        send_last(8)
        transpose_into(normed_t, low_ref)

        def lower(start):
            at = slice(start, start + 256)
            second_ref[:, at] += contract_cols(active_ref[...], d_ref[at, :])

        lower(0)
        lower(2 * block)
        complete(7, 8)
        arrived(X, 7)
        save(D, d_out)
        lower(4 * block)
        lower(6 * block)

        def second(j, sums):
            at = pl.ds(pl.multiple_of(j * chunk, chunk), chunk)
            result, normal, root = norm_forward(second_ref[at, :], vector(G_FFN), vector(S_FFN))
            grads = jnp.concatenate([cotangent_ref[at, lanes_of(owner)] for owner in owners], axis=1)
            for place, owner in enumerate(owners):
                output_ref[at, lanes_of(owner)] = result[:, place * block : (place + 1) * block].astype(BF16)
            hidden, more_gain, more_shift = norm_backward(
                grads.astype(F32), normal, root, vector(G_FFN)
            )
            second_ref[at, :] = hidden
            mixed_ref[at, :] = hidden.astype(BF16)
            more = (jnp.sum(hidden, axis=0), more_gain, more_shift)
            return tuple(a + b[None] for a, b in zip(sums, more))

        zero = jnp.zeros((1, width), F32)
        sums = lax.fori_loop(0, rows // chunk, second, (zero, zero, zero))
        for k in range(3):
            sums_ref[k : k + 1, :] = sums[k]
        transpose_into(mixed_t, mixed_ref)

        def settle(j, carry):
            active_copy(j).wait()
            return carry

        lax.fori_loop(0, units // TILE, settle, 0)
        for j in (units // TILE - 2, units // TILE - 1):
            slope_copy(j).wait()
        for copy in saves:
            copy.wait()
        for copy in copies.values():
            copy.wait_send()

    anywhere, inside = pl.BlockSpec(memory_space=pl.ANY), pl.BlockSpec(memory_space=pltpu.VMEM)
    tall = jax.ShapeDtypeStruct((rows, width), BF16)
    turned = jax.ShapeDtypeStruct((width, rows), BF16)
    return pl.pallas_call(
        body,
        out_shape=[jax.ShapeDtypeStruct(shape, BF16) for shape in full]
        + [
            jax.ShapeDtypeStruct((rows, full[A][1]), BF16),
            tall,
            jax.ShapeDtypeStruct((rows, width), F32),
            jax.ShapeDtypeStruct((rows, units), BF16),
            jax.ShapeDtypeStruct((rows, units), F32),
            tall,
            tall,
            turned,
            turned,
            turned,
            jax.ShapeDtypeStruct((rows, width), F32),
            jax.ShapeDtypeStruct((3, width), F32),
            jax.ShapeDtypeStruct((6, width), F32),
        ],
        in_specs=[inside] * 17 + [pl.BlockSpec(memory_space=pltpu.SMEM)],
        out_specs=[anywhere] * 4 + [inside] * 3 + [anywhere] * 2 + [inside] * 8,
        scratch_shapes=[pltpu.VMEM(shape, BF16) for shape in full]
        + [
            pltpu.VMEM((rows, width), BF16),
            pltpu.VMEM((rows, width), BF16),
            pltpu.VMEM((rows, units), BF16),
            pltpu.VMEM((2, rows, TILE), F32),
            pltpu.VMEM((2, size * attn), F32),
            pltpu.VMEM((1, units), F32),
            pltpu.SemaphoreType.DMA((4,)),
            pltpu.SemaphoreType.DMA((len(pieces), 9)),
            pltpu.SemaphoreType.DMA((len(pieces), 9)),
            pltpu.SemaphoreType.DMA((2, units // TILE)),
        ],
        compiler_params=pltpu.CompilerParams(
            collective_id=FORWARD_ID, has_side_effects=True, vmem_limit_bytes=63 * 2**20
        ),
        cost_estimate=pl.CostEstimate(
            flops=2 * rows * width * sum(shape[1] for shape in full),
            bytes_accessed=4 * width * sum(shape[1] for shape in full),
            transcendentals=rows * units,
        ),
        name="forward_near",
    )(
        *weights, hidden_in, cotangent, *(vector[None] for vector in wide), bias_query[None],
        bias_value[None], bias_units[None], lengths,
    )


def backward_near(mixed_low, mixed_t, normed_t, input_t, context, grad_second, hidden, wide, lengths,
                  active, slope, qkv, weights, vectors, head_size):
    size = lax.axis_size("tensor")
    rows, width = mixed_low.shape
    block = width // len(ORDER)
    middle = width // 2
    half = block // 2
    full = [weight.shape[1] for weight in weights]
    units = full[2]
    units_each = units // size
    attn = full[1] // size
    pieces = pieces_of(size, attn, units_each)
    X = len(pieces) - 1
    A, O, U, D = range(4)
    tiles = [c // TILE for c in full]
    vector_rows = (6 * width + 2 * full[1] + units) // 128
    v_query, v_value, v_up = 6 * width // 128, (6 * width + full[1]) // 128, (6 * width + 2 * full[1]) // 128
    scale = float(head_size) ** (-0.5)

    def body(
        mixed_ref, mixed_t, normed_t, input_t, context_ref, second_in, hidden_in, wide_ref,
        lengths_ref, active_in, slope_in, qkv_in, a_in, o_in, u_in, d_in, vectors_ref,
        q_out, k_out, v_out, o_out, u_out, d_out, grad_out, sums_out,
        w_buf, act_ref, slope_buf, gu_ref, grad_ref, low_ref, low_t, gctx_ref, qkv_buf, send_buf,
        units_sum, a_plane, o_plane, u_plane, d_plane, *rest,
    ):
        count = len(pieces)
        corners, sides, zins = (rest[k * count : (k + 1) * count] for k in range(3))
        (
            v_ref, v_in, load_sem, start_sem, core_send, core_recv, send_sem, recv_sem, v_send, v_recv,
        ) = rest[3 * count :]
        data_at, tensor_at = lax.axis_index("dp"), lax.axis_index("tensor")
        planes = (a_plane, o_plane, u_plane, d_plane)
        outs = (q_out, k_out, v_out, o_out, u_out, u_out, u_out, d_out, d_out, d_out)
        shift_by = (tiles[O], 0, 0, 0)

        def dp_partner(bit):
            return (neighbour(data_at, bit), tensor_at)

        def z_partner(step):
            return (data_at, (tensor_at + size + step) % size)

        by_x, by_y, by_core = dp_partner(BIT_X), dp_partner(BIT_Y), dp_partner(BIT_CORE)

        def column(j, span=TILE):
            return pl.ds(pl.multiple_of(j * span, 128), span)

        def load(row, source, buffer, j):
            return pltpu.make_async_copy(
                source.at[:, column(j)], buffer.at[j % 2], load_sem.at[row, j % 2]
            )

        def over_tiles(first, last, loads, step):
            for row, source, buffer in loads:
                load(row, source, buffer, first).start()

            def one(j, carry):
                @pl.when(j + 1 < last)
                def _():
                    for row, source, buffer in loads:
                        load(row, source, buffer, j + 1).start()

                for row, source, buffer in loads:
                    load(row, source, buffer, j).wait()
                step(j)
                return carry

            lax.fori_loop(first, last, one, 0)

        def remote(source, target, send, receive, device):
            return pltpu.make_async_remote_copy(
                src_ref=source,
                dst_ref=target,
                send_sem=send,
                recv_sem=receive,
                device_id=device,
                device_id_type=pl.DeviceIdType.MESH,
            )

        def core_copy(g, j):
            return remote(
                send_buf.at[:, column(j + shift_by[g])],
                planes[g].at[:, column(j)],
                core_send.at[g, j],
                core_recv.at[g, j],
                by_core,
            )

        copies = {}

        def send(g, slot, source, target, device):
            copies[g, slot] = remote(
                source, target, send_sem.at[g, slot], recv_sem.at[g, slot], device
            )
            copies[g, slot].start()

        def arrived(g, *slots):
            for slot in slots:
                copies[g, slot].wait_recv()

        def other_tile(g, left_t, right, j):
            send_buf[:, column(j + shift_by[g])] = matmul(left_t[middle:, :], right).astype(BF16)
            core_copy(g, j).start()

        def own_tile(g, left_t, right, j):
            core_copy(g, j).wait_recv()
            total = matmul(left_t[:middle, :], right) + planes[g][:, column(j)].astype(F32)
            planes[g][:, column(j)] = total.astype(BF16)

        def span(g):
            _, first, wide_by = pieces[g]
            return first, wide_by if g == X else size * wide_by

        def plane_rows(g, start, count):
            first, wide_by = span(g)
            return planes[pieces[g][0]].at[start : start + count, first : first + wide_by]

        def send_corner(g):
            send(g, 0, plane_rows(g, 3 * block, half), corners[g].at[0], by_x)
            send(g, 1, plane_rows(g, 3 * block + half, half), corners[g].at[1], by_y)

        def add_rows(g, start, count, *more):
            plane = planes[pieces[g][0]]
            first, wide_by = span(g)
            step = min(TILE, wide_by)
            for at in range(0, wide_by, step):
                where = (slice(start, start + count), slice(first + at, first + at + step))
                total = plane[where].astype(F32)
                for ref in more:
                    total += ref[:, at : at + step].astype(F32)
                plane[where] = total.astype(BF16)

        def send_sides(g):
            arrived(g, 0, 1)
            add_rows(g, 2 * block, half, corners[g].at[0])
            add_rows(g, block + half, half, corners[g].at[1])
            send(g, 2, plane_rows(g, block, block), sides[g].at[0], by_x)
            send(g, 3, plane_rows(g, 2 * block, block), sides[g].at[1], by_y)

        def out_of(g):
            weight, first, wide_by = pieces[g]
            start = first // size if weight >= U else 0
            return outs[g].at[:, start : start + wide_by]

        def send_column(g):
            arrived(g, 2, 3)
            weight, first, wide_by = pieces[g]
            for r in range(size):
                at = slice(r * wide_by, (r + 1) * wide_by)
                own = slice(first + r * wide_by, first + (r + 1) * wide_by)
                total = planes[weight][:block, own].astype(F32)
                total += sides[g][0, :, at].astype(F32) + sides[g][1, :, at].astype(F32)
                if r == 0:
                    out_of(g)[...] = total
                else:
                    planes[weight][:block, own] = total.astype(BF16)
                    send(g, 3 + r, planes[weight].at[:block, own], zins[g].at[r - 1], z_partner(-r))

        def finish(g):
            arrived(g, *range(4, 3 + size))
            total = out_of(g)[...]
            for r in range(1, size):
                total += zins[g][r - 1].astype(F32)
            out_of(g)[...] = total

        def late_z():
            weight, first, wide_by = pieces[X]
            for r in range(1, size):
                own = slice(first + r * wide_by, first + (r + 1) * wide_by)
                send(X, 3 + r, planes[weight].at[:, own], zins[X].at[r - 1], z_partner(-r))

        def late_corner():
            arrived(X, *range(4, 3 + size))
            for k in range(4):
                rows_k = slice(k * block, (k + 1) * block)
                add_rows(X, k * block, block, *(zins[X].at[r, rows_k] for r in range(size - 1)))
            send_corner(X)

        def late_finish():
            arrived(X, 2, 3)
            total = plane_rows(X, 0, block)[...].astype(F32)
            out_of(X)[...] = total + sides[X][0].astype(F32) + sides[X][1].astype(F32)

        def feature_rows(k, vector):
            for place, mask in enumerate(ORDER):
                at = block_of(data_at, mask)
                v_ref[0, pl.ds(k * len(ORDER) + at, 1), :] = vector[:, place * 128 : (place + 1) * 128]

        z_near = tensor_at + 1 - 2 * (tensor_at % 2)
        z_across = tensor_at + 2 - 4 * ((tensor_at // 2) % 2)
        v_partners = (by_core, (data_at, z_near), (data_at, z_across), by_x, by_y)

        def v_copy(k):
            return remote(v_ref.at[k], v_in.at[k], v_send.at[k], v_recv.at[k], v_partners[k])

        def v_add(k):
            v_copy(k).wait_recv()
            v_ref[k + 1] = v_ref[k] + v_in[k]

        early = [
            pltpu.make_async_copy(
                active_in.at[:, k * (units // 2) : (k + 1) * (units // 2)],
                act_ref.at[:, k * (units // 2) : (k + 1) * (units // 2)],
                start_sem.at[k],
            )
            for k in range(2)
        ]
        grad_load = pltpu.make_async_copy(second_in, grad_ref, start_sem.at[2])
        for copy in early:
            copy.start()
        grad_load.start()
        greet([by_x, by_y, by_core] + [z_partner(r) for r in range(1, size)])

        def each(first, last, step):
            def one(j, carry):
                step(j)
                return carry

            lax.fori_loop(first, last, one, 0)

        def other_down(j):
            other_tile(D, mixed_t, act_ref[:, column(j)], j)

        def own_down(j):
            own_tile(D, mixed_t, act_ref[:, column(j)], j)

        def other_up(j):
            core_copy(D, j).wait_send()
            other_tile(U, normed_t, gu_ref[:, column(j)], j)

        def own_up(j):
            own_tile(U, normed_t, gu_ref[:, column(j)], j)

        def bounds(g):
            _, first, wide_by = pieces[g]
            return first // TILE, (first + size * wide_by) // TILE

        early[0].wait()
        each(*bounds(7), other_down)
        early[1].wait()
        each(*bounds(X), other_down)
        each(*bounds(8), other_down)
        each(*bounds(7), own_down)
        send_corner(7)
        each(*bounds(X), own_down)
        late_z()
        each(*bounds(8), own_down)
        send_corner(8)
        for k in range(3):
            feature_rows((1, 4, 5)[k], vectors_ref[k : k + 1, :])

        def gelu_step(j):
            low = (matmul(mixed_ref[...], w_buf[j % 2]) * slope_buf[j % 2]).astype(BF16)
            gu_ref[:, column(j)] = low
            units_sum[:, column(j)] = jnp.sum(low.astype(F32), axis=0, keepdims=True)

        gelu_loads = [(1, d_in, w_buf), (2, slope_in, slope_buf)]
        over_tiles(0, tiles[D] // 2, gelu_loads, gelu_step)
        send_sides(7)
        each(*bounds(4), other_up)
        over_tiles(tiles[D] // 2, tiles[D], gelu_loads, gelu_step)
        hidden_loads = [
            pltpu.make_async_copy(hidden_in.at[:, column(k)], slope_buf.at[k], load_sem.at[2, k])
            for k in range(2)
        ]
        for copy in hidden_loads:
            copy.start()
        send_sides(8)
        each(*bounds(4), own_up)
        send_corner(4)
        for g in (5, 6):
            each(*bounds(g), other_up)
        late_corner()
        for g in (5, 6):
            each(*bounds(g), own_up)
            send_corner(g)

        grad_load.wait()

        def up_step(j):
            grad_ref[...] += contract_cols(gu_ref[:, column(j)], w_buf[j % 2])

        over_tiles(0, tiles[U] // 2, [(1, u_in, w_buf)], up_step)
        send_sides(X)
        send_column(7)
        send_sides(4)
        over_tiles(tiles[U] // 2, tiles[U], [(1, u_in, w_buf)], up_step)
        send_column(8)
        for r in range(size):
            for weight, first, wide_by in pieces:
                if weight == U:
                    for k in range(wide_by // 128):
                        place = ((tensor_at + size - r) % size) * (units_each // 128)
                        place += (first // size) // 128 + k
                        at = first + r * wide_by + k * 128
                        v_ref[0, pl.ds(v_up + place, 1), :] = units_sum[:, at : at + 128]

        for copy in hidden_loads:
            copy.wait()
        chunk = 64

        def norm_step(j, sums):
            at = pl.ds(pl.multiple_of(j * chunk, chunk), chunk)
            hidden_rows = jnp.concatenate([slope_buf[0, at, :], slope_buf[1, at, :]], axis=1)
            gain = wide_ref[2:3, :]
            normal, root = norm_forward(hidden_rows, gain, gain)[1:]
            hidden, more_gain, more_shift = norm_backward(grad_ref[at, :], normal, root, gain)
            grad_ref[at, :] = hidden
            low_ref[at, :] = hidden.astype(BF16)
            more = (jnp.sum(hidden, axis=0), more_gain, more_shift)
            return tuple(a + b[None] for a, b in zip(sums, more))

        zero = jnp.zeros((1, width), F32)
        sums = lax.fori_loop(0, rows // chunk, norm_step, (zero, zero, zero))
        for k in range(3):
            feature_rows((0, 2, 3)[k], sums[k])
        for k in range(width // 128):
            at = slice(k * 128, (k + 1) * 128)
            low_t[at, :] = low_ref[:, at].astype(F32).T.astype(BF16)

        send_sides(5)
        late_finish()

        def out_step(j):
            core_copy(U, j).wait_send()
            gctx_ref[:, column(j)] = matmul(low_ref[...], w_buf[j % 2]).astype(BF16)
            other_tile(O, low_t, context_ref[:, column(j)], j)

        over_tiles(0, tiles[O], [(1, o_in, w_buf)], out_step)
        send_sides(6)

        def qkv_load(r):
            return [
                pltpu.make_async_copy(
                    qkv_in.at[:, column(k * size + r, attn)], qkv_buf.at[r % 2, k], load_sem.at[k, r % 2]
                )
                for k in range(3)
            ]

        def attend_step(r):
            @pl.when(r + 1 < size)
            def _():
                for copy in qkv_load(r + 1):
                    copy.start()

            for copy in qkv_load(r):
                copy.wait()
            slot = r % 2
            seen = lax.broadcasted_iota(jnp.int32, (rows, rows), 0) < length
            for start, lanes, held in pairs_of(attn, head_size):
                queries, keys, values = (qkv_buf[slot, k, :, start : start + lanes] for k in range(3))
                grads = gctx_ref[:, pl.ds(pl.multiple_of(r * attn + start, 128), lanes)]
                grad_q = jnp.zeros((rows, lanes), F32)
                grad_k = jnp.zeros((rows, lanes), F32)
                grad_v = jnp.zeros((rows, lanes), F32)
                for which in range(held):
                    mine = keep_head(grads, which, head_size)
                    query = keep_head(queries, which, head_size)
                    scores = jnp.where(seen, contract_cols(keys, query) * scale, MASKED)
                    exponent = jnp.exp(scores - jnp.max(scores, axis=0, keepdims=True))
                    probs = exponent * (1.0 / jnp.sum(exponent, axis=0, keepdims=True))
                    grad_v += matmul(probs.astype(BF16), mine)
                    grad_probs = contract_cols(values, mine)
                    inner = jnp.sum(probs * grad_probs, axis=0, keepdims=True)
                    grad_scores = (probs * (grad_probs - inner)).astype(BF16)
                    grad_q += keep_head(contract_rows(grad_scores, keys), which, head_size)
                    grad_k += matmul(grad_scores, query)
                low_q = (grad_q * scale).astype(BF16)
                low_v = grad_v.astype(BF16)
                for k, low in enumerate((low_q, (grad_k * scale).astype(BF16), low_v)):
                    at = pl.multiple_of((k * size + r) * attn + start, 128)
                    gu_ref[:, pl.ds(at, lanes)] = low
                place = ((tensor_at + size - r) % size) * (attn // 128) + start // 128
                v_ref[0, pl.ds(v_query + place, 1), :] = jnp.sum(
                    low_q.astype(F32), axis=0, keepdims=True
                )
                v_ref[0, pl.ds(v_value + place, 1), :] = jnp.sum(
                    low_v.astype(F32), axis=0, keepdims=True
                )

        length = lengths_ref[tensor_at]
        for copy in qkv_load(0):
            copy.start()
        each(0, 1, attend_step)
        for j in range(tiles[O]):
            own_tile(O, low_t, context_ref[:, j * TILE : (j + 1) * TILE], j)
        send_corner(3)
        send_column(4)
        each(1, 2, attend_step)
        send_column(5)
        finish(7)
        each(2, 3, attend_step)
        send_sides(3)
        send_column(6)
        finish(8)
        each(3, size, attend_step)
        v_copy(0).start()

        def other_qkv(j):
            @pl.when(j + tiles[O] < tiles[U])
            def _():
                core_copy(U, j + tiles[O]).wait_send()

            other_tile(A, input_t, gu_ref[:, column(j)], j)

        def own_qkv(j):
            own_tile(A, input_t, gu_ref[:, column(j)], j)

        each(0, tiles[A], other_qkv)
        for g in range(3):
            each(*bounds(g), own_qkv)
            send_corner(g)
        send_column(3)
        v_add(0)
        v_copy(1).start()

        def input_step(j):
            grad_ref[...] += contract_cols(gu_ref[:, column(j)], w_buf[j % 2])

        over_tiles(0, tiles[A] // 2, [(1, a_in, w_buf)], input_step)
        send_sides(0)
        send_sides(1)
        over_tiles(tiles[A] // 2, tiles[A], [(1, a_in, w_buf)], input_step)
        send_sides(2)
        v_add(1)
        v_copy(2).start()
        for place, mask in enumerate(ORDER):
            at = block_of(data_at, mask)
            grad_out[:, pl.ds(pl.multiple_of(at * block, block), block)] = grad_ref[
                :, place * block : (place + 1) * block
            ].astype(BF16)
        send_column(0)
        for g in (4, 5, 6):
            finish(g)
        send_column(1)
        v_add(2)
        v_copy(3).start()
        send_column(2)
        v_add(3)
        v_copy(4).start()
        finish(3)
        finish(0)
        finish(1)
        v_add(4)
        sums_out[...] = v_ref[5]
        finish(2)
        for g in (A, O):
            for j in range(tiles[g]):
                core_copy(g, j).wait_send()
        for k in range(5):
            v_copy(k).wait_send()
        for copy in copies.values():
            copy.wait_send()

    spans = [piece[2] if g == X else size * piece[2] for g, piece in enumerate(pieces)]
    anywhere, inside = pl.BlockSpec(memory_space=pl.ANY), pl.BlockSpec(memory_space=pltpu.VMEM)
    results = pl.pallas_call(
        body,
        out_shape=[jax.ShapeDtypeStruct((block, attn), F32)] * 4
        + [jax.ShapeDtypeStruct((block, units_each), F32)] * 2
        + [
            jax.ShapeDtypeStruct((rows, width), BF16),
            jax.ShapeDtypeStruct((vector_rows, 128), F32),
        ],
        in_specs=[inside] * 5
        + [anywhere] * 2
        + [inside, pl.BlockSpec(memory_space=pltpu.SMEM)]
        + [anywhere] * 7
        + [inside],
        out_specs=[inside] * 8,
        scratch_shapes=[
            pltpu.VMEM((2, width, TILE), BF16),
            pltpu.VMEM((rows, units), BF16),
            pltpu.VMEM((2, rows, TILE), F32),
            pltpu.VMEM((rows, units), BF16),
            pltpu.VMEM((rows, width), F32),
            pltpu.VMEM((rows, width), BF16),
            pltpu.VMEM((width, rows), BF16),
            pltpu.VMEM((rows, full[1]), BF16),
            pltpu.VMEM((2, 3, rows, attn), BF16),
            pltpu.VMEM((middle, units), BF16),
            pltpu.VMEM((1, units), F32),
        ]
        + [pltpu.VMEM((middle, c), BF16) for c in full]
        + [pltpu.VMEM((2, half, c), BF16) for c in spans]
        + [pltpu.VMEM((2, block, c), BF16) for c in spans]
        + [
            pltpu.VMEM((size - 1, 4 * block if g == X else block, piece[2]), BF16)
            for g, piece in enumerate(pieces)
        ]
        + [
            pltpu.VMEM((6, vector_rows, 128), F32),
            pltpu.VMEM((5, vector_rows, 128), F32),
            pltpu.SemaphoreType.DMA((3, 2)),
            pltpu.SemaphoreType.DMA((3,)),
            pltpu.SemaphoreType.DMA((4, units // TILE)),
            pltpu.SemaphoreType.DMA((4, units // TILE)),
            pltpu.SemaphoreType.DMA((len(pieces), 3 + size)),
            pltpu.SemaphoreType.DMA((len(pieces), 3 + size)),
            pltpu.SemaphoreType.DMA((5,)),
            pltpu.SemaphoreType.DMA((5,)),
        ],
        compiler_params=pltpu.CompilerParams(
            collective_id=BACKWARD_ID, has_side_effects=True, vmem_limit_bytes=63 * 2**20
        ),
        cost_estimate=pl.CostEstimate(
            flops=4 * rows * sum(full) * width,
            bytes_accessed=4 * sum(full) * width,
            transcendentals=0,
        ),
        name="backward_near",
    )(
        mixed_low, mixed_t, normed_t, input_t, context, grad_second, hidden, wide, lengths, active,
        slope, qkv, *weights, vectors,
    )
    return results[:6], results[6], results[7]


def gather_far(shard):
    return lax.all_gather(
        lax.all_gather(shard, "tensor", axis=1, tiled=True), "dp", axis=0, tiled=True
    )


def scatter_far(left_side, right_side):
    whole = contract_rows(left_side, right_side).astype(BF16)
    part = lax.psum_scatter(whole, "dp", scatter_dimension=0, tiled=True)
    return lax.psum_scatter(part, "tensor", scatter_dimension=1, tiled=True).astype(F32)


def soft_weights(queries, keys, visible, scale):
    scores = contract_cols(queries, keys) * scale
    scores = jnp.where(visible, scores, MASKED)
    exponent = jnp.exp(scores - jnp.max(scores, axis=-1, keepdims=True))
    return exponent * (1.0 / jnp.sum(exponent, axis=-1, keepdims=True))


def pairs_of(width, head_size):
    lanes = max(128, head_size)
    return [(start, lanes, lanes // head_size) for start in range(0, width, lanes)]


def keep_head(array, which, head_size):
    lane = lax.broadcasted_iota(jnp.int32, array.shape, 1)
    return jnp.where(lane // head_size == which, array, jnp.zeros_like(array))


def attend_forward(qkv_q, qkv_kv, length, head_size, groups):
    q_rows = qkv_q.shape[0]
    k_rows = qkv_kv.shape[0]
    block = qkv_q.shape[1] // groups
    width = block // 3
    scale = float(head_size) ** (-0.5)

    def body(length_ref, q_ref, kv_ref, out_ref):
        visible = lax.broadcasted_iota(jnp.int32, (q_rows, k_rows), 1) < length_ref[0]
        for start, lanes, held in pairs_of(width, head_size):
            queries = q_ref[:, start : start + lanes]
            keys = kv_ref[:, width + start : width + start + lanes]
            values = kv_ref[:, 2 * width + start : 2 * width + start + lanes]
            total = jnp.zeros((q_rows, lanes), F32)
            for which in range(held):
                probs = soft_weights(keep_head(queries, which, head_size), keys, visible, scale)
                total += keep_head(matmul(probs.astype(BF16), values), which, head_size)
            out_ref[:, start : start + lanes] = total.astype(BF16)

    return pl.pallas_call(
        body,
        out_shape=jax.ShapeDtypeStruct((q_rows, groups * width), BF16),
        grid_spec=pltpu.PrefetchScalarGridSpec(
            num_scalar_prefetch=1,
            grid=(groups,),
            in_specs=[
                pl.BlockSpec((q_rows, block), lambda g, length_ref: (0, g)),
                pl.BlockSpec((k_rows, block), lambda g, length_ref: (0, g)),
            ],
            out_specs=pl.BlockSpec((q_rows, width), lambda g, length_ref: (0, g)),
        ),
        cost_estimate=pl.CostEstimate(
            flops=4 * q_rows * k_rows * width * groups,
            bytes_accessed=2 * (2 * q_rows + 2 * k_rows) * width * groups,
            transcendentals=q_rows * k_rows * groups * width // head_size,
        ),
        name="attend_forward",
    )(length, qkv_q, qkv_kv)


def attend_backward(qkv_q, qkv_kv, grad_context, length, head_size, groups):
    q_rows = qkv_q.shape[0]
    k_rows = qkv_kv.shape[0]
    block = qkv_q.shape[1] // groups
    width = block // 3
    scale = float(head_size) ** (-0.5)

    def body(length_ref, q_ref, kv_ref, grad_ref, dq_ref, dkv_ref):
        visible = lax.broadcasted_iota(jnp.int32, (q_rows, k_rows), 1) < length_ref[0]
        for start, lanes, held in pairs_of(width, head_size):
            queries = q_ref[:, start : start + lanes]
            keys = kv_ref[:, width + start : width + start + lanes]
            values = kv_ref[:, 2 * width + start : 2 * width + start + lanes]
            grads = grad_ref[:, start : start + lanes]
            grad_q = jnp.zeros((q_rows, lanes), F32)
            grad_k = jnp.zeros((k_rows, lanes), F32)
            grad_v = jnp.zeros((k_rows, lanes), F32)
            for which in range(held):
                mine = keep_head(grads, which, head_size)
                query = keep_head(queries, which, head_size)
                probs = soft_weights(query, keys, visible, scale)
                grad_v += contract_rows(probs.astype(BF16), mine)
                grad_probs = contract_cols(mine, values)
                inner = jnp.sum(probs * grad_probs, axis=-1, keepdims=True)
                grad_scores = (probs * (grad_probs - inner)).astype(BF16)
                grad_q += keep_head(matmul(grad_scores, keys), which, head_size)
                grad_k += contract_rows(grad_scores, query)
            dq_ref[:, start : start + lanes] = (grad_q * scale).astype(BF16)
            dkv_ref[:, start : start + lanes] = (grad_k * scale).astype(BF16)
            dkv_ref[:, width + start : width + start + lanes] = grad_v.astype(BF16)

    return pl.pallas_call(
        body,
        out_shape=(
            jax.ShapeDtypeStruct((q_rows, groups * width), BF16),
            jax.ShapeDtypeStruct((k_rows, groups * 2 * width), BF16),
        ),
        grid_spec=pltpu.PrefetchScalarGridSpec(
            num_scalar_prefetch=1,
            grid=(groups,),
            in_specs=[
                pl.BlockSpec((q_rows, block), lambda g, length_ref: (0, g)),
                pl.BlockSpec((k_rows, block), lambda g, length_ref: (0, g)),
                pl.BlockSpec((q_rows, width), lambda g, length_ref: (0, g)),
            ],
            out_specs=[
                pl.BlockSpec((q_rows, width), lambda g, length_ref: (0, g)),
                pl.BlockSpec((k_rows, 2 * width), lambda g, length_ref: (0, g)),
            ],
        ),
        cost_estimate=pl.CostEstimate(
            flops=10 * q_rows * k_rows * width * groups,
            bytes_accessed=2 * (3 * q_rows + 4 * k_rows) * width * groups,
            transcendentals=q_rows * k_rows * groups * width // head_size,
        ),
        name="attend_backward",
    )(length, qkv_q, qkv_kv, grad_context)


def activate(total, bias):
    upper = total + bias
    cumulative = 0.5 * (1.0 + lax.erf(upper * math.sqrt(0.5)))
    density = jnp.exp(-0.5 * upper * upper) * (1.0 / math.sqrt(2.0 * math.pi))
    return upper * cumulative, cumulative + upper * density


def norm_forward(hidden, gain_vec, shift_vec):
    center = hidden - jnp.mean(hidden, axis=-1, keepdims=True)
    variance = jnp.mean(center * center, axis=-1, keepdims=True)
    inv_root = lax.rsqrt(variance + EPSILON)
    normal = center * inv_root
    return (normal * gain_vec + shift_vec, normal, inv_root)


def norm_backward(grad_in, normal, inv_root, gain_vec):
    grad_normal = grad_in * gain_vec
    grad_gain = jnp.sum(grad_in * normal, axis=0)
    grad_shift = jnp.sum(grad_in, axis=0)
    grad_hidden = inv_root * (
        grad_normal
        - jnp.mean(grad_normal, axis=-1, keepdims=True)
        - normal * jnp.mean(grad_normal * normal, axis=-1, keepdims=True)
    )
    return (grad_hidden, grad_gain, grad_shift)


def layer(
    hidden_in,
    cotangent,
    w_query,
    w_key,
    w_value,
    w_out,
    w_up,
    w_down,
    bias_query,
    bias_value,
    bias_out,
    bias_up,
    bias_down,
    gain_attn,
    shift_attn,
    gain_ffn,
    shift_ffn,
    valid_lengths,
):
    rows, model_width = hidden_in.shape
    n_tensor = lax.axis_size("tensor")
    n_data = lax.axis_size("dp")
    tensor_at = lax.axis_index("tensor")
    spread_over = rows * n_tensor // valid_lengths.shape[0] // rows
    head_size = model_width // HEADS
    head_cols = w_query.shape[1]
    factor = 1.0 / math.sqrt(rows * n_tensor * n_data)
    matrices = (w_query, w_key, w_value, w_out, w_up, w_down)
    wide = (bias_out, bias_down, gain_attn, shift_attn, gain_ffn, shift_ffn)

    if n_data == len(ORDER) and spread_over == 1:
        (
            qkv_full, out_full, up_full, down_full, qkv, context, hidden, active, slope, output,
            mixed_low, mixed_t, normed_t, input_t, grad_second, given, arranged,
        ) = forward_near(
            matrices, hidden_in, cotangent, wide, bias_query, bias_value, bias_up, valid_lengths,
            head_size,
        )
        grads, grad_input, sums = backward_near(
            mixed_low, mixed_t, normed_t, input_t, context, grad_second, hidden, arranged,
            valid_lengths, active, slope, qkv, (qkv_full, out_full, up_full, down_full), given,
            head_size,
        )
        sums = sums.reshape(-1) * factor
    else:

        def column_part(vector):
            return vector.reshape(n_tensor, -1)

        query_bias, value_bias = column_part(bias_query), column_part(bias_value)
        bias_qkv = jnp.concatenate(
            [query_bias, jnp.zeros_like(query_bias), value_bias], axis=1
        ).reshape(1, -1)
        length = lax.dynamic_slice_in_dim(valid_lengths, tensor_at // spread_over, 1)
        low = [matrix.astype(BF16) for matrix in matrices]
        shards = [jnp.concatenate(low[:3], axis=1)] + low[3:]
        qkv_full, out_full, up_full, down_full = (gather_far(shard) for shard in shards)
        qkv = (matmul(hidden_in, qkv_full) + bias_qkv).astype(BF16)
        members = [list(range(k, k + spread_over)) for k in range(0, n_tensor, spread_over)]
        qkv_seq = lax.all_gather(qkv, "tensor", axis_index_groups=members, axis=0, tiled=True)
        context = attend_forward(qkv, qkv_seq, length, head_size, n_tensor)
        hidden = hidden_in.astype(F32) + contract_cols(context, out_full) + bias_out
        normed, normal_attn, root_attn = norm_forward(hidden, gain_attn, shift_attn)
        normed_low = normed.astype(BF16)
        active, slope = activate(matmul(normed_low, up_full), bias_up)
        active = active.astype(BF16)
        mixed = contract_cols(active, down_full)
        result, normal_ffn, root_ffn = norm_forward(normed + mixed + bias_down, gain_ffn, shift_ffn)
        output = result.astype(BF16)
        grad_second, grad_gain_ffn, grad_shift_ffn = norm_backward(
            cotangent.astype(F32), normal_ffn, root_ffn, gain_ffn
        )
        grad_bias_down = jnp.sum(grad_second, axis=0)
        mixed_low = grad_second.astype(BF16)
        grad_down = scatter_far(mixed_low, active)
        grad_upper = (matmul(mixed_low, down_full) * slope).astype(BF16)
        grad_bias_up = jnp.sum(grad_upper, axis=0, dtype=F32)
        grad_up = scatter_far(normed_low, grad_upper)
        grad_normed = grad_second + contract_cols(grad_upper, up_full)
        grad_first, grad_gain_attn, grad_shift_attn = norm_backward(
            grad_normed, normal_attn, root_attn, gain_attn
        )
        grad_bias_out = jnp.sum(grad_first, axis=0)
        attn_low = grad_first.astype(BF16)
        grad_context = matmul(attn_low, out_full).astype(BF16)
        grad_out = scatter_far(attn_low, context)
        grad_q, grad_kv = attend_backward(qkv, qkv_seq, grad_context, length, head_size, n_tensor)
        grad_kv = lax.psum_scatter(
            grad_kv.astype(F32),
            "tensor",
            scatter_dimension=0,
            axis_index_groups=members,
            tiled=True,
        ).astype(BF16)
        grad_qkv = jnp.concatenate(
            [grad_q.reshape(rows, n_tensor, -1), grad_kv.reshape(rows, n_tensor, -1)], axis=2
        ).reshape(rows, -1)
        grad_bias_qkv = jnp.sum(grad_qkv, axis=0, dtype=F32).reshape(n_tensor, 3, head_cols)
        grads = jnp.split(scatter_far(hidden_in, grad_qkv), 3, axis=1)
        grads += [grad_out, grad_up, grad_down]
        grad_input = (grad_first + contract_cols(grad_qkv, qkv_full)).astype(BF16)
        sums = jnp.concatenate(
            [
                grad_bias_out,
                grad_bias_down,
                grad_gain_attn,
                grad_shift_attn,
                grad_gain_ffn,
                grad_shift_ffn,
                grad_bias_qkv[:, 0].reshape(-1),
                grad_bias_qkv[:, 2].reshape(-1),
                grad_bias_up,
            ]
        )
        sums = lax.psum(sums, ("dp", "tensor")) * factor
    v_out, v_down, v_gain_attn, v_shift_attn, v_gain_ffn, v_shift_ffn, v_query, v_value = (
        sums[k * model_width : (k + 1) * model_width] for k in range(8)
    )
    v_up = sums[8 * model_width :]
    return (
        output,
        grad_input,
        *(grad * factor for grad in grads),
        v_query,
        v_value,
        v_out,
        v_up,
        v_down,
        v_gain_attn,
        v_shift_attn,
        v_gain_ffn,
        v_shift_ffn,
    )


def solution(mesh):
    tokens, matrix, copied = P(("dp", "tensor"), None), P("dp", "tensor"), P()
    return jax.shard_map(
        layer,
        mesh=mesh,
        in_specs=(tokens,) * 2 + (matrix,) * 6 + (copied,) * 9 + (P("dp"),),
        out_specs=(tokens,) * 2 + (matrix,) * 6 + (copied,) * 9,
        check_vma=False,
    )
```

```python
import math

import jax
import jax.numpy as jnp
from jax import lax
from jax.experimental import pallas as pl
from jax.experimental.pallas import tpu as pltpu
from jax.sharding import PartitionSpec as P

HEADS = 16
EPSILON = 1e-12
MASKED = -1e30
BF16 = jnp.bfloat16
F32 = jnp.float32

ORDER = (0, 2, 4, 6, 1, 3, 5, 7)
BIT_CORE, BIT_X, BIT_Y = 1, 2, 4


def matmul(left_side, right_side):
    return jnp.dot(left_side, right_side, preferred_element_type=F32)


def contract_rows(left_side, right_side):
    return lax.dot_general(
        left_side, right_side, (((0,), (0,)), ((), ())), preferred_element_type=F32
    )


def contract_cols(left_side, right_side):
    return lax.dot_general(
        left_side, right_side, (((1,), (1,)), ((), ())), preferred_element_type=F32
    )


FORWARD_ID = 1
BACKWARD_ID = 2
TILE = 512

FORWARD = (
    "lplane9", "z1", "z3", "lcor9", "col1", "z2", "z5", "z0", "z4", "col3", "col2", "prep",
    "col5", "col0", "cor2", "cor1", "z6", "cor0", "cor3", "z7", "last0", "z8", "col4", "col6",
    "last2", "tr", "last1", "cor5", "cor4", "qkv", "last3", "lz9", "a0", "cor6", "a1", "a2",
    "col7", "a3", "last4", "last5", "last6", "out", "col8", "norm", "up1", "cor7", "cor8",
    "lcore9", "up2", "up3", "last7", "lowX", "last8", "low1", "low2", "ln",
)
BACKWARD = (
    "oth8", "oth7", "gelA", "own8", "cor8", "own7", "cor7", "oth9", "oth4", "sid8", "gelB",
    "own9", "sid7", "oth5", "lz9", "oth6", "upA", "own4", "upB", "own5", "cor4", "cor5", "norm",
    "col8", "sid4", "own6", "out", "col7", "oth3", "a0", "own3", "cor3", "cor6", "a1", "col4",
    "sid5", "sid3", "a2", "a3", "oth1", "sid6", "vec", "oth2", "col5", "fin4", "own1", "cor1",
    "v0", "oth0", "col3", "v1", "own2", "cor2", "fin8", "sid1", "col6", "own0", "cor0", "fin7",
    "sid2", "v2", "col1", "dxA", "sid0", "col2", "lcor9", "dxB", "fin6", "col0", "v3", "sid9",
    "fin2", "v4", "gout", "fin5", "fin1", "fin3", "fin9", "v5", "fin0",
)


def neighbour(index, bit):
    return index + bit - 2 * bit * ((index // bit) % 2)


def block_of(index, mask):
    for bit in (BIT_CORE, BIT_X, BIT_Y):
        if mask & bit:
            index = neighbour(index, bit)
    return index


def pieces_of(size, attn, units_each):
    pieces = [(0, k * size * attn, attn) for k in range(3)] + [(1, 0, attn)]
    for weight in (2, 3):
        start = 0
        for count in (units_each // 2, units_each // 4, units_each // 4):
            pieces.append((weight, start * size, count))
            start += count
    return pieces


def run_events(order, table, attend, size):
    first = order.index("a0")
    last = order.index(f"a{size - 1}")
    for name in order[:first]:
        table[name]()

    def step(r, carry):
        attend(r)
        for k in range(size - 1):
            start = order.index(f"a{k}") + 1
            names = order[start : order.index(f"a{k + 1}")]
            if names:

                @pl.when(r == k)
                def _():
                    for name in names:
                        table[name]()

        return carry

    lax.fori_loop(0, size, step, 0)
    for name in order[last + 1 :]:
        table[name]()


def greet(partners):
    barrier = pltpu.get_barrier_semaphore()
    for partner in partners:
        pl.semaphore_signal(
            barrier, inc=1, device_id=partner, device_id_type=pl.DeviceIdType.MESH
        )
    pl.semaphore_wait(barrier, len(partners))


def forward_near(weights, hidden_in, cotangent, wide, bias_query, bias_value, bias_units, lengths, head_size):
    size = lax.axis_size("tensor")
    rows, width = hidden_in.shape
    block = width // len(ORDER)
    attn, units_each = weights[0].shape[1], weights[4].shape[1]
    cols = [3 * attn, attn, units_each, units_each]
    full = [(width, size * c) for c in cols]
    units = size * units_each
    half = block // 2
    pieces = pieces_of(size, attn, units_each)
    X = len(pieces) - 1
    A, O, U, _ = range(4)
    B_OUT, B_DOWN, G_ATTN, S_ATTN, G_FFN, S_FFN = range(6)

    def body(
        q_in, k_in, v_in, o_in, u_in, d_in, hidden_raw, cotangent_ref, bias_out_in, bias_down_in,
        gain_attn_in, shift_attn_in, gain_ffn_in, shift_ffn_in, bias_q_ref, bias_v_ref, bias_u_ref,
        lengths_ref,
        a_out, o_out, u_out, d_out, qkv_out, context_out, hidden_out, active_out, slope_out, output_ref,
        mixed_ref, mixed_t, normed_t, input_t, second_ref, sums_ref, wide_ref,
        a_ref, o_ref, u_ref, d_ref, x_ref, low_ref, active_ref, slope_ref, bias_ref, units_ref, qkv_ref,
        context_ref, hidden_ref, turned_x, turned_n, local_sem, send_sem, recv_sem,
        tile_sem,
    ):
        data_at, tensor_at = lax.axis_index("dp"), lax.axis_index("tensor")
        places = (a_ref, o_ref, u_ref, d_ref)

        def dp_partner(bit):
            return (neighbour(data_at, bit), tensor_at)

        def z_partner(step):
            return by_z[step]

        by_z = [(data_at, (tensor_at + step) % size) for step in range(size)]
        by_x, by_y, by_core = dp_partner(BIT_X), dp_partner(BIT_Y), dp_partner(BIT_CORE)
        owners = [block_of(data_at, mask) for mask in ORDER]
        copies = {}

        def send(g, slot, source, target, device):
            def copy():
                return pltpu.make_async_remote_copy(
                    src_ref=source,
                    dst_ref=target,
                    send_sem=send_sem.at[g, slot],
                    recv_sem=recv_sem.at[g, slot],
                    device_id=device,
                    device_id_type=pl.DeviceIdType.MESH,
                )

            copies[g, slot] = copy
            copy().start()

        def arrived(g, *slots):
            for slot in slots:
                copies[g, slot]().wait_recv()

        def whole(g, start, count):
            weight, first, wide_by = pieces[g]
            return places[weight].at[start : start + count, first : first + size * wide_by]

        def cell(g, start, count, r):
            weight, first, wide_by = pieces[g]
            at = first + r * wide_by
            return places[weight].at[start : start + count, at : at + wide_by]

        def send_z(g):
            for r in range(1, size):
                send(g, r - 1, cell(g, 0, block, 0), cell(g, 0, block, r), z_partner(r))

        def send_column(g):
            arrived(g, 0, 1, 2)
            send(g, 3, whole(g, 0, block), whole(g, block, block), by_x)
            send(g, 4, whole(g, 0, block), whole(g, 2 * block, block), by_y)

        def send_corner(g):
            arrived(g, 3, 4)
            send(g, 5, whole(g, block, half), whole(g, 3 * block, half), by_y)
            send(g, 6, whole(g, 2 * block + half, half), whole(g, 3 * block + half, half), by_x)
            send(g, 7, whole(g, 0, 3 * block), whole(g, 4 * block, 3 * block), by_core)

        def send_last(g):
            arrived(g, 5, 6)
            send(g, 8, whole(g, 3 * block, block), whole(g, 7 * block, block), by_core)

        def complete(*group):
            for g in group:
                arrived(g, 7, 8)

        def late_plane():
            send(X, 3, cell(X, 0, block, 0), cell(X, block, block, 0), by_x)
            send(X, 4, cell(X, 0, block, 0), cell(X, 2 * block, block, 0), by_y)

        def late_corner():
            arrived(X, 3, 4)
            send(X, 5, cell(X, block, half, 0), cell(X, 3 * block, half, 0), by_y)
            send(X, 6, cell(X, 2 * block + half, half, 0), cell(X, 3 * block + half, half, 0), by_x)

        def late_z():
            arrived(X, 5, 6)
            for r in range(1, size):
                send(X, r - 1, cell(X, 0, 4 * block, 0), cell(X, 0, 4 * block, r), z_partner(r))

        def late_core():
            arrived(X, 0, 1, 2)
            send(X, 7, whole(X, 0, 4 * block), whole(X, 4 * block, 4 * block), by_core)

        saves = []

        def save(slot, source, target):
            copy = pltpu.make_async_copy(source, target, local_sem.at[slot])
            copy.start()
            saves.append(copy)

        def save_weight(slot, g):
            target = (a_out, o_out, u_out, d_out)[g]
            save(slot, places[g], target)

        sources = (q_in, k_in, v_in, o_in, u_in, u_in, u_in, d_in, d_in, d_in)

        def cast(g):
            weight, first, wide_by = pieces[g]
            start = first // size if weight >= U else 0
            places[weight][:block, first : first + wide_by] = sources[g][
                :, start : start + wide_by
            ].astype(BF16)

        for g in range(len(pieces)):
            cast(g)
        greet([by_x, by_y, by_core] + by_z[1:])

        def lanes_of(owner):
            return pl.ds(pl.multiple_of(owner * block, block), block)

        def turn(target, at, rows_of):
            for k in range(width // 128):
                target[k * 128 : (k + 1) * 128, at] = rows_of[:, k * 128 : (k + 1) * 128].T.astype(BF16)

        def vector(k):
            return wide_ref[k : k + 1, :]

        def column_of(r, first, span):
            at = ((tensor_at + size - r) % size) * (first[1]) + first[0]
            return pl.ds(pl.multiple_of(at, 128), span)

        def prepare():
            for place, owner in enumerate(owners):
                at = slice(place * block, (place + 1) * block)
                x_ref[:, at] = hidden_raw[:, lanes_of(owner)]
                for k, ref in enumerate(
                    (bias_out_in, bias_down_in, gain_attn_in, shift_attn_in, gain_ffn_in, shift_ffn_in)
                ):
                    wide_ref[k : k + 1, at] = ref[:, lanes_of(owner)]
            for r in range(size):
                at = slice(r * attn, (r + 1) * attn)
                bias_ref[0:1, at] = bias_q_ref[:, column_of(r, (0, attn), attn)]
                bias_ref[1:2, at] = bias_v_ref[:, column_of(r, (0, attn), attn)]
                for weight, first, wide_by in pieces:
                    if weight == U:
                        at = slice(first + r * wide_by, first + (r + 1) * wide_by)
                        units_ref[:, at] = bias_u_ref[
                            :, column_of(r, (first // size, units_each), wide_by)
                        ]

        def turn_inputs():
            def one(j, carry):
                at = pl.ds(pl.multiple_of(j * 128, 128), 128)
                turn(turned_x, at, x_ref[at, :].astype(F32))
                return carry

            lax.fori_loop(0, rows // 128, one, 0)
            save(4, turned_x, input_t)

        def project(j, carry):
            at = pl.ds(pl.multiple_of(j * attn, attn), attn)
            total = matmul(x_ref[...], a_ref[:, at])
            which = j // size
            bias = bias_ref[:, pl.ds(pl.multiple_of((j % size) * attn, attn), attn)]
            bias = jnp.where(which == 0, bias[0:1], jnp.where(which == 2, bias[1:2], 0.0))
            qkv_ref[:, at] = (total + bias).astype(BF16)
            return carry

        def qkv():
            complete(0, 1, 2)
            save_weight(A, A)
            lax.fori_loop(0, 3 * size, project, 0)
            save(5, qkv_ref, qkv_out)

        scale = float(head_size) ** (-0.5)
        length = lengths_ref[tensor_at]

        def attend(r):
            seen = lax.broadcasted_iota(jnp.int32, (rows, rows), 1) < length
            for start, lanes, held in pairs_of(attn, head_size):
                at = [
                    pl.ds(pl.multiple_of((k * size + r) * attn + start, 128), lanes) for k in range(3)
                ]
                queries, keys, values = (qkv_ref[:, where] for where in at)
                total = jnp.zeros((rows, lanes), F32)
                for which in range(held):
                    probs = soft_weights(keep_head(queries, which, head_size), keys, seen, scale)
                    total += keep_head(matmul(probs.astype(BF16), values), which, head_size)
                context_ref[:, at[0]] = total.astype(BF16)

        def output(j, carry):
            at = pl.ds(pl.multiple_of(j * 256, 256), 256)
            total = contract_cols(context_ref[...], o_ref[at, :])
            hidden_ref[:, at] = x_ref[:, at].astype(F32) + total + wide_ref[B_OUT : B_OUT + 1, at]
            return carry

        def out():
            complete(3)
            save_weight(O, O)
            save(6, context_ref, context_out)
            lax.fori_loop(0, width // 256, output, 0)
            save(7, hidden_ref, hidden_out)

        chunk = 128

        def norm_step(j, carry):
            at = pl.ds(pl.multiple_of(j * chunk, chunk), chunk)
            normed = norm_forward(hidden_ref[at, :], vector(G_ATTN), vector(S_ATTN))[0]
            low_ref[at, :] = normed.astype(BF16)
            second_ref[at, :] = normed + vector(B_DOWN)
            turn(turned_n, at, normed)
            return carry

        def norm():
            lax.fori_loop(0, rows // chunk, norm_step, 0)
            save(8, turned_n, normed_t)

        def tile_at(j):
            return pl.ds(pl.multiple_of(j * TILE, TILE), TILE)

        def slope_copy(j):
            return pltpu.make_async_copy(
                slope_ref.at[j % 2], slope_out.at[:, tile_at(j)], tile_sem.at[1, j % 2]
            )

        def active_copy(j):
            return pltpu.make_async_copy(
                active_ref.at[:, tile_at(j)], active_out.at[:, tile_at(j)], tile_sem.at[0, j]
            )

        def raise_up(j, carry):
            @pl.when(j >= 2)
            def _():
                slope_copy(j - 2).wait()

            total = matmul(low_ref[...], u_ref[:, tile_at(j)])
            active, slope = activate(total, units_ref[:, tile_at(j)])
            active_ref[:, tile_at(j)] = active.astype(BF16)
            slope_ref[j % 2] = slope
            active_copy(j).start()
            slope_copy(j).start()
            return carry

        def span_of(g):
            _, first, wide_by = pieces[g]
            return slice(first, first + size * wide_by)

        def raise_piece(g):
            complete(g)
            save(g + 5, u_ref.at[:, span_of(g)], u_out.at[:, span_of(g)])
            at = span_of(g)
            lax.fori_loop(at.start // TILE, at.stop // TILE, raise_up, 0)

        def lower_piece(g):
            if g == X:
                arrived(X, 7)
            else:
                complete(g)
            at = span_of(g)
            save(g + 5, d_ref.at[:, at], d_out.at[:, at])

            def one(j, carry):
                to = pl.ds(pl.multiple_of(j * 256, 256), 256)
                second_ref[:, to] += contract_cols(active_ref[:, at], d_ref[to, at])
                return carry

            lax.fori_loop(0, width // 256, one, 0)

        def second(j, sums):
            at = pl.ds(pl.multiple_of(j * chunk, chunk), chunk)
            result, normal, root = norm_forward(second_ref[at, :], vector(G_FFN), vector(S_FFN))
            grads = jnp.concatenate([cotangent_ref[at, lanes_of(owner)] for owner in owners], axis=1)
            for place, owner in enumerate(owners):
                output_ref[at, lanes_of(owner)] = result[:, place * block : (place + 1) * block].astype(BF16)
            hidden, more_gain, more_shift = norm_backward(
                grads.astype(F32), normal, root, vector(G_FFN)
            )
            second_ref[at, :] = hidden
            mixed_ref[at, :] = hidden.astype(BF16)
            turn(mixed_t, at, hidden)
            more = (jnp.sum(hidden, axis=0), more_gain, more_shift)
            return tuple(a + b[None] for a, b in zip(sums, more))

        def last_norm():
            zero = jnp.zeros((1, width), F32)
            sums = lax.fori_loop(0, rows // chunk, second, (zero, zero, zero))
            for k in range(3):
                sums_ref[k : k + 1, :] = sums[k]

        def bound(step, *given):
            return lambda: step(*given)

        table = {
            "prep": prepare, "tr": turn_inputs, "qkv": qkv, "out": out, "norm": norm, "ln": last_norm,
            "up1": bound(raise_piece, 4), "up2": bound(raise_piece, 5), "up3": bound(raise_piece, 6),
            "low1": bound(lower_piece, 7), "low2": bound(lower_piece, 8), "lowX": bound(lower_piece, X),
            "lplane9": late_plane, "lcor9": late_corner, "lz9": late_z, "lcore9": late_core,
        }
        for g in range(X):
            table[f"z{g}"] = bound(send_z, g)
            table[f"col{g}"] = bound(send_column, g)
            table[f"cor{g}"] = bound(send_corner, g)
            table[f"last{g}"] = bound(send_last, g)
        run_events(FORWARD, table, attend, size)

        def settle(j, carry):
            active_copy(j).wait()
            return carry

        lax.fori_loop(0, units // TILE, settle, 0)
        for j in (units // TILE - 2, units // TILE - 1):
            slope_copy(j).wait()
        for copy in saves:
            copy.wait()
        for copy in copies.values():
            copy().wait_send()

    anywhere, inside = pl.BlockSpec(memory_space=pl.ANY), pl.BlockSpec(memory_space=pltpu.VMEM)
    tall = jax.ShapeDtypeStruct((rows, width), BF16)
    turned = jax.ShapeDtypeStruct((width, rows), BF16)
    return pl.pallas_call(
        body,
        out_shape=[jax.ShapeDtypeStruct(shape, BF16) for shape in full]
        + [
            jax.ShapeDtypeStruct((rows, full[A][1]), BF16),
            tall,
            jax.ShapeDtypeStruct((rows, width), F32),
            jax.ShapeDtypeStruct((rows, units), BF16),
            jax.ShapeDtypeStruct((rows, units), F32),
            tall,
            tall,
            turned,
            turned,
            turned,
            jax.ShapeDtypeStruct((rows, width), F32),
            jax.ShapeDtypeStruct((3, width), F32),
            jax.ShapeDtypeStruct((6, width), F32),
        ],
        in_specs=[inside] * 17 + [pl.BlockSpec(memory_space=pltpu.SMEM)],
        out_specs=[anywhere] * 9 + [inside] * 3 + [anywhere] * 2 + [inside] * 3,
        scratch_shapes=[pltpu.VMEM(shape, BF16) for shape in full]
        + [
            pltpu.VMEM((rows, width), BF16),
            pltpu.VMEM((rows, width), BF16),
            pltpu.VMEM((rows, units), BF16),
            pltpu.VMEM((2, rows, TILE), F32),
            pltpu.VMEM((2, size * attn), F32),
            pltpu.VMEM((1, units), F32),
            pltpu.VMEM((rows, full[A][1]), BF16),
            pltpu.VMEM((rows, width), BF16),
            pltpu.VMEM((rows, width), F32),
            pltpu.VMEM((width, rows), BF16),
            pltpu.VMEM((width, rows), BF16),
            pltpu.SemaphoreType.DMA((5 + len(pieces),)),
            pltpu.SemaphoreType.DMA((len(pieces), 9)),
            pltpu.SemaphoreType.DMA((len(pieces), 9)),
            pltpu.SemaphoreType.DMA((2, units // TILE)),
        ],
        compiler_params=pltpu.CompilerParams(
            collective_id=FORWARD_ID, has_side_effects=True, vmem_limit_bytes=63 * 2**20
        ),
        cost_estimate=pl.CostEstimate(
            flops=2 * rows * width * sum(shape[1] for shape in full),
            bytes_accessed=4 * width * sum(shape[1] for shape in full),
            transcendentals=rows * units,
        ),
        name="forward_near",
    )(
        *weights, hidden_in, cotangent, *(vector[None] for vector in wide), bias_query[None],
        bias_value[None], bias_units[None], lengths,
    )


def backward_near(mixed_low, mixed_t, normed_t, input_t, context, grad_second, hidden, wide, lengths,
                  active, slope, qkv, weights, vectors, head_size):
    size = lax.axis_size("tensor")
    rows, width = mixed_low.shape
    block = width // len(ORDER)
    middle = width // 2
    half = block // 2
    full = [weight.shape[1] for weight in weights]
    units = full[2]
    units_each = units // size
    attn = full[1] // size
    pieces = pieces_of(size, attn, units_each)
    X = len(pieces) - 1
    A, O, U, D = range(4)
    tiles = [c // TILE for c in full]
    vector_rows = (6 * width + 2 * full[1] + units) // 128
    v_query, v_value, v_up = 6 * width // 128, (6 * width + full[1]) // 128, (6 * width + 2 * full[1]) // 128
    scale = float(head_size) ** (-0.5)

    def body(
        mixed_in, mixed_t, normed_in, input_in, context_in, second_in, hidden_in, wide_ref,
        lengths_ref, active_in, slope_in, qkv_in, a_in, o_in, u_in, d_in, vectors_ref,
        q_out, k_out, v_out, o_out, u_out, d_out, grad_out, sums_out,
        w_buf, act_ref, slope_buf, gu_ref, grad_ref, low_ref, low_t, gctx_ref, qkv_buf, send_buf,
        units_sum, mixed_ref, normed_t, input_t, context_ref, a_plane, o_plane, u_plane, d_plane, *rest,
    ):
        count = len(pieces)
        corners, sides, zins = (rest[k * count : (k + 1) * count] for k in range(3))
        (
            v_ref, v_in, load_sem, start_sem, core_send, core_recv, send_sem, recv_sem, v_send, v_recv,
        ) = rest[3 * count :]
        data_at, tensor_at = lax.axis_index("dp"), lax.axis_index("tensor")
        planes = (a_plane, o_plane, u_plane, d_plane)
        outs = (q_out, k_out, v_out, o_out, u_out, u_out, u_out, d_out, d_out, d_out)
        shift_by = (tiles[O], 0, 0, 0)

        def dp_partner(bit):
            return (neighbour(data_at, bit), tensor_at)

        def z_partner(step):
            return by_z[step % size]

        by_z = [(data_at, (tensor_at + step) % size) for step in range(size)]

        by_x, by_y, by_core = dp_partner(BIT_X), dp_partner(BIT_Y), dp_partner(BIT_CORE)

        def column(j, span=TILE):
            return pl.ds(pl.multiple_of(j * span, 128), span)

        def load(row, source, buffer, j):
            return pltpu.make_async_copy(
                source.at[:, column(j)], buffer.at[j % 2], load_sem.at[row, j % 2]
            )

        def over_tiles(first, last, loads, step):
            for row, source, buffer in loads:
                load(row, source, buffer, first).start()

            def one(j, carry):
                @pl.when(j + 1 < last)
                def _():
                    for row, source, buffer in loads:
                        load(row, source, buffer, j + 1).start()

                for row, source, buffer in loads:
                    load(row, source, buffer, j).wait()
                step(j)
                return carry

            lax.fori_loop(first, last, one, 0)

        def remote(source, target, send, receive, device):
            return pltpu.make_async_remote_copy(
                src_ref=source,
                dst_ref=target,
                send_sem=send,
                recv_sem=receive,
                device_id=device,
                device_id_type=pl.DeviceIdType.MESH,
            )

        def core_copy(g, j):
            return remote(
                send_buf.at[:, column(j + shift_by[g])],
                planes[g].at[:, column(j)],
                core_send.at[g, j],
                core_recv.at[g, j],
                by_core,
            )

        copies = {}

        def send(g, slot, source, target, device):
            def copy():
                return remote(source, target(), send_sem.at[g, slot], recv_sem.at[g, slot], device)

            copies[g, slot] = copy
            copy().start()

        def arrived(g, *slots):
            for slot in slots:
                copies[g, slot]().wait_recv()

        def other_tile(g, left_t, right, j):
            send_buf[:, column(j + shift_by[g])] = matmul(left_t[middle:, :], right).astype(BF16)
            core_copy(g, j).start()

        def own_tile(g, left_t, right, j):
            core_copy(g, j).wait_recv()
            total = matmul(left_t[:middle, :], right) + planes[g][:, column(j)].astype(F32)
            planes[g][:, column(j)] = total.astype(BF16)

        def span(g):
            _, first, wide_by = pieces[g]
            return first, wide_by if g == X else size * wide_by

        def plane_rows(g, start, count):
            first, wide_by = span(g)
            return planes[pieces[g][0]].at[start : start + count, first : first + wide_by]

        def send_corner(g):
            send(g, 0, plane_rows(g, 3 * block, half), lambda: corners[g].at[0], by_x)
            send(g, 1, plane_rows(g, 3 * block + half, half), lambda: corners[g].at[1], by_y)

        def add_rows(g, start, count, *more):
            plane = planes[pieces[g][0]]
            first, wide_by = span(g)
            step = min(TILE, wide_by)
            for at in range(0, wide_by, step):
                where = (slice(start, start + count), slice(first + at, first + at + step))
                total = plane[where].astype(F32)
                for ref in more:
                    total += ref[:, at : at + step].astype(F32)
                plane[where] = total.astype(BF16)

        def send_sides(g):
            arrived(g, 0, 1)
            add_rows(g, 2 * block, half, corners[g].at[0])
            add_rows(g, block + half, half, corners[g].at[1])
            send(g, 2, plane_rows(g, block, block), lambda: sides[g].at[0], by_x)
            send(g, 3, plane_rows(g, 2 * block, block), lambda: sides[g].at[1], by_y)

        def out_of(g):
            weight, first, wide_by = pieces[g]
            start = first // size if weight >= U else 0
            return outs[g].at[:, start : start + wide_by]

        def send_column(g):
            arrived(g, 2, 3)
            weight, first, wide_by = pieces[g]
            for r in range(size):
                at = slice(r * wide_by, (r + 1) * wide_by)
                own = slice(first + r * wide_by, first + (r + 1) * wide_by)
                total = planes[weight][:block, own].astype(F32)
                total += sides[g][0, :, at].astype(F32) + sides[g][1, :, at].astype(F32)
                if r == 0:
                    out_of(g)[...] = total
                else:
                    planes[weight][:block, own] = total.astype(BF16)
                    send(g, 3 + r, planes[weight].at[:block, own], lambda r=r: zins[g].at[r - 1], z_partner(-r))

        def finish(g):
            arrived(g, *range(4, 3 + size))
            total = out_of(g)[...]
            for r in range(1, size):
                total += zins[g][r - 1].astype(F32)
            out_of(g)[...] = total

        def late_z():
            weight, first, wide_by = pieces[X]
            for r in range(1, size):
                own = slice(first + r * wide_by, first + (r + 1) * wide_by)
                send(X, 3 + r, planes[weight].at[:, own], lambda r=r: zins[X].at[r - 1], z_partner(-r))

        def late_corner():
            arrived(X, *range(4, 3 + size))
            for k in range(4):
                rows_k = slice(k * block, (k + 1) * block)
                add_rows(X, k * block, block, *(zins[X].at[r, rows_k] for r in range(size - 1)))
            send_corner(X)

        def late_finish():
            arrived(X, 2, 3)
            total = plane_rows(X, 0, block)[...].astype(F32)
            out_of(X)[...] = total + sides[X][0].astype(F32) + sides[X][1].astype(F32)

        def feature_rows(k, vector):
            for place, mask in enumerate(ORDER):
                at = block_of(data_at, mask)
                v_ref[0, pl.ds(k * len(ORDER) + at, 1), :] = vector[:, place * 128 : (place + 1) * 128]

        z_near = tensor_at + 1 - 2 * (tensor_at % 2)
        z_across = tensor_at + 2 - 4 * ((tensor_at // 2) % 2)
        v_partners = (by_core, (data_at, z_near), (data_at, z_across), by_x, by_y)

        def v_copy(k):
            return remote(v_ref.at[k], v_in.at[k], v_send.at[k], v_recv.at[k], v_partners[k])

        def v_add(k):
            v_copy(k).wait_recv()
            v_ref[k + 1] = v_ref[k] + v_in[k]

        early = [
            pltpu.make_async_copy(
                active_in.at[:, k * (units // 2) : (k + 1) * (units // 2)],
                act_ref.at[:, k * (units // 2) : (k + 1) * (units // 2)],
                start_sem.at[k],
            )
            for k in range(2)
        ]
        grad_load, mixed_load, normed_load, context_load, input_load = (
            pltpu.make_async_copy(source, target, start_sem.at[k])
            for k, (source, target) in enumerate(
                (
                    (second_in, grad_ref),
                    (mixed_in, mixed_ref),
                    (normed_in, normed_t),
                    (context_in, context_ref),
                    (input_in, input_t),
                ),
                2,
            )
        )
        for copy in early:
            copy.start()
        for copy in (mixed_load, normed_load, grad_load, context_load, input_load):
            copy.start()
        greet([by_x, by_y, by_core] + by_z[1:])

        def each(first, last, step):
            def one(j, carry):
                step(j)
                return carry

            lax.fori_loop(first, last, one, 0)

        def other_down(j):
            other_tile(D, mixed_t, act_ref[:, column(j)], j)

        def own_down(j):
            own_tile(D, mixed_t, act_ref[:, column(j)], j)

        def other_up(j):
            core_copy(D, j).wait_send()
            other_tile(U, normed_t, gu_ref[:, column(j)], j)

        def own_up(j):
            own_tile(U, normed_t, gu_ref[:, column(j)], j)

        def bounds(g):
            _, first, wide_by = pieces[g]
            return first // TILE, (first + size * wide_by) // TILE

        early[0].wait()
        early[1].wait()

        def loaded(copy, step):
            def both():
                copy.wait()
                step()

            return both

        def bound(step, *given):
            return lambda: step(*given)

        def gelu_step(j):
            low = (matmul(mixed_ref[...], w_buf[j % 2]) * slope_buf[j % 2]).astype(BF16)
            gu_ref[:, column(j)] = low
            units_sum[:, column(j)] = jnp.sum(low.astype(F32), axis=0, keepdims=True)

        gelu_loads = [(1, d_in, w_buf), (2, slope_in, slope_buf)]
        hidden_loads = [
            pltpu.make_async_copy(hidden_in.at[:, column(k)], slope_buf.at[k], load_sem.at[2, k])
            for k in range(2)
        ]

        def second_gelu():
            over_tiles(tiles[D] // 2, tiles[D], gelu_loads, gelu_step)
            for copy in hidden_loads:
                copy.start()

        def up_step(j):
            grad_ref[...] += contract_cols(gu_ref[:, column(j)], w_buf[j % 2])

        def sum_units():
            for k in range(3):
                feature_rows((1, 4, 5)[k], vectors_ref[k : k + 1, :])
            for r in range(size):
                for weight, first, wide_by in pieces:
                    if weight == U:
                        for k in range(wide_by // 128):
                            place = ((tensor_at + size - r) % size) * (units_each // 128)
                            place += (first // size) // 128 + k
                            at = first + r * wide_by + k * 128
                            v_ref[0, pl.ds(v_up + place, 1), :] = units_sum[:, at : at + 128]

        chunk = 128

        def norm_step(j, sums):
            at = pl.ds(pl.multiple_of(j * chunk, chunk), chunk)
            hidden_rows = jnp.concatenate([slope_buf[0, at, :], slope_buf[1, at, :]], axis=1)
            gain = wide_ref[2:3, :]
            normal, root = norm_forward(hidden_rows, gain, gain)[1:]
            hidden, more_gain, more_shift = norm_backward(grad_ref[at, :], normal, root, gain)
            grad_ref[at, :] = hidden
            low_ref[at, :] = hidden.astype(BF16)
            for k in range(width // 128):
                low_t[k * 128 : (k + 1) * 128, at] = hidden[:, k * 128 : (k + 1) * 128].T.astype(BF16)
            more = (jnp.sum(hidden, axis=0), more_gain, more_shift)
            return tuple(a + b[None] for a, b in zip(sums, more))

        def norm():
            for copy in hidden_loads:
                copy.wait()
            zero = jnp.zeros((1, width), F32)
            sums = lax.fori_loop(0, rows // chunk, norm_step, (zero, zero, zero))
            for k in range(3):
                feature_rows((0, 2, 3)[k], sums[k])

        def out_step(j):
            core_copy(U, j).wait_send()
            gctx_ref[:, column(j)] = matmul(low_ref[...], w_buf[j % 2]).astype(BF16)
            other_tile(O, low_t, context_ref[:, column(j)], j)

        def out():
            context_load.wait()
            over_tiles(0, tiles[O], [(1, o_in, w_buf)], out_step)
            for copy in qkv_load(0):
                copy.start()

        def own_out():
            for j in range(tiles[O]):
                own_tile(O, low_t, context_ref[:, j * TILE : (j + 1) * TILE], j)

        def qkv_load(r):
            return [
                pltpu.make_async_copy(
                    qkv_in.at[:, column(k * size + r, attn)], qkv_buf.at[r % 2, k], load_sem.at[k, r % 2]
                )
                for k in range(3)
            ]

        def attend_step(r):
            @pl.when(r + 1 < size)
            def _():
                for copy in qkv_load(r + 1):
                    copy.start()

            for copy in qkv_load(r):
                copy.wait()
            slot = r % 2
            seen = lax.broadcasted_iota(jnp.int32, (rows, rows), 0) < length
            for start, lanes, held in pairs_of(attn, head_size):
                queries, keys, values = (qkv_buf[slot, k, :, start : start + lanes] for k in range(3))
                grads = gctx_ref[:, pl.ds(pl.multiple_of(r * attn + start, 128), lanes)]
                grad_q = jnp.zeros((rows, lanes), F32)
                grad_k = jnp.zeros((rows, lanes), F32)
                grad_v = jnp.zeros((rows, lanes), F32)
                for which in range(held):
                    mine = keep_head(grads, which, head_size)
                    query = keep_head(queries, which, head_size)
                    scores = jnp.where(seen, contract_cols(keys, query) * scale, MASKED)
                    exponent = jnp.exp(scores - jnp.max(scores, axis=0, keepdims=True))
                    probs = exponent * (1.0 / jnp.sum(exponent, axis=0, keepdims=True))
                    grad_v += matmul(probs.astype(BF16), mine)
                    grad_probs = contract_cols(values, mine)
                    inner = jnp.sum(probs * grad_probs, axis=0, keepdims=True)
                    grad_scores = (probs * (grad_probs - inner)).astype(BF16)
                    grad_q += keep_head(contract_rows(grad_scores, keys), which, head_size)
                    grad_k += matmul(grad_scores, query)
                low_q = (grad_q * scale).astype(BF16)
                low_v = grad_v.astype(BF16)
                for k, low in enumerate((low_q, (grad_k * scale).astype(BF16), low_v)):
                    at = pl.multiple_of((k * size + r) * attn + start, 128)
                    gu_ref[:, pl.ds(at, lanes)] = low
                place = ((tensor_at + size - r) % size) * (attn // 128) + start // 128
                v_ref[0, pl.ds(v_query + place, 1), :] = jnp.sum(
                    low_q.astype(F32), axis=0, keepdims=True
                )
                v_ref[0, pl.ds(v_value + place, 1), :] = jnp.sum(
                    low_v.astype(F32), axis=0, keepdims=True
                )

        length = lengths_ref[tensor_at]

        def other_qkv(j):
            core_copy(U, j + tiles[O]).wait_send()
            other_tile(A, input_t, gu_ref[:, column(j)], j)

        def own_qkv(j):
            own_tile(A, input_t, gu_ref[:, column(j)], j)

        def input_step(j):
            grad_ref[...] += contract_cols(gu_ref[:, column(j)], w_buf[j % 2])

        def give_input():
            for place, mask in enumerate(ORDER):
                at = block_of(data_at, mask)
                grad_out[:, pl.ds(pl.multiple_of(at * block, block), block)] = grad_ref[
                    :, place * block : (place + 1) * block
                ].astype(BF16)

        def give_sums():
            v_add(4)
            sums_out[...] = v_ref[5]

        def next_sum(k):
            v_add(k - 1)
            v_copy(k).start()

        weight_loads = [[(1, ref, w_buf)] for ref in (a_in, o_in, u_in, d_in)]
        parts = (
            (other_qkv, own_qkv), (other_qkv, own_qkv), (other_qkv, own_qkv), (lambda j: None, own_out),
            (other_up, own_up), (other_up, own_up), (other_up, own_up), (other_down, own_down),
            (other_down, own_down), (other_down, own_down),
        )
        halves = [(0, count // 2, count) for count in tiles]
        table = {
            "gelA": loaded(mixed_load, bound(over_tiles, 0, halves[D][1], gelu_loads, gelu_step)),
            "gelB": second_gelu,
            "upA": loaded(grad_load, bound(over_tiles, 0, halves[U][1], weight_loads[U], up_step)),
            "upB": bound(over_tiles, *halves[U][1:], weight_loads[U], up_step),
            "vec": sum_units,
            "norm": norm,
            "out": out,
            "dxA": bound(over_tiles, 0, halves[A][1], weight_loads[A], input_step),
            "dxB": bound(over_tiles, *halves[A][1:], weight_loads[A], input_step),
            "gout": give_input,
            "lz9": late_z,
            "lcor9": late_corner,
            "sid9": bound(send_sides, X),
            "fin9": late_finish,
            "v0": lambda: v_copy(0).start(),
            "v5": give_sums,
        }
        for k in range(1, 5):
            table[f"v{k}"] = bound(next_sum, k)
        for g in range(len(pieces)):
            other, own = parts[g]
            table[f"oth{g}"] = bound(each, *bounds(g), other)
            table[f"own{g}"] = bound(each, *bounds(g), own)
            if g < X:
                table[f"cor{g}"] = bound(send_corner, g)
                table[f"sid{g}"] = bound(send_sides, g)
                table[f"col{g}"] = bound(send_column, g)
                table[f"fin{g}"] = bound(finish, g)
        table["oth3"] = lambda: None
        table["own3"] = own_out
        first_up = [g for g in range(len(pieces)) if f"oth{g}" in BACKWARD and pieces[g][0] == U]
        first_up = min(first_up, key=lambda g: BACKWARD.index(f"oth{g}"))
        table[f"oth{first_up}"] = loaded(normed_load, table[f"oth{first_up}"])
        first_in = min((0, 1, 2), key=lambda g: BACKWARD.index(f"oth{g}"))
        table[f"oth{first_in}"] = loaded(input_load, table[f"oth{first_in}"])
        run_events(BACKWARD, table, attend_step, size)
        for g in (A, O):
            for j in range(tiles[g]):
                core_copy(g, j).wait_send()
        for k in range(5):
            v_copy(k).wait_send()
        for copy in copies.values():
            copy().wait_send()

    spans = [piece[2] if g == X else size * piece[2] for g, piece in enumerate(pieces)]
    anywhere, inside = pl.BlockSpec(memory_space=pl.ANY), pl.BlockSpec(memory_space=pltpu.VMEM)
    results = pl.pallas_call(
        body,
        out_shape=[jax.ShapeDtypeStruct((block, attn), F32)] * 4
        + [jax.ShapeDtypeStruct((block, units_each), F32)] * 2
        + [
            jax.ShapeDtypeStruct((rows, width), BF16),
            jax.ShapeDtypeStruct((vector_rows, 128), F32),
        ],
        in_specs=[anywhere, inside]
        + [anywhere] * 5
        + [inside, pl.BlockSpec(memory_space=pltpu.SMEM)]
        + [anywhere] * 7
        + [inside],
        out_specs=[inside] * 8,
        scratch_shapes=[
            pltpu.VMEM((2, width, TILE), BF16),
            pltpu.VMEM((rows, units), BF16),
            pltpu.VMEM((2, rows, TILE), F32),
            pltpu.VMEM((rows, units), BF16),
            pltpu.VMEM((rows, width), F32),
            pltpu.VMEM((rows, width), BF16),
            pltpu.VMEM((width, rows), BF16),
            pltpu.VMEM((rows, full[1]), BF16),
            pltpu.VMEM((2, 3, rows, attn), BF16),
            pltpu.VMEM((middle, units), BF16),
            pltpu.VMEM((1, units), F32),
            pltpu.VMEM((rows, width), BF16),
            pltpu.VMEM((width, rows), BF16),
            pltpu.VMEM((width, rows), BF16),
            pltpu.VMEM((rows, width), BF16),
        ]
        + [pltpu.VMEM((middle, c), BF16) for c in full]
        + [pltpu.VMEM((2, half, c), BF16) for c in spans]
        + [pltpu.VMEM((2, block, c), BF16) for c in spans]
        + [
            pltpu.VMEM((size - 1, 4 * block if g == X else block, piece[2]), BF16)
            for g, piece in enumerate(pieces)
        ]
        + [
            pltpu.VMEM((6, vector_rows, 128), F32),
            pltpu.VMEM((5, vector_rows, 128), F32),
            pltpu.SemaphoreType.DMA((3, 2)),
            pltpu.SemaphoreType.DMA((7,)),
            pltpu.SemaphoreType.DMA((4, units // TILE)),
            pltpu.SemaphoreType.DMA((4, units // TILE)),
            pltpu.SemaphoreType.DMA((len(pieces), 3 + size)),
            pltpu.SemaphoreType.DMA((len(pieces), 3 + size)),
            pltpu.SemaphoreType.DMA((5,)),
            pltpu.SemaphoreType.DMA((5,)),
        ],
        compiler_params=pltpu.CompilerParams(
            collective_id=BACKWARD_ID, has_side_effects=True, vmem_limit_bytes=63 * 2**20
        ),
        cost_estimate=pl.CostEstimate(
            flops=4 * rows * sum(full) * width,
            bytes_accessed=4 * sum(full) * width,
            transcendentals=0,
        ),
        name="backward_near",
    )(
        mixed_low, mixed_t, normed_t, input_t, context, grad_second, hidden, wide, lengths, active,
        slope, qkv, *weights, vectors,
    )
    return results[:6], results[6], results[7]


def gather_far(shard):
    return lax.all_gather(
        lax.all_gather(shard, "tensor", axis=1, tiled=True), "dp", axis=0, tiled=True
    )


def scatter_far(left_side, right_side):
    whole = contract_rows(left_side, right_side).astype(BF16)
    part = lax.psum_scatter(whole, "dp", scatter_dimension=0, tiled=True)
    return lax.psum_scatter(part, "tensor", scatter_dimension=1, tiled=True).astype(F32)


def soft_weights(queries, keys, visible, scale):
    scores = contract_cols(queries, keys) * scale
    scores = jnp.where(visible, scores, MASKED)
    exponent = jnp.exp(scores - jnp.max(scores, axis=-1, keepdims=True))
    return exponent * (1.0 / jnp.sum(exponent, axis=-1, keepdims=True))


def pairs_of(width, head_size):
    lanes = max(128, head_size)
    return [(start, lanes, lanes // head_size) for start in range(0, width, lanes)]


def keep_head(array, which, head_size):
    lane = lax.broadcasted_iota(jnp.int32, array.shape, 1)
    return jnp.where(lane // head_size == which, array, jnp.zeros_like(array))


def attend_forward(qkv_q, qkv_kv, length, head_size, groups):
    q_rows = qkv_q.shape[0]
    k_rows = qkv_kv.shape[0]
    block = qkv_q.shape[1] // groups
    width = block // 3
    scale = float(head_size) ** (-0.5)

    def body(length_ref, q_ref, kv_ref, out_ref):
        visible = lax.broadcasted_iota(jnp.int32, (q_rows, k_rows), 1) < length_ref[0]
        for start, lanes, held in pairs_of(width, head_size):
            queries = q_ref[:, start : start + lanes]
            keys = kv_ref[:, width + start : width + start + lanes]
            values = kv_ref[:, 2 * width + start : 2 * width + start + lanes]
            total = jnp.zeros((q_rows, lanes), F32)
            for which in range(held):
                probs = soft_weights(keep_head(queries, which, head_size), keys, visible, scale)
                total += keep_head(matmul(probs.astype(BF16), values), which, head_size)
            out_ref[:, start : start + lanes] = total.astype(BF16)

    return pl.pallas_call(
        body,
        out_shape=jax.ShapeDtypeStruct((q_rows, groups * width), BF16),
        grid_spec=pltpu.PrefetchScalarGridSpec(
            num_scalar_prefetch=1,
            grid=(groups,),
            in_specs=[
                pl.BlockSpec((q_rows, block), lambda g, length_ref: (0, g)),
                pl.BlockSpec((k_rows, block), lambda g, length_ref: (0, g)),
            ],
            out_specs=pl.BlockSpec((q_rows, width), lambda g, length_ref: (0, g)),
        ),
        cost_estimate=pl.CostEstimate(
            flops=4 * q_rows * k_rows * width * groups,
            bytes_accessed=2 * (2 * q_rows + 2 * k_rows) * width * groups,
            transcendentals=q_rows * k_rows * groups * width // head_size,
        ),
        name="attend_forward",
    )(length, qkv_q, qkv_kv)


def attend_backward(qkv_q, qkv_kv, grad_context, length, head_size, groups):
    q_rows = qkv_q.shape[0]
    k_rows = qkv_kv.shape[0]
    block = qkv_q.shape[1] // groups
    width = block // 3
    scale = float(head_size) ** (-0.5)

    def body(length_ref, q_ref, kv_ref, grad_ref, dq_ref, dkv_ref):
        visible = lax.broadcasted_iota(jnp.int32, (q_rows, k_rows), 1) < length_ref[0]
        for start, lanes, held in pairs_of(width, head_size):
            queries = q_ref[:, start : start + lanes]
            keys = kv_ref[:, width + start : width + start + lanes]
            values = kv_ref[:, 2 * width + start : 2 * width + start + lanes]
            grads = grad_ref[:, start : start + lanes]
            grad_q = jnp.zeros((q_rows, lanes), F32)
            grad_k = jnp.zeros((k_rows, lanes), F32)
            grad_v = jnp.zeros((k_rows, lanes), F32)
            for which in range(held):
                mine = keep_head(grads, which, head_size)
                query = keep_head(queries, which, head_size)
                probs = soft_weights(query, keys, visible, scale)
                grad_v += contract_rows(probs.astype(BF16), mine)
                grad_probs = contract_cols(mine, values)
                inner = jnp.sum(probs * grad_probs, axis=-1, keepdims=True)
                grad_scores = (probs * (grad_probs - inner)).astype(BF16)
                grad_q += keep_head(matmul(grad_scores, keys), which, head_size)
                grad_k += contract_rows(grad_scores, query)
            dq_ref[:, start : start + lanes] = (grad_q * scale).astype(BF16)
            dkv_ref[:, start : start + lanes] = (grad_k * scale).astype(BF16)
            dkv_ref[:, width + start : width + start + lanes] = grad_v.astype(BF16)

    return pl.pallas_call(
        body,
        out_shape=(
            jax.ShapeDtypeStruct((q_rows, groups * width), BF16),
            jax.ShapeDtypeStruct((k_rows, groups * 2 * width), BF16),
        ),
        grid_spec=pltpu.PrefetchScalarGridSpec(
            num_scalar_prefetch=1,
            grid=(groups,),
            in_specs=[
                pl.BlockSpec((q_rows, block), lambda g, length_ref: (0, g)),
                pl.BlockSpec((k_rows, block), lambda g, length_ref: (0, g)),
                pl.BlockSpec((q_rows, width), lambda g, length_ref: (0, g)),
            ],
            out_specs=[
                pl.BlockSpec((q_rows, width), lambda g, length_ref: (0, g)),
                pl.BlockSpec((k_rows, 2 * width), lambda g, length_ref: (0, g)),
            ],
        ),
        cost_estimate=pl.CostEstimate(
            flops=10 * q_rows * k_rows * width * groups,
            bytes_accessed=2 * (3 * q_rows + 4 * k_rows) * width * groups,
            transcendentals=q_rows * k_rows * groups * width // head_size,
        ),
        name="attend_backward",
    )(length, qkv_q, qkv_kv, grad_context)


def activate(total, bias):
    upper = total + bias
    cumulative = 0.5 * (1.0 + lax.erf(upper * math.sqrt(0.5)))
    density = jnp.exp(-0.5 * upper * upper) * (1.0 / math.sqrt(2.0 * math.pi))
    return upper * cumulative, cumulative + upper * density


def norm_forward(hidden, gain_vec, shift_vec):
    center = hidden - jnp.mean(hidden, axis=-1, keepdims=True)
    variance = jnp.mean(center * center, axis=-1, keepdims=True)
    inv_root = lax.rsqrt(variance + EPSILON)
    normal = center * inv_root
    return (normal * gain_vec + shift_vec, normal, inv_root)


def norm_backward(grad_in, normal, inv_root, gain_vec):
    grad_normal = grad_in * gain_vec
    grad_gain = jnp.sum(grad_in * normal, axis=0)
    grad_shift = jnp.sum(grad_in, axis=0)
    grad_hidden = inv_root * (
        grad_normal
        - jnp.mean(grad_normal, axis=-1, keepdims=True)
        - normal * jnp.mean(grad_normal * normal, axis=-1, keepdims=True)
    )
    return (grad_hidden, grad_gain, grad_shift)


def layer(
    hidden_in,
    cotangent,
    w_query,
    w_key,
    w_value,
    w_out,
    w_up,
    w_down,
    bias_query,
    bias_value,
    bias_out,
    bias_up,
    bias_down,
    gain_attn,
    shift_attn,
    gain_ffn,
    shift_ffn,
    valid_lengths,
):
    rows, model_width = hidden_in.shape
    n_tensor = lax.axis_size("tensor")
    n_data = lax.axis_size("dp")
    tensor_at = lax.axis_index("tensor")
    spread_over = rows * n_tensor // valid_lengths.shape[0] // rows
    head_size = model_width // HEADS
    head_cols = w_query.shape[1]
    factor = 1.0 / math.sqrt(rows * n_tensor * n_data)
    matrices = (w_query, w_key, w_value, w_out, w_up, w_down)
    wide = (bias_out, bias_down, gain_attn, shift_attn, gain_ffn, shift_ffn)

    if n_data == len(ORDER) and spread_over == 1:
        (
            qkv_full, out_full, up_full, down_full, qkv, context, hidden, active, slope, output,
            mixed_low, mixed_t, normed_t, input_t, grad_second, given, arranged,
        ) = forward_near(
            matrices, hidden_in, cotangent, wide, bias_query, bias_value, bias_up, valid_lengths,
            head_size,
        )
        grads, grad_input, sums = backward_near(
            mixed_low, mixed_t, normed_t, input_t, context, grad_second, hidden, arranged,
            valid_lengths, active, slope, qkv, (qkv_full, out_full, up_full, down_full), given,
            head_size,
        )
        sums = sums.reshape(-1) * factor
    else:

        def column_part(vector):
            return vector.reshape(n_tensor, -1)

        query_bias, value_bias = column_part(bias_query), column_part(bias_value)
        bias_qkv = jnp.concatenate(
            [query_bias, jnp.zeros_like(query_bias), value_bias], axis=1
        ).reshape(1, -1)
        length = lax.dynamic_slice_in_dim(valid_lengths, tensor_at // spread_over, 1)
        low = [matrix.astype(BF16) for matrix in matrices]
        shards = [jnp.concatenate(low[:3], axis=1)] + low[3:]
        qkv_full, out_full, up_full, down_full = (gather_far(shard) for shard in shards)
        qkv = (matmul(hidden_in, qkv_full) + bias_qkv).astype(BF16)
        members = [list(range(k, k + spread_over)) for k in range(0, n_tensor, spread_over)]
        qkv_seq = lax.all_gather(qkv, "tensor", axis_index_groups=members, axis=0, tiled=True)
        context = attend_forward(qkv, qkv_seq, length, head_size, n_tensor)
        hidden = hidden_in.astype(F32) + contract_cols(context, out_full) + bias_out
        normed, normal_attn, root_attn = norm_forward(hidden, gain_attn, shift_attn)
        normed_low = normed.astype(BF16)
        active, slope = activate(matmul(normed_low, up_full), bias_up)
        active = active.astype(BF16)
        mixed = contract_cols(active, down_full)
        result, normal_ffn, root_ffn = norm_forward(normed + mixed + bias_down, gain_ffn, shift_ffn)
        output = result.astype(BF16)
        grad_second, grad_gain_ffn, grad_shift_ffn = norm_backward(
            cotangent.astype(F32), normal_ffn, root_ffn, gain_ffn
        )
        grad_bias_down = jnp.sum(grad_second, axis=0)
        mixed_low = grad_second.astype(BF16)
        grad_down = scatter_far(mixed_low, active)
        grad_upper = (matmul(mixed_low, down_full) * slope).astype(BF16)
        grad_bias_up = jnp.sum(grad_upper, axis=0, dtype=F32)
        grad_up = scatter_far(normed_low, grad_upper)
        grad_normed = grad_second + contract_cols(grad_upper, up_full)
        grad_first, grad_gain_attn, grad_shift_attn = norm_backward(
            grad_normed, normal_attn, root_attn, gain_attn
        )
        grad_bias_out = jnp.sum(grad_first, axis=0)
        attn_low = grad_first.astype(BF16)
        grad_context = matmul(attn_low, out_full).astype(BF16)
        grad_out = scatter_far(attn_low, context)
        grad_q, grad_kv = attend_backward(qkv, qkv_seq, grad_context, length, head_size, n_tensor)
        grad_kv = lax.psum_scatter(
            grad_kv.astype(F32),
            "tensor",
            scatter_dimension=0,
            axis_index_groups=members,
            tiled=True,
        ).astype(BF16)
        grad_qkv = jnp.concatenate(
            [grad_q.reshape(rows, n_tensor, -1), grad_kv.reshape(rows, n_tensor, -1)], axis=2
        ).reshape(rows, -1)
        grad_bias_qkv = jnp.sum(grad_qkv, axis=0, dtype=F32).reshape(n_tensor, 3, head_cols)
        grads = jnp.split(scatter_far(hidden_in, grad_qkv), 3, axis=1)
        grads += [grad_out, grad_up, grad_down]
        grad_input = (grad_first + contract_cols(grad_qkv, qkv_full)).astype(BF16)
        sums = jnp.concatenate(
            [
                grad_bias_out,
                grad_bias_down,
                grad_gain_attn,
                grad_shift_attn,
                grad_gain_ffn,
                grad_shift_ffn,
                grad_bias_qkv[:, 0].reshape(-1),
                grad_bias_qkv[:, 2].reshape(-1),
                grad_bias_up,
            ]
        )
        sums = lax.psum(sums, ("dp", "tensor")) * factor
    v_out, v_down, v_gain_attn, v_shift_attn, v_gain_ffn, v_shift_ffn, v_query, v_value = (
        sums[k * model_width : (k + 1) * model_width] for k in range(8)
    )
    v_up = sums[8 * model_width :]
    return (
        output,
        grad_input,
        *(grad * factor for grad in grads),
        v_query,
        v_value,
        v_out,
        v_up,
        v_down,
        v_gain_attn,
        v_shift_attn,
        v_gain_ffn,
        v_shift_ffn,
    )


def solution(mesh):
    tokens, matrix, copied = P(("dp", "tensor"), None), P("dp", "tensor"), P()
    return jax.shard_map(
        layer,
        mesh=mesh,
        in_specs=(tokens,) * 2 + (matrix,) * 6 + (copied,) * 9 + (P("dp"),),
        out_specs=(tokens,) * 2 + (matrix,) * 6 + (copied,) * 9,
        check_vma=False,
    )
```

```python
import math

import jax
import jax.numpy as jnp
from jax import lax
from jax.experimental import pallas as pl
from jax.experimental.pallas import tpu as pltpu
from jax.sharding import PartitionSpec as P

HEADS = 16
EPSILON = 1e-12
MASKED = -1e30
BF16 = jnp.bfloat16
F32 = jnp.float32

ORDER = (0, 2, 4, 6, 1, 3, 5, 7)
BIT_CORE, BIT_X, BIT_Y = 1, 2, 4


def matmul(left_side, right_side):
    return jnp.dot(left_side, right_side, preferred_element_type=F32)


def contract_rows(left_side, right_side):
    return lax.dot_general(
        left_side, right_side, (((0,), (0,)), ((), ())), preferred_element_type=F32
    )


def contract_cols(left_side, right_side):
    return lax.dot_general(
        left_side, right_side, (((1,), (1,)), ((), ())), preferred_element_type=F32
    )


FORWARD_ID = 1
BACKWARD_ID = 2
TILE = 512

FORWARD = (
    "lplane9", "z1", "z3", "lcor9", "col1", "z2", "z5", "z0", "z4", "col3", "col2", "prep",
    "col5", "col0", "cor2", "cor1", "z6", "cor0", "cor3", "z7", "last0", "z8", "col4", "col6",
    "last2", "tr", "last1", "cor5", "cor4", "qkv", "last3", "lz9", "a0", "cor6", "a1", "a2",
    "col7", "a3", "last4", "last5", "last6", "out", "col8", "norm", "up1", "cor7", "cor8",
    "lcore9", "up2", "up3", "last7", "lowX", "last8", "low1", "low2", "ln",
)
BACKWARD = (
    "oth8", "oth7", "gelA", "own8", "cor8", "own7", "cor7", "oth9", "oth4", "sid8", "gelB",
    "own9", "sid7", "oth5", "lz9", "oth6", "upA", "own4", "upB", "own5", "cor4", "cor5", "norm",
    "col8", "sid4", "own6", "out", "col7", "oth3", "a0", "own3", "cor3", "cor6", "a1", "col4",
    "sid5", "sid3", "a2", "a3", "oth1", "sid6", "vec", "oth2", "col5", "fin4", "own1", "cor1",
    "v0", "oth0", "col3", "v1", "own2", "cor2", "fin8", "sid1", "col6", "own0", "cor0", "fin7",
    "sid2", "v2", "col1", "dxA", "sid0", "col2", "lcor9", "dxB", "fin6", "col0", "v3", "sid9",
    "fin2", "v4", "gout", "fin5", "fin1", "fin3", "fin9", "v5", "fin0",
)


def neighbour(index, bit):
    return index + bit - 2 * bit * ((index // bit) % 2)


def block_of(index, mask):
    for bit in (BIT_CORE, BIT_X, BIT_Y):
        if mask & bit:
            index = neighbour(index, bit)
    return index


def pieces_of(size, attn, units_each):
    pieces = [(0, k * size * attn, attn) for k in range(3)] + [(1, 0, attn)]
    for weight in (2, 3):
        start = 0
        for count in (units_each // 2, units_each // 4, units_each // 4):
            pieces.append((weight, start * size, count))
            start += count
    return pieces


def run_events(order, table, attend, size):
    first = order.index("a0")
    last = order.index(f"a{size - 1}")
    for name in order[:first]:
        table[name]()

    def step(r, carry):
        attend(r)
        for k in range(size - 1):
            start = order.index(f"a{k}") + 1
            names = order[start : order.index(f"a{k + 1}")]
            if names:

                @pl.when(r == k)
                def _():
                    for name in names:
                        table[name]()

        return carry

    lax.fori_loop(0, size, step, 0)
    for name in order[last + 1 :]:
        table[name]()


def greet(partners):
    barrier = pltpu.get_barrier_semaphore()
    for partner in partners:
        pl.semaphore_signal(
            barrier, inc=1, device_id=partner, device_id_type=pl.DeviceIdType.MESH
        )


def await_greetings(partners):
    pl.semaphore_wait(pltpu.get_barrier_semaphore(), len(partners))


def scale_and_copy(scaled, copied, sums, lengths, factor):
    arrays = list(scaled) + list(copied)
    starts = [sum(lengths[:k]) for k in range(len(lengths))]

    def body(*refs):
        sums_ref, targets = refs[len(arrays)], refs[len(arrays) + 1 :]
        for k in range(len(arrays)):
            targets[k][...] = refs[k][...] * factor if k < len(scaled) else refs[k][...]
        for start, length, target in zip(starts, lengths, targets[len(arrays) :]):
            target[...] = sums_ref[start : start + length, :] * factor

    return pl.pallas_call(
        body,
        out_shape=[jax.ShapeDtypeStruct(array.shape, array.dtype) for array in arrays]
        + [jax.ShapeDtypeStruct((length, sums.shape[1]), F32) for length in lengths],
        in_specs=[pl.BlockSpec(memory_space=pltpu.VMEM)] * (len(arrays) + 1),
        out_specs=[pl.BlockSpec(memory_space=pltpu.VMEM)] * (len(arrays) + len(lengths)),
    )(*arrays, sums)


def forward_near(weights, hidden_in, cotangent, wide, bias_query, bias_value, bias_units, lengths, head_size):
    size = lax.axis_size("tensor")
    rows, width = hidden_in.shape
    block = width // len(ORDER)
    attn, units_each = weights[0].shape[1], weights[4].shape[1]
    cols = [3 * attn, attn, units_each, units_each]
    full = [(width, size * c) for c in cols]
    units = size * units_each
    half = block // 2
    pieces = pieces_of(size, attn, units_each)
    X = len(pieces) - 1
    A, O, U, _ = range(4)
    B_OUT, B_DOWN, G_ATTN, S_ATTN, G_FFN, S_FFN = range(6)

    def body(
        q_in, k_in, v_in, o_in, u_in, d_in, hidden_raw, cotangent_ref, bias_out_in, bias_down_in,
        gain_attn_in, shift_attn_in, gain_ffn_in, shift_ffn_in, bias_q_ref, bias_v_ref, bias_u_ref,
        lengths_ref,
        a_out, o_out, u_out, d_out, qkv_out, context_out, hidden_out, active_out, slope_out, output_ref,
        mixed_ref, mixed_t, normed_t, input_t, second_ref, sums_ref, wide_ref,
        a_ref, o_ref, u_ref, d_ref, x_ref, low_ref, active_ref, slope_ref, bias_ref, units_ref, qkv_ref,
        context_ref, hidden_ref, turned_x, turned_n, local_sem, send_sem, recv_sem,
        tile_sem,
    ):
        data_at, tensor_at = lax.axis_index("dp"), lax.axis_index("tensor")
        places = (a_ref, o_ref, u_ref, d_ref)

        def dp_partner(bit):
            return (neighbour(data_at, bit), tensor_at)

        def z_partner(step):
            return by_z[step]

        by_z = [(data_at, (tensor_at + step) % size) for step in range(size)]
        by_x, by_y, by_core = dp_partner(BIT_X), dp_partner(BIT_Y), dp_partner(BIT_CORE)
        owners = [block_of(data_at, mask) for mask in ORDER]
        copies = {}

        def send(g, slot, source, target, device):
            def copy():
                return pltpu.make_async_remote_copy(
                    src_ref=source,
                    dst_ref=target,
                    send_sem=send_sem.at[g, slot],
                    recv_sem=recv_sem.at[g, slot],
                    device_id=device,
                    device_id_type=pl.DeviceIdType.MESH,
                )

            copies[g, slot] = copy
            copy().start()

        def arrived(g, *slots):
            for slot in slots:
                copies[g, slot]().wait_recv()

        def whole(g, start, count):
            weight, first, wide_by = pieces[g]
            return places[weight].at[start : start + count, first : first + size * wide_by]

        def cell(g, start, count, r):
            weight, first, wide_by = pieces[g]
            at = first + r * wide_by
            return places[weight].at[start : start + count, at : at + wide_by]

        def send_z(g):
            for r in range(1, size):
                send(g, r - 1, cell(g, 0, block, 0), cell(g, 0, block, r), z_partner(r))

        def send_column(g):
            arrived(g, 0, 1, 2)
            send(g, 3, whole(g, 0, block), whole(g, block, block), by_x)
            send(g, 4, whole(g, 0, block), whole(g, 2 * block, block), by_y)

        def send_corner(g):
            arrived(g, 3, 4)
            send(g, 5, whole(g, block, half), whole(g, 3 * block, half), by_y)
            send(g, 6, whole(g, 2 * block + half, half), whole(g, 3 * block + half, half), by_x)
            send(g, 7, whole(g, 0, 3 * block), whole(g, 4 * block, 3 * block), by_core)

        def send_last(g):
            arrived(g, 5, 6)
            send(g, 8, whole(g, 3 * block, block), whole(g, 7 * block, block), by_core)

        def complete(*group):
            for g in group:
                arrived(g, 7, 8)

        def late_plane():
            send(X, 3, cell(X, 0, block, 0), cell(X, block, block, 0), by_x)
            send(X, 4, cell(X, 0, block, 0), cell(X, 2 * block, block, 0), by_y)

        def late_corner():
            arrived(X, 3, 4)
            send(X, 5, cell(X, block, half, 0), cell(X, 3 * block, half, 0), by_y)
            send(X, 6, cell(X, 2 * block + half, half, 0), cell(X, 3 * block + half, half, 0), by_x)

        def late_z():
            arrived(X, 5, 6)
            for r in range(1, size):
                send(X, r - 1, cell(X, 0, 4 * block, 0), cell(X, 0, 4 * block, r), z_partner(r))

        def late_core():
            arrived(X, 0, 1, 2)
            send(X, 7, whole(X, 0, 4 * block), whole(X, 4 * block, 4 * block), by_core)

        saves = []

        def save(slot, source, target):
            copy = pltpu.make_async_copy(source, target, local_sem.at[slot])
            copy.start()
            saves.append(copy)

        def save_weight(slot, g):
            target = (a_out, o_out, u_out, d_out)[g]
            save(slot, places[g], target)

        sources = (q_in, k_in, v_in, o_in, u_in, u_in, u_in, d_in, d_in, d_in)

        def cast(g):
            weight, first, wide_by = pieces[g]
            start = first // size if weight >= U else 0
            places[weight][:block, first : first + wide_by] = sources[g][
                :, start : start + wide_by
            ].astype(BF16)

        partners = [by_x, by_y, by_core] + by_z[1:]
        greet(partners)
        for g in range(len(pieces)):
            cast(g)
        await_greetings(partners)

        def lanes_of(owner):
            return pl.ds(pl.multiple_of(owner * block, block), block)

        def turn(target, at, rows_of):
            for k in range(width // 128):
                target[k * 128 : (k + 1) * 128, at] = rows_of[:, k * 128 : (k + 1) * 128].T.astype(BF16)

        def vector(k):
            return wide_ref[k : k + 1, :]

        def column_of(r, first, span):
            at = ((tensor_at + size - r) % size) * (first[1]) + first[0]
            return pl.ds(pl.multiple_of(at, 128), span)

        def prepare():
            for place, owner in enumerate(owners):
                at = slice(place * block, (place + 1) * block)
                x_ref[:, at] = hidden_raw[:, lanes_of(owner)]
                for k, ref in enumerate(
                    (bias_out_in, bias_down_in, gain_attn_in, shift_attn_in, gain_ffn_in, shift_ffn_in)
                ):
                    wide_ref[k : k + 1, at] = ref[:, lanes_of(owner)]
            for r in range(size):
                at = slice(r * attn, (r + 1) * attn)
                bias_ref[0:1, at] = bias_q_ref[:, column_of(r, (0, attn), attn)]
                bias_ref[1:2, at] = bias_v_ref[:, column_of(r, (0, attn), attn)]
                for weight, first, wide_by in pieces:
                    if weight == U:
                        at = slice(first + r * wide_by, first + (r + 1) * wide_by)
                        units_ref[:, at] = bias_u_ref[
                            :, column_of(r, (first // size, units_each), wide_by)
                        ]

        def turn_inputs():
            def one(j, carry):
                at = pl.ds(pl.multiple_of(j * 128, 128), 128)
                turn(turned_x, at, x_ref[at, :].astype(F32))
                return carry

            lax.fori_loop(0, rows // 128, one, 0)
            save(4, turned_x, input_t)

        def project(j, carry):
            at = pl.ds(pl.multiple_of(j * attn, attn), attn)
            total = matmul(x_ref[...], a_ref[:, at])
            which = j // size
            bias = bias_ref[:, pl.ds(pl.multiple_of((j % size) * attn, attn), attn)]
            bias = jnp.where(which == 0, bias[0:1], jnp.where(which == 2, bias[1:2], 0.0))
            qkv_ref[:, at] = (total + bias).astype(BF16)
            return carry

        def qkv():
            complete(0, 1, 2)
            save_weight(A, A)
            lax.fori_loop(0, 3 * size, project, 0)
            save(5, qkv_ref, qkv_out)

        scale = float(head_size) ** (-0.5)
        length = lengths_ref[tensor_at]

        def attend(r):
            seen = lax.broadcasted_iota(jnp.int32, (rows, rows), 1) < length
            for start, lanes, held in pairs_of(attn, head_size):
                at = [
                    pl.ds(pl.multiple_of((k * size + r) * attn + start, 128), lanes) for k in range(3)
                ]
                queries, keys, values = (qkv_ref[:, where] for where in at)
                total = jnp.zeros((rows, lanes), F32)
                for which in range(held):
                    probs = soft_weights(keep_head(queries, which, head_size), keys, seen, scale)
                    total += keep_head(matmul(probs.astype(BF16), values), which, head_size)
                context_ref[:, at[0]] = total.astype(BF16)

        def output(j, carry):
            at = pl.ds(pl.multiple_of(j * 256, 256), 256)
            total = contract_cols(context_ref[...], o_ref[at, :])
            hidden_ref[:, at] = x_ref[:, at].astype(F32) + total + wide_ref[B_OUT : B_OUT + 1, at]
            return carry

        def out():
            complete(3)
            save_weight(O, O)
            save(6, context_ref, context_out)
            lax.fori_loop(0, width // 256, output, 0)
            save(7, hidden_ref, hidden_out)

        chunk = 128

        def norm_step(j, carry):
            at = pl.ds(pl.multiple_of(j * chunk, chunk), chunk)
            normed = norm_forward(hidden_ref[at, :], vector(G_ATTN), vector(S_ATTN))[0]
            low_ref[at, :] = normed.astype(BF16)
            second_ref[at, :] = normed + vector(B_DOWN)
            turn(turned_n, at, normed)
            return carry

        def norm():
            lax.fori_loop(0, rows // chunk, norm_step, 0)
            save(8, turned_n, normed_t)

        def tile_at(j):
            return pl.ds(pl.multiple_of(j * TILE, TILE), TILE)

        def slope_copy(j):
            return pltpu.make_async_copy(
                slope_ref.at[j % 2], slope_out.at[:, tile_at(j)], tile_sem.at[1, j % 2]
            )

        def active_copy(j):
            return pltpu.make_async_copy(
                active_ref.at[:, tile_at(j)], active_out.at[:, tile_at(j)], tile_sem.at[0, j]
            )

        def raise_up(j, carry):
            @pl.when(j >= 2)
            def _():
                slope_copy(j - 2).wait()

            total = matmul(low_ref[...], u_ref[:, tile_at(j)])
            active, slope = activate(total, units_ref[:, tile_at(j)])
            active_ref[:, tile_at(j)] = active.astype(BF16)
            slope_ref[j % 2] = slope
            active_copy(j).start()
            slope_copy(j).start()
            return carry

        def span_of(g):
            _, first, wide_by = pieces[g]
            return slice(first, first + size * wide_by)

        def raise_piece(g):
            complete(g)
            save(g + 5, u_ref.at[:, span_of(g)], u_out.at[:, span_of(g)])
            at = span_of(g)
            lax.fori_loop(at.start // TILE, at.stop // TILE, raise_up, 0)

        def lower_piece(g):
            if g == X:
                arrived(X, 7)
            else:
                complete(g)
            at = span_of(g)
            save(g + 5, d_ref.at[:, at], d_out.at[:, at])

            def one(j, carry):
                to = pl.ds(pl.multiple_of(j * 256, 256), 256)
                second_ref[:, to] += contract_cols(active_ref[:, at], d_ref[to, at])
                return carry

            lax.fori_loop(0, width // 256, one, 0)

        def second(j, sums):
            at = pl.ds(pl.multiple_of(j * chunk, chunk), chunk)
            result, normal, root = norm_forward(second_ref[at, :], vector(G_FFN), vector(S_FFN))
            grads = jnp.concatenate([cotangent_ref[at, lanes_of(owner)] for owner in owners], axis=1)
            for place, owner in enumerate(owners):
                output_ref[at, lanes_of(owner)] = result[:, place * block : (place + 1) * block].astype(BF16)
            hidden, more_gain, more_shift = norm_backward(
                grads.astype(F32), normal, root, vector(G_FFN)
            )
            second_ref[at, :] = hidden
            mixed_ref[at, :] = hidden.astype(BF16)
            turn(mixed_t, at, hidden)
            more = (jnp.sum(hidden, axis=0), more_gain, more_shift)
            return tuple(a + b[None] for a, b in zip(sums, more))

        def last_norm():
            zero = jnp.zeros((1, width), F32)
            sums = lax.fori_loop(0, rows // chunk, second, (zero, zero, zero))
            for k in range(3):
                sums_ref[k : k + 1, :] = sums[k]

        def bound(step, *given):
            return lambda: step(*given)

        table = {
            "prep": prepare, "tr": turn_inputs, "qkv": qkv, "out": out, "norm": norm, "ln": last_norm,
            "up1": bound(raise_piece, 4), "up2": bound(raise_piece, 5), "up3": bound(raise_piece, 6),
            "low1": bound(lower_piece, 7), "low2": bound(lower_piece, 8), "lowX": bound(lower_piece, X),
            "lplane9": late_plane, "lcor9": late_corner, "lz9": late_z, "lcore9": late_core,
        }
        for g in range(X):
            table[f"z{g}"] = bound(send_z, g)
            table[f"col{g}"] = bound(send_column, g)
            table[f"cor{g}"] = bound(send_corner, g)
            table[f"last{g}"] = bound(send_last, g)
        run_events(FORWARD, table, attend, size)

        def settle(j, carry):
            active_copy(j).wait()
            return carry

        lax.fori_loop(0, units // TILE, settle, 0)
        for j in (units // TILE - 2, units // TILE - 1):
            slope_copy(j).wait()
        for copy in saves:
            copy.wait()
        for copy in copies.values():
            copy().wait_send()

    anywhere, inside = pl.BlockSpec(memory_space=pl.ANY), pl.BlockSpec(memory_space=pltpu.VMEM)
    tall = jax.ShapeDtypeStruct((rows, width), BF16)
    turned = jax.ShapeDtypeStruct((width, rows), BF16)
    return pl.pallas_call(
        body,
        out_shape=[jax.ShapeDtypeStruct(shape, BF16) for shape in full]
        + [
            jax.ShapeDtypeStruct((rows, full[A][1]), BF16),
            tall,
            jax.ShapeDtypeStruct((rows, width), F32),
            jax.ShapeDtypeStruct((rows, units), BF16),
            jax.ShapeDtypeStruct((rows, units), F32),
            tall,
            tall,
            turned,
            turned,
            turned,
            jax.ShapeDtypeStruct((rows, width), F32),
            jax.ShapeDtypeStruct((3, width), F32),
            jax.ShapeDtypeStruct((6, width), F32),
        ],
        in_specs=[inside] * 17 + [pl.BlockSpec(memory_space=pltpu.SMEM)],
        out_specs=[anywhere] * 9 + [inside] * 3 + [anywhere] * 2 + [inside] * 3,
        scratch_shapes=[pltpu.VMEM(shape, BF16) for shape in full]
        + [
            pltpu.VMEM((rows, width), BF16),
            pltpu.VMEM((rows, width), BF16),
            pltpu.VMEM((rows, units), BF16),
            pltpu.VMEM((2, rows, TILE), F32),
            pltpu.VMEM((2, size * attn), F32),
            pltpu.VMEM((1, units), F32),
            pltpu.VMEM((rows, full[A][1]), BF16),
            pltpu.VMEM((rows, width), BF16),
            pltpu.VMEM((rows, width), F32),
            pltpu.VMEM((width, rows), BF16),
            pltpu.VMEM((width, rows), BF16),
            pltpu.SemaphoreType.DMA((5 + len(pieces),)),
            pltpu.SemaphoreType.DMA((len(pieces), 9)),
            pltpu.SemaphoreType.DMA((len(pieces), 9)),
            pltpu.SemaphoreType.DMA((2, units // TILE)),
        ],
        compiler_params=pltpu.CompilerParams(
            collective_id=FORWARD_ID, has_side_effects=True, vmem_limit_bytes=63 * 2**20
        ),
        cost_estimate=pl.CostEstimate(
            flops=2 * rows * width * sum(shape[1] for shape in full),
            bytes_accessed=4 * width * sum(shape[1] for shape in full),
            transcendentals=rows * units,
        ),
        name="forward_near",
    )(
        *weights, hidden_in, cotangent, *(vector[None] for vector in wide), bias_query[None],
        bias_value[None], bias_units[None], lengths,
    )


def backward_near(mixed_low, mixed_t, normed_t, input_t, context, grad_second, hidden, wide, lengths,
                  active, slope, qkv, weights, vectors, head_size):
    size = lax.axis_size("tensor")
    rows, width = mixed_low.shape
    block = width // len(ORDER)
    middle = width // 2
    half = block // 2
    full = [weight.shape[1] for weight in weights]
    units = full[2]
    units_each = units // size
    attn = full[1] // size
    pieces = pieces_of(size, attn, units_each)
    X = len(pieces) - 1
    A, O, U, D = range(4)
    tiles = [c // TILE for c in full]
    vector_rows = (6 * width + 2 * full[1] + units) // 128
    v_query, v_value, v_up = 6 * width // 128, (6 * width + full[1]) // 128, (6 * width + 2 * full[1]) // 128
    scale = float(head_size) ** (-0.5)

    def body(
        mixed_in, mixed_t, normed_in, input_in, context_in, second_in, hidden_in, wide_ref,
        lengths_ref, active_in, slope_in, qkv_in, a_in, o_in, u_in, d_in, vectors_ref,
        q_out, k_out, v_out, o_out, u_out, d_out, grad_out, sums_out,
        w_buf, act_ref, slope_buf, gu_ref, grad_ref, low_ref, low_t, gctx_ref, qkv_buf, send_buf,
        units_sum, mixed_ref, normed_t, input_t, context_ref, a_plane, o_plane, u_plane, d_plane, *rest,
    ):
        count = len(pieces)
        corners, sides, zins = (rest[k * count : (k + 1) * count] for k in range(3))
        (
            v_ref, v_in, load_sem, start_sem, core_send, core_recv, send_sem, recv_sem, v_send, v_recv,
        ) = rest[3 * count :]
        data_at, tensor_at = lax.axis_index("dp"), lax.axis_index("tensor")
        planes = (a_plane, o_plane, u_plane, d_plane)
        outs = (q_out, k_out, v_out, o_out, u_out, u_out, u_out, d_out, d_out, d_out)
        shift_by = (tiles[O], 0, 0, 0)

        def dp_partner(bit):
            return (neighbour(data_at, bit), tensor_at)

        def z_partner(step):
            return by_z[step % size]

        by_z = [(data_at, (tensor_at + step) % size) for step in range(size)]

        by_x, by_y, by_core = dp_partner(BIT_X), dp_partner(BIT_Y), dp_partner(BIT_CORE)

        def column(j, span=TILE):
            return pl.ds(pl.multiple_of(j * span, 128), span)

        def load(row, source, buffer, j):
            return pltpu.make_async_copy(
                source.at[:, column(j)], buffer.at[j % 2], load_sem.at[row, j % 2]
            )

        def over_tiles(first, last, loads, step):
            for row, source, buffer in loads:
                load(row, source, buffer, first).start()

            def one(j, carry):
                @pl.when(j + 1 < last)
                def _():
                    for row, source, buffer in loads:
                        load(row, source, buffer, j + 1).start()

                for row, source, buffer in loads:
                    load(row, source, buffer, j).wait()
                step(j)
                return carry

            lax.fori_loop(first, last, one, 0)

        def remote(source, target, send, receive, device):
            return pltpu.make_async_remote_copy(
                src_ref=source,
                dst_ref=target,
                send_sem=send,
                recv_sem=receive,
                device_id=device,
                device_id_type=pl.DeviceIdType.MESH,
            )

        def core_copy(g, j):
            return remote(
                send_buf.at[:, column(j + shift_by[g])],
                planes[g].at[:, column(j)],
                core_send.at[g, j],
                core_recv.at[g, j],
                by_core,
            )

        copies = {}

        def send(g, slot, source, target, device):
            def copy():
                return remote(source, target(), send_sem.at[g, slot], recv_sem.at[g, slot], device)

            copies[g, slot] = copy
            copy().start()

        def arrived(g, *slots):
            for slot in slots:
                copies[g, slot]().wait_recv()

        def other_tile(g, left_t, right, j):
            send_buf[:, column(j + shift_by[g])] = matmul(left_t[middle:, :], right).astype(BF16)
            core_copy(g, j).start()

        def own_tile(g, left_t, right, j):
            core_copy(g, j).wait_recv()
            total = matmul(left_t[:middle, :], right) + planes[g][:, column(j)].astype(F32)
            planes[g][:, column(j)] = total.astype(BF16)

        def span(g):
            _, first, wide_by = pieces[g]
            return first, wide_by if g == X else size * wide_by

        def plane_rows(g, start, count):
            first, wide_by = span(g)
            return planes[pieces[g][0]].at[start : start + count, first : first + wide_by]

        def send_corner(g):
            send(g, 0, plane_rows(g, 3 * block, half), lambda: corners[g].at[0], by_x)
            send(g, 1, plane_rows(g, 3 * block + half, half), lambda: corners[g].at[1], by_y)

        def add_rows(g, start, count, *more):
            plane = planes[pieces[g][0]]
            first, wide_by = span(g)
            step = min(TILE, wide_by)
            for at in range(0, wide_by, step):
                where = (slice(start, start + count), slice(first + at, first + at + step))
                total = plane[where].astype(F32)
                for ref in more:
                    total += ref[:, at : at + step].astype(F32)
                plane[where] = total.astype(BF16)

        def send_sides(g):
            arrived(g, 0, 1)
            add_rows(g, 2 * block, half, corners[g].at[0])
            add_rows(g, block + half, half, corners[g].at[1])
            send(g, 2, plane_rows(g, block, block), lambda: sides[g].at[0], by_x)
            send(g, 3, plane_rows(g, 2 * block, block), lambda: sides[g].at[1], by_y)

        def out_of(g):
            weight, first, wide_by = pieces[g]
            start = first // size if weight >= U else 0
            return outs[g].at[:, start : start + wide_by]

        def send_column(g):
            arrived(g, 2, 3)
            weight, first, wide_by = pieces[g]
            for r in range(size):
                at = slice(r * wide_by, (r + 1) * wide_by)
                own = slice(first + r * wide_by, first + (r + 1) * wide_by)
                total = planes[weight][:block, own].astype(F32)
                total += sides[g][0, :, at].astype(F32) + sides[g][1, :, at].astype(F32)
                if r == 0:
                    out_of(g)[...] = total
                else:
                    planes[weight][:block, own] = total.astype(BF16)
                    send(g, 3 + r, planes[weight].at[:block, own], lambda r=r: zins[g].at[r - 1], z_partner(-r))

        def finish(g):
            arrived(g, *range(4, 3 + size))
            total = out_of(g)[...]
            for r in range(1, size):
                total += zins[g][r - 1].astype(F32)
            out_of(g)[...] = total

        def late_z():
            weight, first, wide_by = pieces[X]
            for r in range(1, size):
                own = slice(first + r * wide_by, first + (r + 1) * wide_by)
                send(X, 3 + r, planes[weight].at[:, own], lambda r=r: zins[X].at[r - 1], z_partner(-r))

        def late_corner():
            arrived(X, *range(4, 3 + size))
            for k in range(4):
                rows_k = slice(k * block, (k + 1) * block)
                add_rows(X, k * block, block, *(zins[X].at[r, rows_k] for r in range(size - 1)))
            send_corner(X)

        def late_finish():
            arrived(X, 2, 3)
            total = plane_rows(X, 0, block)[...].astype(F32)
            out_of(X)[...] = total + sides[X][0].astype(F32) + sides[X][1].astype(F32)

        def feature_rows(k, vector):
            for place, mask in enumerate(ORDER):
                at = block_of(data_at, mask)
                v_ref[0, pl.ds(k * len(ORDER) + at, 1), :] = vector[:, place * 128 : (place + 1) * 128]

        z_near = tensor_at + 1 - 2 * (tensor_at % 2)
        z_across = tensor_at + 2 - 4 * ((tensor_at // 2) % 2)
        v_partners = (by_core, (data_at, z_near), (data_at, z_across), by_x, by_y)

        def v_copy(k):
            return remote(v_ref.at[k], v_in.at[k], v_send.at[k], v_recv.at[k], v_partners[k])

        def v_add(k):
            v_copy(k).wait_recv()
            v_ref[k + 1] = v_ref[k] + v_in[k]

        early = [
            pltpu.make_async_copy(
                active_in.at[:, k * (units // 2) : (k + 1) * (units // 2)],
                act_ref.at[:, k * (units // 2) : (k + 1) * (units // 2)],
                start_sem.at[k],
            )
            for k in range(2)
        ]
        grad_load, mixed_load, normed_load, context_load, input_load = (
            pltpu.make_async_copy(source, target, start_sem.at[k])
            for k, (source, target) in enumerate(
                (
                    (second_in, grad_ref),
                    (mixed_in, mixed_ref),
                    (normed_in, normed_t),
                    (context_in, context_ref),
                    (input_in, input_t),
                ),
                2,
            )
        )
        for copy in early:
            copy.start()
        for copy in (mixed_load, normed_load, grad_load, context_load, input_load):
            copy.start()
        partners = [by_x, by_y, by_core] + by_z[1:]
        greet(partners)
        await_greetings(partners)

        def each(first, last, step):
            def one(j, carry):
                step(j)
                return carry

            lax.fori_loop(first, last, one, 0)

        def other_down(j):
            other_tile(D, mixed_t, act_ref[:, column(j)], j)

        def own_down(j):
            own_tile(D, mixed_t, act_ref[:, column(j)], j)

        def other_up(j):
            core_copy(D, j).wait_send()
            other_tile(U, normed_t, gu_ref[:, column(j)], j)

        def own_up(j):
            own_tile(U, normed_t, gu_ref[:, column(j)], j)

        def bounds(g):
            _, first, wide_by = pieces[g]
            return first // TILE, (first + size * wide_by) // TILE

        early[0].wait()
        early[1].wait()

        def loaded(copy, step):
            def both():
                copy.wait()
                step()

            return both

        def bound(step, *given):
            return lambda: step(*given)

        def gelu_step(j):
            low = (matmul(mixed_ref[...], w_buf[j % 2]) * slope_buf[j % 2]).astype(BF16)
            gu_ref[:, column(j)] = low
            units_sum[:, column(j)] = jnp.sum(low.astype(F32), axis=0, keepdims=True)

        gelu_loads = [(1, d_in, w_buf), (2, slope_in, slope_buf)]
        hidden_loads = [
            pltpu.make_async_copy(hidden_in.at[:, column(k)], slope_buf.at[k], load_sem.at[2, k])
            for k in range(2)
        ]

        def second_gelu():
            over_tiles(tiles[D] // 2, tiles[D], gelu_loads, gelu_step)
            for copy in hidden_loads:
                copy.start()

        def up_step(j):
            grad_ref[...] += contract_cols(gu_ref[:, column(j)], w_buf[j % 2])

        def sum_units():
            for k in range(3):
                feature_rows((1, 4, 5)[k], vectors_ref[k : k + 1, :])
            for r in range(size):
                for weight, first, wide_by in pieces:
                    if weight == U:
                        for k in range(wide_by // 128):
                            place = ((tensor_at + size - r) % size) * (units_each // 128)
                            place += (first // size) // 128 + k
                            at = first + r * wide_by + k * 128
                            v_ref[0, pl.ds(v_up + place, 1), :] = units_sum[:, at : at + 128]

        chunk = 128

        def norm_step(j, sums):
            at = pl.ds(pl.multiple_of(j * chunk, chunk), chunk)
            hidden_rows = jnp.concatenate([slope_buf[0, at, :], slope_buf[1, at, :]], axis=1)
            gain = wide_ref[2:3, :]
            normal, root = norm_forward(hidden_rows, gain, gain)[1:]
            hidden, more_gain, more_shift = norm_backward(grad_ref[at, :], normal, root, gain)
            grad_ref[at, :] = hidden
            low_ref[at, :] = hidden.astype(BF16)
            for k in range(width // 128):
                low_t[k * 128 : (k + 1) * 128, at] = hidden[:, k * 128 : (k + 1) * 128].T.astype(BF16)
            more = (jnp.sum(hidden, axis=0), more_gain, more_shift)
            return tuple(a + b[None] for a, b in zip(sums, more))

        def norm():
            for copy in hidden_loads:
                copy.wait()
            zero = jnp.zeros((1, width), F32)
            sums = lax.fori_loop(0, rows // chunk, norm_step, (zero, zero, zero))
            for k in range(3):
                feature_rows((0, 2, 3)[k], sums[k])

        def out_step(j):
            core_copy(U, j).wait_send()
            gctx_ref[:, column(j)] = matmul(low_ref[...], w_buf[j % 2]).astype(BF16)
            other_tile(O, low_t, context_ref[:, column(j)], j)

        def out():
            context_load.wait()
            over_tiles(0, tiles[O], [(1, o_in, w_buf)], out_step)
            for copy in qkv_load(0):
                copy.start()

        def own_out():
            for j in range(tiles[O]):
                own_tile(O, low_t, context_ref[:, j * TILE : (j + 1) * TILE], j)

        def qkv_load(r):
            return [
                pltpu.make_async_copy(
                    qkv_in.at[:, column(k * size + r, attn)], qkv_buf.at[r % 2, k], load_sem.at[k, r % 2]
                )
                for k in range(3)
            ]

        def attend_step(r):
            @pl.when(r + 1 < size)
            def _():
                for copy in qkv_load(r + 1):
                    copy.start()

            for copy in qkv_load(r):
                copy.wait()
            slot = r % 2
            seen = lax.broadcasted_iota(jnp.int32, (rows, rows), 0) < length
            for start, lanes, held in pairs_of(attn, head_size):
                queries, keys, values = (qkv_buf[slot, k, :, start : start + lanes] for k in range(3))
                grads = gctx_ref[:, pl.ds(pl.multiple_of(r * attn + start, 128), lanes)]
                grad_q = jnp.zeros((rows, lanes), F32)
                grad_k = jnp.zeros((rows, lanes), F32)
                grad_v = jnp.zeros((rows, lanes), F32)
                for which in range(held):
                    mine = keep_head(grads, which, head_size)
                    query = keep_head(queries, which, head_size)
                    scores = jnp.where(seen, contract_cols(keys, query) * scale, MASKED)
                    exponent = jnp.exp(scores - jnp.max(scores, axis=0, keepdims=True))
                    probs = exponent * (1.0 / jnp.sum(exponent, axis=0, keepdims=True))
                    grad_v += matmul(probs.astype(BF16), mine)
                    grad_probs = contract_cols(values, mine)
                    inner = jnp.sum(probs * grad_probs, axis=0, keepdims=True)
                    grad_scores = (probs * (grad_probs - inner)).astype(BF16)
                    grad_q += keep_head(contract_rows(grad_scores, keys), which, head_size)
                    grad_k += matmul(grad_scores, query)
                low_q = (grad_q * scale).astype(BF16)
                low_v = grad_v.astype(BF16)
                for k, low in enumerate((low_q, (grad_k * scale).astype(BF16), low_v)):
                    at = pl.multiple_of((k * size + r) * attn + start, 128)
                    gu_ref[:, pl.ds(at, lanes)] = low
                place = ((tensor_at + size - r) % size) * (attn // 128) + start // 128
                v_ref[0, pl.ds(v_query + place, 1), :] = jnp.sum(
                    low_q.astype(F32), axis=0, keepdims=True
                )
                v_ref[0, pl.ds(v_value + place, 1), :] = jnp.sum(
                    low_v.astype(F32), axis=0, keepdims=True
                )

        length = lengths_ref[tensor_at]

        def other_qkv(j):
            core_copy(U, j + tiles[O]).wait_send()
            other_tile(A, input_t, gu_ref[:, column(j)], j)

        def own_qkv(j):
            own_tile(A, input_t, gu_ref[:, column(j)], j)

        def input_step(j):
            grad_ref[...] += contract_cols(gu_ref[:, column(j)], w_buf[j % 2])

        def give_input():
            for place, mask in enumerate(ORDER):
                at = block_of(data_at, mask)
                grad_out[:, pl.ds(pl.multiple_of(at * block, block), block)] = grad_ref[
                    :, place * block : (place + 1) * block
                ].astype(BF16)

        def give_sums():
            v_add(4)
            sums_out[...] = v_ref[5]

        def next_sum(k):
            v_add(k - 1)
            v_copy(k).start()

        weight_loads = [[(1, ref, w_buf)] for ref in (a_in, o_in, u_in, d_in)]
        parts = (
            (other_qkv, own_qkv), (other_qkv, own_qkv), (other_qkv, own_qkv), (lambda j: None, own_out),
            (other_up, own_up), (other_up, own_up), (other_up, own_up), (other_down, own_down),
            (other_down, own_down), (other_down, own_down),
        )
        halves = [(0, count // 2, count) for count in tiles]
        table = {
            "gelA": loaded(mixed_load, bound(over_tiles, 0, halves[D][1], gelu_loads, gelu_step)),
            "gelB": second_gelu,
            "upA": loaded(grad_load, bound(over_tiles, 0, halves[U][1], weight_loads[U], up_step)),
            "upB": bound(over_tiles, *halves[U][1:], weight_loads[U], up_step),
            "vec": sum_units,
            "norm": norm,
            "out": out,
            "dxA": bound(over_tiles, 0, halves[A][1], weight_loads[A], input_step),
            "dxB": bound(over_tiles, *halves[A][1:], weight_loads[A], input_step),
            "gout": give_input,
            "lz9": late_z,
            "lcor9": late_corner,
            "sid9": bound(send_sides, X),
            "fin9": late_finish,
            "v0": lambda: v_copy(0).start(),
            "v5": give_sums,
        }
        for k in range(1, 5):
            table[f"v{k}"] = bound(next_sum, k)
        for g in range(len(pieces)):
            other, own = parts[g]
            table[f"oth{g}"] = bound(each, *bounds(g), other)
            table[f"own{g}"] = bound(each, *bounds(g), own)
            if g < X:
                table[f"cor{g}"] = bound(send_corner, g)
                table[f"sid{g}"] = bound(send_sides, g)
                table[f"col{g}"] = bound(send_column, g)
                table[f"fin{g}"] = bound(finish, g)
        table["oth3"] = lambda: None
        table["own3"] = own_out
        first_up = [g for g in range(len(pieces)) if f"oth{g}" in BACKWARD and pieces[g][0] == U]
        first_up = min(first_up, key=lambda g: BACKWARD.index(f"oth{g}"))
        table[f"oth{first_up}"] = loaded(normed_load, table[f"oth{first_up}"])
        first_in = min((0, 1, 2), key=lambda g: BACKWARD.index(f"oth{g}"))
        table[f"oth{first_in}"] = loaded(input_load, table[f"oth{first_in}"])
        run_events(BACKWARD, table, attend_step, size)
        for g in (A, O):
            for j in range(tiles[g]):
                core_copy(g, j).wait_send()
        for k in range(5):
            v_copy(k).wait_send()
        for copy in copies.values():
            copy().wait_send()

    spans = [piece[2] if g == X else size * piece[2] for g, piece in enumerate(pieces)]
    anywhere, inside = pl.BlockSpec(memory_space=pl.ANY), pl.BlockSpec(memory_space=pltpu.VMEM)
    results = pl.pallas_call(
        body,
        out_shape=[jax.ShapeDtypeStruct((block, attn), F32)] * 4
        + [jax.ShapeDtypeStruct((block, units_each), F32)] * 2
        + [
            jax.ShapeDtypeStruct((rows, width), BF16),
            jax.ShapeDtypeStruct((vector_rows, 128), F32),
        ],
        in_specs=[anywhere, inside]
        + [anywhere] * 5
        + [inside, pl.BlockSpec(memory_space=pltpu.SMEM)]
        + [anywhere] * 7
        + [inside],
        out_specs=[inside] * 8,
        scratch_shapes=[
            pltpu.VMEM((2, width, TILE), BF16),
            pltpu.VMEM((rows, units), BF16),
            pltpu.VMEM((2, rows, TILE), F32),
            pltpu.VMEM((rows, units), BF16),
            pltpu.VMEM((rows, width), F32),
            pltpu.VMEM((rows, width), BF16),
            pltpu.VMEM((width, rows), BF16),
            pltpu.VMEM((rows, full[1]), BF16),
            pltpu.VMEM((2, 3, rows, attn), BF16),
            pltpu.VMEM((middle, units), BF16),
            pltpu.VMEM((1, units), F32),
            pltpu.VMEM((rows, width), BF16),
            pltpu.VMEM((width, rows), BF16),
            pltpu.VMEM((width, rows), BF16),
            pltpu.VMEM((rows, width), BF16),
        ]
        + [pltpu.VMEM((middle, c), BF16) for c in full]
        + [pltpu.VMEM((2, half, c), BF16) for c in spans]
        + [pltpu.VMEM((2, block, c), BF16) for c in spans]
        + [
            pltpu.VMEM((size - 1, 4 * block if g == X else block, piece[2]), BF16)
            for g, piece in enumerate(pieces)
        ]
        + [
            pltpu.VMEM((6, vector_rows, 128), F32),
            pltpu.VMEM((5, vector_rows, 128), F32),
            pltpu.SemaphoreType.DMA((3, 2)),
            pltpu.SemaphoreType.DMA((7,)),
            pltpu.SemaphoreType.DMA((4, units // TILE)),
            pltpu.SemaphoreType.DMA((4, units // TILE)),
            pltpu.SemaphoreType.DMA((len(pieces), 3 + size)),
            pltpu.SemaphoreType.DMA((len(pieces), 3 + size)),
            pltpu.SemaphoreType.DMA((5,)),
            pltpu.SemaphoreType.DMA((5,)),
        ],
        compiler_params=pltpu.CompilerParams(
            collective_id=BACKWARD_ID, has_side_effects=True, vmem_limit_bytes=63 * 2**20
        ),
        cost_estimate=pl.CostEstimate(
            flops=4 * rows * sum(full) * width,
            bytes_accessed=4 * sum(full) * width,
            transcendentals=0,
        ),
        name="backward_near",
    )(
        mixed_low, mixed_t, normed_t, input_t, context, grad_second, hidden, wide, lengths, active,
        slope, qkv, *weights, vectors,
    )
    return results[:6], results[6], results[7]


def gather_far(shard):
    return lax.all_gather(
        lax.all_gather(shard, "tensor", axis=1, tiled=True), "dp", axis=0, tiled=True
    )


def scatter_far(left_side, right_side):
    whole = contract_rows(left_side, right_side).astype(BF16)
    part = lax.psum_scatter(whole, "dp", scatter_dimension=0, tiled=True)
    return lax.psum_scatter(part, "tensor", scatter_dimension=1, tiled=True).astype(F32)


def soft_weights(queries, keys, visible, scale):
    scores = contract_cols(queries, keys) * scale
    scores = jnp.where(visible, scores, MASKED)
    exponent = jnp.exp(scores - jnp.max(scores, axis=-1, keepdims=True))
    return exponent * (1.0 / jnp.sum(exponent, axis=-1, keepdims=True))


def pairs_of(width, head_size):
    lanes = max(128, head_size)
    return [(start, lanes, lanes // head_size) for start in range(0, width, lanes)]


def keep_head(array, which, head_size):
    lane = lax.broadcasted_iota(jnp.int32, array.shape, 1)
    return jnp.where(lane // head_size == which, array, jnp.zeros_like(array))


def attend_forward(qkv_q, qkv_kv, length, head_size, groups):
    q_rows = qkv_q.shape[0]
    k_rows = qkv_kv.shape[0]
    block = qkv_q.shape[1] // groups
    width = block // 3
    scale = float(head_size) ** (-0.5)

    def body(length_ref, q_ref, kv_ref, out_ref):
        visible = lax.broadcasted_iota(jnp.int32, (q_rows, k_rows), 1) < length_ref[0]
        for start, lanes, held in pairs_of(width, head_size):
            queries = q_ref[:, start : start + lanes]
            keys = kv_ref[:, width + start : width + start + lanes]
            values = kv_ref[:, 2 * width + start : 2 * width + start + lanes]
            total = jnp.zeros((q_rows, lanes), F32)
            for which in range(held):
                probs = soft_weights(keep_head(queries, which, head_size), keys, visible, scale)
                total += keep_head(matmul(probs.astype(BF16), values), which, head_size)
            out_ref[:, start : start + lanes] = total.astype(BF16)

    return pl.pallas_call(
        body,
        out_shape=jax.ShapeDtypeStruct((q_rows, groups * width), BF16),
        grid_spec=pltpu.PrefetchScalarGridSpec(
            num_scalar_prefetch=1,
            grid=(groups,),
            in_specs=[
                pl.BlockSpec((q_rows, block), lambda g, length_ref: (0, g)),
                pl.BlockSpec((k_rows, block), lambda g, length_ref: (0, g)),
            ],
            out_specs=pl.BlockSpec((q_rows, width), lambda g, length_ref: (0, g)),
        ),
        cost_estimate=pl.CostEstimate(
            flops=4 * q_rows * k_rows * width * groups,
            bytes_accessed=2 * (2 * q_rows + 2 * k_rows) * width * groups,
            transcendentals=q_rows * k_rows * groups * width // head_size,
        ),
        name="attend_forward",
    )(length, qkv_q, qkv_kv)


def attend_backward(qkv_q, qkv_kv, grad_context, length, head_size, groups):
    q_rows = qkv_q.shape[0]
    k_rows = qkv_kv.shape[0]
    block = qkv_q.shape[1] // groups
    width = block // 3
    scale = float(head_size) ** (-0.5)

    def body(length_ref, q_ref, kv_ref, grad_ref, dq_ref, dkv_ref):
        visible = lax.broadcasted_iota(jnp.int32, (q_rows, k_rows), 1) < length_ref[0]
        for start, lanes, held in pairs_of(width, head_size):
            queries = q_ref[:, start : start + lanes]
            keys = kv_ref[:, width + start : width + start + lanes]
            values = kv_ref[:, 2 * width + start : 2 * width + start + lanes]
            grads = grad_ref[:, start : start + lanes]
            grad_q = jnp.zeros((q_rows, lanes), F32)
            grad_k = jnp.zeros((k_rows, lanes), F32)
            grad_v = jnp.zeros((k_rows, lanes), F32)
            for which in range(held):
                mine = keep_head(grads, which, head_size)
                query = keep_head(queries, which, head_size)
                probs = soft_weights(query, keys, visible, scale)
                grad_v += contract_rows(probs.astype(BF16), mine)
                grad_probs = contract_cols(mine, values)
                inner = jnp.sum(probs * grad_probs, axis=-1, keepdims=True)
                grad_scores = (probs * (grad_probs - inner)).astype(BF16)
                grad_q += keep_head(matmul(grad_scores, keys), which, head_size)
                grad_k += contract_rows(grad_scores, query)
            dq_ref[:, start : start + lanes] = (grad_q * scale).astype(BF16)
            dkv_ref[:, start : start + lanes] = (grad_k * scale).astype(BF16)
            dkv_ref[:, width + start : width + start + lanes] = grad_v.astype(BF16)

    return pl.pallas_call(
        body,
        out_shape=(
            jax.ShapeDtypeStruct((q_rows, groups * width), BF16),
            jax.ShapeDtypeStruct((k_rows, groups * 2 * width), BF16),
        ),
        grid_spec=pltpu.PrefetchScalarGridSpec(
            num_scalar_prefetch=1,
            grid=(groups,),
            in_specs=[
                pl.BlockSpec((q_rows, block), lambda g, length_ref: (0, g)),
                pl.BlockSpec((k_rows, block), lambda g, length_ref: (0, g)),
                pl.BlockSpec((q_rows, width), lambda g, length_ref: (0, g)),
            ],
            out_specs=[
                pl.BlockSpec((q_rows, width), lambda g, length_ref: (0, g)),
                pl.BlockSpec((k_rows, 2 * width), lambda g, length_ref: (0, g)),
            ],
        ),
        cost_estimate=pl.CostEstimate(
            flops=10 * q_rows * k_rows * width * groups,
            bytes_accessed=2 * (3 * q_rows + 4 * k_rows) * width * groups,
            transcendentals=q_rows * k_rows * groups * width // head_size,
        ),
        name="attend_backward",
    )(length, qkv_q, qkv_kv, grad_context)


def activate(total, bias):
    upper = total + bias
    cumulative = 0.5 * (1.0 + lax.erf(upper * math.sqrt(0.5)))
    density = jnp.exp(-0.5 * upper * upper) * (1.0 / math.sqrt(2.0 * math.pi))
    return upper * cumulative, cumulative + upper * density


def norm_forward(hidden, gain_vec, shift_vec):
    center = hidden - jnp.mean(hidden, axis=-1, keepdims=True)
    variance = jnp.mean(center * center, axis=-1, keepdims=True)
    inv_root = lax.rsqrt(variance + EPSILON)
    normal = center * inv_root
    return (normal * gain_vec + shift_vec, normal, inv_root)


def norm_backward(grad_in, normal, inv_root, gain_vec):
    grad_normal = grad_in * gain_vec
    grad_gain = jnp.sum(grad_in * normal, axis=0)
    grad_shift = jnp.sum(grad_in, axis=0)
    grad_hidden = inv_root * (
        grad_normal
        - jnp.mean(grad_normal, axis=-1, keepdims=True)
        - normal * jnp.mean(grad_normal * normal, axis=-1, keepdims=True)
    )
    return (grad_hidden, grad_gain, grad_shift)


def layer(
    hidden_in,
    cotangent,
    w_query,
    w_key,
    w_value,
    w_out,
    w_up,
    w_down,
    bias_query,
    bias_value,
    bias_out,
    bias_up,
    bias_down,
    gain_attn,
    shift_attn,
    gain_ffn,
    shift_ffn,
    valid_lengths,
):
    rows, model_width = hidden_in.shape
    n_tensor = lax.axis_size("tensor")
    n_data = lax.axis_size("dp")
    tensor_at = lax.axis_index("tensor")
    spread_over = rows * n_tensor // valid_lengths.shape[0] // rows
    head_size = model_width // HEADS
    head_cols = w_query.shape[1]
    factor = 1.0 / math.sqrt(rows * n_tensor * n_data)
    matrices = (w_query, w_key, w_value, w_out, w_up, w_down)
    wide = (bias_out, bias_down, gain_attn, shift_attn, gain_ffn, shift_ffn)

    if n_data == len(ORDER) and spread_over == 1:
        (
            qkv_full, out_full, up_full, down_full, qkv, context, hidden, active, slope, output,
            mixed_low, mixed_t, normed_t, input_t, grad_second, given, arranged,
        ) = forward_near(
            matrices, hidden_in, cotangent, wide, bias_query, bias_value, bias_up, valid_lengths,
            head_size,
        )
        grads, grad_input, sums = backward_near(
            mixed_low, mixed_t, normed_t, input_t, context, grad_second, hidden, arranged,
            valid_lengths, active, slope, qkv, (qkv_full, out_full, up_full, down_full), given,
            head_size,
        )
        lengths = [model_width // 128] * 8 + [bias_up.shape[0] // 128]
        results = scale_and_copy(grads, (grad_input, output), sums, lengths, factor)
        grads, (grad_input, output) = results[:6], results[6:8]
        vector_sums = [part.reshape(-1) for part in results[8:]]
    else:

        def column_part(vector):
            return vector.reshape(n_tensor, -1)

        query_bias, value_bias = column_part(bias_query), column_part(bias_value)
        bias_qkv = jnp.concatenate(
            [query_bias, jnp.zeros_like(query_bias), value_bias], axis=1
        ).reshape(1, -1)
        length = lax.dynamic_slice_in_dim(valid_lengths, tensor_at // spread_over, 1)
        low = [matrix.astype(BF16) for matrix in matrices]
        shards = [jnp.concatenate(low[:3], axis=1)] + low[3:]
        qkv_full, out_full, up_full, down_full = (gather_far(shard) for shard in shards)
        qkv = (matmul(hidden_in, qkv_full) + bias_qkv).astype(BF16)
        members = [list(range(k, k + spread_over)) for k in range(0, n_tensor, spread_over)]
        qkv_seq = lax.all_gather(qkv, "tensor", axis_index_groups=members, axis=0, tiled=True)
        context = attend_forward(qkv, qkv_seq, length, head_size, n_tensor)
        hidden = hidden_in.astype(F32) + contract_cols(context, out_full) + bias_out
        normed, normal_attn, root_attn = norm_forward(hidden, gain_attn, shift_attn)
        normed_low = normed.astype(BF16)
        active, slope = activate(matmul(normed_low, up_full), bias_up)
        active = active.astype(BF16)
        mixed = contract_cols(active, down_full)
        result, normal_ffn, root_ffn = norm_forward(normed + mixed + bias_down, gain_ffn, shift_ffn)
        output = result.astype(BF16)
        grad_second, grad_gain_ffn, grad_shift_ffn = norm_backward(
            cotangent.astype(F32), normal_ffn, root_ffn, gain_ffn
        )
        grad_bias_down = jnp.sum(grad_second, axis=0)
        mixed_low = grad_second.astype(BF16)
        grad_down = scatter_far(mixed_low, active)
        grad_upper = (matmul(mixed_low, down_full) * slope).astype(BF16)
        grad_bias_up = jnp.sum(grad_upper, axis=0, dtype=F32)
        grad_up = scatter_far(normed_low, grad_upper)
        grad_normed = grad_second + contract_cols(grad_upper, up_full)
        grad_first, grad_gain_attn, grad_shift_attn = norm_backward(
            grad_normed, normal_attn, root_attn, gain_attn
        )
        grad_bias_out = jnp.sum(grad_first, axis=0)
        attn_low = grad_first.astype(BF16)
        grad_context = matmul(attn_low, out_full).astype(BF16)
        grad_out = scatter_far(attn_low, context)
        grad_q, grad_kv = attend_backward(qkv, qkv_seq, grad_context, length, head_size, n_tensor)
        grad_kv = lax.psum_scatter(
            grad_kv.astype(F32),
            "tensor",
            scatter_dimension=0,
            axis_index_groups=members,
            tiled=True,
        ).astype(BF16)
        grad_qkv = jnp.concatenate(
            [grad_q.reshape(rows, n_tensor, -1), grad_kv.reshape(rows, n_tensor, -1)], axis=2
        ).reshape(rows, -1)
        grad_bias_qkv = jnp.sum(grad_qkv, axis=0, dtype=F32).reshape(n_tensor, 3, head_cols)
        grads = jnp.split(scatter_far(hidden_in, grad_qkv), 3, axis=1)
        grads = [grad * factor for grad in (*grads, grad_out, grad_up, grad_down)]
        grad_input = (grad_first + contract_cols(grad_qkv, qkv_full)).astype(BF16)
        sums = jnp.concatenate(
            [
                grad_bias_out,
                grad_bias_down,
                grad_gain_attn,
                grad_shift_attn,
                grad_gain_ffn,
                grad_shift_ffn,
                grad_bias_qkv[:, 0].reshape(-1),
                grad_bias_qkv[:, 2].reshape(-1),
                grad_bias_up,
            ]
        )
        sums = lax.psum(sums, ("dp", "tensor")) * factor
        vector_sums = jnp.split(sums, [k * model_width for k in range(1, 9)])
    (
        v_out, v_down, v_gain_attn, v_shift_attn, v_gain_ffn, v_shift_ffn, v_query, v_value, v_up,
    ) = vector_sums
    return (
        output,
        grad_input,
        *grads,
        v_query,
        v_value,
        v_out,
        v_up,
        v_down,
        v_gain_attn,
        v_shift_attn,
        v_gain_ffn,
        v_shift_ffn,
    )


def solution(mesh):
    tokens, matrix, copied = P(("dp", "tensor"), None), P("dp", "tensor"), P()
    return jax.shard_map(
        layer,
        mesh=mesh,
        in_specs=(tokens,) * 2 + (matrix,) * 6 + (copied,) * 9 + (P("dp"),),
        out_specs=(tokens,) * 2 + (matrix,) * 6 + (copied,) * 9,
        check_vma=False,
    )
```

```python
import math

import jax
import jax.numpy as jnp
from jax import lax
from jax.experimental import pallas as pl
from jax.experimental.pallas import tpu as pltpu
from jax.sharding import PartitionSpec as P

HEADS = 16
EPSILON = 1e-12
MASKED = -1e30
BF16 = jnp.bfloat16
F32 = jnp.float32

ORDER = (0, 2, 4, 6, 1, 3, 5, 7)
BIT_CORE, BIT_X, BIT_Y = 1, 2, 4


def matmul(left_side, right_side):
    return jnp.dot(left_side, right_side, preferred_element_type=F32)


def contract_rows(left_side, right_side):
    return lax.dot_general(
        left_side, right_side, (((0,), (0,)), ((), ())), preferred_element_type=F32
    )


def contract_cols(left_side, right_side):
    return lax.dot_general(
        left_side, right_side, (((1,), (1,)), ((), ())), preferred_element_type=F32
    )


FORWARD_ID = 1
BACKWARD_ID = 2
TILE = 512

FORWARD = (
    "z3", "lplane9", "fw3", "lcor9", "z1", "col3", "fw1", "z6", "z0", "col1", "fw0", "cor3",
    "z2", "col0", "fw2", "z5", "z4", "prep", "fw6", "z8", "cor1", "fw5", "last3", "col2", "fw4",
    "cor0", "cor2", "tr", "fw8", "col5", "z7", "last1", "last0", "col4", "col6", "last2", "fw7",
    "lz9", "qkv", "a0", "cor5", "cor4", "a1", "a2", "a3", "out", "fw9", "last5", "cor6", "col7",
    "norm", "col8", "last4", "last6", "up1", "cor7", "up2", "lcore9", "cor8", "up3", "last7",
    "lowX", "last8", "low1", "low2", "ln",
)
BACKWARD = (
    "oth8", "oth7", "gelA", "own8", "cor8", "own7", "cor7", "oth9", "oth4", "sid8", "gelB",
    "own9", "sid7", "oth5", "lz9", "oth6", "upA", "own4", "upB", "own5", "cor4", "cor5", "norm",
    "col8", "sid4", "own6", "out", "col7", "oth3", "a0", "own3", "cor3", "cor6", "a1", "col4",
    "sid5", "sid3", "a2", "a3", "oth1", "sid6", "vec", "oth2", "col5", "fin4", "own1", "cor1",
    "v0", "oth0", "col3", "v1", "own2", "cor2", "fin8", "sid1", "col6", "own0", "cor0", "fin7",
    "sid2", "v2", "col1", "dxA", "sid0", "col2", "lcor9", "dxB", "fin6", "col0", "v3", "sid9",
    "fin2", "v4", "gout", "fin5", "fin1", "fin3", "fin9", "v5", "fin0",
)


def neighbour(index, bit):
    return index + bit - 2 * bit * ((index // bit) % 2)


def block_of(index, mask):
    for bit in (BIT_CORE, BIT_X, BIT_Y):
        if mask & bit:
            index = neighbour(index, bit)
    return index


def pieces_of(size, attn, units_each):
    pieces = [(0, k * size * attn, attn) for k in range(3)] + [(1, 0, attn)]
    for weight in (2, 3):
        start = 0
        for count in (units_each // 2, units_each // 4, units_each // 4):
            pieces.append((weight, start * size, count))
            start += count
    return pieces


def run_events(order, table, attend, size):
    first = order.index("a0")
    last = order.index(f"a{size - 1}")
    for name in order[:first]:
        table[name]()

    def step(r, carry):
        attend(r)
        for k in range(size - 1):
            start = order.index(f"a{k}") + 1
            names = order[start : order.index(f"a{k + 1}")]
            if names:

                @pl.when(r == k)
                def _():
                    for name in names:
                        table[name]()

        return carry

    lax.fori_loop(0, size, step, 0)
    for name in order[last + 1 :]:
        table[name]()


def greet(partners):
    barrier = pltpu.get_barrier_semaphore()
    for partner in partners:
        pl.semaphore_signal(
            barrier, inc=1, device_id=partner, device_id_type=pl.DeviceIdType.MESH
        )


def await_greetings(partners):
    pl.semaphore_wait(pltpu.get_barrier_semaphore(), len(partners))


def scale_and_copy(scaled, copied, sums, lengths, factor):
    arrays = list(scaled) + list(copied)
    starts = [sum(lengths[:k]) for k in range(len(lengths))]

    def body(*refs):
        sums_ref, targets = refs[len(arrays)], refs[len(arrays) + 1 :]
        for k in range(len(arrays)):
            targets[k][...] = refs[k][...] * factor if k < len(scaled) else refs[k][...]
        for start, length, target in zip(starts, lengths, targets[len(arrays) :]):
            target[...] = sums_ref[start : start + length, :] * factor

    return pl.pallas_call(
        body,
        out_shape=[jax.ShapeDtypeStruct(array.shape, array.dtype) for array in arrays]
        + [jax.ShapeDtypeStruct((length, sums.shape[1]), F32) for length in lengths],
        in_specs=[pl.BlockSpec(memory_space=pltpu.VMEM)] * (len(arrays) + 1),
        out_specs=[pl.BlockSpec(memory_space=pltpu.VMEM)] * (len(arrays) + len(lengths)),
    )(*arrays, sums)


def forward_near(weights, hidden_in, cotangent, wide, bias_query, bias_value, bias_units, lengths, head_size):
    size = lax.axis_size("tensor")
    rows, width = hidden_in.shape
    block = width // len(ORDER)
    attn, units_each = weights[0].shape[1], weights[4].shape[1]
    cols = [3 * attn, attn, units_each, units_each]
    full = [(width, size * c) for c in cols]
    units = size * units_each
    half = block // 2
    pieces = pieces_of(size, attn, units_each)
    X = len(pieces) - 1
    pieces = pieces[:-3] + [pieces[-2], pieces[-1], pieces[-3]]
    A, O, U, _ = range(4)
    B_OUT, B_DOWN, G_ATTN, S_ATTN, G_FFN, S_FFN = range(6)

    def body(
        q_in, k_in, v_in, o_in, u_in, d_in, hidden_raw, cotangent_ref, bias_out_in, bias_down_in,
        gain_attn_in, shift_attn_in, gain_ffn_in, shift_ffn_in, bias_q_ref, bias_v_ref, bias_u_ref,
        lengths_ref,
        a_out, o_out, u_out, d_out, qkv_out, context_out, hidden_out, active_out, slope_out, output_ref,
        mixed_ref, mixed_t, normed_t, input_t, second_ref, sums_ref, wide_ref,
        a_ref, o_ref, u_ref, d_ref, x_ref, low_ref, active_ref, slope_ref, bias_ref, units_ref, qkv_ref,
        context_ref, hidden_ref, turned_x, turned_n, local_sem, send_sem, recv_sem,
        tile_sem,
    ):
        data_at, tensor_at = lax.axis_index("dp"), lax.axis_index("tensor")
        places = (a_ref, o_ref, u_ref, d_ref)

        def dp_partner(bit):
            return (neighbour(data_at, bit), tensor_at)

        def z_partner(step):
            return by_z[step]

        by_z = [(data_at, (tensor_at + step) % size) for step in range(size)]
        by_x, by_y, by_core = dp_partner(BIT_X), dp_partner(BIT_Y), dp_partner(BIT_CORE)
        owners = [block_of(data_at, mask) for mask in ORDER]
        copies = {}
        sent = {}

        def send(g, slot, source, target, device, when=None, lands=None):
            def copy():
                return pltpu.make_async_remote_copy(
                    src_ref=source,
                    dst_ref=target,
                    send_sem=send_sem.at[g, slot],
                    recv_sem=recv_sem.at[g, slot if lands is None else lands],
                    device_id=device,
                    device_id_type=pl.DeviceIdType.MESH,
                )

            copies[g, slot] = copy
            only(when, lambda: copy().start())
            sent[g, slot] = when

        def only(when, step):
            if when is None:
                step()
            else:
                pl.when(when())(step)

        def arrived(g, *slots):
            for slot in slots:
                copies[g, slot]().wait_recv()

        def whole(g, start, count):
            weight, first, wide_by = pieces[g]
            return places[weight].at[start : start + count, first : first + size * wide_by]

        def cell(g, start, count, r):
            weight, first, wide_by = pieces[g]
            at = first + r * wide_by
            return places[weight].at[start : start + count, at : at + wide_by]

        def send_z(g, count=block):
            send(g, 1, cell(g, 0, count, 0), cell(g, 0, count, 2), z_partner(2))
            send(g, 0, cell(g, 0, count, 0), cell(g, 0, count, 1), z_partner(1), lambda: tensor_at < size - 1)
            send(g, 2, cell(g, 0, count, 0), cell(g, 0, count, 3), z_partner(3), lambda: tensor_at > 0)

        def pass_on(g, count=block):
            arrived(g, 1)
            send(g, 9, cell(g, 0, count, 2), cell(g, 0, count, 1), z_partner(3), lambda: tensor_at == 1, 0)
            send(g, 10, cell(g, 0, count, 2), cell(g, 0, count, 3), z_partner(1), lambda: tensor_at == 2, 2)

        def send_column(g):
            arrived(g, 0, 2)
            send(g, 3, whole(g, 0, block), whole(g, block, block), by_x)
            send(g, 4, whole(g, 0, block), whole(g, 2 * block, block), by_y)

        def send_corner(g):
            arrived(g, 3, 4)
            send(g, 5, whole(g, block, half), whole(g, 3 * block, half), by_y)
            send(g, 6, whole(g, 2 * block + half, half), whole(g, 3 * block + half, half), by_x)
            send(g, 7, whole(g, 0, 3 * block), whole(g, 4 * block, 3 * block), by_core)

        def send_last(g):
            arrived(g, 5, 6)
            send(g, 8, whole(g, 3 * block, block), whole(g, 7 * block, block), by_core)

        def complete(*group):
            for g in group:
                arrived(g, 7, 8)

        def late_plane():
            send(X, 3, cell(X, 0, block, 0), cell(X, block, block, 0), by_x)
            send(X, 4, cell(X, 0, block, 0), cell(X, 2 * block, block, 0), by_y)

        def late_corner():
            arrived(X, 3, 4)
            send(X, 5, cell(X, block, half, 0), cell(X, 3 * block, half, 0), by_y)
            send(X, 6, cell(X, 2 * block + half, half, 0), cell(X, 3 * block + half, half, 0), by_x)

        def late_z():
            arrived(X, 5, 6)
            send_z(X, 4 * block)

        def late_core():
            arrived(X, 0, 2)
            send(X, 7, whole(X, 0, 4 * block), whole(X, 4 * block, 4 * block), by_core)

        saves = []

        def save(slot, source, target):
            copy = pltpu.make_async_copy(source, target, local_sem.at[slot])
            copy.start()
            saves.append(copy)

        def save_weight(slot, g):
            target = (a_out, o_out, u_out, d_out)[g]
            save(slot, places[g], target)

        sources = (q_in, k_in, v_in, o_in, u_in, u_in, u_in, d_in, d_in, d_in)

        def cast(g):
            weight, first, wide_by = pieces[g]
            start = first // size if weight >= U else 0
            places[weight][:block, first : first + wide_by] = sources[g][
                :, start : start + wide_by
            ].astype(BF16)

        partners = [by_x, by_y, by_core] + by_z[1:]
        greet(partners)
        for g in range(len(pieces)):
            cast(g)
        await_greetings(partners)

        def lanes_of(owner):
            return pl.ds(pl.multiple_of(owner * block, block), block)

        def turn(target, at, rows_of):
            for k in range(width // 128):
                target[k * 128 : (k + 1) * 128, at] = rows_of[:, k * 128 : (k + 1) * 128].T.astype(BF16)

        def vector(k):
            return wide_ref[k : k + 1, :]

        def column_of(r, first, span):
            at = ((tensor_at + size - r) % size) * (first[1]) + first[0]
            return pl.ds(pl.multiple_of(at, 128), span)

        def prepare():
            for place, owner in enumerate(owners):
                at = slice(place * block, (place + 1) * block)
                x_ref[:, at] = hidden_raw[:, lanes_of(owner)]
                for k, ref in enumerate(
                    (bias_out_in, bias_down_in, gain_attn_in, shift_attn_in, gain_ffn_in, shift_ffn_in)
                ):
                    wide_ref[k : k + 1, at] = ref[:, lanes_of(owner)]
            for r in range(size):
                at = slice(r * attn, (r + 1) * attn)
                bias_ref[0:1, at] = bias_q_ref[:, column_of(r, (0, attn), attn)]
                bias_ref[1:2, at] = bias_v_ref[:, column_of(r, (0, attn), attn)]
                for weight, first, wide_by in pieces:
                    if weight == U:
                        at = slice(first + r * wide_by, first + (r + 1) * wide_by)
                        units_ref[:, at] = bias_u_ref[
                            :, column_of(r, (first // size, units_each), wide_by)
                        ]

        def turn_inputs():
            def one(j, carry):
                at = pl.ds(pl.multiple_of(j * 128, 128), 128)
                turn(turned_x, at, x_ref[at, :].astype(F32))
                return carry

            lax.fori_loop(0, rows // 128, one, 0)
            save(4, turned_x, input_t)

        def project(j, carry):
            at = pl.ds(pl.multiple_of(j * attn, attn), attn)
            total = matmul(x_ref[...], a_ref[:, at])
            which = j // size
            bias = bias_ref[:, pl.ds(pl.multiple_of((j % size) * attn, attn), attn)]
            bias = jnp.where(which == 0, bias[0:1], jnp.where(which == 2, bias[1:2], 0.0))
            qkv_ref[:, at] = (total + bias).astype(BF16)
            return carry

        def qkv():
            complete(0, 1, 2)
            save_weight(A, A)
            lax.fori_loop(0, 3 * size, project, 0)
            save(5, qkv_ref, qkv_out)

        scale = float(head_size) ** (-0.5)
        length = lengths_ref[tensor_at]

        def attend(r):
            seen = lax.broadcasted_iota(jnp.int32, (rows, rows), 1) < length
            for start, lanes, held in pairs_of(attn, head_size):
                at = [
                    pl.ds(pl.multiple_of((k * size + r) * attn + start, 128), lanes) for k in range(3)
                ]
                queries, keys, values = (qkv_ref[:, where] for where in at)
                total = jnp.zeros((rows, lanes), F32)
                for which in range(held):
                    probs = soft_weights(keep_head(queries, which, head_size), keys, seen, scale)
                    total += keep_head(matmul(probs.astype(BF16), values), which, head_size)
                context_ref[:, at[0]] = total.astype(BF16)

        def output(j, carry):
            at = pl.ds(pl.multiple_of(j * 256, 256), 256)
            total = contract_cols(context_ref[...], o_ref[at, :])
            hidden_ref[:, at] = x_ref[:, at].astype(F32) + total + wide_ref[B_OUT : B_OUT + 1, at]
            return carry

        def out():
            complete(3)
            save_weight(O, O)
            save(6, context_ref, context_out)
            lax.fori_loop(0, width // 256, output, 0)
            save(7, hidden_ref, hidden_out)

        chunk = 128

        def norm_step(j, carry):
            at = pl.ds(pl.multiple_of(j * chunk, chunk), chunk)
            normed = norm_forward(hidden_ref[at, :], vector(G_ATTN), vector(S_ATTN))[0]
            low_ref[at, :] = normed.astype(BF16)
            second_ref[at, :] = normed + vector(B_DOWN)
            turn(turned_n, at, normed)
            return carry

        def norm():
            lax.fori_loop(0, rows // chunk, norm_step, 0)
            save(8, turned_n, normed_t)

        def tile_at(j):
            return pl.ds(pl.multiple_of(j * TILE, TILE), TILE)

        def slope_copy(j):
            return pltpu.make_async_copy(
                slope_ref.at[j % 2], slope_out.at[:, tile_at(j)], tile_sem.at[1, j % 2]
            )

        def active_copy(j):
            return pltpu.make_async_copy(
                active_ref.at[:, tile_at(j)], active_out.at[:, tile_at(j)], tile_sem.at[0, j]
            )

        def raise_up(j, carry):
            @pl.when(j >= 2)
            def _():
                slope_copy(j - 2).wait()

            total = matmul(low_ref[...], u_ref[:, tile_at(j)])
            active, slope = activate(total, units_ref[:, tile_at(j)])
            active_ref[:, tile_at(j)] = active.astype(BF16)
            slope_ref[j % 2] = slope
            active_copy(j).start()
            slope_copy(j).start()
            return carry

        def span_of(g):
            _, first, wide_by = pieces[g]
            return slice(first, first + size * wide_by)

        def raise_piece(g):
            complete(g)
            save(g + 5, u_ref.at[:, span_of(g)], u_out.at[:, span_of(g)])
            at = span_of(g)
            lax.fori_loop(at.start // TILE, at.stop // TILE, raise_up, 0)

        def lower_piece(g):
            if g == X:
                arrived(X, 7)
            else:
                complete(g)
            at = span_of(g)
            save(g + 5, d_ref.at[:, at], d_out.at[:, at])

            def one(j, carry):
                to = pl.ds(pl.multiple_of(j * 256, 256), 256)
                second_ref[:, to] += contract_cols(active_ref[:, at], d_ref[to, at])
                return carry

            lax.fori_loop(0, width // 256, one, 0)

        def second(j, sums):
            at = pl.ds(pl.multiple_of(j * chunk, chunk), chunk)
            result, normal, root = norm_forward(second_ref[at, :], vector(G_FFN), vector(S_FFN))
            grads = jnp.concatenate([cotangent_ref[at, lanes_of(owner)] for owner in owners], axis=1)
            for place, owner in enumerate(owners):
                output_ref[at, lanes_of(owner)] = result[:, place * block : (place + 1) * block].astype(BF16)
            hidden, more_gain, more_shift = norm_backward(
                grads.astype(F32), normal, root, vector(G_FFN)
            )
            second_ref[at, :] = hidden
            mixed_ref[at, :] = hidden.astype(BF16)
            turn(mixed_t, at, hidden)
            more = (jnp.sum(hidden, axis=0), more_gain, more_shift)
            return tuple(a + b[None] for a, b in zip(sums, more))

        def last_norm():
            zero = jnp.zeros((1, width), F32)
            sums = lax.fori_loop(0, rows // chunk, second, (zero, zero, zero))
            for k in range(3):
                sums_ref[k : k + 1, :] = sums[k]

        def bound(step, *given):
            return lambda: step(*given)

        table = {
            "prep": prepare, "tr": turn_inputs, "qkv": qkv, "out": out, "norm": norm, "ln": last_norm,
            "up1": bound(raise_piece, 4), "up2": bound(raise_piece, 5), "up3": bound(raise_piece, 6),
            "low1": bound(lower_piece, 7), "low2": bound(lower_piece, 8), "lowX": bound(lower_piece, X),
            "fw9": bound(pass_on, X, 4 * block), "lplane9": late_plane, "lcor9": late_corner, "lz9": late_z, "lcore9": late_core,
        }
        for g in range(X):
            table[f"z{g}"] = bound(send_z, g)
            table[f"fw{g}"] = bound(pass_on, g)
            table[f"col{g}"] = bound(send_column, g)
            table[f"cor{g}"] = bound(send_corner, g)
            table[f"last{g}"] = bound(send_last, g)
        run_events(FORWARD, table, attend, size)

        def settle(j, carry):
            active_copy(j).wait()
            return carry

        lax.fori_loop(0, units // TILE, settle, 0)
        for j in (units // TILE - 2, units // TILE - 1):
            slope_copy(j).wait()
        for copy in saves:
            copy.wait()
        for key, copy in copies.items():
            only(sent[key], lambda: copy().wait_send())

    anywhere, inside = pl.BlockSpec(memory_space=pl.ANY), pl.BlockSpec(memory_space=pltpu.VMEM)
    tall = jax.ShapeDtypeStruct((rows, width), BF16)
    turned = jax.ShapeDtypeStruct((width, rows), BF16)
    return pl.pallas_call(
        body,
        out_shape=[jax.ShapeDtypeStruct(shape, BF16) for shape in full]
        + [
            jax.ShapeDtypeStruct((rows, full[A][1]), BF16),
            tall,
            jax.ShapeDtypeStruct((rows, width), F32),
            jax.ShapeDtypeStruct((rows, units), BF16),
            jax.ShapeDtypeStruct((rows, units), F32),
            tall,
            tall,
            turned,
            turned,
            turned,
            jax.ShapeDtypeStruct((rows, width), F32),
            jax.ShapeDtypeStruct((3, width), F32),
            jax.ShapeDtypeStruct((6, width), F32),
        ],
        in_specs=[inside] * 17 + [pl.BlockSpec(memory_space=pltpu.SMEM)],
        out_specs=[anywhere] * 9 + [inside] * 3 + [anywhere] * 2 + [inside] * 3,
        scratch_shapes=[pltpu.VMEM(shape, BF16) for shape in full]
        + [
            pltpu.VMEM((rows, width), BF16),
            pltpu.VMEM((rows, width), BF16),
            pltpu.VMEM((rows, units), BF16),
            pltpu.VMEM((2, rows, TILE), F32),
            pltpu.VMEM((2, size * attn), F32),
            pltpu.VMEM((1, units), F32),
            pltpu.VMEM((rows, full[A][1]), BF16),
            pltpu.VMEM((rows, width), BF16),
            pltpu.VMEM((rows, width), F32),
            pltpu.VMEM((width, rows), BF16),
            pltpu.VMEM((width, rows), BF16),
            pltpu.SemaphoreType.DMA((5 + len(pieces),)),
            pltpu.SemaphoreType.DMA((len(pieces), 11)),
            pltpu.SemaphoreType.DMA((len(pieces), 11)),
            pltpu.SemaphoreType.DMA((2, units // TILE)),
        ],
        compiler_params=pltpu.CompilerParams(
            collective_id=FORWARD_ID, has_side_effects=True, vmem_limit_bytes=63 * 2**20
        ),
        cost_estimate=pl.CostEstimate(
            flops=2 * rows * width * sum(shape[1] for shape in full),
            bytes_accessed=4 * width * sum(shape[1] for shape in full),
            transcendentals=rows * units,
        ),
        name="forward_near",
    )(
        *weights, hidden_in, cotangent, *(vector[None] for vector in wide), bias_query[None],
        bias_value[None], bias_units[None], lengths,
    )


def backward_near(mixed_low, mixed_t, normed_t, input_t, context, grad_second, hidden, wide, lengths,
                  active, slope, qkv, weights, vectors, head_size):
    size = lax.axis_size("tensor")
    rows, width = mixed_low.shape
    block = width // len(ORDER)
    middle = width // 2
    half = block // 2
    full = [weight.shape[1] for weight in weights]
    units = full[2]
    units_each = units // size
    attn = full[1] // size
    pieces = pieces_of(size, attn, units_each)
    X = len(pieces) - 1
    A, O, U, D = range(4)
    tiles = [c // TILE for c in full]
    vector_rows = (6 * width + 2 * full[1] + units) // 128
    v_query, v_value, v_up = 6 * width // 128, (6 * width + full[1]) // 128, (6 * width + 2 * full[1]) // 128
    scale = float(head_size) ** (-0.5)

    def body(
        mixed_in, mixed_t, normed_in, input_in, context_in, second_in, hidden_in, wide_ref,
        lengths_ref, active_in, slope_in, qkv_in, a_in, o_in, u_in, d_in, vectors_ref,
        q_out, k_out, v_out, o_out, u_out, d_out, grad_out, sums_out,
        w_buf, act_ref, slope_buf, gu_ref, grad_ref, low_ref, low_t, gctx_ref, qkv_buf, send_buf,
        units_sum, mixed_ref, normed_t, input_t, context_ref, a_plane, o_plane, u_plane, d_plane, *rest,
    ):
        count = len(pieces)
        corners, sides, zins = (rest[k * count : (k + 1) * count] for k in range(3))
        (
            v_ref, v_in, load_sem, start_sem, core_send, core_recv, send_sem, recv_sem, v_send, v_recv,
        ) = rest[3 * count :]
        data_at, tensor_at = lax.axis_index("dp"), lax.axis_index("tensor")
        planes = (a_plane, o_plane, u_plane, d_plane)
        outs = (q_out, k_out, v_out, o_out, u_out, u_out, u_out, d_out, d_out, d_out)
        shift_by = (tiles[O], 0, 0, 0)

        def dp_partner(bit):
            return (neighbour(data_at, bit), tensor_at)

        def z_partner(step):
            return by_z[step % size]

        by_z = [(data_at, (tensor_at + step) % size) for step in range(size)]

        by_x, by_y, by_core = dp_partner(BIT_X), dp_partner(BIT_Y), dp_partner(BIT_CORE)

        def column(j, span=TILE):
            return pl.ds(pl.multiple_of(j * span, 128), span)

        def load(row, source, buffer, j):
            return pltpu.make_async_copy(
                source.at[:, column(j)], buffer.at[j % 2], load_sem.at[row, j % 2]
            )

        def over_tiles(first, last, loads, step):
            for row, source, buffer in loads:
                load(row, source, buffer, first).start()

            def one(j, carry):
                @pl.when(j + 1 < last)
                def _():
                    for row, source, buffer in loads:
                        load(row, source, buffer, j + 1).start()

                for row, source, buffer in loads:
                    load(row, source, buffer, j).wait()
                step(j)
                return carry

            lax.fori_loop(first, last, one, 0)

        def remote(source, target, send, receive, device):
            return pltpu.make_async_remote_copy(
                src_ref=source,
                dst_ref=target,
                send_sem=send,
                recv_sem=receive,
                device_id=device,
                device_id_type=pl.DeviceIdType.MESH,
            )

        def core_copy(g, j):
            return remote(
                send_buf.at[:, column(j + shift_by[g])],
                planes[g].at[:, column(j)],
                core_send.at[g, j],
                core_recv.at[g, j],
                by_core,
            )

        copies = {}

        def send(g, slot, source, target, device):
            def copy():
                return remote(source, target(), send_sem.at[g, slot], recv_sem.at[g, slot], device)

            copies[g, slot] = copy
            copy().start()

        def arrived(g, *slots):
            for slot in slots:
                copies[g, slot]().wait_recv()

        def other_tile(g, left_t, right, j):
            send_buf[:, column(j + shift_by[g])] = matmul(left_t[middle:, :], right).astype(BF16)
            core_copy(g, j).start()

        def own_tile(g, left_t, right, j):
            core_copy(g, j).wait_recv()
            total = matmul(left_t[:middle, :], right) + planes[g][:, column(j)].astype(F32)
            planes[g][:, column(j)] = total.astype(BF16)

        def span(g):
            _, first, wide_by = pieces[g]
            return first, wide_by if g == X else size * wide_by

        def plane_rows(g, start, count):
            first, wide_by = span(g)
            return planes[pieces[g][0]].at[start : start + count, first : first + wide_by]

        def send_corner(g):
            send(g, 0, plane_rows(g, 3 * block, half), lambda: corners[g].at[0], by_x)
            send(g, 1, plane_rows(g, 3 * block + half, half), lambda: corners[g].at[1], by_y)

        def add_rows(g, start, count, *more):
            plane = planes[pieces[g][0]]
            first, wide_by = span(g)
            step = min(TILE, wide_by)
            for at in range(0, wide_by, step):
                where = (slice(start, start + count), slice(first + at, first + at + step))
                total = plane[where].astype(F32)
                for ref in more:
                    total += ref[:, at : at + step].astype(F32)
                plane[where] = total.astype(BF16)

        def send_sides(g):
            arrived(g, 0, 1)
            add_rows(g, 2 * block, half, corners[g].at[0])
            add_rows(g, block + half, half, corners[g].at[1])
            send(g, 2, plane_rows(g, block, block), lambda: sides[g].at[0], by_x)
            send(g, 3, plane_rows(g, 2 * block, block), lambda: sides[g].at[1], by_y)

        def out_of(g):
            weight, first, wide_by = pieces[g]
            start = first // size if weight >= U else 0
            return outs[g].at[:, start : start + wide_by]

        def send_column(g):
            arrived(g, 2, 3)
            weight, first, wide_by = pieces[g]
            for r in range(size):
                at = slice(r * wide_by, (r + 1) * wide_by)
                own = slice(first + r * wide_by, first + (r + 1) * wide_by)
                total = planes[weight][:block, own].astype(F32)
                total += sides[g][0, :, at].astype(F32) + sides[g][1, :, at].astype(F32)
                if r == 0:
                    out_of(g)[...] = total
                else:
                    planes[weight][:block, own] = total.astype(BF16)
                    send(g, 3 + r, planes[weight].at[:block, own], lambda r=r: zins[g].at[r - 1], z_partner(-r))

        def finish(g):
            arrived(g, *range(4, 3 + size))
            total = out_of(g)[...]
            for r in range(1, size):
                total += zins[g][r - 1].astype(F32)
            out_of(g)[...] = total

        def late_z():
            weight, first, wide_by = pieces[X]
            for r in range(1, size):
                own = slice(first + r * wide_by, first + (r + 1) * wide_by)
                send(X, 3 + r, planes[weight].at[:, own], lambda r=r: zins[X].at[r - 1], z_partner(-r))

        def late_corner():
            arrived(X, *range(4, 3 + size))
            for k in range(4):
                rows_k = slice(k * block, (k + 1) * block)
                add_rows(X, k * block, block, *(zins[X].at[r, rows_k] for r in range(size - 1)))
            send_corner(X)

        def late_finish():
            arrived(X, 2, 3)
            total = plane_rows(X, 0, block)[...].astype(F32)
            out_of(X)[...] = total + sides[X][0].astype(F32) + sides[X][1].astype(F32)

        def feature_rows(k, vector):
            for place, mask in enumerate(ORDER):
                at = block_of(data_at, mask)
                v_ref[0, pl.ds(k * len(ORDER) + at, 1), :] = vector[:, place * 128 : (place + 1) * 128]

        z_near = tensor_at + 1 - 2 * (tensor_at % 2)
        z_across = tensor_at + 2 - 4 * ((tensor_at // 2) % 2)
        v_partners = (by_core, (data_at, z_near), (data_at, z_across), by_x, by_y)

        def v_copy(k):
            return remote(v_ref.at[k], v_in.at[k], v_send.at[k], v_recv.at[k], v_partners[k])

        def v_add(k):
            v_copy(k).wait_recv()
            v_ref[k + 1] = v_ref[k] + v_in[k]

        early = [
            pltpu.make_async_copy(
                active_in.at[:, k * (units // 2) : (k + 1) * (units // 2)],
                act_ref.at[:, k * (units // 2) : (k + 1) * (units // 2)],
                start_sem.at[k],
            )
            for k in range(2)
        ]
        grad_load, mixed_load, normed_load, context_load, input_load = (
            pltpu.make_async_copy(source, target, start_sem.at[k])
            for k, (source, target) in enumerate(
                (
                    (second_in, grad_ref),
                    (mixed_in, mixed_ref),
                    (normed_in, normed_t),
                    (context_in, context_ref),
                    (input_in, input_t),
                ),
                2,
            )
        )
        for copy in early:
            copy.start()
        for copy in (mixed_load, normed_load, grad_load, context_load, input_load):
            copy.start()
        partners = [by_x, by_y, by_core] + by_z[1:]
        greet(partners)
        await_greetings(partners)

        def each(first, last, step):
            def one(j, carry):
                step(j)
                return carry

            lax.fori_loop(first, last, one, 0)

        def other_down(j):
            other_tile(D, mixed_t, act_ref[:, column(j)], j)

        def own_down(j):
            own_tile(D, mixed_t, act_ref[:, column(j)], j)

        def other_up(j):
            core_copy(D, j).wait_send()
            other_tile(U, normed_t, gu_ref[:, column(j)], j)

        def own_up(j):
            own_tile(U, normed_t, gu_ref[:, column(j)], j)

        def bounds(g):
            _, first, wide_by = pieces[g]
            return first // TILE, (first + size * wide_by) // TILE

        early[0].wait()
        early[1].wait()

        def loaded(copy, step):
            def both():
                copy.wait()
                step()

            return both

        def bound(step, *given):
            return lambda: step(*given)

        def gelu_step(j):
            low = (matmul(mixed_ref[...], w_buf[j % 2]) * slope_buf[j % 2]).astype(BF16)
            gu_ref[:, column(j)] = low
            units_sum[:, column(j)] = jnp.sum(low.astype(F32), axis=0, keepdims=True)

        gelu_loads = [(1, d_in, w_buf), (2, slope_in, slope_buf)]
        hidden_loads = [
            pltpu.make_async_copy(hidden_in.at[:, column(k)], slope_buf.at[k], load_sem.at[2, k])
            for k in range(2)
        ]

        def second_gelu():
            over_tiles(tiles[D] // 2, tiles[D], gelu_loads, gelu_step)
            for copy in hidden_loads:
                copy.start()

        def up_step(j):
            grad_ref[...] += contract_cols(gu_ref[:, column(j)], w_buf[j % 2])

        def sum_units():
            for k in range(3):
                feature_rows((1, 4, 5)[k], vectors_ref[k : k + 1, :])
            for r in range(size):
                for weight, first, wide_by in pieces:
                    if weight == U:
                        for k in range(wide_by // 128):
                            place = ((tensor_at + size - r) % size) * (units_each // 128)
                            place += (first // size) // 128 + k
                            at = first + r * wide_by + k * 128
                            v_ref[0, pl.ds(v_up + place, 1), :] = units_sum[:, at : at + 128]

        chunk = 128

        def norm_step(j, sums):
            at = pl.ds(pl.multiple_of(j * chunk, chunk), chunk)
            hidden_rows = jnp.concatenate([slope_buf[0, at, :], slope_buf[1, at, :]], axis=1)
            gain = wide_ref[2:3, :]
            normal, root = norm_forward(hidden_rows, gain, gain)[1:]
            hidden, more_gain, more_shift = norm_backward(grad_ref[at, :], normal, root, gain)
            grad_ref[at, :] = hidden
            low_ref[at, :] = hidden.astype(BF16)
            for k in range(width // 128):
                low_t[k * 128 : (k + 1) * 128, at] = hidden[:, k * 128 : (k + 1) * 128].T.astype(BF16)
            more = (jnp.sum(hidden, axis=0), more_gain, more_shift)
            return tuple(a + b[None] for a, b in zip(sums, more))

        def norm():
            for copy in hidden_loads:
                copy.wait()
            zero = jnp.zeros((1, width), F32)
            sums = lax.fori_loop(0, rows // chunk, norm_step, (zero, zero, zero))
            for k in range(3):
                feature_rows((0, 2, 3)[k], sums[k])

        def out_step(j):
            core_copy(U, j).wait_send()
            gctx_ref[:, column(j)] = matmul(low_ref[...], w_buf[j % 2]).astype(BF16)
            other_tile(O, low_t, context_ref[:, column(j)], j)

        def out():
            context_load.wait()
            over_tiles(0, tiles[O], [(1, o_in, w_buf)], out_step)
            for copy in qkv_load(0):
                copy.start()

        def own_out():
            for j in range(tiles[O]):
                own_tile(O, low_t, context_ref[:, j * TILE : (j + 1) * TILE], j)

        def qkv_load(r):
            return [
                pltpu.make_async_copy(
                    qkv_in.at[:, column(k * size + r, attn)], qkv_buf.at[r % 2, k], load_sem.at[k, r % 2]
                )
                for k in range(3)
            ]

        def attend_step(r):
            @pl.when(r + 1 < size)
            def _():
                for copy in qkv_load(r + 1):
                    copy.start()

            for copy in qkv_load(r):
                copy.wait()
            slot = r % 2
            seen = lax.broadcasted_iota(jnp.int32, (rows, rows), 0) < length
            for start, lanes, held in pairs_of(attn, head_size):
                queries, keys, values = (qkv_buf[slot, k, :, start : start + lanes] for k in range(3))
                grads = gctx_ref[:, pl.ds(pl.multiple_of(r * attn + start, 128), lanes)]
                grad_q = jnp.zeros((rows, lanes), F32)
                grad_k = jnp.zeros((rows, lanes), F32)
                grad_v = jnp.zeros((rows, lanes), F32)
                for which in range(held):
                    mine = keep_head(grads, which, head_size)
                    query = keep_head(queries, which, head_size)
                    scores = jnp.where(seen, contract_cols(keys, query) * scale, MASKED)
                    exponent = jnp.exp(scores - jnp.max(scores, axis=0, keepdims=True))
                    probs = exponent * (1.0 / jnp.sum(exponent, axis=0, keepdims=True))
                    grad_v += matmul(probs.astype(BF16), mine)
                    grad_probs = contract_cols(values, mine)
                    inner = jnp.sum(probs * grad_probs, axis=0, keepdims=True)
                    grad_scores = (probs * (grad_probs - inner)).astype(BF16)
                    grad_q += keep_head(contract_rows(grad_scores, keys), which, head_size)
                    grad_k += matmul(grad_scores, query)
                low_q = (grad_q * scale).astype(BF16)
                low_v = grad_v.astype(BF16)
                for k, low in enumerate((low_q, (grad_k * scale).astype(BF16), low_v)):
                    at = pl.multiple_of((k * size + r) * attn + start, 128)
                    gu_ref[:, pl.ds(at, lanes)] = low
                place = ((tensor_at + size - r) % size) * (attn // 128) + start // 128
                v_ref[0, pl.ds(v_query + place, 1), :] = jnp.sum(
                    low_q.astype(F32), axis=0, keepdims=True
                )
                v_ref[0, pl.ds(v_value + place, 1), :] = jnp.sum(
                    low_v.astype(F32), axis=0, keepdims=True
                )

        length = lengths_ref[tensor_at]

        def other_qkv(j):
            core_copy(U, j + tiles[O]).wait_send()
            other_tile(A, input_t, gu_ref[:, column(j)], j)

        def own_qkv(j):
            own_tile(A, input_t, gu_ref[:, column(j)], j)

        def input_step(j):
            grad_ref[...] += contract_cols(gu_ref[:, column(j)], w_buf[j % 2])

        def give_input():
            for place, mask in enumerate(ORDER):
                at = block_of(data_at, mask)
                grad_out[:, pl.ds(pl.multiple_of(at * block, block), block)] = grad_ref[
                    :, place * block : (place + 1) * block
                ].astype(BF16)

        def give_sums():
            v_add(4)
            sums_out[...] = v_ref[5]

        def next_sum(k):
            v_add(k - 1)
            v_copy(k).start()

        weight_loads = [[(1, ref, w_buf)] for ref in (a_in, o_in, u_in, d_in)]
        parts = (
            (other_qkv, own_qkv), (other_qkv, own_qkv), (other_qkv, own_qkv), (lambda j: None, own_out),
            (other_up, own_up), (other_up, own_up), (other_up, own_up), (other_down, own_down),
            (other_down, own_down), (other_down, own_down),
        )
        halves = [(0, count // 2, count) for count in tiles]
        table = {
            "gelA": loaded(mixed_load, bound(over_tiles, 0, halves[D][1], gelu_loads, gelu_step)),
            "gelB": second_gelu,
            "upA": loaded(grad_load, bound(over_tiles, 0, halves[U][1], weight_loads[U], up_step)),
            "upB": bound(over_tiles, *halves[U][1:], weight_loads[U], up_step),
            "vec": sum_units,
            "norm": norm,
            "out": out,
            "dxA": bound(over_tiles, 0, halves[A][1], weight_loads[A], input_step),
            "dxB": bound(over_tiles, *halves[A][1:], weight_loads[A], input_step),
            "gout": give_input,
            "lz9": late_z,
            "lcor9": late_corner,
            "sid9": bound(send_sides, X),
            "fin9": late_finish,
            "v0": lambda: v_copy(0).start(),
            "v5": give_sums,
        }
        for k in range(1, 5):
            table[f"v{k}"] = bound(next_sum, k)
        for g in range(len(pieces)):
            other, own = parts[g]
            table[f"oth{g}"] = bound(each, *bounds(g), other)
            table[f"own{g}"] = bound(each, *bounds(g), own)
            if g < X:
                table[f"cor{g}"] = bound(send_corner, g)
                table[f"sid{g}"] = bound(send_sides, g)
                table[f"col{g}"] = bound(send_column, g)
                table[f"fin{g}"] = bound(finish, g)
        table["oth3"] = lambda: None
        table["own3"] = own_out
        first_up = [g for g in range(len(pieces)) if f"oth{g}" in BACKWARD and pieces[g][0] == U]
        first_up = min(first_up, key=lambda g: BACKWARD.index(f"oth{g}"))
        table[f"oth{first_up}"] = loaded(normed_load, table[f"oth{first_up}"])
        first_in = min((0, 1, 2), key=lambda g: BACKWARD.index(f"oth{g}"))
        table[f"oth{first_in}"] = loaded(input_load, table[f"oth{first_in}"])
        run_events(BACKWARD, table, attend_step, size)
        for g in (A, O):
            for j in range(tiles[g]):
                core_copy(g, j).wait_send()
        for k in range(5):
            v_copy(k).wait_send()
        for copy in copies.values():
            copy().wait_send()

    spans = [piece[2] if g == X else size * piece[2] for g, piece in enumerate(pieces)]
    anywhere, inside = pl.BlockSpec(memory_space=pl.ANY), pl.BlockSpec(memory_space=pltpu.VMEM)
    results = pl.pallas_call(
        body,
        out_shape=[jax.ShapeDtypeStruct((block, attn), F32)] * 4
        + [jax.ShapeDtypeStruct((block, units_each), F32)] * 2
        + [
            jax.ShapeDtypeStruct((rows, width), BF16),
            jax.ShapeDtypeStruct((vector_rows, 128), F32),
        ],
        in_specs=[anywhere, inside]
        + [anywhere] * 5
        + [inside, pl.BlockSpec(memory_space=pltpu.SMEM)]
        + [anywhere] * 7
        + [inside],
        out_specs=[inside] * 8,
        scratch_shapes=[
            pltpu.VMEM((2, width, TILE), BF16),
            pltpu.VMEM((rows, units), BF16),
            pltpu.VMEM((2, rows, TILE), F32),
            pltpu.VMEM((rows, units), BF16),
            pltpu.VMEM((rows, width), F32),
            pltpu.VMEM((rows, width), BF16),
            pltpu.VMEM((width, rows), BF16),
            pltpu.VMEM((rows, full[1]), BF16),
            pltpu.VMEM((2, 3, rows, attn), BF16),
            pltpu.VMEM((middle, units), BF16),
            pltpu.VMEM((1, units), F32),
            pltpu.VMEM((rows, width), BF16),
            pltpu.VMEM((width, rows), BF16),
            pltpu.VMEM((width, rows), BF16),
            pltpu.VMEM((rows, width), BF16),
        ]
        + [pltpu.VMEM((middle, c), BF16) for c in full]
        + [pltpu.VMEM((2, half, c), BF16) for c in spans]
        + [pltpu.VMEM((2, block, c), BF16) for c in spans]
        + [
            pltpu.VMEM((size - 1, 4 * block if g == X else block, piece[2]), BF16)
            for g, piece in enumerate(pieces)
        ]
        + [
            pltpu.VMEM((6, vector_rows, 128), F32),
            pltpu.VMEM((5, vector_rows, 128), F32),
            pltpu.SemaphoreType.DMA((3, 2)),
            pltpu.SemaphoreType.DMA((7,)),
            pltpu.SemaphoreType.DMA((4, units // TILE)),
            pltpu.SemaphoreType.DMA((4, units // TILE)),
            pltpu.SemaphoreType.DMA((len(pieces), 3 + size)),
            pltpu.SemaphoreType.DMA((len(pieces), 3 + size)),
            pltpu.SemaphoreType.DMA((5,)),
            pltpu.SemaphoreType.DMA((5,)),
        ],
        compiler_params=pltpu.CompilerParams(
            collective_id=BACKWARD_ID, has_side_effects=True, vmem_limit_bytes=63 * 2**20
        ),
        cost_estimate=pl.CostEstimate(
            flops=4 * rows * sum(full) * width,
            bytes_accessed=4 * sum(full) * width,
            transcendentals=0,
        ),
        name="backward_near",
    )(
        mixed_low, mixed_t, normed_t, input_t, context, grad_second, hidden, wide, lengths, active,
        slope, qkv, *weights, vectors,
    )
    return results[:6], results[6], results[7]


def gather_far(shard):
    return lax.all_gather(
        lax.all_gather(shard, "tensor", axis=1, tiled=True), "dp", axis=0, tiled=True
    )


def scatter_far(left_side, right_side):
    whole = contract_rows(left_side, right_side).astype(BF16)
    part = lax.psum_scatter(whole, "dp", scatter_dimension=0, tiled=True)
    return lax.psum_scatter(part, "tensor", scatter_dimension=1, tiled=True).astype(F32)


def soft_weights(queries, keys, visible, scale):
    scores = contract_cols(queries, keys) * scale
    scores = jnp.where(visible, scores, MASKED)
    exponent = jnp.exp(scores - jnp.max(scores, axis=-1, keepdims=True))
    return exponent * (1.0 / jnp.sum(exponent, axis=-1, keepdims=True))


def pairs_of(width, head_size):
    lanes = max(128, head_size)
    return [(start, lanes, lanes // head_size) for start in range(0, width, lanes)]


def keep_head(array, which, head_size):
    lane = lax.broadcasted_iota(jnp.int32, array.shape, 1)
    return jnp.where(lane // head_size == which, array, jnp.zeros_like(array))


def attend_forward(qkv_q, qkv_kv, length, head_size, groups):
    q_rows = qkv_q.shape[0]
    k_rows = qkv_kv.shape[0]
    block = qkv_q.shape[1] // groups
    width = block // 3
    scale = float(head_size) ** (-0.5)

    def body(length_ref, q_ref, kv_ref, out_ref):
        visible = lax.broadcasted_iota(jnp.int32, (q_rows, k_rows), 1) < length_ref[0]
        for start, lanes, held in pairs_of(width, head_size):
            queries = q_ref[:, start : start + lanes]
            keys = kv_ref[:, width + start : width + start + lanes]
            values = kv_ref[:, 2 * width + start : 2 * width + start + lanes]
            total = jnp.zeros((q_rows, lanes), F32)
            for which in range(held):
                probs = soft_weights(keep_head(queries, which, head_size), keys, visible, scale)
                total += keep_head(matmul(probs.astype(BF16), values), which, head_size)
            out_ref[:, start : start + lanes] = total.astype(BF16)

    return pl.pallas_call(
        body,
        out_shape=jax.ShapeDtypeStruct((q_rows, groups * width), BF16),
        grid_spec=pltpu.PrefetchScalarGridSpec(
            num_scalar_prefetch=1,
            grid=(groups,),
            in_specs=[
                pl.BlockSpec((q_rows, block), lambda g, length_ref: (0, g)),
                pl.BlockSpec((k_rows, block), lambda g, length_ref: (0, g)),
            ],
            out_specs=pl.BlockSpec((q_rows, width), lambda g, length_ref: (0, g)),
        ),
        cost_estimate=pl.CostEstimate(
            flops=4 * q_rows * k_rows * width * groups,
            bytes_accessed=2 * (2 * q_rows + 2 * k_rows) * width * groups,
            transcendentals=q_rows * k_rows * groups * width // head_size,
        ),
        name="attend_forward",
    )(length, qkv_q, qkv_kv)


def attend_backward(qkv_q, qkv_kv, grad_context, length, head_size, groups):
    q_rows = qkv_q.shape[0]
    k_rows = qkv_kv.shape[0]
    block = qkv_q.shape[1] // groups
    width = block // 3
    scale = float(head_size) ** (-0.5)

    def body(length_ref, q_ref, kv_ref, grad_ref, dq_ref, dkv_ref):
        visible = lax.broadcasted_iota(jnp.int32, (q_rows, k_rows), 1) < length_ref[0]
        for start, lanes, held in pairs_of(width, head_size):
            queries = q_ref[:, start : start + lanes]
            keys = kv_ref[:, width + start : width + start + lanes]
            values = kv_ref[:, 2 * width + start : 2 * width + start + lanes]
            grads = grad_ref[:, start : start + lanes]
            grad_q = jnp.zeros((q_rows, lanes), F32)
            grad_k = jnp.zeros((k_rows, lanes), F32)
            grad_v = jnp.zeros((k_rows, lanes), F32)
            for which in range(held):
                mine = keep_head(grads, which, head_size)
                query = keep_head(queries, which, head_size)
                probs = soft_weights(query, keys, visible, scale)
                grad_v += contract_rows(probs.astype(BF16), mine)
                grad_probs = contract_cols(mine, values)
                inner = jnp.sum(probs * grad_probs, axis=-1, keepdims=True)
                grad_scores = (probs * (grad_probs - inner)).astype(BF16)
                grad_q += keep_head(matmul(grad_scores, keys), which, head_size)
                grad_k += contract_rows(grad_scores, query)
            dq_ref[:, start : start + lanes] = (grad_q * scale).astype(BF16)
            dkv_ref[:, start : start + lanes] = (grad_k * scale).astype(BF16)
            dkv_ref[:, width + start : width + start + lanes] = grad_v.astype(BF16)

    return pl.pallas_call(
        body,
        out_shape=(
            jax.ShapeDtypeStruct((q_rows, groups * width), BF16),
            jax.ShapeDtypeStruct((k_rows, groups * 2 * width), BF16),
        ),
        grid_spec=pltpu.PrefetchScalarGridSpec(
            num_scalar_prefetch=1,
            grid=(groups,),
            in_specs=[
                pl.BlockSpec((q_rows, block), lambda g, length_ref: (0, g)),
                pl.BlockSpec((k_rows, block), lambda g, length_ref: (0, g)),
                pl.BlockSpec((q_rows, width), lambda g, length_ref: (0, g)),
            ],
            out_specs=[
                pl.BlockSpec((q_rows, width), lambda g, length_ref: (0, g)),
                pl.BlockSpec((k_rows, 2 * width), lambda g, length_ref: (0, g)),
            ],
        ),
        cost_estimate=pl.CostEstimate(
            flops=10 * q_rows * k_rows * width * groups,
            bytes_accessed=2 * (3 * q_rows + 4 * k_rows) * width * groups,
            transcendentals=q_rows * k_rows * groups * width // head_size,
        ),
        name="attend_backward",
    )(length, qkv_q, qkv_kv, grad_context)


def activate(total, bias):
    upper = total + bias
    cumulative = 0.5 * (1.0 + lax.erf(upper * math.sqrt(0.5)))
    density = jnp.exp(-0.5 * upper * upper) * (1.0 / math.sqrt(2.0 * math.pi))
    return upper * cumulative, cumulative + upper * density


def norm_forward(hidden, gain_vec, shift_vec):
    center = hidden - jnp.mean(hidden, axis=-1, keepdims=True)
    variance = jnp.mean(center * center, axis=-1, keepdims=True)
    inv_root = lax.rsqrt(variance + EPSILON)
    normal = center * inv_root
    return (normal * gain_vec + shift_vec, normal, inv_root)


def norm_backward(grad_in, normal, inv_root, gain_vec):
    grad_normal = grad_in * gain_vec
    grad_gain = jnp.sum(grad_in * normal, axis=0)
    grad_shift = jnp.sum(grad_in, axis=0)
    grad_hidden = inv_root * (
        grad_normal
        - jnp.mean(grad_normal, axis=-1, keepdims=True)
        - normal * jnp.mean(grad_normal * normal, axis=-1, keepdims=True)
    )
    return (grad_hidden, grad_gain, grad_shift)


def layer(
    hidden_in,
    cotangent,
    w_query,
    w_key,
    w_value,
    w_out,
    w_up,
    w_down,
    bias_query,
    bias_value,
    bias_out,
    bias_up,
    bias_down,
    gain_attn,
    shift_attn,
    gain_ffn,
    shift_ffn,
    valid_lengths,
):
    rows, model_width = hidden_in.shape
    n_tensor = lax.axis_size("tensor")
    n_data = lax.axis_size("dp")
    tensor_at = lax.axis_index("tensor")
    spread_over = rows * n_tensor // valid_lengths.shape[0] // rows
    head_size = model_width // HEADS
    head_cols = w_query.shape[1]
    factor = 1.0 / math.sqrt(rows * n_tensor * n_data)
    matrices = (w_query, w_key, w_value, w_out, w_up, w_down)
    wide = (bias_out, bias_down, gain_attn, shift_attn, gain_ffn, shift_ffn)

    if n_data == len(ORDER) and n_tensor == 4 and spread_over == 1:
        (
            qkv_full, out_full, up_full, down_full, qkv, context, hidden, active, slope, output,
            mixed_low, mixed_t, normed_t, input_t, grad_second, given, arranged,
        ) = forward_near(
            matrices, hidden_in, cotangent, wide, bias_query, bias_value, bias_up, valid_lengths,
            head_size,
        )
        grads, grad_input, sums = backward_near(
            mixed_low, mixed_t, normed_t, input_t, context, grad_second, hidden, arranged,
            valid_lengths, active, slope, qkv, (qkv_full, out_full, up_full, down_full), given,
            head_size,
        )
        lengths = [model_width // 128] * 8 + [bias_up.shape[0] // 128]
        results = scale_and_copy(grads, (grad_input, output), sums, lengths, factor)
        grads, (grad_input, output) = results[:6], results[6:8]
        vector_sums = [part.reshape(-1) for part in results[8:]]
    else:

        def column_part(vector):
            return vector.reshape(n_tensor, -1)

        query_bias, value_bias = column_part(bias_query), column_part(bias_value)
        bias_qkv = jnp.concatenate(
            [query_bias, jnp.zeros_like(query_bias), value_bias], axis=1
        ).reshape(1, -1)
        length = lax.dynamic_slice_in_dim(valid_lengths, tensor_at // spread_over, 1)
        low = [matrix.astype(BF16) for matrix in matrices]
        shards = [jnp.concatenate(low[:3], axis=1)] + low[3:]
        qkv_full, out_full, up_full, down_full = (gather_far(shard) for shard in shards)
        qkv = (matmul(hidden_in, qkv_full) + bias_qkv).astype(BF16)
        members = [list(range(k, k + spread_over)) for k in range(0, n_tensor, spread_over)]
        qkv_seq = lax.all_gather(qkv, "tensor", axis_index_groups=members, axis=0, tiled=True)
        context = attend_forward(qkv, qkv_seq, length, head_size, n_tensor)
        hidden = hidden_in.astype(F32) + contract_cols(context, out_full) + bias_out
        normed, normal_attn, root_attn = norm_forward(hidden, gain_attn, shift_attn)
        normed_low = normed.astype(BF16)
        active, slope = activate(matmul(normed_low, up_full), bias_up)
        active = active.astype(BF16)
        mixed = contract_cols(active, down_full)
        result, normal_ffn, root_ffn = norm_forward(normed + mixed + bias_down, gain_ffn, shift_ffn)
        output = result.astype(BF16)
        grad_second, grad_gain_ffn, grad_shift_ffn = norm_backward(
            cotangent.astype(F32), normal_ffn, root_ffn, gain_ffn
        )
        grad_bias_down = jnp.sum(grad_second, axis=0)
        mixed_low = grad_second.astype(BF16)
        grad_down = scatter_far(mixed_low, active)
        grad_upper = (matmul(mixed_low, down_full) * slope).astype(BF16)
        grad_bias_up = jnp.sum(grad_upper, axis=0, dtype=F32)
        grad_up = scatter_far(normed_low, grad_upper)
        grad_normed = grad_second + contract_cols(grad_upper, up_full)
        grad_first, grad_gain_attn, grad_shift_attn = norm_backward(
            grad_normed, normal_attn, root_attn, gain_attn
        )
        grad_bias_out = jnp.sum(grad_first, axis=0)
        attn_low = grad_first.astype(BF16)
        grad_context = matmul(attn_low, out_full).astype(BF16)
        grad_out = scatter_far(attn_low, context)
        grad_q, grad_kv = attend_backward(qkv, qkv_seq, grad_context, length, head_size, n_tensor)
        grad_kv = lax.psum_scatter(
            grad_kv.astype(F32),
            "tensor",
            scatter_dimension=0,
            axis_index_groups=members,
            tiled=True,
        ).astype(BF16)
        grad_qkv = jnp.concatenate(
            [grad_q.reshape(rows, n_tensor, -1), grad_kv.reshape(rows, n_tensor, -1)], axis=2
        ).reshape(rows, -1)
        grad_bias_qkv = jnp.sum(grad_qkv, axis=0, dtype=F32).reshape(n_tensor, 3, head_cols)
        grads = jnp.split(scatter_far(hidden_in, grad_qkv), 3, axis=1)
        grads = [grad * factor for grad in (*grads, grad_out, grad_up, grad_down)]
        grad_input = (grad_first + contract_cols(grad_qkv, qkv_full)).astype(BF16)
        sums = jnp.concatenate(
            [
                grad_bias_out,
                grad_bias_down,
                grad_gain_attn,
                grad_shift_attn,
                grad_gain_ffn,
                grad_shift_ffn,
                grad_bias_qkv[:, 0].reshape(-1),
                grad_bias_qkv[:, 2].reshape(-1),
                grad_bias_up,
            ]
        )
        sums = lax.psum(sums, ("dp", "tensor")) * factor
        vector_sums = jnp.split(sums, [k * model_width for k in range(1, 9)])
    (
        v_out, v_down, v_gain_attn, v_shift_attn, v_gain_ffn, v_shift_ffn, v_query, v_value, v_up,
    ) = vector_sums
    return (
        output,
        grad_input,
        *grads,
        v_query,
        v_value,
        v_out,
        v_up,
        v_down,
        v_gain_attn,
        v_shift_attn,
        v_gain_ffn,
        v_shift_ffn,
    )


def solution(mesh):
    tokens, matrix, copied = P(("dp", "tensor"), None), P("dp", "tensor"), P()
    return jax.shard_map(
        layer,
        mesh=mesh,
        in_specs=(tokens,) * 2 + (matrix,) * 6 + (copied,) * 9 + (P("dp"),),
        out_specs=(tokens,) * 2 + (matrix,) * 6 + (copied,) * 9,
        check_vma=False,
    )
```

```python
import math

import jax
import jax.numpy as jnp
from jax import lax
from jax.experimental import pallas as pl
from jax.experimental.pallas import tpu as pltpu
from jax.sharding import PartitionSpec as P

HEADS = 16
EPSILON = 1e-12
MASKED = -1e30
BF16 = jnp.bfloat16
F32 = jnp.float32

ORDER = (0, 2, 4, 6, 1, 3, 5, 7)
BIT_CORE, BIT_X, BIT_Y = 1, 2, 4


def matmul(left_side, right_side):
    return jnp.dot(left_side, right_side, preferred_element_type=F32)


def contract_rows(left_side, right_side):
    return lax.dot_general(
        left_side, right_side, (((0,), (0,)), ((), ())), preferred_element_type=F32
    )


def contract_cols(left_side, right_side):
    return lax.dot_general(
        left_side, right_side, (((1,), (1,)), ((), ())), preferred_element_type=F32
    )


FORWARD_ID = 1
BACKWARD_ID = 2
TILE = 512

FORWARD = (
    "lplane9", "z3", "fw3", "z1", "lcor9", "col3", "fw1", "z2", "fw2", "col1", "z0", "col2",
    "cor3", "z8", "z6", "fw0", "cor1", "z4", "z7", "z5", "col0", "cor2", "fw6", "prep", "fw8",
    "cor0", "tr", "col6", "fw4", "fw5", "lz9", "col4", "last2", "last0", "last1", "qkv", "a0",
    "cor6", "col5", "a1", "a2", "fw7", "last3", "a3", "out", "cor4", "fw9", "norm", "cor5",
    "last4", "col7", "col8", "last5", "last6", "up1", "lcore9", "up2", "cor7", "up3", "cor8",
    "lowX", "last7", "last8", "low1", "low2", "ln",
)
BACKWARD = (
    "oth7", "oth9", "gelA", "own7", "oth8", "cor7", "oth4", "gelB", "own9", "own8", "cor8",
    "lz9", "own4", "cor4", "sid7", "upA", "upB", "oth5", "oth6", "sid4", "sid8", "norm", "out",
    "own5", "own6", "cor5", "a0", "col4", "col7", "cor6", "oth3", "a1", "sid5", "own3", "cor3",
    "fw9", "sid6", "a2", "a3", "oth2", "fw4", "sid3", "oth0", "vec", "oth1", "col8", "own2",
    "own0", "cor0", "col5", "own1", "col6", "v0", "cor2", "fw8", "fw7", "cor1", "fin4", "fw5",
    "sid0", "dxA", "fw6", "col3", "sid1", "fin7", "v1", "dxB", "sid2", "fw3", "col0", "v2",
    "col1", "fw0", "lcor9", "gout", "col2", "fin6", "fin8", "fin5", "v3", "sid9", "fw1", "fin0",
    "fin3", "fw2", "v4", "fin9", "fin1", "fin2", "v5",
)


def neighbour(index, bit):
    return index + bit - 2 * bit * ((index // bit) % 2)


def block_of(index, mask):
    for bit in (BIT_CORE, BIT_X, BIT_Y):
        if mask & bit:
            index = neighbour(index, bit)
    return index


def pieces_of(size, attn, units_each):
    pieces = [(0, k * size * attn, attn) for k in range(3)] + [(1, 0, attn)]
    for weight in (2, 3):
        start = 0
        for count in (units_each // 2, units_each // 4, units_each // 4):
            pieces.append((weight, start * size, count))
            start += count
    return pieces


def run_events(order, table, attend, size):
    first = order.index("a0")
    last = order.index(f"a{size - 1}")
    for name in order[:first]:
        table[name]()

    def step(r, carry):
        attend(r)
        for k in range(size - 1):
            start = order.index(f"a{k}") + 1
            names = order[start : order.index(f"a{k + 1}")]
            if names:

                @pl.when(r == k)
                def _():
                    for name in names:
                        table[name]()

        return carry

    lax.fori_loop(0, size, step, 0)
    for name in order[last + 1 :]:
        table[name]()


def greet(partners):
    barrier = pltpu.get_barrier_semaphore()
    for partner in partners:
        pl.semaphore_signal(
            barrier, inc=1, device_id=partner, device_id_type=pl.DeviceIdType.MESH
        )


def await_greetings(partners):
    pl.semaphore_wait(pltpu.get_barrier_semaphore(), len(partners))


def scale_and_copy(scaled, copied, sums, lengths, factor):
    arrays = list(scaled) + list(copied)
    starts = [sum(lengths[:k]) for k in range(len(lengths))]

    def body(*refs):
        sums_ref, targets = refs[len(arrays)], refs[len(arrays) + 1 :]
        for k in range(len(arrays)):
            targets[k][...] = refs[k][...] * factor if k < len(scaled) else refs[k][...]
        for start, length, target in zip(starts, lengths, targets[len(arrays) :]):
            target[...] = sums_ref[start : start + length, :] * factor

    return pl.pallas_call(
        body,
        out_shape=[jax.ShapeDtypeStruct(array.shape, array.dtype) for array in arrays]
        + [jax.ShapeDtypeStruct((length, sums.shape[1]), F32) for length in lengths],
        in_specs=[pl.BlockSpec(memory_space=pltpu.VMEM)] * (len(arrays) + 1),
        out_specs=[pl.BlockSpec(memory_space=pltpu.VMEM)] * (len(arrays) + len(lengths)),
    )(*arrays, sums)


def forward_near(weights, hidden_in, cotangent, wide, bias_query, bias_value, bias_units, lengths, head_size):
    size = lax.axis_size("tensor")
    rows, width = hidden_in.shape
    block = width // len(ORDER)
    attn, units_each = weights[0].shape[1], weights[4].shape[1]
    cols = [3 * attn, attn, units_each, units_each]
    full = [(width, size * c) for c in cols]
    units = size * units_each
    half = block // 2
    pieces = pieces_of(size, attn, units_each)
    X = len(pieces) - 1
    pieces = pieces[:-3] + [pieces[-2], pieces[-1], pieces[-3]]
    A, O, U, _ = range(4)
    B_OUT, B_DOWN, G_ATTN, S_ATTN, G_FFN, S_FFN = range(6)

    def body(
        q_in, k_in, v_in, o_in, u_in, d_in, hidden_raw, cotangent_ref, bias_out_in, bias_down_in,
        gain_attn_in, shift_attn_in, gain_ffn_in, shift_ffn_in, bias_q_ref, bias_v_ref, bias_u_ref,
        lengths_ref,
        a_out, o_out, u_out, d_out, qkv_out, context_out, hidden_out, active_out, slope_out, output_ref,
        mixed_ref, mixed_t, normed_t, input_t, second_ref, sums_ref, wide_ref,
        a_ref, o_ref, u_ref, d_ref, x_ref, low_ref, active_ref, slope_ref, bias_ref, units_ref, qkv_ref,
        context_ref, hidden_ref, turned_x, turned_n, local_sem, send_sem, recv_sem,
        tile_sem,
    ):
        data_at, tensor_at = lax.axis_index("dp"), lax.axis_index("tensor")
        places = (a_ref, o_ref, u_ref, d_ref)

        def dp_partner(bit):
            return (neighbour(data_at, bit), tensor_at)

        def z_partner(step):
            return by_z[step]

        by_z = [(data_at, (tensor_at + step) % size) for step in range(size)]
        by_x, by_y, by_core = dp_partner(BIT_X), dp_partner(BIT_Y), dp_partner(BIT_CORE)
        owners = [block_of(data_at, mask) for mask in ORDER]
        copies = {}
        sent = {}

        def send(g, slot, source, target, device, when=None, lands=None):
            def copy():
                return pltpu.make_async_remote_copy(
                    src_ref=source,
                    dst_ref=target,
                    send_sem=send_sem.at[g, slot],
                    recv_sem=recv_sem.at[g, slot if lands is None else lands],
                    device_id=device,
                    device_id_type=pl.DeviceIdType.MESH,
                )

            copies[g, slot] = copy
            only(when, lambda: copy().start())
            sent[g, slot] = when

        def only(when, step):
            if when is None:
                step()
            else:
                pl.when(when())(step)

        def arrived(g, *slots):
            for slot in slots:
                copies[g, slot]().wait_recv()

        def whole(g, start, count):
            weight, first, wide_by = pieces[g]
            return places[weight].at[start : start + count, first : first + size * wide_by]

        def cell(g, start, count, r):
            weight, first, wide_by = pieces[g]
            at = first + r * wide_by
            return places[weight].at[start : start + count, at : at + wide_by]

        def send_z(g, count=block):
            send(g, 1, cell(g, 0, count, 0), cell(g, 0, count, 2), z_partner(2))
            send(g, 0, cell(g, 0, count, 0), cell(g, 0, count, 1), z_partner(1), lambda: tensor_at < size - 1)
            send(g, 2, cell(g, 0, count, 0), cell(g, 0, count, 3), z_partner(3), lambda: tensor_at > 0)

        def pass_on(g, count=block):
            arrived(g, 1)
            send(g, 9, cell(g, 0, count, 2), cell(g, 0, count, 1), z_partner(3), lambda: tensor_at == 1, 0)
            send(g, 10, cell(g, 0, count, 2), cell(g, 0, count, 3), z_partner(1), lambda: tensor_at == 2, 2)

        def send_column(g):
            arrived(g, 0, 2)
            send(g, 3, whole(g, 0, block), whole(g, block, block), by_x)
            send(g, 4, whole(g, 0, block), whole(g, 2 * block, block), by_y)

        def send_corner(g):
            arrived(g, 3, 4)
            send(g, 5, whole(g, block, half), whole(g, 3 * block, half), by_y)
            send(g, 6, whole(g, 2 * block + half, half), whole(g, 3 * block + half, half), by_x)
            send(g, 7, whole(g, 0, 3 * block), whole(g, 4 * block, 3 * block), by_core)

        def send_last(g):
            arrived(g, 5, 6)
            send(g, 8, whole(g, 3 * block, block), whole(g, 7 * block, block), by_core)

        def complete(*group):
            for g in group:
                arrived(g, 7, 8)

        def late_plane():
            send(X, 3, cell(X, 0, block, 0), cell(X, block, block, 0), by_x)
            send(X, 4, cell(X, 0, block, 0), cell(X, 2 * block, block, 0), by_y)

        def late_corner():
            arrived(X, 3, 4)
            send(X, 5, cell(X, block, half, 0), cell(X, 3 * block, half, 0), by_y)
            send(X, 6, cell(X, 2 * block + half, half, 0), cell(X, 3 * block + half, half, 0), by_x)

        def late_z():
            arrived(X, 5, 6)
            send_z(X, 4 * block)

        def late_core():
            arrived(X, 0, 2)
            send(X, 7, whole(X, 0, 4 * block), whole(X, 4 * block, 4 * block), by_core)

        saves = []

        def save(slot, source, target):
            copy = pltpu.make_async_copy(source, target, local_sem.at[slot])
            copy.start()
            saves.append(copy)

        def save_weight(slot, g):
            target = (a_out, o_out, u_out, d_out)[g]
            save(slot, places[g], target)

        sources = (q_in, k_in, v_in, o_in, u_in, u_in, u_in, d_in, d_in, d_in)

        def cast(g):
            weight, first, wide_by = pieces[g]
            start = first // size if weight >= U else 0
            places[weight][:block, first : first + wide_by] = sources[g][
                :, start : start + wide_by
            ].astype(BF16)

        partners = [by_x, by_y, by_core] + by_z[1:]
        greet(partners)
        for g in range(len(pieces)):
            cast(g)
        await_greetings(partners)

        def lanes_of(owner):
            return pl.ds(pl.multiple_of(owner * block, block), block)

        def turn(target, at, rows_of):
            for k in range(width // 128):
                target[k * 128 : (k + 1) * 128, at] = rows_of[:, k * 128 : (k + 1) * 128].T.astype(BF16)

        def vector(k):
            return wide_ref[k : k + 1, :]

        def column_of(r, first, span):
            at = ((tensor_at + size - r) % size) * (first[1]) + first[0]
            return pl.ds(pl.multiple_of(at, 128), span)

        def prepare():
            for place, owner in enumerate(owners):
                at = slice(place * block, (place + 1) * block)
                x_ref[:, at] = hidden_raw[:, lanes_of(owner)]
                for k, ref in enumerate(
                    (bias_out_in, bias_down_in, gain_attn_in, shift_attn_in, gain_ffn_in, shift_ffn_in)
                ):
                    wide_ref[k : k + 1, at] = ref[:, lanes_of(owner)]
            for r in range(size):
                at = slice(r * attn, (r + 1) * attn)
                bias_ref[0:1, at] = bias_q_ref[:, column_of(r, (0, attn), attn)]
                bias_ref[1:2, at] = bias_v_ref[:, column_of(r, (0, attn), attn)]
                for weight, first, wide_by in pieces:
                    if weight == U:
                        at = slice(first + r * wide_by, first + (r + 1) * wide_by)
                        units_ref[:, at] = bias_u_ref[
                            :, column_of(r, (first // size, units_each), wide_by)
                        ]

        def turn_inputs():
            def one(j, carry):
                at = pl.ds(pl.multiple_of(j * 128, 128), 128)
                turn(turned_x, at, x_ref[at, :].astype(F32))
                return carry

            lax.fori_loop(0, rows // 128, one, 0)
            save(4, turned_x, input_t)

        def project(j, carry):
            at = pl.ds(pl.multiple_of(j * attn, attn), attn)
            total = matmul(x_ref[...], a_ref[:, at])
            which = j // size
            bias = bias_ref[:, pl.ds(pl.multiple_of((j % size) * attn, attn), attn)]
            bias = jnp.where(which == 0, bias[0:1], jnp.where(which == 2, bias[1:2], 0.0))
            qkv_ref[:, at] = (total + bias).astype(BF16)
            return carry

        def qkv():
            complete(0, 1, 2)
            save_weight(A, A)
            lax.fori_loop(0, 3 * size, project, 0)
            save(5, qkv_ref, qkv_out)

        scale = float(head_size) ** (-0.5)
        length = lengths_ref[tensor_at]

        def attend(r):
            seen = lax.broadcasted_iota(jnp.int32, (rows, rows), 1) < length
            for start, lanes, held in pairs_of(attn, head_size):
                at = [
                    pl.ds(pl.multiple_of((k * size + r) * attn + start, 128), lanes) for k in range(3)
                ]
                queries, keys, values = (qkv_ref[:, where] for where in at)
                total = jnp.zeros((rows, lanes), F32)
                for which in range(held):
                    probs = soft_weights(keep_head(queries, which, head_size), keys, seen, scale)
                    total += keep_head(matmul(probs.astype(BF16), values), which, head_size)
                context_ref[:, at[0]] = total.astype(BF16)

        def output(j, carry):
            at = pl.ds(pl.multiple_of(j * 256, 256), 256)
            total = contract_cols(context_ref[...], o_ref[at, :])
            hidden_ref[:, at] = x_ref[:, at].astype(F32) + total + wide_ref[B_OUT : B_OUT + 1, at]
            return carry

        def out():
            complete(3)
            save_weight(O, O)
            save(6, context_ref, context_out)
            lax.fori_loop(0, width // 256, output, 0)
            save(7, hidden_ref, hidden_out)

        chunk = 128

        def norm_step(j, carry):
            at = pl.ds(pl.multiple_of(j * chunk, chunk), chunk)
            normed = norm_forward(hidden_ref[at, :], vector(G_ATTN), vector(S_ATTN))[0]
            low_ref[at, :] = normed.astype(BF16)
            second_ref[at, :] = normed + vector(B_DOWN)
            turn(turned_n, at, normed)
            return carry

        def norm():
            lax.fori_loop(0, rows // chunk, norm_step, 0)
            save(8, turned_n, normed_t)

        def tile_at(j):
            return pl.ds(pl.multiple_of(j * TILE, TILE), TILE)

        def slope_copy(j):
            return pltpu.make_async_copy(
                slope_ref.at[j % 2], slope_out.at[:, tile_at(j)], tile_sem.at[1, j % 2]
            )

        def active_copy(j):
            return pltpu.make_async_copy(
                active_ref.at[:, tile_at(j)], active_out.at[:, tile_at(j)], tile_sem.at[0, j]
            )

        def raise_up(j, carry):
            @pl.when(j >= 2)
            def _():
                slope_copy(j - 2).wait()

            total = matmul(low_ref[...], u_ref[:, tile_at(j)])
            active, slope = activate(total, units_ref[:, tile_at(j)])
            active_ref[:, tile_at(j)] = active.astype(BF16)
            slope_ref[j % 2] = slope
            active_copy(j).start()
            slope_copy(j).start()
            return carry

        def span_of(g):
            _, first, wide_by = pieces[g]
            return slice(first, first + size * wide_by)

        def raise_piece(g):
            complete(g)
            save(g + 5, u_ref.at[:, span_of(g)], u_out.at[:, span_of(g)])
            at = span_of(g)
            lax.fori_loop(at.start // TILE, at.stop // TILE, raise_up, 0)

        def lower_piece(g):
            if g == X:
                arrived(X, 7)
            else:
                complete(g)
            at = span_of(g)
            save(g + 5, d_ref.at[:, at], d_out.at[:, at])

            def one(j, carry):
                to = pl.ds(pl.multiple_of(j * 256, 256), 256)
                second_ref[:, to] += contract_cols(active_ref[:, at], d_ref[to, at])
                return carry

            lax.fori_loop(0, width // 256, one, 0)

        def second(j, sums):
            at = pl.ds(pl.multiple_of(j * chunk, chunk), chunk)
            result, normal, root = norm_forward(second_ref[at, :], vector(G_FFN), vector(S_FFN))
            grads = jnp.concatenate([cotangent_ref[at, lanes_of(owner)] for owner in owners], axis=1)
            for place, owner in enumerate(owners):
                output_ref[at, lanes_of(owner)] = result[:, place * block : (place + 1) * block].astype(BF16)
            hidden, more_gain, more_shift = norm_backward(
                grads.astype(F32), normal, root, vector(G_FFN)
            )
            second_ref[at, :] = hidden
            mixed_ref[at, :] = hidden.astype(BF16)
            turn(mixed_t, at, hidden)
            more = (jnp.sum(hidden, axis=0), more_gain, more_shift)
            return tuple(a + b[None] for a, b in zip(sums, more))

        def last_norm():
            zero = jnp.zeros((1, width), F32)
            sums = lax.fori_loop(0, rows // chunk, second, (zero, zero, zero))
            for k in range(3):
                sums_ref[k : k + 1, :] = sums[k]

        def bound(step, *given):
            return lambda: step(*given)

        table = {
            "prep": prepare, "tr": turn_inputs, "qkv": qkv, "out": out, "norm": norm, "ln": last_norm,
            "up1": bound(raise_piece, 4), "up2": bound(raise_piece, 5), "up3": bound(raise_piece, 6),
            "low1": bound(lower_piece, 7), "low2": bound(lower_piece, 8), "lowX": bound(lower_piece, X),
            "fw9": bound(pass_on, X, 4 * block), "lplane9": late_plane, "lcor9": late_corner, "lz9": late_z, "lcore9": late_core,
        }
        for g in range(X):
            table[f"z{g}"] = bound(send_z, g)
            table[f"fw{g}"] = bound(pass_on, g)
            table[f"col{g}"] = bound(send_column, g)
            table[f"cor{g}"] = bound(send_corner, g)
            table[f"last{g}"] = bound(send_last, g)
        run_events(FORWARD, table, attend, size)

        def settle(j, carry):
            active_copy(j).wait()
            return carry

        lax.fori_loop(0, units // TILE, settle, 0)
        for j in (units // TILE - 2, units // TILE - 1):
            slope_copy(j).wait()
        for copy in saves:
            copy.wait()
        for key, copy in copies.items():
            only(sent[key], lambda: copy().wait_send())

    anywhere, inside = pl.BlockSpec(memory_space=pl.ANY), pl.BlockSpec(memory_space=pltpu.VMEM)
    tall = jax.ShapeDtypeStruct((rows, width), BF16)
    turned = jax.ShapeDtypeStruct((width, rows), BF16)
    return pl.pallas_call(
        body,
        out_shape=[jax.ShapeDtypeStruct(shape, BF16) for shape in full]
        + [
            jax.ShapeDtypeStruct((rows, full[A][1]), BF16),
            tall,
            jax.ShapeDtypeStruct((rows, width), F32),
            jax.ShapeDtypeStruct((rows, units), BF16),
            jax.ShapeDtypeStruct((rows, units), F32),
            tall,
            tall,
            turned,
            turned,
            turned,
            jax.ShapeDtypeStruct((rows, width), F32),
            jax.ShapeDtypeStruct((3, width), F32),
            jax.ShapeDtypeStruct((6, width), F32),
        ],
        in_specs=[inside] * 17 + [pl.BlockSpec(memory_space=pltpu.SMEM)],
        out_specs=[anywhere] * 9 + [inside] * 3 + [anywhere] * 2 + [inside] * 3,
        scratch_shapes=[pltpu.VMEM(shape, BF16) for shape in full]
        + [
            pltpu.VMEM((rows, width), BF16),
            pltpu.VMEM((rows, width), BF16),
            pltpu.VMEM((rows, units), BF16),
            pltpu.VMEM((2, rows, TILE), F32),
            pltpu.VMEM((2, size * attn), F32),
            pltpu.VMEM((1, units), F32),
            pltpu.VMEM((rows, full[A][1]), BF16),
            pltpu.VMEM((rows, width), BF16),
            pltpu.VMEM((rows, width), F32),
            pltpu.VMEM((width, rows), BF16),
            pltpu.VMEM((width, rows), BF16),
            pltpu.SemaphoreType.DMA((5 + len(pieces),)),
            pltpu.SemaphoreType.DMA((len(pieces), 11)),
            pltpu.SemaphoreType.DMA((len(pieces), 11)),
            pltpu.SemaphoreType.DMA((2, units // TILE)),
        ],
        compiler_params=pltpu.CompilerParams(
            collective_id=FORWARD_ID, has_side_effects=True, vmem_limit_bytes=63 * 2**20
        ),
        cost_estimate=pl.CostEstimate(
            flops=2 * rows * width * sum(shape[1] for shape in full),
            bytes_accessed=4 * width * sum(shape[1] for shape in full),
            transcendentals=rows * units,
        ),
        name="forward_near",
    )(
        *weights, hidden_in, cotangent, *(vector[None] for vector in wide), bias_query[None],
        bias_value[None], bias_units[None], lengths,
    )


def backward_near(mixed_low, mixed_t, normed_t, input_t, context, grad_second, hidden, wide, lengths,
                  active, slope, qkv, weights, vectors, head_size):
    size = lax.axis_size("tensor")
    rows, width = mixed_low.shape
    block = width // len(ORDER)
    middle = width // 2
    half = block // 2
    full = [weight.shape[1] for weight in weights]
    units = full[2]
    units_each = units // size
    attn = full[1] // size
    pieces = pieces_of(size, attn, units_each)
    X = len(pieces) - 1
    pieces = pieces[:-3] + [pieces[-2], pieces[-1], pieces[-3]]
    A, O, U, D = range(4)
    tiles = [c // TILE for c in full]
    vector_rows = (6 * width + 2 * full[1] + units) // 128
    v_query, v_value, v_up = 6 * width // 128, (6 * width + full[1]) // 128, (6 * width + 2 * full[1]) // 128
    scale = float(head_size) ** (-0.5)

    def body(
        mixed_in, mixed_t, normed_in, input_in, context_in, second_in, hidden_in, wide_ref,
        lengths_ref, active_in, slope_in, qkv_in, a_in, o_in, u_in, d_in, vectors_ref,
        q_out, k_out, v_out, o_out, u_out, d_out, grad_out, sums_out,
        w_buf, act_ref, slope_buf, gu_ref, grad_ref, low_ref, low_t, gctx_ref, qkv_buf, send_buf,
        units_sum, mixed_ref, normed_t, input_t, context_ref, a_plane, o_plane, u_plane, d_plane, *rest,
    ):
        count = len(pieces)
        corners, sides, zins, relays = (rest[k * count : (k + 1) * count] for k in range(4))
        (
            v_ref, v_in, load_sem, start_sem, core_send, core_recv, send_sem, recv_sem, v_send, v_recv,
        ) = rest[4 * count :]
        data_at, tensor_at = lax.axis_index("dp"), lax.axis_index("tensor")
        planes = (a_plane, o_plane, u_plane, d_plane)
        outs = (q_out, k_out, v_out, o_out, u_out, u_out, u_out, d_out, d_out, d_out)
        shift_by = (tiles[O], 0, 0, 0)

        def dp_partner(bit):
            return (neighbour(data_at, bit), tensor_at)

        def z_partner(step):
            return by_z[step % size]

        by_z = [(data_at, (tensor_at + step) % size) for step in range(size)]

        by_x, by_y, by_core = dp_partner(BIT_X), dp_partner(BIT_Y), dp_partner(BIT_CORE)

        def column(j, span=TILE):
            return pl.ds(pl.multiple_of(j * span, 128), span)

        def load(row, source, buffer, j):
            return pltpu.make_async_copy(
                source.at[:, column(j)], buffer.at[j % 2], load_sem.at[row, j % 2]
            )

        def over_tiles(first, last, loads, step):
            for row, source, buffer in loads:
                load(row, source, buffer, first).start()

            def one(j, carry):
                @pl.when(j + 1 < last)
                def _():
                    for row, source, buffer in loads:
                        load(row, source, buffer, j + 1).start()

                for row, source, buffer in loads:
                    load(row, source, buffer, j).wait()
                step(j)
                return carry

            lax.fori_loop(first, last, one, 0)

        def remote(source, target, send, receive, device):
            return pltpu.make_async_remote_copy(
                src_ref=source,
                dst_ref=target,
                send_sem=send,
                recv_sem=receive,
                device_id=device,
                device_id_type=pl.DeviceIdType.MESH,
            )

        def core_copy(g, j):
            return remote(
                send_buf.at[:, column(j + shift_by[g])],
                planes[g].at[:, column(j)],
                core_send.at[g, j],
                core_recv.at[g, j],
                by_core,
            )

        copies = {}
        sent = {}

        def send(g, slot, source, target, device, when=None, lands=None):
            def copy():
                at = slot if lands is None else lands
                return remote(source, target(), send_sem.at[g, slot], recv_sem.at[g, at], device)

            copies[g, slot] = copy
            sent[g, slot] = when
            only(when, lambda: copy().start())

        def only(when, step):
            if when is None:
                step()
            else:
                pl.when(when())(step)

        def not_first():
            return tensor_at > 0

        def not_last():
            return tensor_at < size - 1

        def first_one():
            return tensor_at == 0

        def last_one():
            return tensor_at == size - 1

        def outer():
            return (tensor_at % (size - 1)) == 0

        def inner():
            return (tensor_at % (size - 1)) > 0

        def z_cell(g, r, count):
            weight, first, wide_by = pieces[g]
            at = first + r * wide_by
            return planes[weight].at[:count, at : at + wide_by]

        def send_z(g, count=block):
            near, far = z_cell(g, 1, count), z_cell(g, 3, count)
            send(g, 7, near, lambda: relays[g], z_partner(1), first_one)
            send(g, 8, far, lambda: relays[g], z_partner(-1), last_one, 7)
            send(g, 4, near, lambda: zins[g].at[0], z_partner(-1), not_first)
            send(g, 6, far, lambda: zins[g].at[2], z_partner(1), not_last)
            send(g, 5, z_cell(g, 2, count), lambda: zins[g].at[1], z_partner(-2), outer)

        def add_on(g, count=block):
            def step():
                arrived(g, 7)
                cell = z_cell(g, 2, count)
                for at in range(0, count, block):
                    rows_k = slice(at, at + block)
                    total = cell[rows_k, :].astype(F32) + relays[g][rows_k, :].astype(F32)
                    cell[rows_k, :] = total.astype(BF16)

            only(inner, step)
            send(g, 9, z_cell(g, 2, count), lambda: zins[g].at[1], z_partner(-2), inner, 5)

        def wait_z(g):
            arrived(g, 5)
            only(not_last, lambda: arrived(g, 4))
            only(not_first, lambda: arrived(g, 6))

        def arrived(g, *slots):
            for slot in slots:
                copies[g, slot]().wait_recv()

        def other_tile(g, left_t, right, j):
            send_buf[:, column(j + shift_by[g])] = matmul(left_t[middle:, :], right).astype(BF16)
            core_copy(g, j).start()

        def own_tile(g, left_t, right, j):
            core_copy(g, j).wait_recv()
            total = matmul(left_t[:middle, :], right) + planes[g][:, column(j)].astype(F32)
            planes[g][:, column(j)] = total.astype(BF16)

        def span(g):
            _, first, wide_by = pieces[g]
            return first, wide_by if g == X else size * wide_by

        def plane_rows(g, start, count):
            first, wide_by = span(g)
            return planes[pieces[g][0]].at[start : start + count, first : first + wide_by]

        def send_corner(g):
            send(g, 0, plane_rows(g, 3 * block, half), lambda: corners[g].at[0], by_x)
            send(g, 1, plane_rows(g, 3 * block + half, half), lambda: corners[g].at[1], by_y)

        def add_rows(g, start, count, *more):
            plane = planes[pieces[g][0]]
            first, wide_by = span(g)
            step = min(TILE, wide_by)
            for at in range(0, wide_by, step):
                where = (slice(start, start + count), slice(first + at, first + at + step))
                total = plane[where].astype(F32)
                for ref in more:
                    total += ref[:, at : at + step].astype(F32)
                plane[where] = total.astype(BF16)

        def send_sides(g):
            arrived(g, 0, 1)
            add_rows(g, 2 * block, half, corners[g].at[0])
            add_rows(g, block + half, half, corners[g].at[1])
            send(g, 2, plane_rows(g, block, block), lambda: sides[g].at[0], by_x)
            send(g, 3, plane_rows(g, 2 * block, block), lambda: sides[g].at[1], by_y)

        def out_of(g):
            weight, first, wide_by = pieces[g]
            start = first // size if weight >= U else 0
            return outs[g].at[:, start : start + wide_by]

        def send_column(g):
            arrived(g, 2, 3)
            weight, first, wide_by = pieces[g]
            for r in range(size):
                at = slice(r * wide_by, (r + 1) * wide_by)
                own = slice(first + r * wide_by, first + (r + 1) * wide_by)
                total = planes[weight][:block, own].astype(F32)
                total += sides[g][0, :, at].astype(F32) + sides[g][1, :, at].astype(F32)
                if r == 0:
                    out_of(g)[...] = total
                else:
                    planes[weight][:block, own] = total.astype(BF16)
            send_z(g)

        def finish(g):
            wait_z(g)

            def add(k):
                out_of(g)[...] += zins[g][k].astype(F32)

            add(1)
            only(not_last, lambda: add(0))
            only(not_first, lambda: add(2))

        def late_corner():
            wait_z(X)

            def add(z):
                for k in range(4):
                    rows_k = slice(k * block, (k + 1) * block)
                    add_rows(X, k * block, block, zins[X].at[z, rows_k])

            add(1)
            only(not_last, lambda: add(0))
            only(not_first, lambda: add(2))
            send_corner(X)

        def late_finish():
            arrived(X, 2, 3)
            total = plane_rows(X, 0, block)[...].astype(F32)
            out_of(X)[...] = total + sides[X][0].astype(F32) + sides[X][1].astype(F32)

        def feature_rows(k, vector):
            for place, mask in enumerate(ORDER):
                at = block_of(data_at, mask)
                v_ref[0, pl.ds(k * len(ORDER) + at, 1), :] = vector[:, place * 128 : (place + 1) * 128]

        z_near = tensor_at + 1 - 2 * (tensor_at % 2)
        z_across = tensor_at + 2 - 4 * ((tensor_at // 2) % 2)
        v_partners = (by_core, (data_at, z_near), (data_at, z_across), by_x, by_y)

        def v_copy(k):
            return remote(v_ref.at[k], v_in.at[k], v_send.at[k], v_recv.at[k], v_partners[k])

        def v_add(k):
            v_copy(k).wait_recv()
            v_ref[k + 1] = v_ref[k] + v_in[k]

        early = [
            pltpu.make_async_copy(
                active_in.at[:, k * (units // 2) : (k + 1) * (units // 2)],
                act_ref.at[:, k * (units // 2) : (k + 1) * (units // 2)],
                start_sem.at[k],
            )
            for k in range(2)
        ]
        grad_load, mixed_load, normed_load, context_load, input_load = (
            pltpu.make_async_copy(source, target, start_sem.at[k])
            for k, (source, target) in enumerate(
                (
                    (second_in, grad_ref),
                    (mixed_in, mixed_ref),
                    (normed_in, normed_t),
                    (context_in, context_ref),
                    (input_in, input_t),
                ),
                2,
            )
        )
        for copy in early:
            copy.start()
        for copy in (mixed_load, normed_load, grad_load, context_load, input_load):
            copy.start()
        partners = [by_x, by_y, by_core] + by_z[1:]
        greet(partners)
        await_greetings(partners)

        def each(first, last, step):
            def one(j, carry):
                step(j)
                return carry

            lax.fori_loop(first, last, one, 0)

        def other_down(j):
            other_tile(D, mixed_t, act_ref[:, column(j)], j)

        def own_down(j):
            own_tile(D, mixed_t, act_ref[:, column(j)], j)

        def other_up(j):
            core_copy(D, j).wait_send()
            other_tile(U, normed_t, gu_ref[:, column(j)], j)

        def own_up(j):
            own_tile(U, normed_t, gu_ref[:, column(j)], j)

        def bounds(g):
            _, first, wide_by = pieces[g]
            return first // TILE, (first + size * wide_by) // TILE

        early[0].wait()
        early[1].wait()

        def loaded(copy, step):
            def both():
                copy.wait()
                step()

            return both

        def bound(step, *given):
            return lambda: step(*given)

        def gelu_step(j):
            low = (matmul(mixed_ref[...], w_buf[j % 2]) * slope_buf[j % 2]).astype(BF16)
            gu_ref[:, column(j)] = low
            units_sum[:, column(j)] = jnp.sum(low.astype(F32), axis=0, keepdims=True)

        gelu_loads = [(1, d_in, w_buf), (2, slope_in, slope_buf)]
        hidden_loads = [
            pltpu.make_async_copy(hidden_in.at[:, column(k)], slope_buf.at[k], load_sem.at[2, k])
            for k in range(2)
        ]

        def second_gelu():
            over_tiles(tiles[D] // 2, tiles[D], gelu_loads, gelu_step)
            for copy in hidden_loads:
                copy.start()

        def up_step(j):
            grad_ref[...] += contract_cols(gu_ref[:, column(j)], w_buf[j % 2])

        def sum_units():
            for k in range(3):
                feature_rows((1, 4, 5)[k], vectors_ref[k : k + 1, :])
            for r in range(size):
                for weight, first, wide_by in pieces:
                    if weight == U:
                        for k in range(wide_by // 128):
                            place = ((tensor_at + size - r) % size) * (units_each // 128)
                            place += (first // size) // 128 + k
                            at = first + r * wide_by + k * 128
                            v_ref[0, pl.ds(v_up + place, 1), :] = units_sum[:, at : at + 128]

        chunk = 128

        def norm_step(j, sums):
            at = pl.ds(pl.multiple_of(j * chunk, chunk), chunk)
            hidden_rows = jnp.concatenate([slope_buf[0, at, :], slope_buf[1, at, :]], axis=1)
            gain = wide_ref[2:3, :]
            normal, root = norm_forward(hidden_rows, gain, gain)[1:]
            hidden, more_gain, more_shift = norm_backward(grad_ref[at, :], normal, root, gain)
            grad_ref[at, :] = hidden
            low_ref[at, :] = hidden.astype(BF16)
            for k in range(width // 128):
                low_t[k * 128 : (k + 1) * 128, at] = hidden[:, k * 128 : (k + 1) * 128].T.astype(BF16)
            more = (jnp.sum(hidden, axis=0), more_gain, more_shift)
            return tuple(a + b[None] for a, b in zip(sums, more))

        def norm():
            for copy in hidden_loads:
                copy.wait()
            zero = jnp.zeros((1, width), F32)
            sums = lax.fori_loop(0, rows // chunk, norm_step, (zero, zero, zero))
            for k in range(3):
                feature_rows((0, 2, 3)[k], sums[k])

        def out_step(j):
            core_copy(U, j).wait_send()
            gctx_ref[:, column(j)] = matmul(low_ref[...], w_buf[j % 2]).astype(BF16)
            other_tile(O, low_t, context_ref[:, column(j)], j)

        def out():
            context_load.wait()
            over_tiles(0, tiles[O], [(1, o_in, w_buf)], out_step)
            for copy in qkv_load(0):
                copy.start()

        def own_out():
            for j in range(tiles[O]):
                own_tile(O, low_t, context_ref[:, j * TILE : (j + 1) * TILE], j)

        def qkv_load(r):
            return [
                pltpu.make_async_copy(
                    qkv_in.at[:, column(k * size + r, attn)], qkv_buf.at[r % 2, k], load_sem.at[k, r % 2]
                )
                for k in range(3)
            ]

        def attend_step(r):
            @pl.when(r + 1 < size)
            def _():
                for copy in qkv_load(r + 1):
                    copy.start()

            for copy in qkv_load(r):
                copy.wait()
            slot = r % 2
            seen = lax.broadcasted_iota(jnp.int32, (rows, rows), 0) < length
            for start, lanes, held in pairs_of(attn, head_size):
                queries, keys, values = (qkv_buf[slot, k, :, start : start + lanes] for k in range(3))
                grads = gctx_ref[:, pl.ds(pl.multiple_of(r * attn + start, 128), lanes)]
                grad_q = jnp.zeros((rows, lanes), F32)
                grad_k = jnp.zeros((rows, lanes), F32)
                grad_v = jnp.zeros((rows, lanes), F32)
                for which in range(held):
                    mine = keep_head(grads, which, head_size)
                    query = keep_head(queries, which, head_size)
                    scores = jnp.where(seen, contract_cols(keys, query) * scale, MASKED)
                    exponent = jnp.exp(scores - jnp.max(scores, axis=0, keepdims=True))
                    probs = exponent * (1.0 / jnp.sum(exponent, axis=0, keepdims=True))
                    grad_v += matmul(probs.astype(BF16), mine)
                    grad_probs = contract_cols(values, mine)
                    inner = jnp.sum(probs * grad_probs, axis=0, keepdims=True)
                    grad_scores = (probs * (grad_probs - inner)).astype(BF16)
                    grad_q += keep_head(contract_rows(grad_scores, keys), which, head_size)
                    grad_k += matmul(grad_scores, query)
                low_q = (grad_q * scale).astype(BF16)
                low_v = grad_v.astype(BF16)
                for k, low in enumerate((low_q, (grad_k * scale).astype(BF16), low_v)):
                    at = pl.multiple_of((k * size + r) * attn + start, 128)
                    gu_ref[:, pl.ds(at, lanes)] = low
                place = ((tensor_at + size - r) % size) * (attn // 128) + start // 128
                v_ref[0, pl.ds(v_query + place, 1), :] = jnp.sum(
                    low_q.astype(F32), axis=0, keepdims=True
                )
                v_ref[0, pl.ds(v_value + place, 1), :] = jnp.sum(
                    low_v.astype(F32), axis=0, keepdims=True
                )

        length = lengths_ref[tensor_at]

        def other_qkv(j):
            core_copy(U, j + tiles[O]).wait_send()
            other_tile(A, input_t, gu_ref[:, column(j)], j)

        def own_qkv(j):
            own_tile(A, input_t, gu_ref[:, column(j)], j)

        def input_step(j):
            grad_ref[...] += contract_cols(gu_ref[:, column(j)], w_buf[j % 2])

        def give_input():
            for place, mask in enumerate(ORDER):
                at = block_of(data_at, mask)
                grad_out[:, pl.ds(pl.multiple_of(at * block, block), block)] = grad_ref[
                    :, place * block : (place + 1) * block
                ].astype(BF16)

        def give_sums():
            v_add(4)
            sums_out[...] = v_ref[5]

        def next_sum(k):
            v_add(k - 1)
            v_copy(k).start()

        weight_loads = [[(1, ref, w_buf)] for ref in (a_in, o_in, u_in, d_in)]
        parts = (
            (other_qkv, own_qkv), (other_qkv, own_qkv), (other_qkv, own_qkv), (lambda j: None, own_out),
            (other_up, own_up), (other_up, own_up), (other_up, own_up), (other_down, own_down),
            (other_down, own_down), (other_down, own_down),
        )
        halves = [(0, count // 2, count) for count in tiles]
        table = {
            "gelA": loaded(mixed_load, bound(over_tiles, 0, halves[D][1], gelu_loads, gelu_step)),
            "gelB": second_gelu,
            "upA": loaded(grad_load, bound(over_tiles, 0, halves[U][1], weight_loads[U], up_step)),
            "upB": bound(over_tiles, *halves[U][1:], weight_loads[U], up_step),
            "vec": sum_units,
            "norm": norm,
            "out": out,
            "dxA": bound(over_tiles, 0, halves[A][1], weight_loads[A], input_step),
            "dxB": bound(over_tiles, *halves[A][1:], weight_loads[A], input_step),
            "gout": give_input,
            "lz9": bound(send_z, X, 4 * block),
            "fw9": bound(add_on, X, 4 * block),
            "lcor9": late_corner,
            "sid9": bound(send_sides, X),
            "fin9": late_finish,
            "v0": lambda: v_copy(0).start(),
            "v5": give_sums,
        }
        for k in range(1, 5):
            table[f"v{k}"] = bound(next_sum, k)
        for g in range(len(pieces)):
            other, own = parts[g]
            table[f"oth{g}"] = bound(each, *bounds(g), other)
            table[f"own{g}"] = bound(each, *bounds(g), own)
            if g < X:
                table[f"cor{g}"] = bound(send_corner, g)
                table[f"sid{g}"] = bound(send_sides, g)
                table[f"col{g}"] = bound(send_column, g)
                table[f"fin{g}"] = bound(finish, g)
                table[f"fw{g}"] = bound(add_on, g)
        table["oth3"] = lambda: None
        table["own3"] = own_out
        first_up = [g for g in range(len(pieces)) if f"oth{g}" in BACKWARD and pieces[g][0] == U]
        first_up = min(first_up, key=lambda g: BACKWARD.index(f"oth{g}"))
        table[f"oth{first_up}"] = loaded(normed_load, table[f"oth{first_up}"])
        first_in = min((0, 1, 2), key=lambda g: BACKWARD.index(f"oth{g}"))
        table[f"oth{first_in}"] = loaded(input_load, table[f"oth{first_in}"])
        run_events(BACKWARD, table, attend_step, size)
        for g in (A, O):
            for j in range(tiles[g]):
                core_copy(g, j).wait_send()
        for k in range(5):
            v_copy(k).wait_send()
        for key, copy in copies.items():
            only(sent[key], lambda: copy().wait_send())

    spans = [piece[2] if g == X else size * piece[2] for g, piece in enumerate(pieces)]
    anywhere, inside = pl.BlockSpec(memory_space=pl.ANY), pl.BlockSpec(memory_space=pltpu.VMEM)
    results = pl.pallas_call(
        body,
        out_shape=[jax.ShapeDtypeStruct((block, attn), F32)] * 4
        + [jax.ShapeDtypeStruct((block, units_each), F32)] * 2
        + [
            jax.ShapeDtypeStruct((rows, width), BF16),
            jax.ShapeDtypeStruct((vector_rows, 128), F32),
        ],
        in_specs=[anywhere, inside]
        + [anywhere] * 5
        + [inside, pl.BlockSpec(memory_space=pltpu.SMEM)]
        + [anywhere] * 7
        + [inside],
        out_specs=[inside] * 8,
        scratch_shapes=[
            pltpu.VMEM((2, width, TILE), BF16),
            pltpu.VMEM((rows, units), BF16),
            pltpu.VMEM((2, rows, TILE), F32),
            pltpu.VMEM((rows, units), BF16),
            pltpu.VMEM((rows, width), F32),
            pltpu.VMEM((rows, width), BF16),
            pltpu.VMEM((width, rows), BF16),
            pltpu.VMEM((rows, full[1]), BF16),
            pltpu.VMEM((2, 3, rows, attn), BF16),
            pltpu.VMEM((middle, units), BF16),
            pltpu.VMEM((1, units), F32),
            pltpu.VMEM((rows, width), BF16),
            pltpu.VMEM((width, rows), BF16),
            pltpu.VMEM((width, rows), BF16),
            pltpu.VMEM((rows, width), BF16),
        ]
        + [pltpu.VMEM((middle, c), BF16) for c in full]
        + [pltpu.VMEM((2, half, c), BF16) for c in spans]
        + [pltpu.VMEM((2, block, c), BF16) for c in spans]
        + [
            pltpu.VMEM((size - 1, 4 * block if g == X else block, piece[2]), BF16)
            for g, piece in enumerate(pieces)
        ]
        + [
            pltpu.VMEM((4 * block if g == X else block, piece[2]), BF16)
            for g, piece in enumerate(pieces)
        ]
        + [
            pltpu.VMEM((6, vector_rows, 128), F32),
            pltpu.VMEM((5, vector_rows, 128), F32),
            pltpu.SemaphoreType.DMA((3, 2)),
            pltpu.SemaphoreType.DMA((7,)),
            pltpu.SemaphoreType.DMA((4, units // TILE)),
            pltpu.SemaphoreType.DMA((4, units // TILE)),
            pltpu.SemaphoreType.DMA((len(pieces), 10)),
            pltpu.SemaphoreType.DMA((len(pieces), 10)),
            pltpu.SemaphoreType.DMA((5,)),
            pltpu.SemaphoreType.DMA((5,)),
        ],
        compiler_params=pltpu.CompilerParams(
            collective_id=BACKWARD_ID, has_side_effects=True, vmem_limit_bytes=63 * 2**20
        ),
        cost_estimate=pl.CostEstimate(
            flops=4 * rows * sum(full) * width,
            bytes_accessed=4 * sum(full) * width,
            transcendentals=0,
        ),
        name="backward_near",
    )(
        mixed_low, mixed_t, normed_t, input_t, context, grad_second, hidden, wide, lengths, active,
        slope, qkv, *weights, vectors,
    )
    return results[:6], results[6], results[7]


def gather_far(shard):
    return lax.all_gather(
        lax.all_gather(shard, "tensor", axis=1, tiled=True), "dp", axis=0, tiled=True
    )


def scatter_far(left_side, right_side):
    whole = contract_rows(left_side, right_side).astype(BF16)
    part = lax.psum_scatter(whole, "dp", scatter_dimension=0, tiled=True)
    return lax.psum_scatter(part, "tensor", scatter_dimension=1, tiled=True).astype(F32)


def soft_weights(queries, keys, visible, scale):
    scores = contract_cols(queries, keys) * scale
    scores = jnp.where(visible, scores, MASKED)
    exponent = jnp.exp(scores - jnp.max(scores, axis=-1, keepdims=True))
    return exponent * (1.0 / jnp.sum(exponent, axis=-1, keepdims=True))


def pairs_of(width, head_size):
    lanes = max(128, head_size)
    return [(start, lanes, lanes // head_size) for start in range(0, width, lanes)]


def keep_head(array, which, head_size):
    lane = lax.broadcasted_iota(jnp.int32, array.shape, 1)
    return jnp.where(lane // head_size == which, array, jnp.zeros_like(array))


def attend_forward(qkv_q, qkv_kv, length, head_size, groups):
    q_rows = qkv_q.shape[0]
    k_rows = qkv_kv.shape[0]
    block = qkv_q.shape[1] // groups
    width = block // 3
    scale = float(head_size) ** (-0.5)

    def body(length_ref, q_ref, kv_ref, out_ref):
        visible = lax.broadcasted_iota(jnp.int32, (q_rows, k_rows), 1) < length_ref[0]
        for start, lanes, held in pairs_of(width, head_size):
            queries = q_ref[:, start : start + lanes]
            keys = kv_ref[:, width + start : width + start + lanes]
            values = kv_ref[:, 2 * width + start : 2 * width + start + lanes]
            total = jnp.zeros((q_rows, lanes), F32)
            for which in range(held):
                probs = soft_weights(keep_head(queries, which, head_size), keys, visible, scale)
                total += keep_head(matmul(probs.astype(BF16), values), which, head_size)
            out_ref[:, start : start + lanes] = total.astype(BF16)

    return pl.pallas_call(
        body,
        out_shape=jax.ShapeDtypeStruct((q_rows, groups * width), BF16),
        grid_spec=pltpu.PrefetchScalarGridSpec(
            num_scalar_prefetch=1,
            grid=(groups,),
            in_specs=[
                pl.BlockSpec((q_rows, block), lambda g, length_ref: (0, g)),
                pl.BlockSpec((k_rows, block), lambda g, length_ref: (0, g)),
            ],
            out_specs=pl.BlockSpec((q_rows, width), lambda g, length_ref: (0, g)),
        ),
        cost_estimate=pl.CostEstimate(
            flops=4 * q_rows * k_rows * width * groups,
            bytes_accessed=2 * (2 * q_rows + 2 * k_rows) * width * groups,
            transcendentals=q_rows * k_rows * groups * width // head_size,
        ),
        name="attend_forward",
    )(length, qkv_q, qkv_kv)


def attend_backward(qkv_q, qkv_kv, grad_context, length, head_size, groups):
    q_rows = qkv_q.shape[0]
    k_rows = qkv_kv.shape[0]
    block = qkv_q.shape[1] // groups
    width = block // 3
    scale = float(head_size) ** (-0.5)

    def body(length_ref, q_ref, kv_ref, grad_ref, dq_ref, dkv_ref):
        visible = lax.broadcasted_iota(jnp.int32, (q_rows, k_rows), 1) < length_ref[0]
        for start, lanes, held in pairs_of(width, head_size):
            queries = q_ref[:, start : start + lanes]
            keys = kv_ref[:, width + start : width + start + lanes]
            values = kv_ref[:, 2 * width + start : 2 * width + start + lanes]
            grads = grad_ref[:, start : start + lanes]
            grad_q = jnp.zeros((q_rows, lanes), F32)
            grad_k = jnp.zeros((k_rows, lanes), F32)
            grad_v = jnp.zeros((k_rows, lanes), F32)
            for which in range(held):
                mine = keep_head(grads, which, head_size)
                query = keep_head(queries, which, head_size)
                probs = soft_weights(query, keys, visible, scale)
                grad_v += contract_rows(probs.astype(BF16), mine)
                grad_probs = contract_cols(mine, values)
                inner = jnp.sum(probs * grad_probs, axis=-1, keepdims=True)
                grad_scores = (probs * (grad_probs - inner)).astype(BF16)
                grad_q += keep_head(matmul(grad_scores, keys), which, head_size)
                grad_k += contract_rows(grad_scores, query)
            dq_ref[:, start : start + lanes] = (grad_q * scale).astype(BF16)
            dkv_ref[:, start : start + lanes] = (grad_k * scale).astype(BF16)
            dkv_ref[:, width + start : width + start + lanes] = grad_v.astype(BF16)

    return pl.pallas_call(
        body,
        out_shape=(
            jax.ShapeDtypeStruct((q_rows, groups * width), BF16),
            jax.ShapeDtypeStruct((k_rows, groups * 2 * width), BF16),
        ),
        grid_spec=pltpu.PrefetchScalarGridSpec(
            num_scalar_prefetch=1,
            grid=(groups,),
            in_specs=[
                pl.BlockSpec((q_rows, block), lambda g, length_ref: (0, g)),
                pl.BlockSpec((k_rows, block), lambda g, length_ref: (0, g)),
                pl.BlockSpec((q_rows, width), lambda g, length_ref: (0, g)),
            ],
            out_specs=[
                pl.BlockSpec((q_rows, width), lambda g, length_ref: (0, g)),
                pl.BlockSpec((k_rows, 2 * width), lambda g, length_ref: (0, g)),
            ],
        ),
        cost_estimate=pl.CostEstimate(
            flops=10 * q_rows * k_rows * width * groups,
            bytes_accessed=2 * (3 * q_rows + 4 * k_rows) * width * groups,
            transcendentals=q_rows * k_rows * groups * width // head_size,
        ),
        name="attend_backward",
    )(length, qkv_q, qkv_kv, grad_context)


def activate(total, bias):
    upper = total + bias
    cumulative = 0.5 * (1.0 + lax.erf(upper * math.sqrt(0.5)))
    density = jnp.exp(-0.5 * upper * upper) * (1.0 / math.sqrt(2.0 * math.pi))
    return upper * cumulative, cumulative + upper * density


def norm_forward(hidden, gain_vec, shift_vec):
    center = hidden - jnp.mean(hidden, axis=-1, keepdims=True)
    variance = jnp.mean(center * center, axis=-1, keepdims=True)
    inv_root = lax.rsqrt(variance + EPSILON)
    normal = center * inv_root
    return (normal * gain_vec + shift_vec, normal, inv_root)


def norm_backward(grad_in, normal, inv_root, gain_vec):
    grad_normal = grad_in * gain_vec
    grad_gain = jnp.sum(grad_in * normal, axis=0)
    grad_shift = jnp.sum(grad_in, axis=0)
    grad_hidden = inv_root * (
        grad_normal
        - jnp.mean(grad_normal, axis=-1, keepdims=True)
        - normal * jnp.mean(grad_normal * normal, axis=-1, keepdims=True)
    )
    return (grad_hidden, grad_gain, grad_shift)


def layer(
    hidden_in,
    cotangent,
    w_query,
    w_key,
    w_value,
    w_out,
    w_up,
    w_down,
    bias_query,
    bias_value,
    bias_out,
    bias_up,
    bias_down,
    gain_attn,
    shift_attn,
    gain_ffn,
    shift_ffn,
    valid_lengths,
):
    rows, model_width = hidden_in.shape
    n_tensor = lax.axis_size("tensor")
    n_data = lax.axis_size("dp")
    tensor_at = lax.axis_index("tensor")
    spread_over = rows * n_tensor // valid_lengths.shape[0] // rows
    head_size = model_width // HEADS
    head_cols = w_query.shape[1]
    factor = 1.0 / math.sqrt(rows * n_tensor * n_data)
    matrices = (w_query, w_key, w_value, w_out, w_up, w_down)
    wide = (bias_out, bias_down, gain_attn, shift_attn, gain_ffn, shift_ffn)

    if n_data == len(ORDER) and n_tensor == 4 and spread_over == 1:
        (
            qkv_full, out_full, up_full, down_full, qkv, context, hidden, active, slope, output,
            mixed_low, mixed_t, normed_t, input_t, grad_second, given, arranged,
        ) = forward_near(
            matrices, hidden_in, cotangent, wide, bias_query, bias_value, bias_up, valid_lengths,
            head_size,
        )
        grads, grad_input, sums = backward_near(
            mixed_low, mixed_t, normed_t, input_t, context, grad_second, hidden, arranged,
            valid_lengths, active, slope, qkv, (qkv_full, out_full, up_full, down_full), given,
            head_size,
        )
        lengths = [model_width // 128] * 8 + [bias_up.shape[0] // 128]
        results = scale_and_copy(grads, (grad_input, output), sums, lengths, factor)
        grads, (grad_input, output) = results[:6], results[6:8]
        vector_sums = [part.reshape(-1) for part in results[8:]]
    else:

        def column_part(vector):
            return vector.reshape(n_tensor, -1)

        query_bias, value_bias = column_part(bias_query), column_part(bias_value)
        bias_qkv = jnp.concatenate(
            [query_bias, jnp.zeros_like(query_bias), value_bias], axis=1
        ).reshape(1, -1)
        length = lax.dynamic_slice_in_dim(valid_lengths, tensor_at // spread_over, 1)
        low = [matrix.astype(BF16) for matrix in matrices]
        shards = [jnp.concatenate(low[:3], axis=1)] + low[3:]
        qkv_full, out_full, up_full, down_full = (gather_far(shard) for shard in shards)
        qkv = (matmul(hidden_in, qkv_full) + bias_qkv).astype(BF16)
        members = [list(range(k, k + spread_over)) for k in range(0, n_tensor, spread_over)]
        qkv_seq = lax.all_gather(qkv, "tensor", axis_index_groups=members, axis=0, tiled=True)
        context = attend_forward(qkv, qkv_seq, length, head_size, n_tensor)
        hidden = hidden_in.astype(F32) + contract_cols(context, out_full) + bias_out
        normed, normal_attn, root_attn = norm_forward(hidden, gain_attn, shift_attn)
        normed_low = normed.astype(BF16)
        active, slope = activate(matmul(normed_low, up_full), bias_up)
        active = active.astype(BF16)
        mixed = contract_cols(active, down_full)
        result, normal_ffn, root_ffn = norm_forward(normed + mixed + bias_down, gain_ffn, shift_ffn)
        output = result.astype(BF16)
        grad_second, grad_gain_ffn, grad_shift_ffn = norm_backward(
            cotangent.astype(F32), normal_ffn, root_ffn, gain_ffn
        )
        grad_bias_down = jnp.sum(grad_second, axis=0)
        mixed_low = grad_second.astype(BF16)
        grad_down = scatter_far(mixed_low, active)
        grad_upper = (matmul(mixed_low, down_full) * slope).astype(BF16)
        grad_bias_up = jnp.sum(grad_upper, axis=0, dtype=F32)
        grad_up = scatter_far(normed_low, grad_upper)
        grad_normed = grad_second + contract_cols(grad_upper, up_full)
        grad_first, grad_gain_attn, grad_shift_attn = norm_backward(
            grad_normed, normal_attn, root_attn, gain_attn
        )
        grad_bias_out = jnp.sum(grad_first, axis=0)
        attn_low = grad_first.astype(BF16)
        grad_context = matmul(attn_low, out_full).astype(BF16)
        grad_out = scatter_far(attn_low, context)
        grad_q, grad_kv = attend_backward(qkv, qkv_seq, grad_context, length, head_size, n_tensor)
        grad_kv = lax.psum_scatter(
            grad_kv.astype(F32),
            "tensor",
            scatter_dimension=0,
            axis_index_groups=members,
            tiled=True,
        ).astype(BF16)
        grad_qkv = jnp.concatenate(
            [grad_q.reshape(rows, n_tensor, -1), grad_kv.reshape(rows, n_tensor, -1)], axis=2
        ).reshape(rows, -1)
        grad_bias_qkv = jnp.sum(grad_qkv, axis=0, dtype=F32).reshape(n_tensor, 3, head_cols)
        grads = jnp.split(scatter_far(hidden_in, grad_qkv), 3, axis=1)
        grads = [grad * factor for grad in (*grads, grad_out, grad_up, grad_down)]
        grad_input = (grad_first + contract_cols(grad_qkv, qkv_full)).astype(BF16)
        sums = jnp.concatenate(
            [
                grad_bias_out,
                grad_bias_down,
                grad_gain_attn,
                grad_shift_attn,
                grad_gain_ffn,
                grad_shift_ffn,
                grad_bias_qkv[:, 0].reshape(-1),
                grad_bias_qkv[:, 2].reshape(-1),
                grad_bias_up,
            ]
        )
        sums = lax.psum(sums, ("dp", "tensor")) * factor
        vector_sums = jnp.split(sums, [k * model_width for k in range(1, 9)])
    (
        v_out, v_down, v_gain_attn, v_shift_attn, v_gain_ffn, v_shift_ffn, v_query, v_value, v_up,
    ) = vector_sums
    return (
        output,
        grad_input,
        *grads,
        v_query,
        v_value,
        v_out,
        v_up,
        v_down,
        v_gain_attn,
        v_shift_attn,
        v_gain_ffn,
        v_shift_ffn,
    )


def solution(mesh):
    tokens, matrix, copied = P(("dp", "tensor"), None), P("dp", "tensor"), P()
    return jax.shard_map(
        layer,
        mesh=mesh,
        in_specs=(tokens,) * 2 + (matrix,) * 6 + (copied,) * 9 + (P("dp"),),
        out_specs=(tokens,) * 2 + (matrix,) * 6 + (copied,) * 9,
        check_vma=False,
    )
```

```python
import math

import jax
import jax.numpy as jnp
from jax import lax
from jax.experimental import pallas as pl
from jax.experimental.pallas import tpu as pltpu
from jax.sharding import PartitionSpec as P

HEADS = 16
EPSILON = 1e-12
MASKED = -1e30
BF16 = jnp.bfloat16
F32 = jnp.float32

ORDER = (0, 2, 4, 6, 1, 3, 5, 7)
BIT_CORE, BIT_X, BIT_Y = 1, 2, 4


def matmul(left_side, right_side):
    return jnp.dot(left_side, right_side, preferred_element_type=F32)


def contract_rows(left_side, right_side):
    return lax.dot_general(
        left_side, right_side, (((0,), (0,)), ((), ())), preferred_element_type=F32
    )


def contract_cols(left_side, right_side):
    return lax.dot_general(
        left_side, right_side, (((1,), (1,)), ((), ())), preferred_element_type=F32
    )


FORWARD_ID = 1
BACKWARD_ID = 2
TILE = 512

FORWARD = (
    "lplane9", "z3", "fw3", "z1", "lcor9", "col3", "fw1", "z2", "fw2", "col1", "z0", "col2",
    "cor3", "z8", "z6", "fw0", "cor1", "z4", "z7", "z5", "col0", "cor2", "fw6", "prep", "fw8",
    "cor0", "tr", "col6", "fw4", "fw5", "lz9", "col4", "last2", "last0", "last1", "qkv", "a0",
    "cor6", "col5", "a1", "a2", "fw7", "last3", "a3", "out", "cor4", "fw9", "norm", "cor5",
    "last4", "col7", "col8", "last5", "last6", "up1", "lcore9", "up2", "cor7", "up3", "cor8",
    "lowX", "last7", "last8", "low1", "low2", "ln",
)
BACKWARD = (
    "oth8", "oth7", "gelA", "own8", "cor8", "own7", "cor7", "oth9", "oth4", "sid8", "gelB",
    "own9", "sid7", "oth5", "lz9", "oth6", "upA", "own4", "upB", "own5", "cor4", "cor5", "norm",
    "col8", "sid4", "own6", "out", "col7", "oth3", "a0", "own3", "cor3", "cor6", "a1", "col4",
    "sid5", "sid3", "a2", "a3", "oth1", "sid6", "vec", "oth2", "col5", "fin4", "own1", "cor1",
    "v0", "oth0", "col3", "v1", "own2", "cor2", "fin8", "sid1", "col6", "own0", "cor0", "fin7",
    "sid2", "v2", "col1", "dxA", "sid0", "col2", "lcor9", "dxB", "fin6", "col0", "v3", "sid9",
    "fin2", "v4", "gout", "fin5", "fin1", "fin3", "fin9", "v5", "fin0",
)


def neighbour(index, bit):
    return index + bit - 2 * bit * ((index // bit) % 2)


def block_of(index, mask):
    for bit in (BIT_CORE, BIT_X, BIT_Y):
        if mask & bit:
            index = neighbour(index, bit)
    return index


def pieces_of(size, attn, units_each):
    pieces = [(0, k * size * attn, attn) for k in range(3)] + [(1, 0, attn)]
    for weight in (2, 3):
        start = 0
        for count in (units_each // 2, units_each // 4, units_each // 4):
            pieces.append((weight, start * size, count))
            start += count
    return pieces


def run_events(order, table, attend, size):
    first = order.index("a0")
    last = order.index(f"a{size - 1}")
    for name in order[:first]:
        table[name]()

    def step(r, carry):
        attend(r)
        for k in range(size - 1):
            start = order.index(f"a{k}") + 1
            names = order[start : order.index(f"a{k + 1}")]
            if names:

                @pl.when(r == k)
                def _():
                    for name in names:
                        table[name]()

        return carry

    lax.fori_loop(0, size, step, 0)
    for name in order[last + 1 :]:
        table[name]()


def greet(partners):
    barrier = pltpu.get_barrier_semaphore()
    for partner in partners:
        pl.semaphore_signal(
            barrier, inc=1, device_id=partner, device_id_type=pl.DeviceIdType.MESH
        )


def await_greetings(partners):
    pl.semaphore_wait(pltpu.get_barrier_semaphore(), len(partners))


def scale_and_copy(scaled, copied, sums, lengths, factor):
    arrays = list(scaled) + list(copied)
    starts = [sum(lengths[:k]) for k in range(len(lengths))]

    def body(*refs):
        sums_ref, targets = refs[len(arrays)], refs[len(arrays) + 1 :]
        for k in range(len(arrays)):
            targets[k][...] = refs[k][...] * factor if k < len(scaled) else refs[k][...]
        for start, length, target in zip(starts, lengths, targets[len(arrays) :]):
            target[...] = sums_ref[start : start + length, :] * factor

    return pl.pallas_call(
        body,
        out_shape=[jax.ShapeDtypeStruct(array.shape, array.dtype) for array in arrays]
        + [jax.ShapeDtypeStruct((length, sums.shape[1]), F32) for length in lengths],
        in_specs=[pl.BlockSpec(memory_space=pltpu.VMEM)] * (len(arrays) + 1),
        out_specs=[pl.BlockSpec(memory_space=pltpu.VMEM)] * (len(arrays) + len(lengths)),
    )(*arrays, sums)


def forward_near(weights, hidden_in, cotangent, wide, bias_query, bias_value, bias_units, lengths, head_size):
    size = lax.axis_size("tensor")
    rows, width = hidden_in.shape
    block = width // len(ORDER)
    attn, units_each = weights[0].shape[1], weights[4].shape[1]
    cols = [3 * attn, attn, units_each, units_each]
    full = [(width, size * c) for c in cols]
    units = size * units_each
    half = block // 2
    pieces = pieces_of(size, attn, units_each)
    X = len(pieces) - 1
    pieces = pieces[:-3] + [pieces[-2], pieces[-1], pieces[-3]]
    A, O, U, _ = range(4)
    B_OUT, B_DOWN, G_ATTN, S_ATTN, G_FFN, S_FFN = range(6)

    def body(
        q_in, k_in, v_in, o_in, u_in, d_in, hidden_raw, cotangent_ref, bias_out_in, bias_down_in,
        gain_attn_in, shift_attn_in, gain_ffn_in, shift_ffn_in, bias_q_ref, bias_v_ref, bias_u_ref,
        lengths_ref,
        a_out, o_out, u_out, d_out, qkv_out, context_out, hidden_out, active_out, slope_out, output_ref,
        mixed_ref, mixed_t, normed_t, input_t, second_ref, sums_ref, wide_ref,
        a_ref, o_ref, u_ref, d_ref, x_ref, low_ref, active_ref, slope_ref, bias_ref, units_ref, qkv_ref,
        context_ref, hidden_ref, turned_x, turned_n, local_sem, send_sem, recv_sem,
        tile_sem,
    ):
        data_at, tensor_at = lax.axis_index("dp"), lax.axis_index("tensor")
        places = (a_ref, o_ref, u_ref, d_ref)

        def dp_partner(bit):
            return (neighbour(data_at, bit), tensor_at)

        def z_partner(step):
            return by_z[step]

        by_z = [(data_at, (tensor_at + step) % size) for step in range(size)]
        by_x, by_y, by_core = dp_partner(BIT_X), dp_partner(BIT_Y), dp_partner(BIT_CORE)
        owners = [block_of(data_at, mask) for mask in ORDER]
        copies = {}
        sent = {}

        def send(g, slot, source, target, device, when=None, lands=None):
            def copy():
                return pltpu.make_async_remote_copy(
                    src_ref=source,
                    dst_ref=target,
                    send_sem=send_sem.at[g, slot],
                    recv_sem=recv_sem.at[g, slot if lands is None else lands],
                    device_id=device,
                    device_id_type=pl.DeviceIdType.MESH,
                )

            copies[g, slot] = copy
            only(when, lambda: copy().start())
            sent[g, slot] = when

        def only(when, step):
            if when is None:
                step()
            else:
                pl.when(when())(step)

        def arrived(g, *slots):
            for slot in slots:
                copies[g, slot]().wait_recv()

        def whole(g, start, count):
            weight, first, wide_by = pieces[g]
            return places[weight].at[start : start + count, first : first + size * wide_by]

        def cell(g, start, count, r):
            weight, first, wide_by = pieces[g]
            at = first + r * wide_by
            return places[weight].at[start : start + count, at : at + wide_by]

        def send_z(g, count=block):
            send(g, 1, cell(g, 0, count, 0), cell(g, 0, count, 2), z_partner(2))
            send(g, 0, cell(g, 0, count, 0), cell(g, 0, count, 1), z_partner(1), lambda: tensor_at < size - 1)
            send(g, 2, cell(g, 0, count, 0), cell(g, 0, count, 3), z_partner(3), lambda: tensor_at > 0)

        def pass_on(g, count=block):
            arrived(g, 1)
            send(g, 9, cell(g, 0, count, 2), cell(g, 0, count, 1), z_partner(3), lambda: tensor_at == 1, 0)
            send(g, 10, cell(g, 0, count, 2), cell(g, 0, count, 3), z_partner(1), lambda: tensor_at == 2, 2)

        def send_column(g):
            arrived(g, 0, 2)
            send(g, 3, whole(g, 0, block), whole(g, block, block), by_x)
            send(g, 4, whole(g, 0, block), whole(g, 2 * block, block), by_y)

        def send_corner(g):
            arrived(g, 3, 4)
            send(g, 5, whole(g, block, half), whole(g, 3 * block, half), by_y)
            send(g, 6, whole(g, 2 * block + half, half), whole(g, 3 * block + half, half), by_x)
            send(g, 7, whole(g, 0, 3 * block), whole(g, 4 * block, 3 * block), by_core)

        def send_last(g):
            arrived(g, 5, 6)
            send(g, 8, whole(g, 3 * block, block), whole(g, 7 * block, block), by_core)

        def complete(*group):
            for g in group:
                arrived(g, 7, 8)

        def late_plane():
            send(X, 3, cell(X, 0, block, 0), cell(X, block, block, 0), by_x)
            send(X, 4, cell(X, 0, block, 0), cell(X, 2 * block, block, 0), by_y)

        def late_corner():
            arrived(X, 3, 4)
            send(X, 5, cell(X, block, half, 0), cell(X, 3 * block, half, 0), by_y)
            send(X, 6, cell(X, 2 * block + half, half, 0), cell(X, 3 * block + half, half, 0), by_x)

        def late_z():
            arrived(X, 5, 6)
            send_z(X, 4 * block)

        def late_core():
            arrived(X, 0, 2)
            send(X, 7, whole(X, 0, 4 * block), whole(X, 4 * block, 4 * block), by_core)

        saves = []

        def save(slot, source, target):
            copy = pltpu.make_async_copy(source, target, local_sem.at[slot])
            copy.start()
            saves.append(copy)

        def save_weight(slot, g):
            target = (a_out, o_out, u_out, d_out)[g]
            save(slot, places[g], target)

        sources = (q_in, k_in, v_in, o_in, u_in, u_in, u_in, d_in, d_in, d_in)

        def cast(g):
            weight, first, wide_by = pieces[g]
            start = first // size if weight >= U else 0
            places[weight][:block, first : first + wide_by] = sources[g][
                :, start : start + wide_by
            ].astype(BF16)

        partners = [by_x, by_y, by_core] + by_z[1:]
        greet(partners)
        for g in range(len(pieces)):
            cast(g)
        await_greetings(partners)

        def lanes_of(owner):
            return pl.ds(pl.multiple_of(owner * block, block), block)

        def turn(target, at, rows_of):
            for k in range(width // 128):
                target[k * 128 : (k + 1) * 128, at] = rows_of[:, k * 128 : (k + 1) * 128].T.astype(BF16)

        def vector(k):
            return wide_ref[k : k + 1, :]

        def column_of(r, first, span):
            at = ((tensor_at + size - r) % size) * (first[1]) + first[0]
            return pl.ds(pl.multiple_of(at, 128), span)

        def prepare():
            for place, owner in enumerate(owners):
                at = slice(place * block, (place + 1) * block)
                x_ref[:, at] = hidden_raw[:, lanes_of(owner)]
                for k, ref in enumerate(
                    (bias_out_in, bias_down_in, gain_attn_in, shift_attn_in, gain_ffn_in, shift_ffn_in)
                ):
                    wide_ref[k : k + 1, at] = ref[:, lanes_of(owner)]
            for r in range(size):
                at = slice(r * attn, (r + 1) * attn)
                bias_ref[0:1, at] = bias_q_ref[:, column_of(r, (0, attn), attn)]
                bias_ref[1:2, at] = bias_v_ref[:, column_of(r, (0, attn), attn)]
                for weight, first, wide_by in pieces:
                    if weight == U:
                        at = slice(first + r * wide_by, first + (r + 1) * wide_by)
                        units_ref[:, at] = bias_u_ref[
                            :, column_of(r, (first // size, units_each), wide_by)
                        ]

        def turn_inputs():
            def one(j, carry):
                at = pl.ds(pl.multiple_of(j * 128, 128), 128)
                turn(turned_x, at, x_ref[at, :].astype(F32))
                return carry

            lax.fori_loop(0, rows // 128, one, 0)
            save(4, turned_x, input_t)

        def project(j, carry):
            at = pl.ds(pl.multiple_of(j * attn, attn), attn)
            total = matmul(x_ref[...], a_ref[:, at])
            which = j // size
            bias = bias_ref[:, pl.ds(pl.multiple_of((j % size) * attn, attn), attn)]
            bias = jnp.where(which == 0, bias[0:1], jnp.where(which == 2, bias[1:2], 0.0))
            qkv_ref[:, at] = (total + bias).astype(BF16)
            return carry

        def qkv():
            complete(0, 1, 2)
            save_weight(A, A)
            lax.fori_loop(0, 3 * size, project, 0)
            save(5, qkv_ref, qkv_out)

        scale = float(head_size) ** (-0.5)
        length = lengths_ref[tensor_at]

        def attend(r):
            seen = lax.broadcasted_iota(jnp.int32, (rows, rows), 1) < length
            for start, lanes, held in pairs_of(attn, head_size):
                at = [
                    pl.ds(pl.multiple_of((k * size + r) * attn + start, 128), lanes) for k in range(3)
                ]
                queries, keys, values = (qkv_ref[:, where] for where in at)
                total = jnp.zeros((rows, lanes), F32)
                for which in range(held):
                    probs = soft_weights(keep_head(queries, which, head_size), keys, seen, scale)
                    total += keep_head(matmul(probs.astype(BF16), values), which, head_size)
                context_ref[:, at[0]] = total.astype(BF16)

        def output(j, carry):
            at = pl.ds(pl.multiple_of(j * 256, 256), 256)
            total = contract_cols(context_ref[...], o_ref[at, :])
            hidden_ref[:, at] = x_ref[:, at].astype(F32) + total + wide_ref[B_OUT : B_OUT + 1, at]
            return carry

        def out():
            complete(3)
            save_weight(O, O)
            save(6, context_ref, context_out)
            lax.fori_loop(0, width // 256, output, 0)
            save(7, hidden_ref, hidden_out)

        chunk = 128

        def norm_step(j, carry):
            at = pl.ds(pl.multiple_of(j * chunk, chunk), chunk)
            normed = norm_forward(hidden_ref[at, :], vector(G_ATTN), vector(S_ATTN))[0]
            low_ref[at, :] = normed.astype(BF16)
            second_ref[at, :] = normed + vector(B_DOWN)
            turn(turned_n, at, normed)
            return carry

        def norm():
            lax.fori_loop(0, rows // chunk, norm_step, 0)
            save(8, turned_n, normed_t)

        def tile_at(j):
            return pl.ds(pl.multiple_of(j * TILE, TILE), TILE)

        def slope_copy(j):
            return pltpu.make_async_copy(
                slope_ref.at[j % 2], slope_out.at[:, tile_at(j)], tile_sem.at[1, j % 2]
            )

        def active_copy(j):
            return pltpu.make_async_copy(
                active_ref.at[:, tile_at(j)], active_out.at[:, tile_at(j)], tile_sem.at[0, j]
            )

        def raise_up(j, carry):
            @pl.when(j >= 2)
            def _():
                slope_copy(j - 2).wait()

            total = matmul(low_ref[...], u_ref[:, tile_at(j)])
            active, slope = activate(total, units_ref[:, tile_at(j)])
            active_ref[:, tile_at(j)] = active.astype(BF16)
            slope_ref[j % 2] = slope
            active_copy(j).start()
            slope_copy(j).start()
            return carry

        def span_of(g):
            _, first, wide_by = pieces[g]
            return slice(first, first + size * wide_by)

        def raise_piece(g):
            complete(g)
            save(g + 5, u_ref.at[:, span_of(g)], u_out.at[:, span_of(g)])
            at = span_of(g)
            lax.fori_loop(at.start // TILE, at.stop // TILE, raise_up, 0)

        def lower_piece(g):
            if g == X:
                arrived(X, 7)
            else:
                complete(g)
            at = span_of(g)
            save(g + 5, d_ref.at[:, at], d_out.at[:, at])

            def one(j, carry):
                to = pl.ds(pl.multiple_of(j * 256, 256), 256)
                second_ref[:, to] += contract_cols(active_ref[:, at], d_ref[to, at])
                return carry

            lax.fori_loop(0, width // 256, one, 0)

        def second(j, sums):
            at = pl.ds(pl.multiple_of(j * chunk, chunk), chunk)
            result, normal, root = norm_forward(second_ref[at, :], vector(G_FFN), vector(S_FFN))
            grads = jnp.concatenate([cotangent_ref[at, lanes_of(owner)] for owner in owners], axis=1)
            for place, owner in enumerate(owners):
                output_ref[at, lanes_of(owner)] = result[:, place * block : (place + 1) * block].astype(BF16)
            hidden, more_gain, more_shift = norm_backward(
                grads.astype(F32), normal, root, vector(G_FFN)
            )
            second_ref[at, :] = hidden
            mixed_ref[at, :] = hidden.astype(BF16)
            turn(mixed_t, at, hidden)
            more = (jnp.sum(hidden, axis=0), more_gain, more_shift)
            return tuple(a + b[None] for a, b in zip(sums, more))

        def last_norm():
            zero = jnp.zeros((1, width), F32)
            sums = lax.fori_loop(0, rows // chunk, second, (zero, zero, zero))
            for k in range(3):
                sums_ref[k : k + 1, :] = sums[k]

        def bound(step, *given):
            return lambda: step(*given)

        table = {
            "prep": prepare, "tr": turn_inputs, "qkv": qkv, "out": out, "norm": norm, "ln": last_norm,
            "up1": bound(raise_piece, 4), "up2": bound(raise_piece, 5), "up3": bound(raise_piece, 6),
            "low1": bound(lower_piece, 7), "low2": bound(lower_piece, 8), "lowX": bound(lower_piece, X),
            "fw9": bound(pass_on, X, 4 * block), "lplane9": late_plane, "lcor9": late_corner, "lz9": late_z, "lcore9": late_core,
        }
        for g in range(X):
            table[f"z{g}"] = bound(send_z, g)
            table[f"fw{g}"] = bound(pass_on, g)
            table[f"col{g}"] = bound(send_column, g)
            table[f"cor{g}"] = bound(send_corner, g)
            table[f"last{g}"] = bound(send_last, g)
        run_events(FORWARD, table, attend, size)

        def settle(j, carry):
            active_copy(j).wait()
            return carry

        lax.fori_loop(0, units // TILE, settle, 0)
        for j in (units // TILE - 2, units // TILE - 1):
            slope_copy(j).wait()
        for copy in saves:
            copy.wait()
        for key, copy in copies.items():
            only(sent[key], lambda: copy().wait_send())

    anywhere, inside = pl.BlockSpec(memory_space=pl.ANY), pl.BlockSpec(memory_space=pltpu.VMEM)
    tall = jax.ShapeDtypeStruct((rows, width), BF16)
    turned = jax.ShapeDtypeStruct((width, rows), BF16)
    return pl.pallas_call(
        body,
        out_shape=[jax.ShapeDtypeStruct(shape, BF16) for shape in full]
        + [
            jax.ShapeDtypeStruct((rows, full[A][1]), BF16),
            tall,
            jax.ShapeDtypeStruct((rows, width), F32),
            jax.ShapeDtypeStruct((rows, units), BF16),
            jax.ShapeDtypeStruct((rows, units), F32),
            tall,
            tall,
            turned,
            turned,
            turned,
            jax.ShapeDtypeStruct((rows, width), F32),
            jax.ShapeDtypeStruct((3, width), F32),
            jax.ShapeDtypeStruct((6, width), F32),
        ],
        in_specs=[inside] * 17 + [pl.BlockSpec(memory_space=pltpu.SMEM)],
        out_specs=[anywhere] * 9 + [inside] * 3 + [anywhere] * 2 + [inside] * 3,
        scratch_shapes=[pltpu.VMEM(shape, BF16) for shape in full]
        + [
            pltpu.VMEM((rows, width), BF16),
            pltpu.VMEM((rows, width), BF16),
            pltpu.VMEM((rows, units), BF16),
            pltpu.VMEM((2, rows, TILE), F32),
            pltpu.VMEM((2, size * attn), F32),
            pltpu.VMEM((1, units), F32),
            pltpu.VMEM((rows, full[A][1]), BF16),
            pltpu.VMEM((rows, width), BF16),
            pltpu.VMEM((rows, width), F32),
            pltpu.VMEM((width, rows), BF16),
            pltpu.VMEM((width, rows), BF16),
            pltpu.SemaphoreType.DMA((5 + len(pieces),)),
            pltpu.SemaphoreType.DMA((len(pieces), 11)),
            pltpu.SemaphoreType.DMA((len(pieces), 11)),
            pltpu.SemaphoreType.DMA((2, units // TILE)),
        ],
        compiler_params=pltpu.CompilerParams(
            collective_id=FORWARD_ID, has_side_effects=True, vmem_limit_bytes=63 * 2**20
        ),
        cost_estimate=pl.CostEstimate(
            flops=2 * rows * width * sum(shape[1] for shape in full),
            bytes_accessed=4 * width * sum(shape[1] for shape in full),
            transcendentals=rows * units,
        ),
        name="forward_near",
    )(
        *weights, hidden_in, cotangent, *(vector[None] for vector in wide), bias_query[None],
        bias_value[None], bias_units[None], lengths,
    )


def backward_near(mixed_low, mixed_t, normed_t, input_t, context, grad_second, hidden, wide, lengths,
                  active, slope, qkv, weights, vectors, head_size):
    size = lax.axis_size("tensor")
    rows, width = mixed_low.shape
    block = width // len(ORDER)
    middle = width // 2
    half = block // 2
    full = [weight.shape[1] for weight in weights]
    units = full[2]
    units_each = units // size
    attn = full[1] // size
    pieces = pieces_of(size, attn, units_each)
    X = len(pieces) - 1
    A, O, U, D = range(4)
    tiles = [c // TILE for c in full]
    vector_rows = (6 * width + 2 * full[1] + units) // 128
    v_query, v_value, v_up = 6 * width // 128, (6 * width + full[1]) // 128, (6 * width + 2 * full[1]) // 128
    scale = float(head_size) ** (-0.5)

    def body(
        mixed_in, mixed_t, normed_in, input_in, context_in, second_in, hidden_in, wide_ref,
        lengths_ref, active_in, slope_in, qkv_in, a_in, o_in, u_in, d_in, vectors_ref,
        q_out, k_out, v_out, o_out, u_out, d_out, grad_out, sums_out,
        w_buf, act_ref, slope_buf, gu_ref, grad_ref, low_ref, low_t, gctx_ref, qkv_buf, send_buf,
        units_sum, mixed_ref, normed_t, input_t, context_ref, a_plane, o_plane, u_plane, d_plane, *rest,
    ):
        count = len(pieces)
        corners, sides, zins = (rest[k * count : (k + 1) * count] for k in range(3))
        (
            v_ref, v_in, load_sem, start_sem, core_send, core_recv, send_sem, recv_sem, v_send, v_recv,
        ) = rest[3 * count :]
        data_at, tensor_at = lax.axis_index("dp"), lax.axis_index("tensor")
        planes = (a_plane, o_plane, u_plane, d_plane)
        outs = (q_out, k_out, v_out, o_out, u_out, u_out, u_out, d_out, d_out, d_out)
        shift_by = (tiles[O], 0, 0, 0)

        def dp_partner(bit):
            return (neighbour(data_at, bit), tensor_at)

        def z_partner(step):
            return by_z[step % size]

        by_z = [(data_at, (tensor_at + step) % size) for step in range(size)]

        by_x, by_y, by_core = dp_partner(BIT_X), dp_partner(BIT_Y), dp_partner(BIT_CORE)

        def column(j, span=TILE):
            return pl.ds(pl.multiple_of(j * span, 128), span)

        def load(row, source, buffer, j):
            return pltpu.make_async_copy(
                source.at[:, column(j)], buffer.at[j % 2], load_sem.at[row, j % 2]
            )

        def over_tiles(first, last, loads, step):
            for row, source, buffer in loads:
                load(row, source, buffer, first).start()

            def one(j, carry):
                @pl.when(j + 1 < last)
                def _():
                    for row, source, buffer in loads:
                        load(row, source, buffer, j + 1).start()

                for row, source, buffer in loads:
                    load(row, source, buffer, j).wait()
                step(j)
                return carry

            lax.fori_loop(first, last, one, 0)

        def remote(source, target, send, receive, device):
            return pltpu.make_async_remote_copy(
                src_ref=source,
                dst_ref=target,
                send_sem=send,
                recv_sem=receive,
                device_id=device,
                device_id_type=pl.DeviceIdType.MESH,
            )

        def core_copy(g, j):
            return remote(
                send_buf.at[:, column(j + shift_by[g])],
                planes[g].at[:, column(j)],
                core_send.at[g, j],
                core_recv.at[g, j],
                by_core,
            )

        copies = {}

        def send(g, slot, source, target, device):
            def copy():
                return remote(source, target(), send_sem.at[g, slot], recv_sem.at[g, slot], device)

            copies[g, slot] = copy
            copy().start()

        def arrived(g, *slots):
            for slot in slots:
                copies[g, slot]().wait_recv()

        def other_tile(g, left_t, right, j):
            send_buf[:, column(j + shift_by[g])] = matmul(left_t[middle:, :], right).astype(BF16)
            core_copy(g, j).start()

        def own_tile(g, left_t, right, j):
            core_copy(g, j).wait_recv()
            total = matmul(left_t[:middle, :], right) + planes[g][:, column(j)].astype(F32)
            planes[g][:, column(j)] = total.astype(BF16)

        def span(g):
            _, first, wide_by = pieces[g]
            return first, wide_by if g == X else size * wide_by

        def plane_rows(g, start, count):
            first, wide_by = span(g)
            return planes[pieces[g][0]].at[start : start + count, first : first + wide_by]

        def send_corner(g):
            send(g, 0, plane_rows(g, 3 * block, half), lambda: corners[g].at[0], by_x)
            send(g, 1, plane_rows(g, 3 * block + half, half), lambda: corners[g].at[1], by_y)

        def add_rows(g, start, count, *more):
            plane = planes[pieces[g][0]]
            first, wide_by = span(g)
            step = min(TILE, wide_by)
            for at in range(0, wide_by, step):
                where = (slice(start, start + count), slice(first + at, first + at + step))
                total = plane[where].astype(F32)
                for ref in more:
                    total += ref[:, at : at + step].astype(F32)
                plane[where] = total.astype(BF16)

        def send_sides(g):
            arrived(g, 0, 1)
            add_rows(g, 2 * block, half, corners[g].at[0])
            add_rows(g, block + half, half, corners[g].at[1])
            send(g, 2, plane_rows(g, block, block), lambda: sides[g].at[0], by_x)
            send(g, 3, plane_rows(g, 2 * block, block), lambda: sides[g].at[1], by_y)

        def out_of(g):
            weight, first, wide_by = pieces[g]
            start = first // size if weight >= U else 0
            return outs[g].at[:, start : start + wide_by]

        def send_column(g):
            arrived(g, 2, 3)
            weight, first, wide_by = pieces[g]
            for r in range(size):
                at = slice(r * wide_by, (r + 1) * wide_by)
                own = slice(first + r * wide_by, first + (r + 1) * wide_by)
                total = planes[weight][:block, own].astype(F32)
                total += sides[g][0, :, at].astype(F32) + sides[g][1, :, at].astype(F32)
                if r == 0:
                    out_of(g)[...] = total
                else:
                    planes[weight][:block, own] = total.astype(BF16)
                    send(g, 3 + r, planes[weight].at[:block, own], lambda r=r: zins[g].at[r - 1], z_partner(-r))

        def finish(g):
            arrived(g, *range(4, 3 + size))
            total = out_of(g)[...]
            for r in range(1, size):
                total += zins[g][r - 1].astype(F32)
            out_of(g)[...] = total

        def late_z():
            weight, first, wide_by = pieces[X]
            for r in range(1, size):
                own = slice(first + r * wide_by, first + (r + 1) * wide_by)
                send(X, 3 + r, planes[weight].at[:, own], lambda r=r: zins[X].at[r - 1], z_partner(-r))

        def late_corner():
            arrived(X, *range(4, 3 + size))
            for k in range(4):
                rows_k = slice(k * block, (k + 1) * block)
                add_rows(X, k * block, block, *(zins[X].at[r, rows_k] for r in range(size - 1)))
            send_corner(X)

        def late_finish():
            arrived(X, 2, 3)
            total = plane_rows(X, 0, block)[...].astype(F32)
            out_of(X)[...] = total + sides[X][0].astype(F32) + sides[X][1].astype(F32)

        def feature_rows(k, vector):
            for place, mask in enumerate(ORDER):
                at = block_of(data_at, mask)
                v_ref[0, pl.ds(k * len(ORDER) + at, 1), :] = vector[:, place * 128 : (place + 1) * 128]

        z_near = tensor_at + 1 - 2 * (tensor_at % 2)
        z_across = tensor_at + 2 - 4 * ((tensor_at // 2) % 2)
        v_partners = (by_core, (data_at, z_near), (data_at, z_across), by_x, by_y)

        def v_copy(k):
            return remote(v_ref.at[k], v_in.at[k], v_send.at[k], v_recv.at[k], v_partners[k])

        def v_add(k):
            v_copy(k).wait_recv()
            v_ref[k + 1] = v_ref[k] + v_in[k]

        early = [
            pltpu.make_async_copy(
                active_in.at[:, k * (units // 2) : (k + 1) * (units // 2)],
                act_ref.at[:, k * (units // 2) : (k + 1) * (units // 2)],
                start_sem.at[k],
            )
            for k in range(2)
        ]
        grad_load, mixed_load, normed_load, context_load, input_load = (
            pltpu.make_async_copy(source, target, start_sem.at[k])
            for k, (source, target) in enumerate(
                (
                    (second_in, grad_ref),
                    (mixed_in, mixed_ref),
                    (normed_in, normed_t),
                    (context_in, context_ref),
                    (input_in, input_t),
                ),
                2,
            )
        )
        for copy in early:
            copy.start()
        for copy in (mixed_load, normed_load, grad_load, context_load, input_load):
            copy.start()
        partners = [by_x, by_y, by_core] + by_z[1:]
        greet(partners)
        await_greetings(partners)

        def each(first, last, step):
            def one(j, carry):
                step(j)
                return carry

            lax.fori_loop(first, last, one, 0)

        def other_down(j):
            other_tile(D, mixed_t, act_ref[:, column(j)], j)

        def own_down(j):
            own_tile(D, mixed_t, act_ref[:, column(j)], j)

        def other_up(j):
            core_copy(D, j).wait_send()
            other_tile(U, normed_t, gu_ref[:, column(j)], j)

        def own_up(j):
            own_tile(U, normed_t, gu_ref[:, column(j)], j)

        def bounds(g):
            _, first, wide_by = pieces[g]
            return first // TILE, (first + size * wide_by) // TILE

        early[0].wait()
        early[1].wait()

        def loaded(copy, step):
            def both():
                copy.wait()
                step()

            return both

        def bound(step, *given):
            return lambda: step(*given)

        def gelu_step(j):
            low = (matmul(mixed_ref[...], w_buf[j % 2]) * slope_buf[j % 2]).astype(BF16)
            gu_ref[:, column(j)] = low
            units_sum[:, column(j)] = jnp.sum(low.astype(F32), axis=0, keepdims=True)

        gelu_loads = [(1, d_in, w_buf), (2, slope_in, slope_buf)]
        hidden_loads = [
            pltpu.make_async_copy(hidden_in.at[:, column(k)], slope_buf.at[k], load_sem.at[2, k])
            for k in range(2)
        ]

        def second_gelu():
            over_tiles(tiles[D] // 2, tiles[D], gelu_loads, gelu_step)
            for copy in hidden_loads:
                copy.start()

        def up_step(j):
            grad_ref[...] += contract_cols(gu_ref[:, column(j)], w_buf[j % 2])

        def sum_units():
            for k in range(3):
                feature_rows((1, 4, 5)[k], vectors_ref[k : k + 1, :])
            for r in range(size):
                for weight, first, wide_by in pieces:
                    if weight == U:
                        for k in range(wide_by // 128):
                            place = ((tensor_at + size - r) % size) * (units_each // 128)
                            place += (first // size) // 128 + k
                            at = first + r * wide_by + k * 128
                            v_ref[0, pl.ds(v_up + place, 1), :] = units_sum[:, at : at + 128]

        chunk = 128

        def norm_step(j, sums):
            at = pl.ds(pl.multiple_of(j * chunk, chunk), chunk)
            hidden_rows = jnp.concatenate([slope_buf[0, at, :], slope_buf[1, at, :]], axis=1)
            gain = wide_ref[2:3, :]
            normal, root = norm_forward(hidden_rows, gain, gain)[1:]
            hidden, more_gain, more_shift = norm_backward(grad_ref[at, :], normal, root, gain)
            grad_ref[at, :] = hidden
            low_ref[at, :] = hidden.astype(BF16)
            for k in range(width // 128):
                low_t[k * 128 : (k + 1) * 128, at] = hidden[:, k * 128 : (k + 1) * 128].T.astype(BF16)
            more = (jnp.sum(hidden, axis=0), more_gain, more_shift)
            return tuple(a + b[None] for a, b in zip(sums, more))

        def norm():
            for copy in hidden_loads:
                copy.wait()
            zero = jnp.zeros((1, width), F32)
            sums = lax.fori_loop(0, rows // chunk, norm_step, (zero, zero, zero))
            for k in range(3):
                feature_rows((0, 2, 3)[k], sums[k])

        def out_step(j):
            core_copy(U, j).wait_send()
            gctx_ref[:, column(j)] = matmul(low_ref[...], w_buf[j % 2]).astype(BF16)
            other_tile(O, low_t, context_ref[:, column(j)], j)

        def out():
            context_load.wait()
            over_tiles(0, tiles[O], [(1, o_in, w_buf)], out_step)
            for copy in qkv_load(0):
                copy.start()

        def own_out():
            for j in range(tiles[O]):
                own_tile(O, low_t, context_ref[:, j * TILE : (j + 1) * TILE], j)

        def qkv_load(r):
            return [
                pltpu.make_async_copy(
                    qkv_in.at[:, column(k * size + r, attn)], qkv_buf.at[r % 2, k], load_sem.at[k, r % 2]
                )
                for k in range(3)
            ]

        def attend_step(r):
            @pl.when(r + 1 < size)
            def _():
                for copy in qkv_load(r + 1):
                    copy.start()

            for copy in qkv_load(r):
                copy.wait()
            slot = r % 2
            seen = lax.broadcasted_iota(jnp.int32, (rows, rows), 0) < length
            for start, lanes, held in pairs_of(attn, head_size):
                queries, keys, values = (qkv_buf[slot, k, :, start : start + lanes] for k in range(3))
                grads = gctx_ref[:, pl.ds(pl.multiple_of(r * attn + start, 128), lanes)]
                grad_q = jnp.zeros((rows, lanes), F32)
                grad_k = jnp.zeros((rows, lanes), F32)
                grad_v = jnp.zeros((rows, lanes), F32)
                for which in range(held):
                    mine = keep_head(grads, which, head_size)
                    query = keep_head(queries, which, head_size)
                    scores = jnp.where(seen, contract_cols(keys, query) * scale, MASKED)
                    exponent = jnp.exp(scores - jnp.max(scores, axis=0, keepdims=True))
                    probs = exponent * (1.0 / jnp.sum(exponent, axis=0, keepdims=True))
                    grad_v += matmul(probs.astype(BF16), mine)
                    grad_probs = contract_cols(values, mine)
                    inner = jnp.sum(probs * grad_probs, axis=0, keepdims=True)
                    grad_scores = (probs * (grad_probs - inner)).astype(BF16)
                    grad_q += keep_head(contract_rows(grad_scores, keys), which, head_size)
                    grad_k += matmul(grad_scores, query)
                low_q = (grad_q * scale).astype(BF16)
                low_v = grad_v.astype(BF16)
                for k, low in enumerate((low_q, (grad_k * scale).astype(BF16), low_v)):
                    at = pl.multiple_of((k * size + r) * attn + start, 128)
                    gu_ref[:, pl.ds(at, lanes)] = low
                place = ((tensor_at + size - r) % size) * (attn // 128) + start // 128
                v_ref[0, pl.ds(v_query + place, 1), :] = jnp.sum(
                    low_q.astype(F32), axis=0, keepdims=True
                )
                v_ref[0, pl.ds(v_value + place, 1), :] = jnp.sum(
                    low_v.astype(F32), axis=0, keepdims=True
                )

        length = lengths_ref[tensor_at]

        def other_qkv(j):
            core_copy(U, j + tiles[O]).wait_send()
            other_tile(A, input_t, gu_ref[:, column(j)], j)

        def own_qkv(j):
            own_tile(A, input_t, gu_ref[:, column(j)], j)

        def input_step(j):
            grad_ref[...] += contract_cols(gu_ref[:, column(j)], w_buf[j % 2])

        def give_input():
            for place, mask in enumerate(ORDER):
                at = block_of(data_at, mask)
                grad_out[:, pl.ds(pl.multiple_of(at * block, block), block)] = grad_ref[
                    :, place * block : (place + 1) * block
                ].astype(BF16)

        def give_sums():
            v_add(4)
            sums_out[...] = v_ref[5]

        def next_sum(k):
            v_add(k - 1)
            v_copy(k).start()

        weight_loads = [[(1, ref, w_buf)] for ref in (a_in, o_in, u_in, d_in)]
        parts = (
            (other_qkv, own_qkv), (other_qkv, own_qkv), (other_qkv, own_qkv), (lambda j: None, own_out),
            (other_up, own_up), (other_up, own_up), (other_up, own_up), (other_down, own_down),
            (other_down, own_down), (other_down, own_down),
        )
        halves = [(0, count // 2, count) for count in tiles]
        table = {
            "gelA": loaded(mixed_load, bound(over_tiles, 0, halves[D][1], gelu_loads, gelu_step)),
            "gelB": second_gelu,
            "upA": loaded(grad_load, bound(over_tiles, 0, halves[U][1], weight_loads[U], up_step)),
            "upB": bound(over_tiles, *halves[U][1:], weight_loads[U], up_step),
            "vec": sum_units,
            "norm": norm,
            "out": out,
            "dxA": bound(over_tiles, 0, halves[A][1], weight_loads[A], input_step),
            "dxB": bound(over_tiles, *halves[A][1:], weight_loads[A], input_step),
            "gout": give_input,
            "lz9": late_z,
            "lcor9": late_corner,
            "sid9": bound(send_sides, X),
            "fin9": late_finish,
            "v0": lambda: v_copy(0).start(),
            "v5": give_sums,
        }
        for k in range(1, 5):
            table[f"v{k}"] = bound(next_sum, k)
        for g in range(len(pieces)):
            other, own = parts[g]
            table[f"oth{g}"] = bound(each, *bounds(g), other)
            table[f"own{g}"] = bound(each, *bounds(g), own)
            if g < X:
                table[f"cor{g}"] = bound(send_corner, g)
                table[f"sid{g}"] = bound(send_sides, g)
                table[f"col{g}"] = bound(send_column, g)
                table[f"fin{g}"] = bound(finish, g)
        table["oth3"] = lambda: None
        table["own3"] = own_out
        first_up = [g for g in range(len(pieces)) if f"oth{g}" in BACKWARD and pieces[g][0] == U]
        first_up = min(first_up, key=lambda g: BACKWARD.index(f"oth{g}"))
        table[f"oth{first_up}"] = loaded(normed_load, table[f"oth{first_up}"])
        first_in = min((0, 1, 2), key=lambda g: BACKWARD.index(f"oth{g}"))
        table[f"oth{first_in}"] = loaded(input_load, table[f"oth{first_in}"])
        run_events(BACKWARD, table, attend_step, size)
        for g in (A, O):
            for j in range(tiles[g]):
                core_copy(g, j).wait_send()
        for k in range(5):
            v_copy(k).wait_send()
        for copy in copies.values():
            copy().wait_send()

    spans = [piece[2] if g == X else size * piece[2] for g, piece in enumerate(pieces)]
    anywhere, inside = pl.BlockSpec(memory_space=pl.ANY), pl.BlockSpec(memory_space=pltpu.VMEM)
    results = pl.pallas_call(
        body,
        out_shape=[jax.ShapeDtypeStruct((block, attn), F32)] * 4
        + [jax.ShapeDtypeStruct((block, units_each), F32)] * 2
        + [
            jax.ShapeDtypeStruct((rows, width), BF16),
            jax.ShapeDtypeStruct((vector_rows, 128), F32),
        ],
        in_specs=[anywhere, inside]
        + [anywhere] * 5
        + [inside, pl.BlockSpec(memory_space=pltpu.SMEM)]
        + [anywhere] * 7
        + [inside],
        out_specs=[inside] * 8,
        scratch_shapes=[
            pltpu.VMEM((2, width, TILE), BF16),
            pltpu.VMEM((rows, units), BF16),
            pltpu.VMEM((2, rows, TILE), F32),
            pltpu.VMEM((rows, units), BF16),
            pltpu.VMEM((rows, width), F32),
            pltpu.VMEM((rows, width), BF16),
            pltpu.VMEM((width, rows), BF16),
            pltpu.VMEM((rows, full[1]), BF16),
            pltpu.VMEM((2, 3, rows, attn), BF16),
            pltpu.VMEM((middle, units), BF16),
            pltpu.VMEM((1, units), F32),
            pltpu.VMEM((rows, width), BF16),
            pltpu.VMEM((width, rows), BF16),
            pltpu.VMEM((width, rows), BF16),
            pltpu.VMEM((rows, width), BF16),
        ]
        + [pltpu.VMEM((middle, c), BF16) for c in full]
        + [pltpu.VMEM((2, half, c), BF16) for c in spans]
        + [pltpu.VMEM((2, block, c), BF16) for c in spans]
        + [
            pltpu.VMEM((size - 1, 4 * block if g == X else block, piece[2]), BF16)
            for g, piece in enumerate(pieces)
        ]
        + [
            pltpu.VMEM((6, vector_rows, 128), F32),
            pltpu.VMEM((5, vector_rows, 128), F32),
            pltpu.SemaphoreType.DMA((3, 2)),
            pltpu.SemaphoreType.DMA((7,)),
            pltpu.SemaphoreType.DMA((4, units // TILE)),
            pltpu.SemaphoreType.DMA((4, units // TILE)),
            pltpu.SemaphoreType.DMA((len(pieces), 3 + size)),
            pltpu.SemaphoreType.DMA((len(pieces), 3 + size)),
            pltpu.SemaphoreType.DMA((5,)),
            pltpu.SemaphoreType.DMA((5,)),
        ],
        compiler_params=pltpu.CompilerParams(
            collective_id=BACKWARD_ID, has_side_effects=True, vmem_limit_bytes=63 * 2**20
        ),
        cost_estimate=pl.CostEstimate(
            flops=4 * rows * sum(full) * width,
            bytes_accessed=4 * sum(full) * width,
            transcendentals=0,
        ),
        name="backward_near",
    )(
        mixed_low, mixed_t, normed_t, input_t, context, grad_second, hidden, wide, lengths, active,
        slope, qkv, *weights, vectors,
    )
    return results[:6], results[6], results[7]


def gather_far(shard):
    return lax.all_gather(
        lax.all_gather(shard, "tensor", axis=1, tiled=True), "dp", axis=0, tiled=True
    )


def scatter_far(left_side, right_side):
    whole = contract_rows(left_side, right_side).astype(BF16)
    part = lax.psum_scatter(whole, "dp", scatter_dimension=0, tiled=True)
    return lax.psum_scatter(part, "tensor", scatter_dimension=1, tiled=True).astype(F32)


def soft_weights(queries, keys, visible, scale):
    scores = contract_cols(queries, keys) * scale
    scores = jnp.where(visible, scores, MASKED)
    exponent = jnp.exp(scores - jnp.max(scores, axis=-1, keepdims=True))
    return exponent * (1.0 / jnp.sum(exponent, axis=-1, keepdims=True))


def pairs_of(width, head_size):
    lanes = max(128, head_size)
    return [(start, lanes, lanes // head_size) for start in range(0, width, lanes)]


def keep_head(array, which, head_size):
    lane = lax.broadcasted_iota(jnp.int32, array.shape, 1)
    return jnp.where(lane // head_size == which, array, jnp.zeros_like(array))


def attend_forward(qkv_q, qkv_kv, length, head_size, groups):
    q_rows = qkv_q.shape[0]
    k_rows = qkv_kv.shape[0]
    block = qkv_q.shape[1] // groups
    width = block // 3
    scale = float(head_size) ** (-0.5)

    def body(length_ref, q_ref, kv_ref, out_ref):
        visible = lax.broadcasted_iota(jnp.int32, (q_rows, k_rows), 1) < length_ref[0]
        for start, lanes, held in pairs_of(width, head_size):
            queries = q_ref[:, start : start + lanes]
            keys = kv_ref[:, width + start : width + start + lanes]
            values = kv_ref[:, 2 * width + start : 2 * width + start + lanes]
            total = jnp.zeros((q_rows, lanes), F32)
            for which in range(held):
                probs = soft_weights(keep_head(queries, which, head_size), keys, visible, scale)
                total += keep_head(matmul(probs.astype(BF16), values), which, head_size)
            out_ref[:, start : start + lanes] = total.astype(BF16)

    return pl.pallas_call(
        body,
        out_shape=jax.ShapeDtypeStruct((q_rows, groups * width), BF16),
        grid_spec=pltpu.PrefetchScalarGridSpec(
            num_scalar_prefetch=1,
            grid=(groups,),
            in_specs=[
                pl.BlockSpec((q_rows, block), lambda g, length_ref: (0, g)),
                pl.BlockSpec((k_rows, block), lambda g, length_ref: (0, g)),
            ],
            out_specs=pl.BlockSpec((q_rows, width), lambda g, length_ref: (0, g)),
        ),
        cost_estimate=pl.CostEstimate(
            flops=4 * q_rows * k_rows * width * groups,
            bytes_accessed=2 * (2 * q_rows + 2 * k_rows) * width * groups,
            transcendentals=q_rows * k_rows * groups * width // head_size,
        ),
        name="attend_forward",
    )(length, qkv_q, qkv_kv)


def attend_backward(qkv_q, qkv_kv, grad_context, length, head_size, groups):
    q_rows = qkv_q.shape[0]
    k_rows = qkv_kv.shape[0]
    block = qkv_q.shape[1] // groups
    width = block // 3
    scale = float(head_size) ** (-0.5)

    def body(length_ref, q_ref, kv_ref, grad_ref, dq_ref, dkv_ref):
        visible = lax.broadcasted_iota(jnp.int32, (q_rows, k_rows), 1) < length_ref[0]
        for start, lanes, held in pairs_of(width, head_size):
            queries = q_ref[:, start : start + lanes]
            keys = kv_ref[:, width + start : width + start + lanes]
            values = kv_ref[:, 2 * width + start : 2 * width + start + lanes]
            grads = grad_ref[:, start : start + lanes]
            grad_q = jnp.zeros((q_rows, lanes), F32)
            grad_k = jnp.zeros((k_rows, lanes), F32)
            grad_v = jnp.zeros((k_rows, lanes), F32)
            for which in range(held):
                mine = keep_head(grads, which, head_size)
                query = keep_head(queries, which, head_size)
                probs = soft_weights(query, keys, visible, scale)
                grad_v += contract_rows(probs.astype(BF16), mine)
                grad_probs = contract_cols(mine, values)
                inner = jnp.sum(probs * grad_probs, axis=-1, keepdims=True)
                grad_scores = (probs * (grad_probs - inner)).astype(BF16)
                grad_q += keep_head(matmul(grad_scores, keys), which, head_size)
                grad_k += contract_rows(grad_scores, query)
            dq_ref[:, start : start + lanes] = (grad_q * scale).astype(BF16)
            dkv_ref[:, start : start + lanes] = (grad_k * scale).astype(BF16)
            dkv_ref[:, width + start : width + start + lanes] = grad_v.astype(BF16)

    return pl.pallas_call(
        body,
        out_shape=(
            jax.ShapeDtypeStruct((q_rows, groups * width), BF16),
            jax.ShapeDtypeStruct((k_rows, groups * 2 * width), BF16),
        ),
        grid_spec=pltpu.PrefetchScalarGridSpec(
            num_scalar_prefetch=1,
            grid=(groups,),
            in_specs=[
                pl.BlockSpec((q_rows, block), lambda g, length_ref: (0, g)),
                pl.BlockSpec((k_rows, block), lambda g, length_ref: (0, g)),
                pl.BlockSpec((q_rows, width), lambda g, length_ref: (0, g)),
            ],
            out_specs=[
                pl.BlockSpec((q_rows, width), lambda g, length_ref: (0, g)),
                pl.BlockSpec((k_rows, 2 * width), lambda g, length_ref: (0, g)),
            ],
        ),
        cost_estimate=pl.CostEstimate(
            flops=10 * q_rows * k_rows * width * groups,
            bytes_accessed=2 * (3 * q_rows + 4 * k_rows) * width * groups,
            transcendentals=q_rows * k_rows * groups * width // head_size,
        ),
        name="attend_backward",
    )(length, qkv_q, qkv_kv, grad_context)


def activate(total, bias):
    upper = total + bias
    cumulative = 0.5 * (1.0 + lax.erf(upper * math.sqrt(0.5)))
    density = jnp.exp(-0.5 * upper * upper) * (1.0 / math.sqrt(2.0 * math.pi))
    return upper * cumulative, cumulative + upper * density


def norm_forward(hidden, gain_vec, shift_vec):
    center = hidden - jnp.mean(hidden, axis=-1, keepdims=True)
    variance = jnp.mean(center * center, axis=-1, keepdims=True)
    inv_root = lax.rsqrt(variance + EPSILON)
    normal = center * inv_root
    return (normal * gain_vec + shift_vec, normal, inv_root)


def norm_backward(grad_in, normal, inv_root, gain_vec):
    grad_normal = grad_in * gain_vec
    grad_gain = jnp.sum(grad_in * normal, axis=0)
    grad_shift = jnp.sum(grad_in, axis=0)
    grad_hidden = inv_root * (
        grad_normal
        - jnp.mean(grad_normal, axis=-1, keepdims=True)
        - normal * jnp.mean(grad_normal * normal, axis=-1, keepdims=True)
    )
    return (grad_hidden, grad_gain, grad_shift)


def layer(
    hidden_in,
    cotangent,
    w_query,
    w_key,
    w_value,
    w_out,
    w_up,
    w_down,
    bias_query,
    bias_value,
    bias_out,
    bias_up,
    bias_down,
    gain_attn,
    shift_attn,
    gain_ffn,
    shift_ffn,
    valid_lengths,
):
    rows, model_width = hidden_in.shape
    n_tensor = lax.axis_size("tensor")
    n_data = lax.axis_size("dp")
    tensor_at = lax.axis_index("tensor")
    spread_over = rows * n_tensor // valid_lengths.shape[0] // rows
    head_size = model_width // HEADS
    head_cols = w_query.shape[1]
    factor = 1.0 / math.sqrt(rows * n_tensor * n_data)
    matrices = (w_query, w_key, w_value, w_out, w_up, w_down)
    wide = (bias_out, bias_down, gain_attn, shift_attn, gain_ffn, shift_ffn)

    if n_data == len(ORDER) and n_tensor == 4 and spread_over == 1:
        (
            qkv_full, out_full, up_full, down_full, qkv, context, hidden, active, slope, output,
            mixed_low, mixed_t, normed_t, input_t, grad_second, given, arranged,
        ) = forward_near(
            matrices, hidden_in, cotangent, wide, bias_query, bias_value, bias_up, valid_lengths,
            head_size,
        )
        grads, grad_input, sums = backward_near(
            mixed_low, mixed_t, normed_t, input_t, context, grad_second, hidden, arranged,
            valid_lengths, active, slope, qkv, (qkv_full, out_full, up_full, down_full), given,
            head_size,
        )
        lengths = [model_width // 128] * 8 + [bias_up.shape[0] // 128]
        results = scale_and_copy(grads, (grad_input, output), sums, lengths, factor)
        grads, (grad_input, output) = results[:6], results[6:8]
        vector_sums = [part.reshape(-1) for part in results[8:]]
    else:

        def column_part(vector):
            return vector.reshape(n_tensor, -1)

        query_bias, value_bias = column_part(bias_query), column_part(bias_value)
        bias_qkv = jnp.concatenate(
            [query_bias, jnp.zeros_like(query_bias), value_bias], axis=1
        ).reshape(1, -1)
        length = lax.dynamic_slice_in_dim(valid_lengths, tensor_at // spread_over, 1)
        low = [matrix.astype(BF16) for matrix in matrices]
        shards = [jnp.concatenate(low[:3], axis=1)] + low[3:]
        qkv_full, out_full, up_full, down_full = (gather_far(shard) for shard in shards)
        qkv = (matmul(hidden_in, qkv_full) + bias_qkv).astype(BF16)
        members = [list(range(k, k + spread_over)) for k in range(0, n_tensor, spread_over)]
        qkv_seq = lax.all_gather(qkv, "tensor", axis_index_groups=members, axis=0, tiled=True)
        context = attend_forward(qkv, qkv_seq, length, head_size, n_tensor)
        hidden = hidden_in.astype(F32) + contract_cols(context, out_full) + bias_out
        normed, normal_attn, root_attn = norm_forward(hidden, gain_attn, shift_attn)
        normed_low = normed.astype(BF16)
        active, slope = activate(matmul(normed_low, up_full), bias_up)
        active = active.astype(BF16)
        mixed = contract_cols(active, down_full)
        result, normal_ffn, root_ffn = norm_forward(normed + mixed + bias_down, gain_ffn, shift_ffn)
        output = result.astype(BF16)
        grad_second, grad_gain_ffn, grad_shift_ffn = norm_backward(
            cotangent.astype(F32), normal_ffn, root_ffn, gain_ffn
        )
        grad_bias_down = jnp.sum(grad_second, axis=0)
        mixed_low = grad_second.astype(BF16)
        grad_down = scatter_far(mixed_low, active)
        grad_upper = (matmul(mixed_low, down_full) * slope).astype(BF16)
        grad_bias_up = jnp.sum(grad_upper, axis=0, dtype=F32)
        grad_up = scatter_far(normed_low, grad_upper)
        grad_normed = grad_second + contract_cols(grad_upper, up_full)
        grad_first, grad_gain_attn, grad_shift_attn = norm_backward(
            grad_normed, normal_attn, root_attn, gain_attn
        )
        grad_bias_out = jnp.sum(grad_first, axis=0)
        attn_low = grad_first.astype(BF16)
        grad_context = matmul(attn_low, out_full).astype(BF16)
        grad_out = scatter_far(attn_low, context)
        grad_q, grad_kv = attend_backward(qkv, qkv_seq, grad_context, length, head_size, n_tensor)
        grad_kv = lax.psum_scatter(
            grad_kv.astype(F32),
            "tensor",
            scatter_dimension=0,
            axis_index_groups=members,
            tiled=True,
        ).astype(BF16)
        grad_qkv = jnp.concatenate(
            [grad_q.reshape(rows, n_tensor, -1), grad_kv.reshape(rows, n_tensor, -1)], axis=2
        ).reshape(rows, -1)
        grad_bias_qkv = jnp.sum(grad_qkv, axis=0, dtype=F32).reshape(n_tensor, 3, head_cols)
        grads = jnp.split(scatter_far(hidden_in, grad_qkv), 3, axis=1)
        grads = [grad * factor for grad in (*grads, grad_out, grad_up, grad_down)]
        grad_input = (grad_first + contract_cols(grad_qkv, qkv_full)).astype(BF16)
        sums = jnp.concatenate(
            [
                grad_bias_out,
                grad_bias_down,
                grad_gain_attn,
                grad_shift_attn,
                grad_gain_ffn,
                grad_shift_ffn,
                grad_bias_qkv[:, 0].reshape(-1),
                grad_bias_qkv[:, 2].reshape(-1),
                grad_bias_up,
            ]
        )
        sums = lax.psum(sums, ("dp", "tensor")) * factor
        vector_sums = jnp.split(sums, [k * model_width for k in range(1, 9)])
    (
        v_out, v_down, v_gain_attn, v_shift_attn, v_gain_ffn, v_shift_ffn, v_query, v_value, v_up,
    ) = vector_sums
    return (
        output,
        grad_input,
        *grads,
        v_query,
        v_value,
        v_out,
        v_up,
        v_down,
        v_gain_attn,
        v_shift_attn,
        v_gain_ffn,
        v_shift_ffn,
    )


def solution(mesh):
    tokens, matrix, copied = P(("dp", "tensor"), None), P("dp", "tensor"), P()
    return jax.shard_map(
        layer,
        mesh=mesh,
        in_specs=(tokens,) * 2 + (matrix,) * 6 + (copied,) * 9 + (P("dp"),),
        out_specs=(tokens,) * 2 + (matrix,) * 6 + (copied,) * 9,
        check_vma=False,
    )
```
